32 devices in a mesh: dp: 4 (over y, core), fsdp: 2 (over x), seq: 4 (over z).
Axes of the slice: x: 2, y: 2, z: 4, core: 2. Of those that a mesh axis runs over, the one named last changes fastest.
Arguments:
- frames_in: float32 [8, 1536, 768], P(('dp', 'fsdp'), 'seq'), may hold values from -8 to 8
- cotangent: float32 [8, 1536, 768], P(('dp', 'fsdp'), 'seq'), may hold values from -6 to 6
- attention_weight: float32 [4, 768, 768], P(None, 'fsdp'), may hold values from -16 to 16
- expand_weight: float32 [768, 3072], P('fsdp'), may hold values from -0.21875 to 0.21875
- contract_weight: float32 [3072, 768], P('fsdp'), may hold values from -0.109375 to 0.109375
- vectors: float32 [12, 768], P(None, 'fsdp'), may hold values from -2 to 2
- first_attention: float32 [4, 768, 768], P(None, 'fsdp'), may hold values from -32 to 32
- first_expand: float32 [768, 3072], P('fsdp'), may hold values from -32 to 32
- first_contract: float32 [3072, 768], P('fsdp'), may hold values from -32 to 32
- first_vectors: float32 [12, 768], P(None, 'fsdp'), may hold values from -32 to 32
- second_attention: float32 [4, 768, 768], P(None, 'fsdp'), may hold values from 0.24576 to 4.9152
- second_expand: float32 [768, 3072], P('fsdp'), may hold values from 0.24576 to 4.9152
- second_contract: float32 [3072, 768], P('fsdp'), may hold values from 0.24576 to 4.9152
- second_vectors: float32 [12, 768], P(None, 'fsdp'), may hold values from 0.24576 to 4.9152
Outputs:
- frames_out: float32 [8, 1536, 768], P(('dp', 'fsdp'), 'seq')
- input_gradient: float32 [8, 1536, 768], P(('dp', 'fsdp'), 'seq')
- gradient_attention: float32 [4, 768, 768], P(None, 'fsdp')
- gradient_expand: float32 [768, 3072], P('fsdp')
- gradient_contract: float32 [3072, 768], P('fsdp')
- gradient_vectors: float32 [12, 768], P(None, 'fsdp')
- updated_attention: float32 [4, 768, 768], P(None, 'fsdp')
- updated_expand: float32 [768, 3072], P('fsdp')
- updated_contract: float32 [3072, 768], P('fsdp')
- updated_vectors: float32 [12, 768], P(None, 'fsdp')
- average_attention: float32 [4, 768, 768], P(None, 'fsdp')
- average_expand: float32 [768, 3072], P('fsdp')
- average_contract: float32 [3072, 768], P('fsdp')
- average_vectors: float32 [12, 768], P(None, 'fsdp')
- variance_attention: float32 [4, 768, 768], P(None, 'fsdp')
- variance_expand: float32 [768, 3072], P('fsdp')
- variance_contract: float32 [3072, 768], P('fsdp')
- variance_vectors: float32 [12, 768], P(None, 'fsdp')
The draws below stay inside these ranges and needn't reach their ends.
All inputs are finite; a program needn't handle non-finite values.
Results may differ from the reference program's by a relative error of at most 0.0095.
The reference program's roundings to bfloat16 on the way count: a program that leaves them out, or rounds other values in their place, can miss the bound.
Values may be sent and summed in bfloat16 or wider, within the bound.
A program may use at most 320 MiB of HBM per device.

```python
import math
import jax
import jax.numpy as jnp
from jax import lax

D = 768
HEADS = 12
FF = 3072
VEC_ROWS = 12
FRAMES = 1536
CLIPS = 8
ROWS_ALL = 12288


def draw_frames_in(key, part):
    shape = (CLIPS, FRAMES, D)
    return jnp.clip(jax.random.normal(key, shape, jnp.float32), -6.0, 6.0)


def draw_attention_weight(key, part):
    factors = jnp.array([1.5, 1.5, 1.0, 3.6], jnp.float32)[:, None, None] / math.sqrt(D)
    shape = (4, D, D)
    return jnp.clip(jax.random.normal(key, shape, jnp.float32), -6.0, 6.0) * factors


def draw_vectors(key, part):
    rows = jnp.arange(VEC_ROWS)[:, None]
    is_gain = jnp.logical_or(rows == 0, rows == 5)
    shape = (VEC_ROWS, D)
    noise = jnp.clip(jax.random.normal(key, shape, jnp.float32), -5.0, 5.0)
    return jnp.where(is_gain, 1.0 + 0.1 * noise, 0.3 * noise)


def steps_of(stream_key, shape, shards, low, high):
    level = 1.0
    for axis_at, blocks in shards:
        steps = jax.random.uniform(jax.random.fold_in(jax.random.fold_in(stream_key, 6), axis_at), (blocks,), jnp.float32, low / len(shards), high / len(shards))
        level = level * jnp.repeat(jnp.exp(steps), shape[axis_at] // blocks).reshape((-1,) + (1,) * (len(shape) - 1 - axis_at))
    return level


def bell_draw(own_key, extent, scale, bound, pieces=(), held_as=jnp.bfloat16):
    values = jax.random.normal(own_key, extent, jnp.float32) * scale
    if len(pieces) > 0:
        values = steps_of(own_key, extent, pieces, -0.22, 0.18) * values
    return jnp.clip(values, min=-bound, max=bound).astype(held_as)


def setup_inputs(seed: int = 0) -> dict:
    key_list = jax.random.split(jax.random.key(seed), 15)
    return {
        "frames_in": draw_frames_in(jax.random.fold_in(key_list[14], 71), 0),
        "cotangent": bell_draw(key_list[1], (CLIPS, FRAMES, D), 1.0, 6.0, ((0, 8), (1, 4)), jnp.float32),
        "attention_weight": draw_attention_weight(jax.random.fold_in(key_list[14], 71), 0),
        "expand_weight": bell_draw(key_list[3], (D, FF), D ** -0.5, 0.21875, ((0, 2),), jnp.float32),
        "contract_weight": bell_draw(key_list[4], (FF, D), FF ** -0.5, 0.109375, ((0, 2),), jnp.float32),
        "vectors": draw_vectors(jax.random.fold_in(key_list[14], 71), 0),
        "first_attention": bell_draw(key_list[6], (4, D, D), (0.05 * ROWS_ALL ** 0.5), 32.0, ((1, 2),), jnp.float32),
        "first_expand": bell_draw(key_list[7], (D, FF), (0.05 * ROWS_ALL ** 0.5), 32.0, ((0, 2),), jnp.float32),
        "first_contract": bell_draw(key_list[8], (FF, D), (0.05 * ROWS_ALL ** 0.5), 32.0, ((0, 2),), jnp.float32),
        "first_vectors": bell_draw(key_list[9], (VEC_ROWS, D), (0.05 * ROWS_ALL ** 0.5), 32.0, ((1, 2),), jnp.float32),
        "second_attention": jnp.clip(jnp.exp(math.log(4.9152) - 2.9957323 * jax.random.uniform(key_list[10], (4, D, D), jnp.float32) ** steps_of(key_list[10], (4, D, D), ((1, 2),), -0.2, 0.2)), 0.24576, 4.9152),
        "second_expand": jnp.clip(jnp.exp(math.log(4.9152) - 2.9957323 * jax.random.uniform(key_list[11], (D, FF), jnp.float32) ** steps_of(key_list[11], (D, FF), ((0, 2),), -0.2, 0.2)), 0.24576, 4.9152),
        "second_contract": jnp.clip(jnp.exp(math.log(4.9152) - 2.9957323 * jax.random.uniform(key_list[12], (FF, D), jnp.float32) ** steps_of(key_list[12], (FF, D), ((0, 2),), -0.2, 0.2)), 0.24576, 4.9152),
        "second_vectors": jnp.clip(jnp.exp(math.log(4.9152) - 2.9957323 * jax.random.uniform(key_list[13], (VEC_ROWS, D), jnp.float32) ** steps_of(key_list[13], (VEC_ROWS, D), ((1, 2),), -0.2, 0.2)), 0.24576, 4.9152),
    }


norm_eps = 1e-05
beta_one = 0.9
beta_two = 0.999
adam_eps = 1e-08
adam_count = 5.0
rate_matrix = 0.02
rate_vector = 0.1
decay_matrix = 0.1
score_scale = 0.125

def layer_norm(values, gain, offset):
    center = values - lax.optimization_barrier(jnp.mean(values, axis=-1, keepdims=True))
    inverse = lax.rsqrt(lax.optimization_barrier(jnp.mean(center * center, axis=-1, keepdims=True)) + norm_eps)
    normed = center * inverse
    return (normed * gain + offset, normed, inverse)

def norm_back(upstream, normed, inverse, gain):
    scaled = upstream * gain
    inner = scaled - lax.optimization_barrier(jnp.mean(scaled, axis=-1, keepdims=True)) - normed * lax.optimization_barrier(jnp.mean(scaled * normed, axis=-1, keepdims=True))
    return (inverse * inner, lax.optimization_barrier(jnp.sum(upstream * normed, axis=0)), lax.optimization_barrier(jnp.sum(upstream, axis=0)))

def gelu_exact(values):
    return 0.5 * values * (1.0 + lax.erf(values * 0.7071067811865476))

def gelu_slope(values):
    return 0.5 * (1.0 + lax.erf(values * 0.7071067811865476)) + values * jnp.exp(-0.5 * values * values) * 0.3989422804014327

def product_nt(left, right):
    return lax.dot_general(left, right, (((1,), (1,)), ((), ())), preferred_element_type=jnp.float32)

def product_tn(left, right):
    return lax.dot_general(left, right, (((0,), (0,)), ((), ())), preferred_element_type=jnp.float32)

def split_heads(matrix):
    return jnp.transpose(matrix.reshape(matrix.shape[0], HEADS, -1), (1, 0, 2))

def join_heads(stacked):
    return jnp.transpose(stacked, (1, 0, 2)).reshape(stacked.shape[1], -1)

def head_forward(operands):
    queries, key_rows, value_rows = operands
    scores = product_nt(queries, key_rows) * score_scale
    largest = lax.optimization_barrier(jnp.max(scores, axis=-1, keepdims=True))
    totals = lax.optimization_barrier(jnp.sum(jnp.exp(scores - largest), axis=-1, keepdims=True))
    log_total = largest + jnp.log(totals)
    weights = jnp.exp(scores - log_total).astype(jnp.bfloat16)
    return (jnp.dot(weights, value_rows, preferred_element_type=jnp.float32), log_total[:, 0])

def head_backward(operands):
    queries, key_rows, value_rows, upstream, log_total = operands
    scores = product_nt(queries, key_rows) * score_scale
    probs = jnp.exp(scores - log_total[:, None])
    weights = probs.astype(jnp.bfloat16)
    slopes = product_nt(upstream, value_rows)
    value_grad = product_tn(weights, upstream)
    row_dot = lax.optimization_barrier(jnp.sum(probs * slopes, axis=-1, keepdims=True))
    score_grad = (probs * (slopes - row_dot) * score_scale).astype(jnp.bfloat16)
    query_grad = jnp.dot(score_grad, key_rows, preferred_element_type=jnp.float32)
    key_grad = product_tn(score_grad, queries)
    return (query_grad, key_grad, value_grad)

def clip_pass(frames, upstream, attention_bf, expand_bf, contract_bf, vector_work):
    width = frames.shape[1]
    bias_expand = vector_work[8:].reshape(-1)
    hidden_one, normed_one, inverse_one = layer_norm(frames, vector_work[0], vector_work[1])
    hidden_one = hidden_one.astype(jnp.bfloat16)
    queries = (jnp.dot(hidden_one, attention_bf[0], preferred_element_type=jnp.float32) + vector_work[2]).astype(jnp.bfloat16)
    key_rows = jnp.dot(hidden_one, attention_bf[1], preferred_element_type=jnp.float32).astype(jnp.bfloat16)
    value_rows = (jnp.dot(hidden_one, attention_bf[2], preferred_element_type=jnp.float32) + vector_work[3]).astype(jnp.bfloat16)
    query_heads = split_heads(queries)
    key_heads = split_heads(key_rows)
    value_heads = split_heads(value_rows)
    context_heads, log_total = lax.map(head_forward, (query_heads, key_heads, value_heads))
    context = join_heads(context_heads).astype(jnp.bfloat16)
    middle = frames + jnp.dot(context, attention_bf[3], preferred_element_type=jnp.float32) + vector_work[4]
    hidden_two, normed_two, inverse_two = layer_norm(middle, vector_work[5], vector_work[6])
    hidden_two = hidden_two.astype(jnp.bfloat16)
    expanded = jnp.dot(hidden_two, expand_bf, preferred_element_type=jnp.float32) + bias_expand
    activated = gelu_exact(expanded).astype(jnp.bfloat16)
    output = middle + jnp.dot(activated, contract_bf, preferred_element_type=jnp.float32) + vector_work[7]
    upstream_bf = upstream.astype(jnp.bfloat16)
    grad_contract_w = product_tn(activated, upstream_bf)
    grad_expanded = product_nt(upstream_bf, contract_bf) * gelu_slope(expanded)
    grad_expanded_bf = grad_expanded.astype(jnp.bfloat16)
    grad_expand_w = product_tn(hidden_two, grad_expanded_bf)
    grad_hidden_two = product_nt(grad_expanded_bf, expand_bf)
    back_two, gain_two_grad, bias_two_grad = norm_back(grad_hidden_two, normed_two, inverse_two, vector_work[5])
    grad_middle = upstream + back_two
    grad_middle_bf = grad_middle.astype(jnp.bfloat16)
    grad_output_w = product_tn(context, grad_middle_bf)
    grad_context = product_nt(grad_middle_bf, attention_bf[3]).astype(jnp.bfloat16)
    query_parts, key_parts, value_parts = lax.map(head_backward, (query_heads, key_heads, value_heads, split_heads(grad_context), log_total))
    query_grad = join_heads(query_parts)
    key_grad = join_heads(key_parts)
    value_grad = join_heads(value_parts)
    query_grad_bf = query_grad.astype(jnp.bfloat16)
    key_grad_bf = key_grad.astype(jnp.bfloat16)
    value_grad_bf = value_grad.astype(jnp.bfloat16)
    grad_query_w = product_tn(hidden_one, query_grad_bf)
    grad_key_w = product_tn(hidden_one, key_grad_bf)
    grad_value_w = product_tn(hidden_one, value_grad_bf)
    grad_hidden_one = product_nt(query_grad_bf, attention_bf[0]) + product_nt(key_grad_bf, attention_bf[1]) + product_nt(value_grad_bf, attention_bf[2])
    back_one, gain_one_grad, bias_one_grad = norm_back(grad_hidden_one, normed_one, inverse_one, vector_work[0])
    input_grad = grad_middle + back_one
    small_rows = jnp.stack([gain_one_grad, bias_one_grad, lax.optimization_barrier(jnp.sum(query_grad, axis=0)), lax.optimization_barrier(jnp.sum(value_grad, axis=0)), lax.optimization_barrier(jnp.sum(grad_middle, axis=0)), gain_two_grad, bias_two_grad, lax.optimization_barrier(jnp.sum(upstream, axis=0))])
    grad_vectors = jnp.concatenate([small_rows, lax.optimization_barrier(jnp.sum(grad_expanded, axis=0)).reshape(-1, width)], axis=0)
    grad_attention = jnp.stack([grad_query_w, grad_key_w, grad_value_w, grad_output_w])
    return (output, input_grad, (grad_attention, grad_expand_w, grad_contract_w, grad_vectors))

def adam_update(weight, gradient, first, second, rate, decay):
    first_new = beta_one * first + (1.0 - beta_one) * gradient
    second_new = beta_two * second + (1.0 - beta_two) * gradient * gradient
    first_hat = first_new / (1.0 - beta_one ** adam_count)
    second_hat = second_new / (1.0 - beta_two ** adam_count)
    updated = weight - rate * (first_hat / (jnp.sqrt(second_hat) + adam_eps) + decay * weight)
    return (updated, first_new, second_new)

def reference(frames_in, cotangent, attention_weight, expand_weight, contract_weight, vectors, first_attention, first_expand, first_contract, first_vectors, second_attention, second_expand, second_contract, second_vectors):
    attention_bf = attention_weight.astype(jnp.bfloat16)
    expand_bf = expand_weight.astype(jnp.bfloat16)
    contract_bf = contract_weight.astype(jnp.bfloat16)
    vector_work = lax.optimization_barrier(vectors.astype(jnp.bfloat16)).astype(jnp.float32)
    initial = (jnp.zeros(attention_weight.shape, jnp.float32), jnp.zeros(expand_weight.shape, jnp.float32), jnp.zeros(contract_weight.shape, jnp.float32), jnp.zeros(vectors.shape, jnp.float32))

    def per_clip(totals, operands):
        output, input_grad, grads = clip_pass(operands[0], operands[1], attention_bf, expand_bf, contract_bf, vector_work)
        return (jax.tree.map(jnp.add, totals, grads), (output, input_grad))
    totals, outputs = lax.scan(per_clip, initial, (frames_in, cotangent))
    frames_out, input_gradient = outputs
    new_attention = adam_update(attention_weight, totals[0], first_attention, second_attention, rate_matrix, decay_matrix)
    new_expand = adam_update(expand_weight, totals[1], first_expand, second_expand, rate_matrix, decay_matrix)
    new_contract = adam_update(contract_weight, totals[2], first_contract, second_contract, rate_matrix, decay_matrix)
    new_vectors = adam_update(vectors, totals[3], first_vectors, second_vectors, rate_vector, 0.0)
    return (frames_out, input_gradient, totals[0], totals[1], totals[2], totals[3], new_attention[0], new_expand[0], new_contract[0], new_vectors[0], new_attention[1], new_expand[1], new_contract[1], new_vectors[1], new_attention[2], new_expand[2], new_contract[2], new_vectors[2])
```

```python
import functools

import jax
import jax.numpy as jnp
from jax import lax
from jax.experimental import pallas as pl
from jax.experimental.pallas import tpu as pltpu
from jax.sharding import PartitionSpec as P

HEADS = 12
norm_eps = 1e-05
beta_one = 0.9
beta_two = 0.999
adam_eps = 1e-08
adam_count = 5.0
rate_matrix = 0.02
rate_vector = 0.1
decay_matrix = 0.1
score_scale = 0.125
VMEM_LIMIT = 60 << 20
MESH = pl.DeviceIdType.MESH
BF = jnp.bfloat16
F32 = jnp.float32


def nt(left, right):
    return lax.dot_general(left, right, (((1,), (1,)), ((), ())), preferred_element_type=F32)


def nn(left, right):
    return lax.dot_general(left, right, (((1,), (0,)), ((), ())), preferred_element_type=F32)


def tn(left, right):
    return lax.dot_general(left, right, (((0,), (0,)), ((), ())), preferred_element_type=F32)


def vmem():
    return pl.BlockSpec(memory_space=pltpu.VMEM)


def normalize(values):
    center = values - jnp.mean(values, axis=-1, keepdims=True)
    inverse = lax.rsqrt(jnp.mean(center * center, axis=-1, keepdims=True) + norm_eps)
    return center * inverse, inverse


def norm_back(upstream, normed, inverse, gain):
    scaled = upstream * gain
    inner = (
        scaled
        - jnp.mean(scaled, axis=-1, keepdims=True)
        - normed * jnp.mean(scaled * normed, axis=-1, keepdims=True)
    )
    return (inverse * inner, jnp.sum(upstream * normed, axis=0), jnp.sum(upstream, axis=0))


def gelu_exact(values):
    return 0.5 * values * (1.0 + lax.erf(values * 0.7071067811865476))


def gelu_slope(values):
    return (
        0.5 * (1.0 + lax.erf(values * 0.7071067811865476))
        + values * jnp.exp(-0.5 * values * values) * 0.3989422804014327
    )


def adam_update(weight, gradient, first, second, rate, decay):
    first_new = beta_one * first + (1.0 - beta_one) * gradient
    second_new = beta_two * second + (1.0 - beta_two) * gradient * gradient
    first_hat = first_new / (1.0 - beta_one**adam_count)
    second_hat = second_new / (1.0 - beta_two**adam_count)
    updated = weight - rate * (first_hat / (jnp.sqrt(second_hat) + adam_eps) + decay * weight)
    return (updated, first_new, second_new)


class Place:
    def __init__(self, sizes):
        self.nd, self.nf, self.ns = sizes
        self.nh = self.nd // 2
        self.dp = lax.axis_index("dp")
        self.x = lax.axis_index("fsdp")
        self.z = lax.axis_index("seq")
        self.core = lax.rem(self.dp, 2)
        self.hi = self.dp // 2

    def sibling(self):
        return {"dp": self.hi * 2 + 1 - self.core}

    def x_peer(self, k):
        return {"fsdp": lax.rem(self.x + k, self.nf)}

    def y_hi(self, k):
        return lax.rem(self.hi + k, self.nh)

    def y_peer(self, k):
        return {"dp": self.y_hi(k) * 2 + self.core}

    def z_at(self, k):
        return lax.rem(self.z + k + self.ns, self.ns)

    def z_peer(self, k):
        return {"seq": self.z_at(k)}

    def everyone(self):
        out = [self.sibling()]
        out += [self.x_peer(k) for k in range(1, self.nf)]
        out += [self.y_peer(k) for k in range(1, self.nh)]
        out += [self.z_peer(k) for k in range(1, self.ns)]
        return out

    def barrier(self):
        sem = pltpu.get_barrier_semaphore()
        peers = self.everyone()
        for peer in peers:
            pl.semaphore_signal(sem, inc=1, device_id=peer, device_id_type=MESH)
        pl.semaphore_wait(sem, len(peers))


def remote(src, dst, send, recv, peer):
    return pltpu.make_async_remote_copy(
        src_ref=src, dst_ref=dst, send_sem=send, recv_sem=recv, device_id=peer, device_id_type=MESH
    )


def gather_kernel(
    sizes, frames_ref, aw_ref, ew_ref, cw_ref, vec_ref,
    a_ref, e_ref, c_ref, v_ref, h_ref,
    xs, xr, ys, yr, s1s, s1r, s2s, s2r, vs, vr, rs, ls, hr,
):
    at = Place(sizes)
    nf, nh, ns = at.nf, at.nh, at.ns
    rows, width = frames_ref.shape
    shard = aw_ref.shape[1]
    half = shard // 2
    at.barrier()
    v_ref[at.x] = vec_ref[...].astype(BF)
    vec_copies = []
    for k in range(1, nf):
        copy = remote(v_ref.at[at.x], v_ref.at[at.x], vs.at[k], vr.at[k], at.x_peer(k))
        copy.start()
        vec_copies.append(copy)

    def view(chunk, j, hi, core):
        if chunk < 2:
            first, count = ((0, 3), (3, 1))[chunk]
            cols = width // nh
            return a_ref.at[
                pl.ds(first, count),
                pl.ds(pl.multiple_of(j * shard + core * half, 16), half),
                pl.ds(pl.multiple_of(hi * cols, 128), cols),
            ]
        if chunk == 2:
            cols = e_ref.shape[1] // nh
            return e_ref.at[
                pl.ds(pl.multiple_of(j * shard + core * half, 16), half),
                pl.ds(pl.multiple_of(hi * cols, 128), cols),
            ]
        cols = width // nh
        deep = c_ref.shape[0] // nf
        return c_ref.at[
            pl.ds(pl.multiple_of(j * deep + core * (deep // 2), 16), deep // 2),
            pl.ds(pl.multiple_of(hi * cols, 128), cols),
        ]

    own = pl.multiple_of(at.x * shard, 16)
    x_copies = {}

    def send_chunk(chunk):
        for k in range(1, nf):
            piece = view(chunk, at.x, at.hi, at.core)
            copy = remote(piece, piece, xs.at[chunk, k], xr.at[chunk, k], at.x_peer(k))
            copy.start()
            x_copies[chunk, k] = copy

    for u in range(3):
        a_ref[u, pl.ds(own, shard), :] = aw_ref[u].astype(BF)
    send_chunk(0)
    normed, _ = normalize(frames_ref[...])
    for copy in vec_copies:
        copy.wait()
    gain = jnp.concatenate([v_ref[j, 0:1, :] for j in range(nf)], axis=1).astype(F32)
    offset = jnp.concatenate([v_ref[j, 1:2, :] for j in range(nf)], axis=1).astype(F32)
    h_ref[pl.ds(pl.multiple_of(at.z * rows, 16), rows), :] = (normed * gain + offset).astype(BF)

    def block(b):
        return h_ref.at[pl.ds(pl.multiple_of(b * rows, 16), rows), :]

    def to_right(b):
        return remote(block(b), block(b), rs.at[b], hr.at[b], {"seq": at.z + 1})

    def to_left(b):
        return remote(block(b), block(b), ls.at[b], hr.at[b], {"seq": at.z - 1})

    @pl.when(at.z < ns - 1)
    def _():
        to_right(at.z).start()

    @pl.when(at.z > 0)
    def _():
        to_left(at.z).start()

    a_ref[3, pl.ds(own, shard), :] = aw_ref[3].astype(BF)
    send_chunk(1)
    e_ref[pl.ds(own, shard), :] = ew_ref[...].astype(BF)
    send_chunk(2)
    deep = cw_ref.shape[0]
    c_ref[pl.ds(pl.multiple_of(at.x * deep, 16), deep), :] = cw_ref[...].astype(BF)
    send_chunk(3)

    pending = []

    def forward(chunk):
        for k in range(1, nf):
            x_copies[chunk, k].wait_recv()
            j = lax.rem(at.x - k + nf, nf)
            piece = view(chunk, j, at.hi, at.core)
            copy = remote(piece, piece, s1s.at[chunk, k], s1r.at[chunk, k], at.sibling())
            copy.start()
            pending.append(copy)
            for m in range(1, nh):
                copy = remote(piece, piece, ys.at[chunk, k, m], yr.at[chunk, k, m], at.y_peer(m))
                copy.start()
                pending.append((copy, chunk, k, m))

    def relay(chunk):
        for k in range(1, nf):
            for m in range(1, nh):
                j = lax.rem(at.x - k + nf, nf)
                hi = lax.rem(at.hi - m + nh, nh)
                piece = view(chunk, j, hi, at.core)
                remote(piece, piece, ys.at[chunk, k, m], yr.at[chunk, k, m], at.y_peer(m)).wait_recv()
                copy = remote(piece, piece, s2s.at[chunk, k, m], s2r.at[chunk, k, m], at.sibling())
                copy.start()
                pending.append(copy)

    def hop(s):
        b = at.z - s

        @pl.when(b >= 0)
        def _():
            to_right(b).wait_recv()

            @pl.when(at.z < ns - 1)
            def _():
                to_right(b).start()

        d = at.z + s

        @pl.when(d < ns)
        def _():
            to_left(d).wait_recv()

            @pl.when(at.z > 0)
            def _():
                to_left(d).start()

    forward(0)
    hop(1)
    forward(1)
    relay(0)
    relay(1)
    for s in range(2, ns - 1):
        hop(s)
    forward(2)
    relay(2)
    if ns > 2:
        hop(ns - 1)
    forward(3)
    relay(3)
    for entry in pending:
        if isinstance(entry, tuple):
            entry[0].wait_send()
        else:
            entry.wait()
    for copy in x_copies.values():
        copy.wait_send()
    for b in range(ns):
        @pl.when(jnp.logical_and(b <= at.z, at.z < ns - 1))
        def _():
            to_right(b).wait_send()

        @pl.when(jnp.logical_and(b >= at.z, at.z > 0))
        def _():
            to_left(b).wait_send()


def gather_all(sizes, frames, aw, ew, cw, vec):
    nd, nf, ns = sizes
    nh = nd // 2
    rows, width = frames.shape
    deep = cw.shape[0] * nf
    dma = pltpu.SemaphoreType.DMA
    return pl.pallas_call(
        functools.partial(gather_kernel, sizes),
        out_shape=(
            jax.ShapeDtypeStruct((4, width, width), BF),
            jax.ShapeDtypeStruct((width, ew.shape[1]), BF),
            jax.ShapeDtypeStruct((deep, width), BF),
            jax.ShapeDtypeStruct((nf, 16, vec.shape[1]), BF),
            jax.ShapeDtypeStruct((rows * ns, width), BF),
        ),
        in_specs=[vmem()] * 5,
        out_specs=(vmem(),) * 5,
        scratch_shapes=[
            dma((4, nf)), dma((4, nf)),
            dma((4, nf, nh)), dma((4, nf, nh)),
            dma((4, nf)), dma((4, nf)),
            dma((4, nf, nh)), dma((4, nf, nh)),
            dma((nf,)), dma((nf,)),
            dma((ns,)), dma((ns,)), dma((ns,)),
        ],
        name="gather",
        compiler_params=pltpu.CompilerParams(
            collective_id=0, has_side_effects=True, vmem_limit_bytes=VMEM_LIMIT
        ),
    )(frames, aw, ew, cw, vec)


def attention_kernel(chunk, q_ref, k_ref, v_ref, ctx_ref, lse_ref):
    rows = q_ref.shape[0]
    lo = lax.broadcasted_iota(jnp.int32, (chunk, 128), 1) < 64

    def pair(p, carry):
        col = pl.ds(pl.multiple_of(p * 128, 128), 128)
        k2 = k_ref[:, col]
        v2 = v_ref[:, col]
        for c in range(rows // chunk):
            part = pl.ds(c * chunk, chunk)
            q2 = q_ref[part, col]
            ctx, lse = [], []
            for h in range(2):
                mask = lo if h == 0 else jnp.logical_not(lo)
                s = nt(jnp.where(mask, q2, jnp.zeros_like(q2)), k2) * score_scale
                largest = jnp.max(s, axis=-1, keepdims=True)
                e = jnp.exp(s - largest)
                total = jnp.sum(e, axis=-1, keepdims=True)
                ctx.append(nn((e * (1.0 / total)).astype(BF), v2))
                lse.append(largest + jnp.log(total))
            ctx_ref[part, col] = jnp.where(lo, ctx[0], ctx[1])
            lse_ref[p, part, :] = jnp.where(lo, lse[0], lse[1])
        return carry

    lax.fori_loop(0, q_ref.shape[1] // 128, pair, 0)


def attention(q, k, v):
    rows, width = q.shape
    return pl.pallas_call(
        functools.partial(attention_kernel, rows),
        out_shape=(
            jax.ShapeDtypeStruct((rows, width), F32),
            jax.ShapeDtypeStruct((width // 128, rows, 128), F32),
        ),
        in_specs=[vmem()] * 3,
        out_specs=(vmem(), vmem()),
        name="attention",
        compiler_params=pltpu.CompilerParams(vmem_limit_bytes=VMEM_LIMIT),
    )(q, k, v)


def attention_back_kernel(chunk, q_ref, k_ref, v_ref, dc_ref, ctx_ref, lse_ref, dq_ref, dk_ref, dv_ref):
    rows = q_ref.shape[0]
    lo = lax.broadcasted_iota(jnp.int32, (chunk, 128), 1) < 64

    def pair(p, carry):
        col = pl.ds(pl.multiple_of(p * 128, 128), 128)
        k2 = k_ref[:, col]
        v2 = v_ref[:, col]
        dk = dv = None
        for c in range(rows // chunk):
            part = pl.ds(c * chunk, chunk)
            q2 = q_ref[part, col]
            dc2 = dc_ref[part, col]
            both = dc2.astype(F32) * ctx_ref[part, col]
            lse2 = lse_ref[p, part, :]
            dq = []
            for h in range(2):
                mask = lo if h == 0 else jnp.logical_not(lo)
                qm = jnp.where(mask, q2, jnp.zeros_like(q2))
                dm = jnp.where(mask, dc2, jnp.zeros_like(q2))
                lse = lse2[:, 0:1] if h == 0 else lse2[:, 64:65]
                dot = jnp.sum(jnp.where(mask, both, 0.0), axis=-1, keepdims=True)
                probs = jnp.exp(nt(qm, k2) * score_scale - lse)
                slopes = nt(dm, v2)
                ds = (probs * (slopes - dot) * score_scale).astype(BF)
                dq.append(nn(ds, k2))
                a = nn(dm.T, probs.astype(BF))
                b = nn(qm.T, ds)
                dv = a if dv is None else dv + a
                dk = b if dk is None else dk + b
            dq_ref[part, col] = jnp.where(lo, dq[0], dq[1])
        dk_ref[col, :] = dk.astype(dk_ref.dtype)
        dv_ref[col, :] = dv.astype(dv_ref.dtype)
        return carry

    lax.fori_loop(0, q_ref.shape[1] // 128, pair, 0)


def attention_back(q, k, v, dc, ctx, lse):
    rows, width = q.shape
    every = k.shape[0]
    return pl.pallas_call(
        functools.partial(attention_back_kernel, rows),
        out_shape=(
            jax.ShapeDtypeStruct((rows, width), F32),
            jax.ShapeDtypeStruct((width, every), F32),
            jax.ShapeDtypeStruct((width, every), F32),
        ),
        in_specs=[vmem()] * 6,
        out_specs=(vmem(),) * 3,
        name="attention_back",
        compiler_params=pltpu.CompilerParams(vmem_limit_bytes=VMEM_LIMIT),
    )(q, k, v, dc, ctx, lse)


def reduce_kernel(
    sizes, ga_ref, ge_ref, gc_ref, gv_ref, dh_ref,
    oa_ref, oe_ref, oc_ref, ov_ref, od_ref,
    ca, ce, cc, xa, xe, xc, ya, ye, yc, za, ze, zc, dr, vb, vx, vy, vz,
    cs, cr, xs, xr, ys, yr, zs, zr, azs, azr, ays, ayr, acs, acr, ds, dm, vs, vr,
):
    at = Place(sizes)
    nf, nh, ns = at.nf, at.nh, at.ns
    half = ga_ref.shape[2] // 2
    width = ga_ref.shape[3]
    cols = width // nh
    wide = ge_ref.shape[2] // nh
    piece = wide // ns
    at.barrier()
    mine = pl.ds(pl.multiple_of(at.core * half, 16), half)
    other = pl.ds(pl.multiple_of((1 - at.core) * half, 16), half)
    sends = []

    def go(copy):
        copy.start()
        sends.append(copy)
        return copy

    held = (cc, ce, ca)
    c_copies = []
    for g, ref in enumerate((gc_ref, ge_ref, ga_ref)):
        src = ref.at[:, other, :] if g == 1 else ref.at[:, :, other, :]
        c_copies.append(go(remote(src, held[g], cs.at[g], cr.at[g], at.sibling())))

    d_copies = []
    for k in range(1, ns):
        d_copies.append(
            go(remote(dh_ref.at[at.z_at(k)], dr.at[k - 1], ds.at[k - 1], dm.at[k - 1], at.z_peer(k)))
        )

    def vector_start():
        return go(remote(gv_ref, vb, vs.at[0], vr.at[0], at.sibling()))

    v_core = vector_start()

    def stage_c(g):
        c_copies[g].wait_recv()
        if g == 0:
            for j in range(nf):
                for u in range(4):
                    cc[j, u] = (cc[j, u].astype(F32) + gc_ref[j, u, mine, :].astype(F32)).astype(BF)
        elif g == 1:
            for j in range(nf):
                ce[j] = (ce[j].astype(F32) + ge_ref[j, mine, :].astype(F32)).astype(BF)
        else:
            for u in range(4):
                for j in range(nf):
                    ca[u, j] = (ca[u, j].astype(F32) + ga_ref[u, j, mine, :].astype(F32)).astype(BF)
        out = []
        for k in range(1, nf):
            j = lax.rem(at.x + k, nf)
            src = ca.at[:, j] if g == 2 else held[g].at[j]
            dst = (xc, xe, xa)[g].at[k - 1]
            out.append(go(remote(src, dst, xs.at[g, k - 1], xr.at[g, k - 1], at.x_peer(k))))
        return out

    def stage_x(g, copies):
        for copy in copies:
            copy.wait_recv()
        got = (xc, xe, xa)[g]

        def mix(u):
            if g == 1:
                total = ce[at.x].astype(F32)
                for k in range(nf - 1):
                    total += got[k].astype(F32)
                got[0] = total.astype(BF)
            else:
                total = (cc[at.x, u] if g == 0 else ca[u, at.x]).astype(F32)
                for k in range(nf - 1):
                    total += got[k, u].astype(F32)
                got[0, u] = total.astype(BF)

        for u in range(1 if g == 1 else 4):
            mix(u)
        out = []
        for m in range(1, nh):
            hi = at.y_hi(m)
            if g == 1:
                src = got.at[0, :, pl.ds(pl.multiple_of(hi * wide, 128), wide)]
            else:
                src = got.at[0, :, :, pl.ds(pl.multiple_of(hi * cols, 128), cols)]
            dst = (yc, ye, ya)[g].at[m - 1]
            out.append(go(remote(src, dst, ys.at[g, m - 1], yr.at[g, m - 1], at.y_peer(m))))
        return out

    def stage_y(g, copies):
        for copy in copies:
            copy.wait_recv()
        kept = (xc, xe, xa)[g]
        got = (yc, ye, ya)[g]
        if g == 1:
            total = kept[0, :, pl.ds(pl.multiple_of(at.hi * wide, 128), wide)].astype(F32)
            for m in range(nh - 1):
                total += got[m].astype(F32)
            got[0] = total.astype(BF)
        else:
            for u in range(4):
                total = kept[0, u, :, pl.ds(pl.multiple_of(at.hi * cols, 128), cols)].astype(F32)
                for m in range(nh - 1):
                    total += got[m, u].astype(F32)
                got[0, u] = total.astype(BF)
        out = []
        for k in range(1, ns):
            b = at.z_at(k)
            if g == 1:
                src = got.at[0, :, pl.ds(pl.multiple_of(b * piece, 128), piece)]
            else:
                src = got.at[0, b]
            dst = (zc, ze, za)[g].at[k - 1]
            out.append(go(remote(src, dst, zs.at[g, k - 1], zr.at[g, k - 1], at.z_peer(k))))
        return out

    def home(g, z, hi):
        if g == 1:
            return oe_ref.at[mine, pl.ds(pl.multiple_of(hi * wide + z * piece, 128), piece)]
        out = oc_ref if g == 0 else oa_ref
        return out.at[z, mine, pl.ds(pl.multiple_of(hi * cols, 128), cols)]

    def stage_z(g, copies):
        for copy in copies:
            copy.wait_recv()
        kept = (yc, ye, ya)[g]
        got = (zc, ze, za)[g]
        if g == 1:
            total = kept[0, :, pl.ds(pl.multiple_of(at.z * piece, 128), piece)].astype(F32)
        else:
            total = kept[0, at.z].astype(F32)
        for k in range(ns - 1):
            total += got[k].astype(F32)
        spot = home(g, at.z, at.hi)
        spot[...] = total.astype(BF)
        out = []
        for k in range(1, ns):
            out.append(go(remote(spot, spot, azs.at[g, k - 1], azr.at[g, k - 1], at.z_peer(k))))
        return out

    def strip(g, hi):
        if g == 1:
            return oe_ref.at[mine, pl.ds(pl.multiple_of(hi * wide, 128), wide)]
        out = oc_ref if g == 0 else oa_ref
        return out.at[:, mine, pl.ds(pl.multiple_of(hi * cols, 128), cols)]

    def gather_y(g, copies):
        for copy in copies:
            copy.wait_recv()
        out = []
        for m in range(1, nh):
            spot = strip(g, at.hi)
            out.append(go(remote(spot, spot, ays.at[g, m - 1], ayr.at[g, m - 1], at.y_peer(m))))
        return out

    def gather_c(g, copies):
        for copy in copies:
            copy.wait_recv()
        if g == 1:
            spot = oe_ref.at[mine, :]
        else:
            spot = (oc_ref if g == 0 else oa_ref).at[:, mine, :]
        return [go(remote(spot, spot, acs.at[g], acr.at[g], at.sibling()))]

    def finish(copies):
        for copy in copies:
            copy.wait_recv()

    x0 = stage_c(0)
    x1 = stage_c(1)
    x2 = stage_c(2)
    v_core.wait_recv()
    vx[at.x] = gv_ref[...] + vb[...]
    v_x = [
        go(remote(vx.at[at.x], vx.at[at.x], vs.at[k], vr.at[k], at.x_peer(k)))
        for k in range(1, nf)
    ]
    y0 = stage_x(0, x0)
    finish(v_x)
    total = vx[0]
    for j in range(1, nf):
        total += vx[j]
    vy[at.hi] = total
    v_y = [
        go(remote(vy.at[at.hi], vy.at[at.hi], vs.at[nf + m], vr.at[nf + m], at.y_peer(m)))
        for m in range(1, nh)
    ]
    z0 = stage_y(0, y0)
    y1 = stage_x(1, x1)
    finish(v_y)
    total = vy[0]
    for j in range(1, nh):
        total += vy[j]
    vz[at.z] = total
    v_z = [
        go(remote(vz.at[at.z], vz.at[at.z], vs.at[nf + nh + k], vr.at[nf + nh + k], at.z_peer(k)))
        for k in range(1, ns)
    ]
    az0 = stage_z(0, z0)
    z1 = stage_y(1, y1)
    ay0 = gather_y(0, az0)
    y2 = stage_x(2, x2)
    az1 = stage_z(1, z1)
    ac0 = gather_c(0, ay0)
    z2 = stage_y(2, y2)
    ay1 = gather_y(1, az1)
    finish(v_z)
    total = vz[0]
    for j in range(1, ns):
        total += vz[j]
    ov_ref[...] = total
    finish(d_copies)
    total = dh_ref[at.z].astype(F32)
    for k in range(ns - 1):
        total += dr[k].astype(F32)
    od_ref[...] = total
    az2 = stage_z(2, z2)
    ac1 = gather_c(1, ay1)
    ay2 = gather_y(2, az2)
    ac2 = gather_c(2, ay2)
    finish(ac0)
    finish(ac1)
    finish(ac2)
    for copy in sends:
        copy.wait_send()


def reduce_all(sizes, ga, ge, gc, gv, dh):
    nd, nf, ns = sizes
    nh = nd // 2
    _, _, shard, width = ga.shape
    half = shard // 2
    full = ge.shape[2]
    cols, wide = width // nh, full // nh
    rows = dh.shape[1]
    dma = pltpu.SemaphoreType.DMA
    xn, yn, zn = max(nf - 1, 1), max(nh - 1, 1), max(ns - 1, 1)
    vec = gv.shape
    return pl.pallas_call(
        functools.partial(reduce_kernel, sizes),
        out_shape=(
            jax.ShapeDtypeStruct((4, shard, width), BF),
            jax.ShapeDtypeStruct((shard, full), BF),
            jax.ShapeDtypeStruct((4, shard, width), BF),
            jax.ShapeDtypeStruct(vec, F32),
            jax.ShapeDtypeStruct((rows, width), F32),
        ),
        in_specs=[vmem()] * 5,
        out_specs=(vmem(),) * 5,
        scratch_shapes=[
            pltpu.VMEM((4, nf, half, width), BF),
            pltpu.VMEM((nf, half, full), BF),
            pltpu.VMEM((nf, 4, half, width), BF),
            pltpu.VMEM((xn, 4, half, width), BF),
            pltpu.VMEM((xn, half, full), BF),
            pltpu.VMEM((xn, 4, half, width), BF),
            pltpu.VMEM((yn, 4, half, cols), BF),
            pltpu.VMEM((yn, half, wide), BF),
            pltpu.VMEM((yn, 4, half, cols), BF),
            pltpu.VMEM((zn, half, cols), BF),
            pltpu.VMEM((zn, half, wide // ns), BF),
            pltpu.VMEM((zn, half, cols), BF),
            pltpu.VMEM((zn, rows, width), BF),
            pltpu.VMEM(vec, F32),
            pltpu.VMEM((nf,) + vec, F32),
            pltpu.VMEM((nh,) + vec, F32),
            pltpu.VMEM((ns,) + vec, F32),
            dma((3,)), dma((3,)),
            dma((3, xn)), dma((3, xn)),
            dma((3, yn)), dma((3, yn)),
            dma((3, zn)), dma((3, zn)),
            dma((3, zn)), dma((3, zn)),
            dma((3, yn)), dma((3, yn)),
            dma((3,)), dma((3,)),
            dma((zn,)), dma((zn,)),
            dma((nf + nh + ns,)), dma((nf + nh + ns,)),
        ],
        name="reduce",
        compiler_params=pltpu.CompilerParams(
            collective_id=1, has_side_effects=True, vmem_limit_bytes=VMEM_LIMIT
        ),
    )(ga, ge, gc, gv, dh)


def on_device(
    sizes,
    frames_in,
    cotangent,
    attention_weight,
    expand_weight,
    contract_weight,
    vectors,
    first_attention,
    first_expand,
    first_contract,
    first_vectors,
    second_attention,
    second_expand,
    second_contract,
    second_vectors,
):
    nd, nf, ns = sizes
    frames = frames_in[0]
    upstream = cotangent[0]
    rows, width = frames.shape
    shard = attention_weight.shape[1]
    full = expand_weight.shape[1]
    vec_pad = jnp.pad(vectors, ((0, 4), (0, 0)))
    aw, ew, cw, vw, h_all = gather_all(
        sizes, frames, attention_weight, expand_weight, contract_weight, vec_pad
    )
    vec = jnp.transpose(vw, (1, 0, 2)).reshape(16, width)[:12].astype(F32)
    bias_expand = vec[8:].reshape(-1)
    normed_one, inverse_one = normalize(frames)
    h_own = lax.dynamic_slice_in_dim(h_all, lax.axis_index("seq") * rows, rows, 0)
    queries = (nn(h_own, aw[0]) + vec[2]).astype(BF)
    key_rows = nn(h_all, aw[1]).astype(BF)
    value_rows = (nn(h_all, aw[2]) + vec[3]).astype(BF)
    context_wide, log_total = attention(queries, key_rows, value_rows)
    context = context_wide.astype(BF)
    middle = frames + nn(context, aw[3]) + vec[4]
    normed_two, inverse_two = normalize(middle)
    hidden_two = (normed_two * vec[5] + vec[6]).astype(BF)
    expanded = nn(hidden_two, ew) + bias_expand
    activated = gelu_exact(expanded).astype(BF)
    frames_out = middle + nn(activated, cw) + vec[7]
    upstream_bf = upstream.astype(BF)
    grad_contract = tn(activated, upstream_bf).astype(BF)
    grad_expanded = nt(upstream_bf, cw) * gelu_slope(expanded)
    grad_expanded_bf = grad_expanded.astype(BF)
    grad_expand = tn(hidden_two, grad_expanded_bf).astype(BF)
    grad_hidden_two = nt(grad_expanded_bf, ew)
    back_two, gain_two_grad, bias_two_grad = norm_back(
        grad_hidden_two, normed_two, inverse_two, vec[5]
    )
    grad_middle = upstream + back_two
    grad_middle_bf = grad_middle.astype(BF)
    grad_output_w = tn(context, grad_middle_bf).astype(BF)
    grad_context = nt(grad_middle_bf, aw[3]).astype(BF)
    dq, dkt, dvt = attention_back(
        queries, key_rows, value_rows, grad_context, context_wide, log_total
    )
    dq_bf = dq.astype(BF)
    dkt_bf = dkt.astype(BF)
    dvt_bf = dvt.astype(BF)
    grad_query_w = tn(h_own, dq_bf).astype(BF)
    grad_key_w = lax.dot_general(
        h_all, dkt_bf, (((0,), (1,)), ((), ())), preferred_element_type=F32
    ).astype(BF)
    grad_value_w = lax.dot_general(
        h_all, dvt_bf, (((0,), (1,)), ((), ())), preferred_element_type=F32
    ).astype(BF)
    spread = (
        lax.dot_general(dkt_bf, aw[1], (((0,), (1,)), ((), ())), preferred_element_type=F32)
        + lax.dot_general(dvt_bf, aw[2], (((0,), (1,)), ((), ())), preferred_element_type=F32)
    ).astype(BF)
    gv = jnp.zeros((16, width), F32)
    small = jnp.stack(
        [
            jnp.sum(dq, axis=0),
            jnp.sum(dvt, axis=1),
            jnp.sum(grad_middle, axis=0),
            gain_two_grad,
            bias_two_grad,
            jnp.sum(upstream, axis=0),
        ]
    )
    gv = jnp.concatenate(
        [jnp.zeros((2, width), F32), small, jnp.sum(grad_expanded, axis=0).reshape(-1, width),
         jnp.zeros((4, width), F32)], axis=0
    )
    ga = jnp.stack([grad_query_w, grad_key_w, grad_value_w, grad_output_w])
    oa, oe, oc, ov, od = reduce_all(
        sizes,
        ga.reshape(4, nf, shard, width),
        grad_expand.reshape(nf, shard, full),
        grad_contract.reshape(nf, 4, shard, width),
        gv,
        spread.reshape(ns, rows, width),
    )
    grad_hidden_one = od + nt(dq_bf, aw[0])
    back_one, gain_one_grad, bias_one_grad = norm_back(
        grad_hidden_one, normed_one, inverse_one, vec[0]
    )
    ends = lax.psum(jnp.stack([gain_one_grad, bias_one_grad]), ("dp", "fsdp", "seq"))
    gv_sum = jnp.concatenate([ends, ov[2:12]], axis=0)
    owned_vec = lax.dynamic_slice_in_dim(
        gv_sum, lax.axis_index("fsdp") * (width // nf), width // nf, 1
    )
    owned = (
        oa.astype(F32),
        oe.astype(F32),
        oc.reshape(4 * shard, width).astype(F32),
        owned_vec,
    )
    new_attention = adam_update(
        attention_weight, owned[0], first_attention, second_attention, rate_matrix, decay_matrix
    )
    new_expand = adam_update(
        expand_weight, owned[1], first_expand, second_expand, rate_matrix, decay_matrix
    )
    new_contract = adam_update(
        contract_weight, owned[2], first_contract, second_contract, rate_matrix, decay_matrix
    )
    new_vectors = adam_update(vectors, owned[3], first_vectors, second_vectors, rate_vector, 0.0)
    return (
        frames_out[None],
        (grad_middle + back_one)[None],
        owned[0],
        owned[1],
        owned[2],
        owned[3],
        new_attention[0],
        new_expand[0],
        new_contract[0],
        new_vectors[0],
        new_attention[1],
        new_expand[1],
        new_contract[1],
        new_vectors[1],
        new_attention[2],
        new_expand[2],
        new_contract[2],
        new_vectors[2],
    )


def solution(mesh):
    sizes = (mesh.shape["dp"], mesh.shape["fsdp"], mesh.shape["seq"])
    data = P(("dp", "fsdp"), "seq", None)
    state = (P(None, "fsdp", None), P("fsdp", None), P("fsdp", None), P(None, "fsdp"))
    return jax.shard_map(
        functools.partial(on_device, sizes),
        mesh=mesh,
        in_specs=(data, data) + state * 3,
        out_specs=(data, data) + state * 4,
        check_vma=False,
    )
```

```python
import functools

import jax
import jax.numpy as jnp
from jax import lax
from jax.experimental import pallas as pl
from jax.experimental.pallas import tpu as pltpu
from jax.sharding import PartitionSpec as P

HEADS = 12
norm_eps = 1e-05
beta_one = 0.9
beta_two = 0.999
adam_eps = 1e-08
adam_count = 5.0
rate_matrix = 0.02
rate_vector = 0.1
decay_matrix = 0.1
score_scale = 0.125
VMEM_LIMIT = 60 << 20
MESH = pl.DeviceIdType.MESH
BF = jnp.bfloat16
F32 = jnp.float32


def nt(left, right):
    return lax.dot_general(left, right, (((1,), (1,)), ((), ())), preferred_element_type=F32)


def nn(left, right):
    return lax.dot_general(left, right, (((1,), (0,)), ((), ())), preferred_element_type=F32)


def tn(left, right):
    return lax.dot_general(left, right, (((0,), (0,)), ((), ())), preferred_element_type=F32)


def vmem():
    return pl.BlockSpec(memory_space=pltpu.VMEM)


def normalize(values):
    center = values - jnp.mean(values, axis=-1, keepdims=True)
    inverse = lax.rsqrt(jnp.mean(center * center, axis=-1, keepdims=True) + norm_eps)
    return center * inverse, inverse


def norm_back(upstream, normed, inverse, gain):
    scaled = upstream * gain
    inner = (
        scaled
        - jnp.mean(scaled, axis=-1, keepdims=True)
        - normed * jnp.mean(scaled * normed, axis=-1, keepdims=True)
    )
    return (inverse * inner, jnp.sum(upstream * normed, axis=0), jnp.sum(upstream, axis=0))


def gelu_exact(values):
    return 0.5 * values * (1.0 + lax.erf(values * 0.7071067811865476))


def gelu_slope(values):
    return (
        0.5 * (1.0 + lax.erf(values * 0.7071067811865476))
        + values * jnp.exp(-0.5 * values * values) * 0.3989422804014327
    )


def adam_update(weight, gradient, first, second, rate, decay):
    first_new = beta_one * first + (1.0 - beta_one) * gradient
    second_new = beta_two * second + (1.0 - beta_two) * gradient * gradient
    first_hat = first_new / (1.0 - beta_one**adam_count)
    second_hat = second_new / (1.0 - beta_two**adam_count)
    updated = weight - rate * (first_hat / (jnp.sqrt(second_hat) + adam_eps) + decay * weight)
    return (updated, first_new, second_new)


class Place:
    def __init__(self, sizes):
        self.nd, self.nf, self.ns = sizes
        self.nh = self.nd // 2
        self.dp = lax.axis_index("dp")
        self.x = lax.axis_index("fsdp")
        self.z = lax.axis_index("seq")
        self.core = lax.rem(self.dp, 2)
        self.hi = self.dp // 2

    def sibling(self):
        return {"dp": self.hi * 2 + 1 - self.core}

    def x_peer(self, k):
        return {"fsdp": lax.rem(self.x + k, self.nf)}

    def y_hi(self, k):
        return lax.rem(self.hi + k, self.nh)

    def y_peer(self, k):
        return {"dp": self.y_hi(k) * 2 + self.core}

    def z_at(self, k):
        return lax.rem(self.z + k + self.ns, self.ns)

    def z_peer(self, k):
        return {"seq": self.z_at(k)}

    def everyone(self):
        out = [self.sibling()]
        out += [self.x_peer(k) for k in range(1, self.nf)]
        out += [self.y_peer(k) for k in range(1, self.nh)]
        out += [self.z_peer(k) for k in range(1, self.ns)]
        return out

    def barrier(self):
        sem = pltpu.get_barrier_semaphore()
        peers = self.everyone()
        for peer in peers:
            pl.semaphore_signal(sem, inc=1, device_id=peer, device_id_type=MESH)
        pl.semaphore_wait(sem, len(peers))


def remote(src, dst, send, recv, peer):
    return pltpu.make_async_remote_copy(
        src_ref=src, dst_ref=dst, send_sem=send, recv_sem=recv, device_id=peer, device_id_type=MESH
    )


def gather_kernel(
    sizes, frames_ref, aw_ref, ew_ref, cw_ref, vec_ref,
    a_ref, e_ref, c_ref, v_ref, h_ref,
    xs, xr, ys, yr, s1s, s1r, s2s, s2r, vs, vr, rs, ls, hr,
):
    at = Place(sizes)
    nf, nh, ns = at.nf, at.nh, at.ns
    rows, width = frames_ref.shape
    shard = aw_ref.shape[1]
    half = shard // 2
    at.barrier()
    v_ref[at.x] = vec_ref[...].astype(BF)
    vec_copies = []
    for k in range(1, nf):
        copy = remote(v_ref.at[at.x], v_ref.at[at.x], vs.at[k], vr.at[k], at.x_peer(k))
        copy.start()
        vec_copies.append(copy)

    def view(chunk, j, hi, core):
        if chunk < 2:
            first, count = ((0, 3), (3, 1))[chunk]
            cols = width // nh
            return a_ref.at[
                pl.ds(first, count),
                pl.ds(pl.multiple_of(j * shard + core * half, 16), half),
                pl.ds(pl.multiple_of(hi * cols, 128), cols),
            ]
        if chunk == 2:
            cols = e_ref.shape[1] // nh
            return e_ref.at[
                pl.ds(pl.multiple_of(j * shard + core * half, 16), half),
                pl.ds(pl.multiple_of(hi * cols, 128), cols),
            ]
        cols = width // nh
        deep = c_ref.shape[0] // nf
        return c_ref.at[
            pl.ds(pl.multiple_of(j * deep + core * (deep // 2), 16), deep // 2),
            pl.ds(pl.multiple_of(hi * cols, 128), cols),
        ]

    own = pl.multiple_of(at.x * shard, 16)
    x_copies = {}

    def send_chunk(chunk):
        for k in range(1, nf):
            piece = view(chunk, at.x, at.hi, at.core)
            copy = remote(piece, piece, xs.at[chunk, k], xr.at[chunk, k], at.x_peer(k))
            copy.start()
            x_copies[chunk, k] = copy

    for u in range(3):
        a_ref[u, pl.ds(own, shard), :] = aw_ref[u].astype(BF)
    send_chunk(0)
    normed, _ = normalize(frames_ref[...])
    for copy in vec_copies:
        copy.wait()
    gain = jnp.concatenate([v_ref[j, 0:1, :] for j in range(nf)], axis=1).astype(F32)
    offset = jnp.concatenate([v_ref[j, 1:2, :] for j in range(nf)], axis=1).astype(F32)
    h_ref[pl.ds(pl.multiple_of(at.z * rows, 16), rows), :] = (normed * gain + offset).astype(BF)

    def block(b):
        return h_ref.at[pl.ds(pl.multiple_of(b * rows, 16), rows), :]

    def to_right(b):
        return remote(block(b), block(b), rs.at[b], hr.at[b], {"seq": at.z + 1})

    def to_left(b):
        return remote(block(b), block(b), ls.at[b], hr.at[b], {"seq": at.z - 1})

    @pl.when(at.z < ns - 1)
    def _():
        to_right(at.z).start()

    @pl.when(at.z > 0)
    def _():
        to_left(at.z).start()

    a_ref[3, pl.ds(own, shard), :] = aw_ref[3].astype(BF)
    send_chunk(1)
    e_ref[pl.ds(own, shard), :] = ew_ref[...].astype(BF)
    send_chunk(2)
    deep = cw_ref.shape[0]
    c_ref[pl.ds(pl.multiple_of(at.x * deep, 16), deep), :] = cw_ref[...].astype(BF)
    send_chunk(3)

    pending = []

    def forward(chunk):
        for k in range(1, nf):
            x_copies[chunk, k].wait_recv()
            j = lax.rem(at.x - k + nf, nf)
            piece = view(chunk, j, at.hi, at.core)
            copy = remote(piece, piece, s1s.at[chunk, k], s1r.at[chunk, k], at.sibling())
            copy.start()
            pending.append(copy)
            for m in range(1, nh):
                copy = remote(piece, piece, ys.at[chunk, k, m], yr.at[chunk, k, m], at.y_peer(m))
                copy.start()
                pending.append((copy, chunk, k, m))

    def relay(chunk):
        for k in range(1, nf):
            for m in range(1, nh):
                j = lax.rem(at.x - k + nf, nf)
                hi = lax.rem(at.hi - m + nh, nh)
                piece = view(chunk, j, hi, at.core)
                remote(piece, piece, ys.at[chunk, k, m], yr.at[chunk, k, m], at.y_peer(m)).wait_recv()
                copy = remote(piece, piece, s2s.at[chunk, k, m], s2r.at[chunk, k, m], at.sibling())
                copy.start()
                pending.append(copy)

    def hop(s):
        b = at.z - s

        @pl.when(b >= 0)
        def _():
            to_right(b).wait_recv()

            @pl.when(at.z < ns - 1)
            def _():
                to_right(b).start()

        d = at.z + s

        @pl.when(d < ns)
        def _():
            to_left(d).wait_recv()

            @pl.when(at.z > 0)
            def _():
                to_left(d).start()

    forward(0)
    hop(1)
    forward(1)
    relay(0)
    relay(1)
    for s in range(2, ns - 1):
        hop(s)
    forward(2)
    relay(2)
    if ns > 2:
        hop(ns - 1)
    forward(3)
    relay(3)
    for entry in pending:
        if isinstance(entry, tuple):
            entry[0].wait_send()
        else:
            entry.wait()
    for copy in x_copies.values():
        copy.wait_send()
    for b in range(ns):
        @pl.when(jnp.logical_and(b <= at.z, at.z < ns - 1))
        def _():
            to_right(b).wait_send()

        @pl.when(jnp.logical_and(b >= at.z, at.z > 0))
        def _():
            to_left(b).wait_send()


def gather_all(sizes, frames, aw, ew, cw, vec):
    nd, nf, ns = sizes
    nh = nd // 2
    rows, width = frames.shape
    deep = cw.shape[0] * nf
    dma = pltpu.SemaphoreType.DMA
    return pl.pallas_call(
        functools.partial(gather_kernel, sizes),
        out_shape=(
            jax.ShapeDtypeStruct((4, width, width), BF),
            jax.ShapeDtypeStruct((width, ew.shape[1]), BF),
            jax.ShapeDtypeStruct((deep, width), BF),
            jax.ShapeDtypeStruct((nf, 16, vec.shape[1]), BF),
            jax.ShapeDtypeStruct((rows * ns, width), BF),
        ),
        in_specs=[vmem()] * 5,
        out_specs=(vmem(),) * 5,
        scratch_shapes=[
            dma((4, nf)), dma((4, nf)),
            dma((4, nf, nh)), dma((4, nf, nh)),
            dma((4, nf)), dma((4, nf)),
            dma((4, nf, nh)), dma((4, nf, nh)),
            dma((nf,)), dma((nf,)),
            dma((ns,)), dma((ns,)), dma((ns,)),
        ],
        name="gather",
        compiler_params=pltpu.CompilerParams(
            collective_id=0, has_side_effects=True, vmem_limit_bytes=VMEM_LIMIT
        ),
    )(frames, aw, ew, cw, vec)


def attention_kernel(chunk, q_ref, k_ref, v_ref, ctx_ref, lse_ref):
    rows = q_ref.shape[0]
    lo = lax.broadcasted_iota(jnp.int32, (chunk, 128), 1) < 64

    def pair(p, carry):
        col = pl.ds(pl.multiple_of(p * 128, 128), 128)
        k2 = k_ref[:, col]
        v2 = v_ref[:, col]
        for c in range(rows // chunk):
            part = pl.ds(c * chunk, chunk)
            q2 = q_ref[part, col]
            ctx, lse = [], []
            for h in range(2):
                mask = lo if h == 0 else jnp.logical_not(lo)
                s = nt(jnp.where(mask, q2, jnp.zeros_like(q2)), k2) * score_scale
                largest = jnp.max(s, axis=-1, keepdims=True)
                e = jnp.exp(s - largest)
                total = jnp.sum(e, axis=-1, keepdims=True)
                ctx.append(nn((e * (1.0 / total)).astype(BF), v2))
                lse.append(largest + jnp.log(total))
            ctx_ref[part, col] = jnp.where(lo, ctx[0], ctx[1])
            lse_ref[p, part, :] = jnp.where(lo, lse[0], lse[1])
        return carry

    lax.fori_loop(0, q_ref.shape[1] // 128, pair, 0)


def attention(q, k, v):
    rows, width = q.shape
    return pl.pallas_call(
        functools.partial(attention_kernel, rows),
        out_shape=(
            jax.ShapeDtypeStruct((rows, width), F32),
            jax.ShapeDtypeStruct((width // 128, rows, 128), F32),
        ),
        in_specs=[vmem()] * 3,
        out_specs=(vmem(), vmem()),
        name="attention",
        compiler_params=pltpu.CompilerParams(vmem_limit_bytes=VMEM_LIMIT),
    )(q, k, v)


def back_kernel(
    sizes, q_ref, k_ref, v_ref, dc_ref, ctx_ref, lse_ref, ht_ref, w_ref, gm_ref, frames_ref,
    vec_ref, gv_ref, gc_ref, ge_ref, go_ref,
    out_ref, ig_ref, ov_ref,
    ga, own, rc, rx, ry, rz, dkt, dvt, dqt, dhs, dhr, dho, vb, vx, vy, vz,
    os, cs, cr, xs, xr, ys, yr, zs, zr, azs, azr, ays, ayr, acs, acr, ds, dm, vs, vr,
):
    at = Place(sizes)
    nf, nh, ns = at.nf, at.nh, at.ns
    rows, width = q_ref.shape
    half = rc.shape[4]
    cols = width // nh
    chunks = rc.shape[0]
    per = chunks // 3
    at.barrier()
    mine = pl.ds(pl.multiple_of(at.core * half, 16), half)
    other = pl.ds(pl.multiple_of((1 - at.core) * half, 16), half)

    def lanes(s, hi):
        return pl.ds(pl.multiple_of(hi * cols + s * 128, 128), 128)

    for s in range(per):
        for hi in range(nh):
            for part in range(2):
                pltpu.make_async_copy(
                    go_ref.at[:, pl.ds(part * half, half), pl.ds(hi * cols + s * 128, 128)],
                    ga.at[s, hi, :, part, 3],
                    os.at[2],
                ).start()

    def own_whole(slot):
        return pltpu.make_async_copy(own.at[slot], own.at[slot], os.at[slot])

    def c_whole(n):
        return remote(rc.at[n], rc.at[n], cs.at[n], cr.at[n], at.sibling())

    def c_send(n):
        slot = lax.rem(n, 2)

        @pl.when(n < per)
        def _():
            for hi in range(nh):
                block = lanes(n, hi)
                remote(
                    gc_ref.at[:, :, other, block], rc.at[n, hi], cs.at[n], cr.at[n], at.sibling()
                ).start()
                pltpu.make_async_copy(
                    gc_ref.at[:, :, mine, block], own.at[slot, hi], os.at[slot]
                ).start()

        @pl.when(jnp.logical_and(n >= per, n < 2 * per))
        def _():
            for hi in range(nh):
                for u in range(4):
                    block = pl.ds(pl.multiple_of(u * width + hi * cols + (n - per) * 128, 128), 128)
                    remote(
                        ge_ref.at[:, other, block], rc.at[n, hi, :, u], cs.at[n], cr.at[n], at.sibling()
                    ).start()
                    pltpu.make_async_copy(
                        ge_ref.at[:, mine, block], own.at[slot, hi, :, u], os.at[slot]
                    ).start()

        @pl.when(jnp.logical_and(n >= 2 * per, n < chunks))
        def _():
            remote(
                ga.at[n - 2 * per, :, :, 1 - at.core], rc.at[n], cs.at[n], cr.at[n], at.sibling()
            ).start()

    def x_copy(n, k):
        peer = lax.rem(at.x + k, nf)
        return remote(rc.at[n, :, peer], rx.at[n, k - 1], xs.at[n, k - 1], xr.at[n, k - 1], at.x_peer(k))

    def y_copy(n, m):
        return remote(
            rx.at[n, 0, at.y_hi(m)], ry.at[n, m - 1], ys.at[n, m - 1], yr.at[n, m - 1], at.y_peer(m)
        )

    def z_copy(n, k):
        return remote(
            ry.at[n, 0, at.z_at(k)], rz.at[n, k - 1], zs.at[n, k - 1], zr.at[n, k - 1], at.z_peer(k)
        )

    def spot(n):
        return n // per, lax.rem(n, per)

    def az_copy(n, k, z=None):
        g, s = spot(n)
        place = out_ref.at[g, at.z if z is None else z, mine, lanes(s, at.hi)]
        return remote(place, place, azs.at[n, k - 1], azr.at[n, k - 1], at.z_peer(k))

    def ay_copy(n, m):
        g, s = spot(n)
        place = out_ref.at[g, :, mine, lanes(s, at.hi)]
        return remote(place, place, ays.at[n, m - 1], ayr.at[n, m - 1], at.y_peer(m))

    def ac_start(n):
        g, s = spot(n)
        for hi in range(nh):
            place = out_ref.at[g, :, mine, lanes(s, hi)]
            remote(place, place, acs.at[n], acr.at[n], at.sibling()).start()

    def ac_whole(n):
        return remote(rx.at[n, 0], rx.at[n, 0], acs.at[n], acr.at[n], at.sibling())

    def stage_c(n):
        c_whole(n).wait_recv()
        slot = lax.rem(n, 2)

        @pl.when(n < 2 * per)
        def _():
            own_whole(slot).wait()

            def add(i, carry):
                hi, j, u = i // (nf * 4), lax.rem(i // 4, nf), lax.rem(i, 4)
                rc[n, hi, j, u] = (rc[n, hi, j, u].astype(F32) + own[slot, hi, j, u].astype(F32)).astype(BF)
                return carry

            lax.fori_loop(0, nh * nf * 4, add, 0)

        @pl.when(n >= 2 * per)
        def _():
            def add(i, carry):
                hi, j, u = i // (nf * 4), lax.rem(i // 4, nf), lax.rem(i, 4)
                rc[n, hi, j, u] = (
                    rc[n, hi, j, u].astype(F32) + ga[n - 2 * per, hi, j, at.core, u].astype(F32)
                ).astype(BF)
                return carry

            lax.fori_loop(0, nh * nf * 4, add, 0)

        for k in range(1, nf):
            x_copy(n, k).start()

    def stage_x(n):
        for k in range(1, nf):
            x_copy(n, k).wait_recv()

        def add(i, carry):
            hi, u = i // 4, lax.rem(i, 4)
            total = rc[n, hi, at.x, u].astype(F32)
            for k in range(nf - 1):
                total += rx[n, k, hi, u].astype(F32)
            rx[n, 0, hi, u] = total.astype(BF)
            return carry

        lax.fori_loop(0, nh * 4, add, 0)
        for m in range(1, nh):
            y_copy(n, m).start()

    def stage_y(n):
        for m in range(1, nh):
            y_copy(n, m).wait_recv()

        def add(u, carry):
            total = rx[n, 0, at.hi, u].astype(F32)
            for m in range(nh - 1):
                total += ry[n, m, u].astype(F32)
            ry[n, 0, u] = total.astype(BF)
            return carry

        lax.fori_loop(0, 4, add, 0)
        for k in range(1, ns):
            z_copy(n, k).start()

    def stage_z(n):
        for k in range(1, ns):
            z_copy(n, k).wait_recv()
        total = ry[n, 0, at.z].astype(F32)
        for k in range(ns - 1):
            total += rz[n, k].astype(F32)
        g, s = spot(n)
        out_ref[g, at.z, mine, lanes(s, at.hi)] = total.astype(BF)
        for k in range(1, ns):
            az_copy(n, k).start()

    def stage_az(n):
        for k in range(1, ns):
            az_copy(n, k, at.z_at(-k)).wait_recv()
        for m in range(1, nh):
            ay_copy(n, m).start()

    def stage_ay(n):
        for m in range(1, nh):
            ay_copy(n, m).wait_recv()
        ac_start(n)

    lo = lax.broadcasted_iota(jnp.int32, (rows, 128), 1) < 64

    def pair(step):
        s, hi = step // nh, lax.rem(step, nh)
        p = hi * per + s
        col = pl.ds(pl.multiple_of(p * 128, 128), 128)
        k2 = k_ref[:, col]
        v2 = v_ref[:, col]
        q2 = q_ref[:, col]
        dc2 = dc_ref[:, col]
        both = dc2.astype(F32) * ctx_ref[:, col]
        lse2 = lse_ref[p]
        dq, dk, dv = [], None, None
        for h in range(2):
            mask = lo if h == 0 else jnp.logical_not(lo)
            qm = jnp.where(mask, q2, jnp.zeros_like(q2))
            dmask = jnp.where(mask, dc2, jnp.zeros_like(q2))
            lse = lse2[:, 0:1] if h == 0 else lse2[:, 64:65]
            dot = jnp.sum(jnp.where(mask, both, 0.0), axis=-1, keepdims=True)
            probs = jnp.exp(nt(qm, k2) * score_scale - lse)
            slopes = nt(dmask, v2)
            dscore = (probs * (slopes - dot) * score_scale).astype(BF)
            dq.append(nn(dscore, k2))
            a = nn(dmask.T, probs.astype(BF))
            b = nn(qm.T, dscore)
            dv = a if dv is None else dv + a
            dk = b if dk is None else dk + b
        dq2 = jnp.where(lo, dq[0], dq[1])
        gv_ref_row = jnp.sum(dq2, axis=0, keepdims=True)
        vb[2, 0:1, col] = gv_ref_row
        dq2 = dq2.astype(BF)
        dqt[col, :] = dq2.T
        dkb = dk.astype(BF)
        dvb = dv.astype(BF)
        dkt[col, :] = dkb
        dvt[col, :] = dvb
        shard = 2 * half
        for j in range(nf):
            for part in range(2):
                here = pl.ds(j * shard + part * half, half)
                ga[s, hi, j, part, 0] = nn(
                    ht_ref[here, pl.ds(pl.multiple_of(at.z * rows, 128), rows)], dq2
                ).astype(BF)
                ga[s, hi, j, part, 1] = nt(ht_ref[here, :], dkb).astype(BF)
                ga[s, hi, j, part, 2] = nt(ht_ref[here, :], dvb).astype(BF)

    def spread():
        def block(b):
            part = pl.ds(pl.multiple_of(b * rows, 128), rows)
            return nn(w_ref[1], dkt[:, part]) + nn(w_ref[2], dvt[:, part])

        for k in range(1, ns):
            dhs[k - 1] = block(at.z_at(k)).astype(BF)
            d_copy(k).start()
        dho[...] = block(at.z) + nn(w_ref[0], dqt[...])

    def d_copy(k):
        return remote(dhs.at[k - 1], dhr.at[k - 1], ds.at[k - 1], dm.at[k - 1], at.z_peer(k))

    def first_norm():
        for k in range(1, ns):
            d_copy(k).wait_recv()
        total = dho[...]
        for k in range(ns - 1):
            total += dhr[k].astype(F32)
        total = total.T
        normed, inverse = normalize(frames_ref[...])
        scaled = total * vec_ref[0:1, :]
        inner = (
            scaled
            - jnp.mean(scaled, axis=-1, keepdims=True)
            - normed * jnp.mean(scaled * normed, axis=-1, keepdims=True)
        )
        ig_ref[...] = gm_ref[...] + inverse * inner
        vb[1] = gv_ref[...]
        vb[1, 0:1, :] = jnp.sum(total * normed, axis=0, keepdims=True)
        vb[1, 1:2, :] = jnp.sum(total, axis=0, keepdims=True)
        vb[1, 2:3, :] = vb[2, 0:1, :]

    def v_core():
        return remote(vb.at[1], vb.at[0], vs.at[0], vr.at[0], at.sibling())

    def v_x(k):
        return remote(vx.at[at.x], vx.at[at.x], vs.at[k], vr.at[k], at.x_peer(k))

    def v_y(m):
        return remote(vy.at[at.hi], vy.at[at.hi], vs.at[nf + m], vr.at[nf + m], at.y_peer(m))

    def v_z(k):
        return remote(
            vz.at[at.z], vz.at[at.z], vs.at[nf + nh + k], vr.at[nf + nh + k], at.z_peer(k)
        )

    def v_step(i):
        if i == 0:
            v_core().start()
        elif i == 1:
            v_core().wait_recv()
            vx[at.x] = vb[0] + vb[1]
            for k in range(1, nf):
                v_x(k).start()
        elif i == 2:
            for k in range(1, nf):
                v_x(k).wait_recv()
            total = vx[0]
            for j in range(1, nf):
                total += vx[j]
            vy[at.hi] = total
            for m in range(1, nh):
                v_y(m).start()
        elif i == 3:
            for m in range(1, nh):
                v_y(m).wait_recv()
            total = vy[0]
            for j in range(1, nh):
                total += vy[j]
            vz[at.z] = total
            for k in range(1, ns):
                v_z(k).start()
        else:
            for k in range(1, ns):
                v_z(k).wait_recv()
            total = vz[0]
            for j in range(1, ns):
                total += vz[j]
            ov_ref[...] = total

    c_send(0)
    c_send(1)
    pairs = width // 128

    def step(n, carry):
        @pl.when(n < chunks)
        def _():
            stage_c(n)

        @pl.when(n < pairs)
        def _():
            pair(n)

        @pl.when(n == 2 * per - 2)
        def _():
            pltpu.make_async_copy(ga.at[:, :, :, :, 3], ga.at[:, :, :, :, 3], os.at[2]).wait()

        @pl.when(n + 2 < chunks)
        def _():
            c_send(n + 2)

        @pl.when(n == pairs)
        def _():
            spread()

        for lag, stage in ((1, stage_x), (2, stage_y), (3, stage_z), (4, stage_az), (5, stage_ay)):
            @pl.when(jnp.logical_and(n >= lag, n < chunks + lag))
            def _(lag=lag, stage=stage):
                stage(n - lag)

        @pl.when(n == chunks + 2)
        def _():
            first_norm()
            v_step(0)

        @pl.when(n == chunks + 3)
        def _():
            v_step(1)

        @pl.when(n == chunks + 4)
        def _():
            v_step(2)

        return carry

    lax.fori_loop(0, chunks + 5, step, 0)
    v_step(3)
    for n in range(chunks):
        ac_whole(n).wait()
    v_step(4)

    def drain(n, carry):
        c_whole(n).wait_send()
        for k in range(1, nf):
            x_copy(n, k).wait_send()
        for m in range(1, nh):
            y_copy(n, m).wait_send()
            ay_copy(n, m).wait_send()
        for k in range(1, ns):
            z_copy(n, k).wait_send()
            az_copy(n, k).wait_send()
        return carry

    lax.fori_loop(0, chunks, drain, 0)
    for k in range(1, ns):
        d_copy(k).wait_send()
        v_z(k).wait_send()
    for k in range(1, nf):
        v_x(k).wait_send()
    for m in range(1, nh):
        v_y(m).wait_send()
    v_core().wait_send()


def back_all(sizes, q, k, v, dc, ctx, lse, ht, w, gm, frames, vec, gv, gc, ge, go):
    nd, nf, ns = sizes
    nh = nd // 2
    rows, width = q.shape
    shard = go.shape[1]
    half = shard // 2
    every = k.shape[0]
    per = width // nh // 128
    chunks = 3 * per
    xn, yn, zn = max(nf - 1, 1), max(nh - 1, 1), max(ns - 1, 1)
    dma = pltpu.SemaphoreType.DMA
    anywhere = pl.BlockSpec(memory_space=pl.ANY)
    return pl.pallas_call(
        functools.partial(back_kernel, sizes),
        out_shape=(
            jax.ShapeDtypeStruct((3, 4, shard, width), BF),
            jax.ShapeDtypeStruct((rows, width), F32),
            jax.ShapeDtypeStruct((16, width), F32),
        ),
        in_specs=[vmem()] * 12 + [anywhere] * 3,
        out_specs=(vmem(),) * 3,
        scratch_shapes=[
            pltpu.VMEM((per, nh, nf, 2, 4, half, 128), BF),
            pltpu.VMEM((2, nh, nf, 4, half, 128), BF),
            pltpu.VMEM((chunks, nh, nf, 4, half, 128), BF),
            pltpu.VMEM((chunks, xn, nh, 4, half, 128), BF),
            pltpu.VMEM((chunks, yn, 4, half, 128), BF),
            pltpu.VMEM((chunks, zn, half, 128), BF),
            pltpu.VMEM((width, every), BF),
            pltpu.VMEM((width, every), BF),
            pltpu.VMEM((width, rows), BF),
            pltpu.VMEM((zn, width, rows), BF),
            pltpu.VMEM((zn, width, rows), BF),
            pltpu.VMEM((width, rows), F32),
            pltpu.VMEM((3, 16, width), F32),
            pltpu.VMEM((nf, 16, width), F32),
            pltpu.VMEM((nh, 16, width), F32),
            pltpu.VMEM((ns, 16, width), F32),
            dma((3,)),
            dma((chunks,)), dma((chunks,)),
            dma((chunks, xn)), dma((chunks, xn)),
            dma((chunks, yn)), dma((chunks, yn)),
            dma((chunks, zn)), dma((chunks, zn)),
            dma((chunks, zn)), dma((chunks, zn)),
            dma((chunks, yn)), dma((chunks, yn)),
            dma((chunks,)), dma((chunks,)),
            dma((zn,)), dma((zn,)),
            dma((nf + nh + ns,)), dma((nf + nh + ns,)),
        ],
        name="back",
        compiler_params=pltpu.CompilerParams(
            collective_id=1, has_side_effects=True, vmem_limit_bytes=67043328
        ),
    )(q, k, v, dc, ctx, lse, ht, w, gm, frames, vec, gv, gc, ge, go)


def adam_kernel(g_ref, w_ref, m_ref, v_ref, go_ref, wo_ref, mo_ref, vo_ref):
    gradient = g_ref[...].reshape(w_ref.shape).astype(F32)
    go_ref[...] = gradient
    wo_ref[...], mo_ref[...], vo_ref[...] = adam_update(
        w_ref[...], gradient, m_ref[...], v_ref[...], rate_matrix, decay_matrix
    )


def adam(group, out, weight, first, second, name):
    shard, width = out.shape[2:]
    rows = min(192, shard)
    parts = shard // rows
    if group == 1:
        grid_map = lambda u, r: (r, u)
    else:
        grid_map = lambda u, r: (u * parts + r, 0)
    spec = pl.BlockSpec((rows, width), grid_map)
    shape = jax.ShapeDtypeStruct(weight.shape, F32)
    return pl.pallas_call(
        adam_kernel,
        grid=(4, parts),
        out_shape=(shape,) * 4,
        in_specs=[pl.BlockSpec((None, None, rows, width), lambda u, r: (group, u, r, 0))] + [spec] * 3,
        out_specs=(spec,) * 4,
        name=name,
        compiler_params=pltpu.CompilerParams(vmem_limit_bytes=67043328),
    )(out, weight, first, second)


def on_device(
    sizes,
    frames_in,
    cotangent,
    attention_weight,
    expand_weight,
    contract_weight,
    vectors,
    first_attention,
    first_expand,
    first_contract,
    first_vectors,
    second_attention,
    second_expand,
    second_contract,
    second_vectors,
):
    nd, nf, ns = sizes
    frames = frames_in[0]
    upstream = cotangent[0]
    rows, width = frames.shape
    shard = attention_weight.shape[1]
    full = expand_weight.shape[1]
    vec_pad = jnp.pad(vectors, ((0, 4), (0, 0)))
    aw, ew, cw, vw, h_all = gather_all(
        sizes, frames, attention_weight, expand_weight, contract_weight, vec_pad
    )
    vec = jnp.transpose(vw, (1, 0, 2)).reshape(16, width)[:12].astype(F32)
    bias_expand = vec[8:].reshape(-1)
    h_own = lax.dynamic_slice_in_dim(h_all, lax.axis_index("seq") * rows, rows, 0)
    queries = (nn(h_own, aw[0]) + vec[2]).astype(BF)
    key_rows = nn(h_all, aw[1]).astype(BF)
    value_rows = (nn(h_all, aw[2]) + vec[3]).astype(BF)
    context_wide, log_total = attention(queries, key_rows, value_rows)
    context = context_wide.astype(BF)
    middle = frames + nn(context, aw[3]) + vec[4]
    normed_two, inverse_two = normalize(middle)
    hidden_two = (normed_two * vec[5] + vec[6]).astype(BF)
    expanded = nn(hidden_two, ew) + bias_expand
    activated = gelu_exact(expanded).astype(BF)
    frames_out = middle + nn(activated, cw) + vec[7]
    upstream_bf = upstream.astype(BF)
    grad_contract = tn(activated, upstream_bf).astype(BF)
    grad_expanded = nt(upstream_bf, cw) * gelu_slope(expanded)
    grad_expanded_bf = grad_expanded.astype(BF)
    grad_expand = tn(hidden_two, grad_expanded_bf).astype(BF)
    grad_hidden_two = nt(grad_expanded_bf, ew)
    back_two, gain_two_grad, bias_two_grad = norm_back(
        grad_hidden_two, normed_two, inverse_two, vec[5]
    )
    grad_middle = upstream + back_two
    grad_middle_bf = grad_middle.astype(BF)
    grad_output_w = tn(context, grad_middle_bf).astype(BF)
    grad_context = nt(grad_middle_bf, aw[3]).astype(BF)
    small = jnp.stack(
        [
            jnp.sum(grad_context.astype(F32), axis=0),
            jnp.sum(grad_middle, axis=0),
            gain_two_grad,
            bias_two_grad,
            jnp.sum(upstream, axis=0),
        ]
    )
    gv = jnp.concatenate(
        [jnp.zeros((3, width), F32), small, jnp.sum(grad_expanded, axis=0).reshape(-1, width),
         jnp.zeros((4, width), F32)], axis=0
    )
    out, input_gradient, gv_sum = back_all(
        sizes,
        queries,
        key_rows,
        value_rows,
        grad_context,
        context_wide,
        log_total,
        h_all.T,
        aw,
        grad_middle,
        frames,
        vec[:8],
        gv,
        grad_contract.reshape(nf, 4, shard, width),
        grad_expand.reshape(nf, shard, full),
        grad_output_w.reshape(nf, shard, width),
    )
    owned_vec = lax.dynamic_slice_in_dim(
        gv_sum[:12], lax.axis_index("fsdp") * (width // nf), width // nf, 1
    )
    flat = (4 * shard, width)
    contract_out = adam(0, out, contract_weight, first_contract, second_contract, "adam_contract")
    expand_out = adam(1, out, expand_weight, first_expand, second_expand, "adam_expand")
    attention_out = adam(
        2, out, attention_weight.reshape(flat), first_attention.reshape(flat),
        second_attention.reshape(flat), "adam_attention"
    )
    attention_out = [each.reshape(attention_weight.shape) for each in attention_out]
    vector_out = (owned_vec,) + adam_update(
        vectors, owned_vec, first_vectors, second_vectors, rate_vector, 0.0
    )
    result = [frames_out[None], input_gradient[None]]
    for i in range(4):
        result += [attention_out[i], expand_out[i], contract_out[i], vector_out[i]]
    return tuple(result)


def solution(mesh):
    sizes = (mesh.shape["dp"], mesh.shape["fsdp"], mesh.shape["seq"])
    data = P(("dp", "fsdp"), "seq", None)
    state = (P(None, "fsdp", None), P("fsdp", None), P("fsdp", None), P(None, "fsdp"))
    return jax.shard_map(
        functools.partial(on_device, sizes),
        mesh=mesh,
        in_specs=(data, data) + state * 3,
        out_specs=(data, data) + state * 4,
        check_vma=False,
    )
```

```python
import functools

import jax
import jax.numpy as jnp
from jax import lax
from jax.experimental import pallas as pl
from jax.experimental.pallas import tpu as pltpu
from jax.sharding import PartitionSpec as P

HEADS = 12
norm_eps = 1e-05
beta_one = 0.9
beta_two = 0.999
adam_eps = 1e-08
adam_count = 5.0
rate_matrix = 0.02
rate_vector = 0.1
decay_matrix = 0.1
score_scale = 0.125
VMEM_LIMIT = 60 << 20
MESH = pl.DeviceIdType.MESH
BF = jnp.bfloat16
F32 = jnp.float32


def nt(left, right):
    return lax.dot_general(left, right, (((1,), (1,)), ((), ())), preferred_element_type=F32)


def nn(left, right):
    return lax.dot_general(left, right, (((1,), (0,)), ((), ())), preferred_element_type=F32)


def tn(left, right):
    return lax.dot_general(left, right, (((0,), (0,)), ((), ())), preferred_element_type=F32)


def vmem():
    return pl.BlockSpec(memory_space=pltpu.VMEM)


def normalize(values):
    center = values - jnp.mean(values, axis=-1, keepdims=True)
    inverse = lax.rsqrt(jnp.mean(center * center, axis=-1, keepdims=True) + norm_eps)
    return center * inverse, inverse


def norm_back(upstream, normed, inverse, gain):
    scaled = upstream * gain
    inner = (
        scaled
        - jnp.mean(scaled, axis=-1, keepdims=True)
        - normed * jnp.mean(scaled * normed, axis=-1, keepdims=True)
    )
    return (inverse * inner, jnp.sum(upstream * normed, axis=0), jnp.sum(upstream, axis=0))


def gelu_exact(values):
    return 0.5 * values * (1.0 + lax.erf(values * 0.7071067811865476))


def gelu_slope(values):
    return (
        0.5 * (1.0 + lax.erf(values * 0.7071067811865476))
        + values * jnp.exp(-0.5 * values * values) * 0.3989422804014327
    )


def adam_update(weight, gradient, first, second, rate, decay):
    first_new = beta_one * first + (1.0 - beta_one) * gradient
    second_new = beta_two * second + (1.0 - beta_two) * gradient * gradient
    first_hat = first_new / (1.0 - beta_one**adam_count)
    second_hat = second_new / (1.0 - beta_two**adam_count)
    updated = weight - rate * (first_hat / (jnp.sqrt(second_hat) + adam_eps) + decay * weight)
    return (updated, first_new, second_new)


class Place:
    def __init__(self, sizes):
        self.nd, self.nf, self.ns = sizes
        self.nh = self.nd // 2
        self.dp = lax.axis_index("dp")
        self.x = lax.axis_index("fsdp")
        self.z = lax.axis_index("seq")
        self.core = lax.rem(self.dp, 2)
        self.hi = self.dp // 2

    def sibling(self):
        return {"dp": self.hi * 2 + 1 - self.core}

    def x_peer(self, k):
        return {"fsdp": lax.rem(self.x + k, self.nf)}

    def y_hi(self, k):
        return lax.rem(self.hi + k, self.nh)

    def y_peer(self, k):
        return {"dp": self.y_hi(k) * 2 + self.core}

    def z_at(self, k):
        return lax.rem(self.z + k + self.ns, self.ns)

    def z_peer(self, k):
        return {"seq": self.z_at(k)}

    def everyone(self):
        out = [self.sibling()]
        out += [self.x_peer(k) for k in range(1, self.nf)]
        out += [self.y_peer(k) for k in range(1, self.nh)]
        out += [self.z_peer(k) for k in range(1, self.ns)]
        return out

    def barrier(self):
        sem = pltpu.get_barrier_semaphore()
        peers = self.everyone()
        for peer in peers:
            pl.semaphore_signal(sem, inc=1, device_id=peer, device_id_type=MESH)
        pl.semaphore_wait(sem, len(peers))


def remote(src, dst, send, recv, peer):
    return pltpu.make_async_remote_copy(
        src_ref=src, dst_ref=dst, send_sem=send, recv_sem=recv, device_id=peer, device_id_type=MESH
    )


def gather_kernel(
    sizes, frames_ref, aw_ref, ew_ref, cw_ref, vec_ref,
    a_ref, e_ref, c_ref, v_ref, h_ref,
    xs, xr, ys, yr, s1s, s1r, s2s, s2r, vs, vr, rs, ls, hr,
):
    at = Place(sizes)
    nf, nh, ns = at.nf, at.nh, at.ns
    rows, width = frames_ref.shape
    shard = aw_ref.shape[1]
    half = shard // 2
    at.barrier()
    v_ref[at.x] = vec_ref[...].astype(BF)
    vec_copies = []
    for k in range(1, nf):
        copy = remote(v_ref.at[at.x], v_ref.at[at.x], vs.at[k], vr.at[k], at.x_peer(k))
        copy.start()
        vec_copies.append(copy)

    def view(chunk, j, hi, core):
        if chunk < 2:
            first, count = ((0, 3), (3, 1))[chunk]
            cols = width // nh
            return a_ref.at[
                pl.ds(first, count),
                pl.ds(pl.multiple_of(j * shard + core * half, 16), half),
                pl.ds(pl.multiple_of(hi * cols, 128), cols),
            ]
        if chunk == 2:
            cols = e_ref.shape[1] // nh
            return e_ref.at[
                pl.ds(pl.multiple_of(j * shard + core * half, 16), half),
                pl.ds(pl.multiple_of(hi * cols, 128), cols),
            ]
        cols = width // nh
        deep = c_ref.shape[0] // nf
        return c_ref.at[
            pl.ds(pl.multiple_of(j * deep + core * (deep // 2), 16), deep // 2),
            pl.ds(pl.multiple_of(hi * cols, 128), cols),
        ]

    own = pl.multiple_of(at.x * shard, 16)
    x_copies = {}

    def send_chunk(chunk):
        for k in range(1, nf):
            piece = view(chunk, at.x, at.hi, at.core)
            copy = remote(piece, piece, xs.at[chunk, k], xr.at[chunk, k], at.x_peer(k))
            copy.start()
            x_copies[chunk, k] = copy

    for u in range(3):
        a_ref[u, pl.ds(own, shard), :] = aw_ref[u].astype(BF)
    send_chunk(0)
    normed, _ = normalize(frames_ref[...])
    for copy in vec_copies:
        copy.wait()
    gain = jnp.concatenate([v_ref[j, 0:1, :] for j in range(nf)], axis=1).astype(F32)
    offset = jnp.concatenate([v_ref[j, 1:2, :] for j in range(nf)], axis=1).astype(F32)
    h_ref[pl.ds(pl.multiple_of(at.z * rows, 16), rows), :] = (normed * gain + offset).astype(BF)

    def block(b):
        return h_ref.at[pl.ds(pl.multiple_of(b * rows, 16), rows), :]

    def to_right(b):
        return remote(block(b), block(b), rs.at[b], hr.at[b], {"seq": at.z + 1})

    def to_left(b):
        return remote(block(b), block(b), ls.at[b], hr.at[b], {"seq": at.z - 1})

    @pl.when(at.z < ns - 1)
    def _():
        to_right(at.z).start()

    @pl.when(at.z > 0)
    def _():
        to_left(at.z).start()

    a_ref[3, pl.ds(own, shard), :] = aw_ref[3].astype(BF)
    send_chunk(1)
    e_ref[pl.ds(own, shard), :] = ew_ref[...].astype(BF)
    send_chunk(2)
    deep = cw_ref.shape[0]
    c_ref[pl.ds(pl.multiple_of(at.x * deep, 16), deep), :] = cw_ref[...].astype(BF)
    send_chunk(3)

    pending = []

    def forward(chunk):
        for k in range(1, nf):
            x_copies[chunk, k].wait_recv()
            j = lax.rem(at.x - k + nf, nf)
            piece = view(chunk, j, at.hi, at.core)
            copy = remote(piece, piece, s1s.at[chunk, k], s1r.at[chunk, k], at.sibling())
            copy.start()
            pending.append(copy)
            for m in range(1, nh):
                copy = remote(piece, piece, ys.at[chunk, k, m], yr.at[chunk, k, m], at.y_peer(m))
                copy.start()
                pending.append((copy, chunk, k, m))

    def relay(chunk):
        for k in range(1, nf):
            for m in range(1, nh):
                j = lax.rem(at.x - k + nf, nf)
                hi = lax.rem(at.hi - m + nh, nh)
                piece = view(chunk, j, hi, at.core)
                remote(piece, piece, ys.at[chunk, k, m], yr.at[chunk, k, m], at.y_peer(m)).wait_recv()
                copy = remote(piece, piece, s2s.at[chunk, k, m], s2r.at[chunk, k, m], at.sibling())
                copy.start()
                pending.append(copy)

    def hop(s):
        b = at.z - s

        @pl.when(b >= 0)
        def _():
            to_right(b).wait_recv()

            @pl.when(at.z < ns - 1)
            def _():
                to_right(b).start()

        d = at.z + s

        @pl.when(d < ns)
        def _():
            to_left(d).wait_recv()

            @pl.when(at.z > 0)
            def _():
                to_left(d).start()

    forward(0)
    hop(1)
    forward(1)
    relay(0)
    relay(1)
    for s in range(2, ns - 1):
        hop(s)
    forward(2)
    relay(2)
    if ns > 2:
        hop(ns - 1)
    forward(3)
    relay(3)
    for entry in pending:
        if isinstance(entry, tuple):
            entry[0].wait_send()
        else:
            entry.wait()
    for copy in x_copies.values():
        copy.wait_send()
    for b in range(ns):
        @pl.when(jnp.logical_and(b <= at.z, at.z < ns - 1))
        def _():
            to_right(b).wait_send()

        @pl.when(jnp.logical_and(b >= at.z, at.z > 0))
        def _():
            to_left(b).wait_send()


def gather_all(sizes, frames, aw, ew, cw, vec):
    nd, nf, ns = sizes
    nh = nd // 2
    rows, width = frames.shape
    deep = cw.shape[0] * nf
    dma = pltpu.SemaphoreType.DMA
    return pl.pallas_call(
        functools.partial(gather_kernel, sizes),
        out_shape=(
            jax.ShapeDtypeStruct((4, width, width), BF),
            jax.ShapeDtypeStruct((width, ew.shape[1]), BF),
            jax.ShapeDtypeStruct((deep, width), BF),
            jax.ShapeDtypeStruct((nf, 16, vec.shape[1]), BF),
            jax.ShapeDtypeStruct((rows * ns, width), BF),
        ),
        in_specs=[vmem()] * 5,
        out_specs=(vmem(),) * 5,
        scratch_shapes=[
            dma((4, nf)), dma((4, nf)),
            dma((4, nf, nh)), dma((4, nf, nh)),
            dma((4, nf)), dma((4, nf)),
            dma((4, nf, nh)), dma((4, nf, nh)),
            dma((nf,)), dma((nf,)),
            dma((ns,)), dma((ns,)), dma((ns,)),
        ],
        name="gather",
        compiler_params=pltpu.CompilerParams(
            collective_id=0, has_side_effects=True, vmem_limit_bytes=VMEM_LIMIT
        ),
    )(frames, aw, ew, cw, vec)


def attention_kernel(chunk, q_ref, k_ref, v_ref, ctx_ref, lse_ref):
    rows = q_ref.shape[0]
    lo = lax.broadcasted_iota(jnp.int32, (chunk, 128), 1) < 64

    def pair(p, carry):
        col = pl.ds(pl.multiple_of(p * 128, 128), 128)
        k2 = k_ref[:, col]
        v2 = v_ref[:, col]
        for c in range(rows // chunk):
            part = pl.ds(c * chunk, chunk)
            q2 = q_ref[part, col]
            ctx, lse = [], []
            for h in range(2):
                mask = lo if h == 0 else jnp.logical_not(lo)
                s = nt(jnp.where(mask, q2, jnp.zeros_like(q2)), k2) * score_scale
                largest = jnp.max(s, axis=-1, keepdims=True)
                e = jnp.exp(s - largest)
                total = jnp.sum(e, axis=-1, keepdims=True)
                ctx.append(nn((e * (1.0 / total)).astype(BF), v2))
                lse.append(largest + jnp.log(total))
            ctx_ref[part, col] = jnp.where(lo, ctx[0], ctx[1])
            lse_ref[p, part, :] = jnp.where(lo, lse[0], lse[1])
        return carry

    lax.fori_loop(0, q_ref.shape[1] // 128, pair, 0)


def attention(q, k, v):
    rows, width = q.shape
    return pl.pallas_call(
        functools.partial(attention_kernel, rows),
        out_shape=(
            jax.ShapeDtypeStruct((rows, width), F32),
            jax.ShapeDtypeStruct((width // 128, rows, 128), F32),
        ),
        in_specs=[vmem()] * 3,
        out_specs=(vmem(), vmem()),
        name="attention",
        compiler_params=pltpu.CompilerParams(vmem_limit_bytes=VMEM_LIMIT),
    )(q, k, v)


def back_kernel(
    sizes, q_ref, k_ref, v_ref, dc_ref, ctx_ref, lse_ref, ht_ref, w_ref, gm_ref, frames_ref,
    vec_ref, gv_ref, gc_ref, ge_ref, go_ref,
    out_ref, ig_ref, ov_ref,
    ga, own, rc, rx, ry, rza, rzb, dkt, dvt, dqa, dhs, dhr, vb, vx, vy, vz,
    os, cs, cr, xs, xr, ys, yr, zas, zar, zbs, zbr, gbs, gbr, gas, gar, ays, ayr, acs, acr,
    das, dar, vs, vr,
):
    at = Place(sizes)
    nf, nh, ns = at.nf, at.nh, at.ns
    rows, width = q_ref.shape
    q = rc.shape[5]
    cols = width // nh
    per = cols // 128
    chunks = rc.shape[0]
    split = chunks // (3 * per)
    half = q * split
    group = per * split
    b0 = lax.rem(at.z, 2)
    b1 = at.z // 2
    at.barrier()

    def strip(core, r):
        return pl.ds(pl.multiple_of(core * half + r * q, 16), q)

    def lanes(s, hi):
        return pl.ds(pl.multiple_of(hi * cols + s * 128, 128), 128)

    def place_of(n):
        return n // group, lax.rem(n, group) // split, lax.rem(n, split)

    for s in range(per):
        for hi in range(nh):
            for part in range(2):
                for r in range(split):
                    pltpu.make_async_copy(
                        go_ref.at[:, pl.ds(part * half + r * q, q), pl.ds(hi * cols + s * 128, 128)],
                        ga.at[s, r, hi, :, part, 1, 1],
                        os.at[4],
                    ).start()

    def own_whole(slot):
        return pltpu.make_async_copy(own.at[slot], own.at[slot], os.at[slot])

    def c_whole(n):
        return remote(rc.at[n], rc.at[n], cs.at[n], cr.at[n], at.sibling())

    def c_send(n):
        slot = lax.rem(n, 4)
        g, s, r = place_of(n)

        @pl.when(n < group)
        def _():
            for hi in range(nh):
                for u in range(4):
                    block = lanes(s, hi)
                    remote(
                        gc_ref.at[:, u, strip(1 - at.core, r), block],
                        rc.at[n, hi, :, u // 2, u % 2], cs.at[n], cr.at[n], at.sibling(),
                    ).start()
                    pltpu.make_async_copy(
                        gc_ref.at[:, u, strip(at.core, r), block],
                        own.at[slot, hi, :, u // 2, u % 2], os.at[slot],
                    ).start()

        @pl.when(jnp.logical_and(n >= group, n < 2 * group))
        def _():
            for hi in range(nh):
                for u in range(4):
                    block = pl.ds(pl.multiple_of(u * width + hi * cols + s * 128, 128), 128)
                    remote(
                        ge_ref.at[:, strip(1 - at.core, r), block],
                        rc.at[n, hi, :, u // 2, u % 2], cs.at[n], cr.at[n], at.sibling(),
                    ).start()
                    pltpu.make_async_copy(
                        ge_ref.at[:, strip(at.core, r), block],
                        own.at[slot, hi, :, u // 2, u % 2], os.at[slot],
                    ).start()

        @pl.when(jnp.logical_and(n >= 2 * group, n < chunks))
        def _():
            remote(
                ga.at[s, r, :, :, 1 - at.core], rc.at[n], cs.at[n], cr.at[n], at.sibling()
            ).start()

    def x_copy(n, k):
        peer = lax.rem(at.x + k, nf)
        return remote(rc.at[n, :, peer], rx.at[n, k - 1], xs.at[n, k - 1], xr.at[n, k - 1], at.x_peer(k))

    def y_copy(n, m):
        return remote(
            rx.at[n, 0, at.y_hi(m)], ry.at[n, m - 1], ys.at[n, m - 1], yr.at[n, m - 1], at.y_peer(m)
        )

    near = {"seq": at.z + 1 - 2 * b0}
    far = {"seq": at.z + 2 - 4 * b1}

    def za_copy(n):
        return remote(ry.at[n, 0, :, 1 - b0], rza.at[n], zas.at[n], zar.at[n], near)

    def zb_copy(n):
        return remote(rza.at[n, 1 - b1], rzb.at[n], zbs.at[n], zbr.at[n], far)

    def gb_copy(n):
        g, s, r = place_of(n)
        place = out_ref.at[g, b1, b0, strip(at.core, r), lanes(s, at.hi)]
        return remote(place, place, gbs.at[n], gbr.at[n], far)

    def ga_copy(n):
        g, s, r = place_of(n)
        place = out_ref.at[g, :, b0, strip(at.core, r), lanes(s, at.hi)]
        return remote(place, place, gas.at[n], gar.at[n], near)

    def ay_copy(n, m):
        g, s, r = place_of(n)
        place = out_ref.at[g, :, :, strip(at.core, r), lanes(s, at.hi)]
        return remote(place, place, ays.at[n, m - 1], ayr.at[n, m - 1], at.y_peer(m))

    def ac_start(n):
        g, s, r = place_of(n)
        for hi in range(nh):
            place = out_ref.at[g, :, :, strip(at.core, r), lanes(s, hi)]
            remote(place, place, acs.at[n], acr.at[n], at.sibling()).start()

    def ac_whole(n):
        return remote(rx.at[n, 0], rx.at[n, 0], acs.at[n], acr.at[n], at.sibling())

    def split_index(i):
        return i // (nf * 4), lax.rem(i // 4, nf), lax.rem(i, 4) // 2, lax.rem(i, 2)

    def stage_c(n):
        c_whole(n).wait_recv()
        slot = lax.rem(n, 4)
        _, s, r = place_of(n)

        @pl.when(n < 2 * group)
        def _():
            own_whole(slot).wait()

            def add(i, carry):
                at_i = split_index(i)
                rc[(n,) + at_i] = (
                    rc[(n,) + at_i].astype(F32) + own[(slot,) + at_i].astype(F32)
                ).astype(BF)
                return carry

            lax.fori_loop(0, nh * nf * 4, add, 0)

        @pl.when(n >= 2 * group)
        def _():
            def add(i, carry):
                hi, j, ua, ub = split_index(i)
                rc[n, hi, j, ua, ub] = (
                    rc[n, hi, j, ua, ub].astype(F32) + ga[s, r, hi, j, at.core, ua, ub].astype(F32)
                ).astype(BF)
                return carry

            lax.fori_loop(0, nh * nf * 4, add, 0)

        for k in range(1, nf):
            x_copy(n, k).start()

    def stage_x(n):
        for k in range(1, nf):
            x_copy(n, k).wait_recv()

        def add(i, carry):
            hi, ua, ub = i // 4, lax.rem(i, 4) // 2, lax.rem(i, 2)
            total = rc[n, hi, at.x, ua, ub].astype(F32)
            for k in range(nf - 1):
                total += rx[n, k, hi, ua, ub].astype(F32)
            rx[n, 0, hi, ua, ub] = total.astype(BF)
            return carry

        lax.fori_loop(0, nh * 4, add, 0)
        for m in range(1, nh):
            y_copy(n, m).start()

    def stage_y(n):
        for m in range(1, nh):
            y_copy(n, m).wait_recv()

        def add(i, carry):
            ua, ub = i // 2, lax.rem(i, 2)
            total = rx[n, 0, at.hi, ua, ub].astype(F32)
            for m in range(nh - 1):
                total += ry[n, m, ua, ub].astype(F32)
            ry[n, 0, ua, ub] = total.astype(BF)
            return carry

        lax.fori_loop(0, 4, add, 0)
        za_copy(n).start()

    def stage_za(n):
        za_copy(n).wait_recv()
        for ua in range(2):
            rza[n, ua] = (ry[n, 0, ua, b0].astype(F32) + rza[n, ua].astype(F32)).astype(BF)
        zb_copy(n).start()

    def stage_zb(n):
        zb_copy(n).wait_recv()
        g, s, r = place_of(n)
        out_ref[g, b1, b0, strip(at.core, r), lanes(s, at.hi)] = (
            rza[n, b1].astype(F32) + rzb[n].astype(F32)
        ).astype(BF)
        gb_copy(n).start()

    def stage_gb(n):
        gb_copy(n).wait_recv()
        ga_copy(n).start()

    def stage_ga(n):
        ga_copy(n).wait_recv()
        for m in range(1, nh):
            ay_copy(n, m).start()

    def stage_ay(n):
        for m in range(1, nh):
            ay_copy(n, m).wait_recv()
        ac_start(n)

    lo = lax.broadcasted_iota(jnp.int32, (rows, 128), 1) < 64
    pairs = width // 128

    def block_of(i):
        return lax.rem(at.z + 1 + i, ns)

    def unit(index):
        i, p = index // pairs, lax.rem(index, pairs)
        there = block_of(i)
        keys = pl.ds(pl.multiple_of(there * rows, 128), rows)
        col = pl.ds(pl.multiple_of(p * 128, 128), 128)
        k2 = k_ref[keys, col]
        v2 = v_ref[keys, col]
        q2 = q_ref[:, col]
        dc2 = dc_ref[:, col]
        both = dc2.astype(F32) * ctx_ref[:, col]
        lse2 = lse_ref[p]
        dq, dk, dv = [], None, None
        for h in range(2):
            mask = lo if h == 0 else jnp.logical_not(lo)
            qm = jnp.where(mask, q2, jnp.zeros_like(q2))
            dmask = jnp.where(mask, dc2, jnp.zeros_like(q2))
            lse = lse2[:, 0:1] if h == 0 else lse2[:, 64:65]
            dot = jnp.sum(jnp.where(mask, both, 0.0), axis=-1, keepdims=True)
            probs = jnp.exp(nt(qm, k2) * score_scale - lse)
            slopes = nt(dmask, v2)
            dscore = (probs * (slopes - dot) * score_scale).astype(BF)
            dq.append(nn(dscore, k2))
            a = nn(dmask.T, probs.astype(BF))
            b = nn(qm.T, dscore)
            dv = a if dv is None else dv + a
            dk = b if dk is None else dk + b
        dq2 = jnp.where(lo, dq[0], dq[1])

        @pl.when(i == 0)
        def _():
            dqa[:, col] = dq2

        @pl.when(i > 0)
        def _():
            dqa[:, col] += dq2

        dkt[col, keys] = dk.astype(BF)
        dvt[col, keys] = dv.astype(BF)

    def weights(s):
        frames = pl.ds(pl.multiple_of(at.z * rows, 128), rows)
        for hi in range(nh):
            col = pl.ds(hi * cols + s * 128, 128)
            dq2 = dqa[:, col]
            vb[2, 0:1, col] = jnp.sum(dq2, axis=0, keepdims=True)
            dq2 = dq2.astype(BF)
            dk2 = dkt[col, :]
            dv2 = dvt[col, :]
            for j in range(nf):
                for part in range(2):
                    for r in range(split):
                        here = pl.ds((2 * j + part) * half + r * q, q)
                        ga[s, r, hi, j, part, 0, 0] = nn(ht_ref[here, frames], dq2).astype(BF)
                        ga[s, r, hi, j, part, 0, 1] = nt(ht_ref[here, :], dk2).astype(BF)
                        ga[s, r, hi, j, part, 1, 0] = nt(ht_ref[here, :], dv2).astype(BF)

    pieces = 8

    def d_copy(i, t):
        part = pl.ds(t * (width // pieces), width // pieces)
        return remote(dhs.at[i, part], dhr.at[i, part], das.at[i], dar.at[i], at.z_peer(i + 1))

    def d_whole(i):
        return remote(dhs.at[i], dhr.at[i], das.at[i], dar.at[i], at.z_peer(i + 1))

    def spread(i):
        part = pl.ds(pl.multiple_of(block_of(i) * rows, 128), rows)
        total = nn(w_ref[1], dkt[:, part]) + nn(w_ref[2], dvt[:, part])
        if i == ns - 1:
            total += nt(w_ref[0], dqa[...].astype(BF))
        dhs[i] = total.astype(BF)

    def first_norm():
        total = dhs[ns - 1].astype(F32)
        for i in range(ns - 1):
            d_whole(i).wait_recv()
            total += dhr[i].astype(F32)
        total = total.T
        normed, inverse = normalize(frames_ref[...])
        scaled = total * vec_ref[0:1, :]
        inner = (
            scaled
            - jnp.mean(scaled, axis=-1, keepdims=True)
            - normed * jnp.mean(scaled * normed, axis=-1, keepdims=True)
        )
        ig_ref[...] = gm_ref[...] + inverse * inner
        vb[1] = gv_ref[...]
        vb[1, 0:1, :] = jnp.sum(total * normed, axis=0, keepdims=True)
        vb[1, 1:2, :] = jnp.sum(total, axis=0, keepdims=True)
        vb[1, 2:3, :] = vb[2, 0:1, :]

    def v_core():
        return remote(vb.at[1], vb.at[0], vs.at[0], vr.at[0], at.sibling())

    def v_x(k):
        return remote(vx.at[at.x], vx.at[at.x], vs.at[k], vr.at[k], at.x_peer(k))

    def v_y(m):
        return remote(vy.at[at.hi], vy.at[at.hi], vs.at[nf + m], vr.at[nf + m], at.y_peer(m))

    def v_z(k):
        return remote(
            vz.at[at.z], vz.at[at.z], vs.at[nf + nh + k], vr.at[nf + nh + k], at.z_peer(k)
        )

    def v_step(i):
        if i == 0:
            v_core().start()
        elif i == 1:
            v_core().wait_recv()
            vx[at.x] = vb[0] + vb[1]
            for k in range(1, nf):
                v_x(k).start()
        elif i == 2:
            for k in range(1, nf):
                v_x(k).wait_recv()
            total = vx[0]
            for j in range(1, nf):
                total += vx[j]
            vy[at.hi] = total
            for m in range(1, nh):
                v_y(m).start()
        elif i == 3:
            for m in range(1, nh):
                v_y(m).wait_recv()
            total = vy[0]
            for j in range(1, nh):
                total += vy[j]
            vz[at.z] = total
            for k in range(1, ns):
                v_z(k).start()
        else:
            for k in range(1, ns):
                v_z(k).wait_recv()
            total = vz[0]
            for j in range(1, ns):
                total += vz[j]
            ov_ref[...] = total

    ready = group + 2
    each = -(-ns * pairs // ready)
    done = [-(-pairs * (i + 1) // each) - 1 for i in range(ns)]
    norm = done[ns - 1] + 6
    stages = (stage_x, stage_y, stage_za, stage_zb, stage_gb, stage_ga, stage_ay)
    last = max(chunks + len(stages), norm + 6)
    for n in range(4):
        c_send(n)

    def step(n, carry):
        for k in range(2):
            @pl.when(2 * n + k < 2 * group)
            def _(k=k):
                stage_c(2 * n + k)

                @pl.when(2 * n + k + 4 < 2 * group)
                def _():
                    c_send(2 * n + k + 4)

        for s in range(per):
            @pl.when(n == ready + s + 1)
            def _(s=s):
                for r in range(split):
                    stage_c(2 * group + s * split + r)

        @pl.when(n < ready)
        def _():
            def one(k, carry):
                @pl.when(n * each + k < ns * pairs)
                def _():
                    unit(n * each + k)

                return carry

            lax.fori_loop(0, each, one, 0)

        for i in range(ns):
            @pl.when(n == done[i])
            def _(i=i):
                spread(i)

            if i < ns - 1:
                for late in range(2):
                    @pl.when(n == done[i] + late)
                    def _(i=i, late=late):
                        for t in range(pieces // 2):
                            d_copy(i, late * (pieces // 2) + t).start()

        @pl.when(n == norm)
        def _():
            first_norm()

        for s in range(per):
            @pl.when(n == ready + s)
            def _(s=s):
                weights(s)
                if s == 0:
                    whole = ga.at[:, :, :, :, :, 1, 1]
                    pltpu.make_async_copy(whole, whole, os.at[4]).wait()
                for r in range(split):
                    c_send(2 * group + s * split + r)

        for lag, stage in enumerate(stages):
            @pl.when(jnp.logical_and(n >= lag, n < chunks + lag))
            def _(lag=lag, stage=stage):
                stage(n - lag)

        for i in range(5):
            @pl.when(n == norm + i)
            def _(i=i):
                v_step(i)

        return carry

    lax.fori_loop(0, last, step, 0)
    for n in range(chunks):
        ac_whole(n).wait()

    def drain(n, carry):
        c_whole(n).wait_send()
        za_copy(n).wait_send()
        zb_copy(n).wait_send()
        gb_copy(n).wait_send()
        ga_copy(n).wait_send()
        for k in range(1, nf):
            x_copy(n, k).wait_send()
        for m in range(1, nh):
            y_copy(n, m).wait_send()
            ay_copy(n, m).wait_send()
        return carry

    lax.fori_loop(0, chunks, drain, 0)
    for i in range(ns - 1):
        d_whole(i).wait_send()
    for k in range(1, ns):
        v_z(k).wait_send()
    for k in range(1, nf):
        v_x(k).wait_send()
    for m in range(1, nh):
        v_y(m).wait_send()
    v_core().wait_send()


def back_all(sizes, q, k, v, dc, ctx, lse, ht, w, gm, frames, vec, gv, gc, ge, go):
    nd, nf, ns = sizes
    nh = nd // 2
    rows, width = q.shape
    shard = go.shape[1]
    half = shard // 2
    every = k.shape[0]
    split = 2 if half % 32 == 0 else 1
    strip = half // split
    per = width // nh // 128
    chunks = 3 * per * split
    xn, yn = max(nf - 1, 1), max(nh - 1, 1)
    dma = pltpu.SemaphoreType.DMA
    anywhere = pl.BlockSpec(memory_space=pl.ANY)
    return pl.pallas_call(
        functools.partial(back_kernel, sizes),
        out_shape=(
            jax.ShapeDtypeStruct((3, 2, 2, shard, width), BF),
            jax.ShapeDtypeStruct((rows, width), F32),
            jax.ShapeDtypeStruct((16, width), F32),
        ),
        in_specs=[vmem()] * 12 + [anywhere] * 3,
        out_specs=(vmem(),) * 3,
        scratch_shapes=[
            pltpu.VMEM((per, split, nh, nf, 2, 2, 2, strip, 128), BF),
            pltpu.VMEM((4, nh, nf, 2, 2, strip, 128), BF),
            pltpu.VMEM((chunks, nh, nf, 2, 2, strip, 128), BF),
            pltpu.VMEM((chunks, xn, nh, 2, 2, strip, 128), BF),
            pltpu.VMEM((chunks, yn, 2, 2, strip, 128), BF),
            pltpu.VMEM((chunks, 2, strip, 128), BF),
            pltpu.VMEM((chunks, strip, 128), BF),
            pltpu.VMEM((width, every), BF),
            pltpu.VMEM((width, every), BF),
            pltpu.VMEM((rows, width), F32),
            pltpu.VMEM((ns, width, rows), BF),
            pltpu.VMEM((ns - 1, width, rows), BF),
            pltpu.VMEM((3, 16, width), F32),
            pltpu.VMEM((nf, 16, width), F32),
            pltpu.VMEM((nh, 16, width), F32),
            pltpu.VMEM((ns, 16, width), F32),
            dma((5,)),
            dma((chunks,)), dma((chunks,)),
            dma((chunks, xn)), dma((chunks, xn)),
            dma((chunks, yn)), dma((chunks, yn)),
            dma((chunks,)), dma((chunks,)),
            dma((chunks,)), dma((chunks,)),
            dma((chunks,)), dma((chunks,)),
            dma((chunks,)), dma((chunks,)),
            dma((chunks, yn)), dma((chunks, yn)),
            dma((chunks,)), dma((chunks,)),
            dma((ns,)), dma((ns,)),
            dma((nf + nh + ns,)), dma((nf + nh + ns,)),
        ],
        name="back",
        compiler_params=pltpu.CompilerParams(
            collective_id=1, has_side_effects=True, vmem_limit_bytes=67043328
        ),
    )(q, k, v, dc, ctx, lse, ht, w, gm, frames, vec, gv, gc, ge, go)


def feed_kernel(
    ctx_ref, frames_ref, cot_ref, vec_ref, wo_ref, win_ref, wout_ref,
    fo_ref, gm_ref, dc_ref, gi_ref, gout_ref, go_ref, gv_ref,
    mid, h2, h2t, dyb, acc, dh2,
):
    b = pl.program_id(0)

    @pl.when(b == 0)
    def _():
        middle = frames_ref[...] + nn(ctx_ref[...].astype(BF), wo_ref[...]) + vec_ref[4:5, :]
        mid[...] = middle
        normed, _ = normalize(middle)
        hidden = (normed * vec_ref[5:6, :] + vec_ref[6:7, :]).astype(BF)
        h2[...] = hidden
        h2t[...] = hidden.T
        dyb[...] = cot_ref[...].astype(BF)
        acc[...] = middle + vec_ref[7:8, :]
        dh2[...] = jnp.zeros_like(dh2)
        gv_ref[...] = jnp.zeros_like(gv_ref)

    up = dyb[...]
    u = nn(h2[...], win_ref[...]) + vec_ref[pl.ds(8 + b, 1), :]
    phi = 0.5 * (1.0 + lax.erf(u * 0.7071067811865476))
    activated = (u * phi).astype(BF)
    acc[...] += nn(activated, wout_ref[...])
    gout_ref[...] = tn(activated, up).astype(BF)
    du = nt(up, wout_ref[...]) * (phi + u * jnp.exp(-0.5 * u * u) * 0.3989422804014327)
    gv_ref[pl.ds(8 + b, 1), :] = jnp.sum(du, axis=0, keepdims=True)
    dub = du.astype(BF)
    gi_ref[...] = nn(h2t[...], dub).astype(BF)
    dh2[...] += nt(dub, win_ref[...])

    @pl.when(b == pl.num_programs(0) - 1)
    def _():
        fo_ref[...] = acc[...]
        normed, inverse = normalize(mid[...])
        back, gain, offset = norm_back(dh2[...], normed, inverse, vec_ref[5:6, :])
        upstream = cot_ref[...]
        middle = upstream + back
        gm_ref[...] = middle
        dab = middle.astype(BF)
        go_ref[...] = tn(ctx_ref[...].astype(BF), dab).astype(BF)
        dctx = nt(dab, wo_ref[...]).astype(BF)
        dc_ref[...] = dctx
        gv_ref[3:4, :] = jnp.sum(dctx.astype(F32), axis=0, keepdims=True)
        gv_ref[4:5, :] = jnp.sum(middle, axis=0, keepdims=True)
        gv_ref[5:6, :] = gain[None]
        gv_ref[6:7, :] = offset[None]
        gv_ref[7:8, :] = jnp.sum(upstream, axis=0, keepdims=True)


def feed_all(ctx, frames, cot, vec, aw, ew, cw):
    rows, width = frames.shape
    full = ew.shape[1]
    whole = lambda shape: pl.BlockSpec(shape, lambda b: (0,) * len(shape))
    blocks = full // width
    return pl.pallas_call(
        feed_kernel,
        grid=(blocks,),
        out_shape=(
            jax.ShapeDtypeStruct((rows, width), F32),
            jax.ShapeDtypeStruct((rows, width), F32),
            jax.ShapeDtypeStruct((rows, width), BF),
            jax.ShapeDtypeStruct((width, full), BF),
            jax.ShapeDtypeStruct((full, width), BF),
            jax.ShapeDtypeStruct((width, width), BF),
            jax.ShapeDtypeStruct((16, width), F32),
        ),
        in_specs=[
            whole((rows, width)), whole((rows, width)), whole((rows, width)), whole((16, width)),
            pl.BlockSpec((None, width, width), lambda b: (3, 0, 0)),
            pl.BlockSpec((width, width), lambda b: (0, b)),
            pl.BlockSpec((width, width), lambda b: (b, 0)),
        ],
        out_specs=(
            whole((rows, width)), whole((rows, width)), whole((rows, width)),
            pl.BlockSpec((width, width), lambda b: (0, b)),
            pl.BlockSpec((width, width), lambda b: (b, 0)),
            whole((width, width)), whole((16, width)),
        ),
        scratch_shapes=[
            pltpu.VMEM((rows, width), F32),
            pltpu.VMEM((rows, width), BF),
            pltpu.VMEM((width, rows), BF),
            pltpu.VMEM((rows, width), BF),
            pltpu.VMEM((rows, width), F32),
            pltpu.VMEM((rows, width), F32),
        ],
        name="feed",
        compiler_params=pltpu.CompilerParams(vmem_limit_bytes=67043328),
    )(ctx, frames, cot, vec, aw, ew, cw)


def adam_kernel(parts, g_ref, *refs):
    step = pl.program_id(0)
    for i, group in enumerate((2, 1, 0)):
        w_ref, m_ref, v_ref = refs[3 * i : 3 * i + 3]
        go_ref, wo_ref, mo_ref, vo_ref = refs[9 + 4 * i : 13 + 4 * i]

        @pl.when(step // parts == i)
        def _():
            gradient = g_ref[...].astype(F32)
            go_ref[...] = gradient
            wo_ref[...], mo_ref[...], vo_ref[...] = adam_update(
                w_ref[...], gradient, m_ref[...], v_ref[...], rate_matrix, decay_matrix
            )


def adam_all(out, arrays):
    shard, width = out.shape[3:]
    rows = 96 if shard % 96 == 0 else shard
    deep = shard // rows
    parts = 4 * deep

    def local(step, i):
        t = jnp.clip(step - i * parts, 0, parts - 1)
        return t // deep, lax.rem(t, deep)

    def g_map(step):
        i = step // parts
        t = step - i * parts
        u = t // deep
        return 2 - i, u // 2, lax.rem(u, 2), lax.rem(t, deep), 0

    def map_of(i):
        def rows_map(step):
            u, r = local(step, i)
            return u * deep + r, 0

        def cols_map(step):
            u, r = local(step, i)
            return r, u

        return cols_map if i == 1 else rows_map

    in_specs = [pl.BlockSpec((None, None, None, rows, width), g_map)]
    out_specs, shapes = [], []
    for i in range(3):
        spec = pl.BlockSpec((rows, width), map_of(i))
        in_specs += [spec] * 3
        out_specs += [spec] * 4
        shapes += [jax.ShapeDtypeStruct(arrays[i][0].shape, F32)] * 4
    return pl.pallas_call(
        functools.partial(adam_kernel, parts),
        grid=(3 * parts,),
        out_shape=tuple(shapes),
        in_specs=in_specs,
        out_specs=tuple(out_specs),
        name="adam",
        compiler_params=pltpu.CompilerParams(vmem_limit_bytes=67043328),
    )(out, *[each for group in arrays for each in group])


def on_device(
    sizes,
    frames_in,
    cotangent,
    attention_weight,
    expand_weight,
    contract_weight,
    vectors,
    first_attention,
    first_expand,
    first_contract,
    first_vectors,
    second_attention,
    second_expand,
    second_contract,
    second_vectors,
):
    nd, nf, ns = sizes
    frames = frames_in[0]
    upstream = cotangent[0]
    rows, width = frames.shape
    shard = attention_weight.shape[1]
    full = expand_weight.shape[1]
    vec_pad = jnp.pad(vectors, ((0, 4), (0, 0)))
    aw, ew, cw, vw, h_all = gather_all(
        sizes, frames, attention_weight, expand_weight, contract_weight, vec_pad
    )
    vec = jnp.transpose(vw, (1, 0, 2)).reshape(16, width).astype(F32)
    h_own = lax.dynamic_slice_in_dim(h_all, lax.axis_index("seq") * rows, rows, 0)
    queries = (nn(h_own, aw[0]) + vec[2]).astype(BF)
    key_rows = nn(h_all, aw[1]).astype(BF)
    value_rows = (nn(h_all, aw[2]) + vec[3]).astype(BF)
    context_wide, log_total = attention(queries, key_rows, value_rows)
    frames_out, grad_middle, grad_context, grad_expand, grad_contract, grad_output_w, gv = feed_all(
        context_wide, frames, upstream, vec, aw, ew, cw
    )
    out, input_gradient, gv_sum = back_all(
        sizes,
        queries,
        key_rows,
        value_rows,
        grad_context,
        context_wide,
        log_total,
        h_all.T,
        aw,
        grad_middle,
        frames,
        vec,
        gv,
        grad_contract.reshape(nf, 4, shard, width),
        grad_expand.reshape(nf, shard, full),
        grad_output_w.reshape(nf, shard, width),
    )
    owned_vec = lax.dynamic_slice_in_dim(
        gv_sum[:12], lax.axis_index("fsdp") * (width // nf), width // nf, 1
    )
    flat = (4 * shard, width)
    done = adam_all(
        out,
        (
            [x.reshape(flat) for x in (attention_weight, first_attention, second_attention)],
            [expand_weight, first_expand, second_expand],
            [contract_weight, first_contract, second_contract],
        ),
    )
    attention_out = [each.reshape(attention_weight.shape) for each in done[:4]]
    expand_out, contract_out = done[4:8], done[8:]
    vector_out = (owned_vec,) + adam_update(
        vectors, owned_vec, first_vectors, second_vectors, rate_vector, 0.0
    )
    result = [frames_out[None], input_gradient[None]]
    for i in range(4):
        result += [attention_out[i], expand_out[i], contract_out[i], vector_out[i]]
    return tuple(result)


def solution(mesh):
    sizes = (mesh.shape["dp"], mesh.shape["fsdp"], mesh.shape["seq"])
    data = P(("dp", "fsdp"), "seq", None)
    state = (P(None, "fsdp", None), P("fsdp", None), P("fsdp", None), P(None, "fsdp"))
    return jax.shard_map(
        functools.partial(on_device, sizes),
        mesh=mesh,
        in_specs=(data, data) + state * 3,
        out_specs=(data, data) + state * 4,
        check_vma=False,
    )
```

```python
import functools

import jax
import jax.numpy as jnp
from jax import lax
from jax.experimental import pallas as pl
from jax.experimental.pallas import tpu as pltpu
from jax.sharding import PartitionSpec as P

HEADS = 12
norm_eps = 1e-05
beta_one = 0.9
beta_two = 0.999
adam_eps = 1e-08
adam_count = 5.0
rate_matrix = 0.02
rate_vector = 0.1
decay_matrix = 0.1
score_scale = 0.125
VMEM_LIMIT = 60 << 20
MESH = pl.DeviceIdType.MESH
BF = jnp.bfloat16
F32 = jnp.float32


def nt(left, right):
    return lax.dot_general(left, right, (((1,), (1,)), ((), ())), preferred_element_type=F32)


def nn(left, right):
    return lax.dot_general(left, right, (((1,), (0,)), ((), ())), preferred_element_type=F32)


def tn(left, right):
    return lax.dot_general(left, right, (((0,), (0,)), ((), ())), preferred_element_type=F32)


def vmem():
    return pl.BlockSpec(memory_space=pltpu.VMEM)


def normalize(values):
    center = values - jnp.mean(values, axis=-1, keepdims=True)
    inverse = lax.rsqrt(jnp.mean(center * center, axis=-1, keepdims=True) + norm_eps)
    return center * inverse, inverse


def norm_back(upstream, normed, inverse, gain):
    scaled = upstream * gain
    inner = (
        scaled
        - jnp.mean(scaled, axis=-1, keepdims=True)
        - normed * jnp.mean(scaled * normed, axis=-1, keepdims=True)
    )
    return (inverse * inner, jnp.sum(upstream * normed, axis=0), jnp.sum(upstream, axis=0))


def adam_update(weight, gradient, first, second, rate, decay):
    first_new = beta_one * first + (1.0 - beta_one) * gradient
    second_new = beta_two * second + (1.0 - beta_two) * gradient * gradient
    first_hat = first_new / (1.0 - beta_one**adam_count)
    second_hat = second_new / (1.0 - beta_two**adam_count)
    updated = weight - rate * (first_hat / (jnp.sqrt(second_hat) + adam_eps) + decay * weight)
    return (updated, first_new, second_new)


class Place:
    def __init__(self, sizes):
        self.nd, self.nf, self.ns = sizes
        self.nh = self.nd // 2
        self.dp = lax.axis_index("dp")
        self.x = lax.axis_index("fsdp")
        self.z = lax.axis_index("seq")
        self.core = lax.rem(self.dp, 2)
        self.hi = self.dp // 2

    def sibling(self):
        return {"dp": self.hi * 2 + 1 - self.core}

    def x_peer(self, k):
        return {"fsdp": lax.rem(self.x + k, self.nf)}

    def y_hi(self, k):
        return lax.rem(self.hi + k, self.nh)

    def y_peer(self, k):
        return {"dp": self.y_hi(k) * 2 + self.core}

    def z_at(self, k):
        return lax.rem(self.z + k + self.ns, self.ns)

    def z_peer(self, k):
        return {"seq": self.z_at(k)}

    def everyone(self):
        out = [self.sibling()]
        out += [self.x_peer(k) for k in range(1, self.nf)]
        out += [self.y_peer(k) for k in range(1, self.nh)]
        out += [self.z_peer(k) for k in range(1, self.ns)]
        return out

    def barrier(self):
        sem = pltpu.get_barrier_semaphore()
        peers = self.everyone()
        for peer in peers:
            pl.semaphore_signal(sem, inc=1, device_id=peer, device_id_type=MESH)
        pl.semaphore_wait(sem, len(peers))


def remote(src, dst, send, recv, peer):
    return pltpu.make_async_remote_copy(
        src_ref=src, dst_ref=dst, send_sem=send, recv_sem=recv, device_id=peer, device_id_type=MESH
    )


def front_kernel(
    sizes, frames_ref, vec_ref, aw_ref, ew_ref, cw_ref,
    a_out, e_ref, c_ref, vec_out, ht_out, q_out, k_out, v_out, ctx_out, lse_ref,
    a_ref, v_buf, h_ref, ht, q_buf, k_buf, v_buf2, ctx_buf, af, ef, cf, eb, cb,
    ls, xs, xr, ys, yr, s1s, s1r, s2s, s2r, vs, vr, rs, hs, hr,
):
    at = Place(sizes)
    nf, nh, ns = at.nf, at.nh, at.ns
    rows, width = frames_ref.shape
    shard = aw_ref.shape[1]
    half = shard // 2
    deep = cw_ref.shape[0]

    def load(i, src, dst):
        return pltpu.make_async_copy(src, dst, ls.at[i])

    loads = [
        load(0, aw_ref.at[pl.ds(0, 3)], af.at[pl.ds(0, 3)]),
        load(1, aw_ref.at[pl.ds(3, 1)], af.at[pl.ds(3, 1)]),
        load(2, ew_ref, ef),
        load(3, cw_ref, cf),
    ]
    for copy in loads:
        copy.start()
    at.barrier()
    v_buf[at.x] = jnp.zeros(v_buf.shape[1:], BF)
    v_buf[at.x, 0 : vec_ref.shape[0], :] = vec_ref[...].astype(BF)
    vec_copies = []
    for k in range(1, nf):
        copy = remote(v_buf.at[at.x], v_buf.at[at.x], vs.at[k], vr.at[k], at.x_peer(k))
        copy.start()
        vec_copies.append(copy)

    def view(chunk, j, hi, core, own=False):
        if chunk < 2:
            first, count = ((0, 3), (3, 1))[chunk]
            cols = width // nh
            return a_ref.at[
                pl.ds(first, count),
                pl.ds(pl.multiple_of(j * shard + core * half, 16), half),
                pl.ds(pl.multiple_of(hi * cols, 128), cols),
            ]
        ref, stage, size = ((e_ref, eb, shard), (c_ref, cb, deep))[chunk - 2]
        cols = ref.shape[1] // nh
        start = core * (size // 2)
        if own:
            ref = stage
        else:
            start = j * size + start
        return ref.at[
            pl.ds(pl.multiple_of(start, 16), size // 2),
            pl.ds(pl.multiple_of(hi * cols, 128), cols),
        ]

    own = pl.multiple_of(at.x * shard, 16)
    x_copies = {}

    def send_chunk(chunk):
        for k in range(1, nf):
            copy = remote(
                view(chunk, at.x, at.hi, at.core, True), view(chunk, at.x, at.hi, at.core),
                xs.at[chunk, k], xr.at[chunk, k], at.x_peer(k),
            )
            copy.start()
            x_copies[chunk, k] = copy

    loads[0].wait()
    for u in range(3):
        a_ref[u, pl.ds(own, shard), :] = af[u].astype(BF)
    send_chunk(0)
    normed, _ = normalize(frames_ref[...])
    for copy in vec_copies:
        copy.wait()
    vec = jnp.concatenate([v_buf[j] for j in range(nf)], axis=1).astype(F32)
    vec_out[...] = vec
    mine = pl.ds(pl.multiple_of(at.z * rows, 128), rows)
    hidden = (normed * vec[0:1] + vec[1:2]).astype(BF)
    h_ref[mine, :] = hidden

    def block(b):
        return h_ref.at[pl.ds(pl.multiple_of(b * rows, 128), rows), :]

    def to_right(b):
        return remote(block(b), block(b), rs.at[b], hr.at[b], {"seq": at.z + 1})

    def to_left(b):
        return remote(block(b), block(b), hs.at[b], hr.at[b], {"seq": at.z - 1})

    @pl.when(at.z < ns - 1)
    def _():
        to_right(at.z).start()

    @pl.when(at.z > 0)
    def _():
        to_left(at.z).start()

    loads[1].wait()
    a_ref[3, pl.ds(own, shard), :] = af[3].astype(BF)
    send_chunk(1)
    loads[2].wait()
    eb[...] = ef[...].astype(BF)
    send_chunk(2)
    loads[3].wait()
    cb[...] = cf[...].astype(BF)
    send_chunk(3)
    stores = [
        load(4, eb, e_ref.at[pl.ds(own, shard), :]),
        load(5, cb, c_ref.at[pl.ds(pl.multiple_of(at.x * deep, 16), deep), :]),
    ]
    for copy in stores:
        copy.start()
    ht[:, mine] = hidden.T

    def first_copy(chunk, k):
        j = lax.rem(at.x - k + nf, nf)
        piece = view(chunk, j, at.hi, at.core)
        return remote(piece, piece, s1s.at[chunk, k], s1r.at[chunk, k], at.sibling())

    def y_copy(chunk, k, m):
        j = lax.rem(at.x - k + nf, nf)
        piece = view(chunk, j, at.hi, at.core)
        return remote(piece, piece, ys.at[chunk, k, m], yr.at[chunk, k, m], at.y_peer(m))

    def second_copy(chunk, k, m):
        j = lax.rem(at.x - k + nf, nf)
        piece = view(chunk, j, lax.rem(at.hi - m + nh, nh), at.core)
        return remote(piece, piece, s2s.at[chunk, k, m], s2r.at[chunk, k, m], at.sibling())

    def forward(chunk):
        for k in range(1, nf):
            x_copies[chunk, k].wait_recv()
            first_copy(chunk, k).start()
            for m in range(1, nh):
                y_copy(chunk, k, m).start()

    def relay(chunk):
        for k in range(1, nf):
            for m in range(1, nh):
                y_copy(chunk, k, m).wait_recv()
                second_copy(chunk, k, m).start()

    def arrived(chunk):
        for k in range(1, nf):
            first_copy(chunk, k).wait_recv()
            for m in range(1, nh):
                second_copy(chunk, k, m).wait_recv()

    def rows_of(b):
        part = pl.ds(pl.multiple_of(b * rows, 128), rows)
        k_buf[part, :] = nn(h_ref[part, :], a_ref[1]).astype(BF)
        v_buf2[part, :] = (nn(h_ref[part, :], a_ref[2]) + vec[3:4]).astype(BF)

    def turn(b):
        part = pl.ds(pl.multiple_of(b * rows, 128), rows)
        ht[:, part] = h_ref[part, :].T

    def hop(s):
        b = at.z - s
        d = at.z + s

        @pl.when(b >= 0)
        def _():
            to_right(b).wait_recv()

            @pl.when(at.z < ns - 1)
            def _():
                to_right(b).start()

        @pl.when(d < ns)
        def _():
            to_left(d).wait_recv()

            @pl.when(at.z > 0)
            def _():
                to_left(d).start()

    def use(s):
        b = at.z - s
        d = at.z + s

        @pl.when(b >= 0)
        def _():
            rows_of(b)
            turn(b)

        @pl.when(d < ns)
        def _():
            rows_of(d)
            turn(d)

    forward(0)
    hop(1)
    forward(1)
    relay(0)
    arrived(0)
    q_buf[...] = (nn(h_ref[mine, :], a_ref[0]) + vec[2:3]).astype(BF)
    stores.append(load(6, q_buf, q_out))
    stores[-1].start()
    rows_of(at.z)
    use(1)
    relay(1)
    forward(2)
    for s in range(2, ns):
        hop(s)
        use(s)
    arrived(1)
    for i, (src, dst) in enumerate(((a_ref, a_out), (ht, ht_out), (k_buf, k_out), (v_buf2, v_out))):
        stores.append(load(7 + i, src, dst))
        stores[-1].start()
    forward(3)
    relay(2)
    lo = lax.broadcasted_iota(jnp.int32, (rows, 128), 1) < 64

    def pair(p, carry):
        col = pl.ds(pl.multiple_of(p * 128, 128), 128)
        k2 = k_buf[:, col]
        v2 = v_buf2[:, col]
        q2 = q_buf[:, col]
        ctx, lse = [], []
        for h in range(2):
            mask = lo if h == 0 else jnp.logical_not(lo)
            s = nt(jnp.where(mask, q2, jnp.zeros_like(q2)), k2) * score_scale
            largest = jnp.max(s, axis=-1, keepdims=True)
            e = jnp.exp(s - largest)
            total = jnp.sum(e, axis=-1, keepdims=True)
            ctx.append(nn((e * (1.0 / total)).astype(BF), v2))
            lse.append(largest + jnp.log(total))
        ctx_buf[:, col] = jnp.where(lo, ctx[0], ctx[1])
        lse_ref[p] = jnp.where(lo, lse[0], lse[1])

        @pl.when(p == 1)
        def _():
            relay(3)

        return carry

    lax.fori_loop(0, width // 128, pair, 0)
    stores.append(load(11, ctx_buf, ctx_out))
    stores[-1].start()
    arrived(2)
    arrived(3)
    for copy in stores:
        copy.wait()
    for copy in x_copies.values():
        copy.wait_send()
    for chunk in range(4):
        for k in range(1, nf):
            first_copy(chunk, k).wait_send()
            for m in range(1, nh):
                y_copy(chunk, k, m).wait_send()
                second_copy(chunk, k, m).wait_send()
    for b in range(ns):
        @pl.when(jnp.logical_and(b <= at.z, at.z < ns - 1))
        def _():
            to_right(b).wait_send()

        @pl.when(jnp.logical_and(b >= at.z, at.z > 0))
        def _():
            to_left(b).wait_send()


def front_all(sizes, frames, vec, aw, ew, cw):
    nd, nf, ns = sizes
    nh = nd // 2
    rows, width = frames.shape
    shard, full = ew.shape
    deep = cw.shape[0]
    every = rows * ns
    dma = pltpu.SemaphoreType.DMA
    anywhere = pl.BlockSpec(memory_space=pl.ANY)
    return pl.pallas_call(
        functools.partial(front_kernel, sizes),
        out_shape=(
            jax.ShapeDtypeStruct((4, width, width), BF),
            jax.ShapeDtypeStruct((width, full), BF),
            jax.ShapeDtypeStruct((deep * nf, width), BF),
            jax.ShapeDtypeStruct((16, width), F32),
            jax.ShapeDtypeStruct((width, every), BF),
            jax.ShapeDtypeStruct((rows, width), BF),
            jax.ShapeDtypeStruct((every, width), BF),
            jax.ShapeDtypeStruct((every, width), BF),
            jax.ShapeDtypeStruct((rows, width), F32),
            jax.ShapeDtypeStruct((width // 128, rows, 128), F32),
        ),
        in_specs=[vmem(), vmem(), anywhere, anywhere, anywhere],
        out_specs=(anywhere, anywhere, anywhere, vmem()) + (anywhere,) * 5 + (vmem(),),
        scratch_shapes=[
            pltpu.VMEM((4, width, width), BF),
            pltpu.VMEM((nf, 16, vec.shape[1]), BF),
            pltpu.VMEM((every, width), BF),
            pltpu.VMEM((width, every), BF),
            pltpu.VMEM((rows, width), BF),
            pltpu.VMEM((every, width), BF),
            pltpu.VMEM((every, width), BF),
            pltpu.VMEM((rows, width), F32),
            pltpu.VMEM((4, shard, width), F32),
            pltpu.VMEM((shard, full), F32),
            pltpu.VMEM((deep, width), F32),
            pltpu.VMEM((shard, full), BF),
            pltpu.VMEM((deep, width), BF),
            dma((12,)),
            dma((4, nf)), dma((4, nf)),
            dma((4, nf, nh)), dma((4, nf, nh)),
            dma((4, nf)), dma((4, nf)),
            dma((4, nf, nh)), dma((4, nf, nh)),
            dma((nf,)), dma((nf,)),
            dma((ns,)), dma((ns,)), dma((ns,)),
        ],
        name="front",
        compiler_params=pltpu.CompilerParams(
            collective_id=0, has_side_effects=True, vmem_limit_bytes=67043328
        ),
    )(frames, vec, aw, ew, cw)


def back_kernel(
    sizes, q_ref, k_ref, v_ref, dc_ref, ctx_ref, lse_ref, ht_ref, w_ref, gm_ref, frames_ref,
    vec_ref, gv_ref, gc_ref, ge_ref, go_ref,
    out_ref, ig_ref, ov_ref,
    ga, own, rc, rx, ry, rza, rzb, dkt, dvt, dqa, dhs, dhr, vb, vx, vy, vz,
    os, cs, cr, xs, xr, ys, yr, zas, zar, zbs, zbr, gbs, gbr, gas, gar, ays, ayr, acs, acr,
    das, dar, vs, vr,
):
    at = Place(sizes)
    nf, nh, ns = at.nf, at.nh, at.ns
    rows, width = q_ref.shape
    q = rc.shape[5]
    cols = width // nh
    per = cols // 128
    chunks = rc.shape[0]
    split = chunks // (3 * per)
    half = q * split
    group = per * split
    b0 = lax.rem(at.z, 2)
    b1 = at.z // 2
    at.barrier()

    def strip(core, r):
        return pl.ds(pl.multiple_of(core * half + r * q, 16), q)

    def lanes(s, hi):
        return pl.ds(pl.multiple_of(hi * cols + s * 128, 128), 128)

    def place_of(n):
        return n // group, lax.rem(n, group) // split, lax.rem(n, split)

    for s in range(per):
        for hi in range(nh):
            for part in range(2):
                for r in range(split):
                    pltpu.make_async_copy(
                        go_ref.at[:, pl.ds(part * half + r * q, q), pl.ds(hi * cols + s * 128, 128)],
                        ga.at[s, r, hi, :, part, 1, 1],
                        os.at[4],
                    ).start()

    def own_whole(slot):
        return pltpu.make_async_copy(own.at[slot], own.at[slot], os.at[slot])

    def c_whole(n):
        return remote(rc.at[n], rc.at[n], cs.at[n], cr.at[n], at.sibling())

    def c_send(n):
        slot = lax.rem(n, 4)
        g, s, r = place_of(n)

        @pl.when(n < group)
        def _():
            for hi in range(nh):
                for u in range(4):
                    block = lanes(s, hi)
                    remote(
                        gc_ref.at[:, u, strip(1 - at.core, r), block],
                        rc.at[n, hi, :, u // 2, u % 2], cs.at[n], cr.at[n], at.sibling(),
                    ).start()
                    pltpu.make_async_copy(
                        gc_ref.at[:, u, strip(at.core, r), block],
                        own.at[slot, hi, :, u // 2, u % 2], os.at[slot],
                    ).start()

        @pl.when(jnp.logical_and(n >= group, n < 2 * group))
        def _():
            for hi in range(nh):
                for u in range(4):
                    block = pl.ds(pl.multiple_of(u * width + hi * cols + s * 128, 128), 128)
                    remote(
                        ge_ref.at[:, strip(1 - at.core, r), block],
                        rc.at[n, hi, :, u // 2, u % 2], cs.at[n], cr.at[n], at.sibling(),
                    ).start()
                    pltpu.make_async_copy(
                        ge_ref.at[:, strip(at.core, r), block],
                        own.at[slot, hi, :, u // 2, u % 2], os.at[slot],
                    ).start()

        @pl.when(jnp.logical_and(n >= 2 * group, n < chunks))
        def _():
            remote(
                ga.at[s, r, :, :, 1 - at.core], rc.at[n], cs.at[n], cr.at[n], at.sibling()
            ).start()

    def x_copy(n, k):
        peer = lax.rem(at.x + k, nf)
        return remote(rc.at[n, :, peer], rx.at[n, k - 1], xs.at[n, k - 1], xr.at[n, k - 1], at.x_peer(k))

    def y_copy(n, m):
        return remote(
            rx.at[n, 0, at.y_hi(m)], ry.at[n, m - 1], ys.at[n, m - 1], yr.at[n, m - 1], at.y_peer(m)
        )

    near = {"seq": at.z + 1 - 2 * b0}
    far = {"seq": at.z + 2 - 4 * b1}

    def za_copy(n):
        return remote(ry.at[n, 0, :, 1 - b0], rza.at[n], zas.at[n], zar.at[n], near)

    def zb_copy(n):
        return remote(rza.at[n, 1 - b1], rzb.at[n], zbs.at[n], zbr.at[n], far)

    def gb_copy(n):
        g, s, r = place_of(n)
        place = out_ref.at[g, b1, b0, strip(at.core, r), lanes(s, at.hi)]
        return remote(place, place, gbs.at[n], gbr.at[n], far)

    def ga_copy(n):
        g, s, r = place_of(n)
        place = out_ref.at[g, :, b0, strip(at.core, r), lanes(s, at.hi)]
        return remote(place, place, gas.at[n], gar.at[n], near)

    def ay_copy(n, m):
        g, s, r = place_of(n)
        place = out_ref.at[g, :, :, strip(at.core, r), lanes(s, at.hi)]
        return remote(place, place, ays.at[n, m - 1], ayr.at[n, m - 1], at.y_peer(m))

    def ac_start(n):
        g, s, r = place_of(n)
        for hi in range(nh):
            place = out_ref.at[g, :, :, strip(at.core, r), lanes(s, hi)]
            remote(place, place, acs.at[n], acr.at[n], at.sibling()).start()

    def ac_whole(n):
        return remote(rx.at[n, 0], rx.at[n, 0], acs.at[n], acr.at[n], at.sibling())

    def split_index(i):
        return i // (nf * 4), lax.rem(i // 4, nf), lax.rem(i, 4) // 2, lax.rem(i, 2)

    def stage_c(n):
        c_whole(n).wait_recv()
        slot = lax.rem(n, 4)
        _, s, r = place_of(n)

        @pl.when(n < 2 * group)
        def _():
            own_whole(slot).wait()

            def add(i, carry):
                at_i = split_index(i)
                rc[(n,) + at_i] = (
                    rc[(n,) + at_i].astype(F32) + own[(slot,) + at_i].astype(F32)
                ).astype(BF)
                return carry

            lax.fori_loop(0, nh * nf * 4, add, 0)

        @pl.when(n >= 2 * group)
        def _():
            def add(i, carry):
                hi, j, ua, ub = split_index(i)
                rc[n, hi, j, ua, ub] = (
                    rc[n, hi, j, ua, ub].astype(F32) + ga[s, r, hi, j, at.core, ua, ub].astype(F32)
                ).astype(BF)
                return carry

            lax.fori_loop(0, nh * nf * 4, add, 0)

        for k in range(1, nf):
            x_copy(n, k).start()

    def stage_x(n):
        for k in range(1, nf):
            x_copy(n, k).wait_recv()

        def add(i, carry):
            hi, ua, ub = i // 4, lax.rem(i, 4) // 2, lax.rem(i, 2)
            total = rc[n, hi, at.x, ua, ub].astype(F32)
            for k in range(nf - 1):
                total += rx[n, k, hi, ua, ub].astype(F32)
            rx[n, 0, hi, ua, ub] = total.astype(BF)
            return carry

        lax.fori_loop(0, nh * 4, add, 0)
        for m in range(1, nh):
            y_copy(n, m).start()

    def stage_y(n):
        for m in range(1, nh):
            y_copy(n, m).wait_recv()

        def add(i, carry):
            ua, ub = i // 2, lax.rem(i, 2)
            total = rx[n, 0, at.hi, ua, ub].astype(F32)
            for m in range(nh - 1):
                total += ry[n, m, ua, ub].astype(F32)
            ry[n, 0, ua, ub] = total.astype(BF)
            return carry

        lax.fori_loop(0, 4, add, 0)
        za_copy(n).start()

    def stage_za(n):
        za_copy(n).wait_recv()
        for ua in range(2):
            rza[n, ua] = (ry[n, 0, ua, b0].astype(F32) + rza[n, ua].astype(F32)).astype(BF)
        zb_copy(n).start()

    def stage_zb(n):
        zb_copy(n).wait_recv()
        g, s, r = place_of(n)
        out_ref[g, b1, b0, strip(at.core, r), lanes(s, at.hi)] = (
            rza[n, b1].astype(F32) + rzb[n].astype(F32)
        ).astype(BF)
        gb_copy(n).start()

    def stage_gb(n):
        gb_copy(n).wait_recv()
        ga_copy(n).start()

    def stage_ga(n):
        ga_copy(n).wait_recv()
        for m in range(1, nh):
            ay_copy(n, m).start()

    def stage_ay(n):
        for m in range(1, nh):
            ay_copy(n, m).wait_recv()
        ac_start(n)

    lo = lax.broadcasted_iota(jnp.int32, (rows, 128), 1) < 64
    pairs = width // 128

    def block_of(i):
        return lax.rem(at.z + 1 + i, ns)

    def unit(index):
        i, p = index // pairs, lax.rem(index, pairs)
        there = block_of(i)
        keys = pl.ds(pl.multiple_of(there * rows, 128), rows)
        col = pl.ds(pl.multiple_of(p * 128, 128), 128)
        k2 = k_ref[keys, col]
        v2 = v_ref[keys, col]
        q2 = q_ref[:, col]
        dc2 = dc_ref[:, col]
        both = dc2.astype(F32) * ctx_ref[:, col]
        lse2 = lse_ref[p]
        dq, dk, dv = [], None, None
        for h in range(2):
            mask = lo if h == 0 else jnp.logical_not(lo)
            qm = jnp.where(mask, q2, jnp.zeros_like(q2))
            dmask = jnp.where(mask, dc2, jnp.zeros_like(q2))
            lse = lse2[:, 0:1] if h == 0 else lse2[:, 64:65]
            dot = jnp.sum(jnp.where(mask, both, 0.0), axis=-1, keepdims=True)
            probs = jnp.exp(nt(qm, k2) * score_scale - lse)
            slopes = nt(dmask, v2)
            dscore = (probs * (slopes - dot) * score_scale).astype(BF)
            dq.append(nn(dscore, k2))
            a = nn(dmask.T, probs.astype(BF))
            b = nn(qm.T, dscore)
            dv = a if dv is None else dv + a
            dk = b if dk is None else dk + b
        dq2 = jnp.where(lo, dq[0], dq[1])

        @pl.when(i == 0)
        def _():
            dqa[:, col] = dq2

        @pl.when(i > 0)
        def _():
            dqa[:, col] += dq2

        dkt[col, keys] = dk.astype(BF)
        dvt[col, keys] = dv.astype(BF)

    def weights(s):
        frames = pl.ds(pl.multiple_of(at.z * rows, 128), rows)
        for hi in range(nh):
            col = pl.ds(hi * cols + s * 128, 128)
            dq2 = dqa[:, col]
            vb[2, 0:1, col] = jnp.sum(dq2, axis=0, keepdims=True)
            dq2 = dq2.astype(BF)
            dk2 = dkt[col, :]
            dv2 = dvt[col, :]
            for j in range(nf):
                for part in range(2):
                    for r in range(split):
                        here = pl.ds((2 * j + part) * half + r * q, q)
                        ga[s, r, hi, j, part, 0, 0] = nn(ht_ref[here, frames], dq2).astype(BF)
                        ga[s, r, hi, j, part, 0, 1] = nt(ht_ref[here, :], dk2).astype(BF)
                        ga[s, r, hi, j, part, 1, 0] = nt(ht_ref[here, :], dv2).astype(BF)

    pieces = 8

    def d_copy(i, t):
        part = pl.ds(t * (width // pieces), width // pieces)
        return remote(dhs.at[i, part], dhr.at[i, part], das.at[i], dar.at[i], at.z_peer(i + 1))

    def d_whole(i):
        return remote(dhs.at[i], dhr.at[i], das.at[i], dar.at[i], at.z_peer(i + 1))

    def spread(i):
        part = pl.ds(pl.multiple_of(block_of(i) * rows, 128), rows)
        total = nn(w_ref[1], dkt[:, part]) + nn(w_ref[2], dvt[:, part])
        if i == ns - 1:
            total += nt(w_ref[0], dqa[...].astype(BF))
        dhs[i] = total.astype(BF)

    def first_norm():
        total = dhs[ns - 1].astype(F32)
        for i in range(ns - 1):
            d_whole(i).wait_recv()
            total += dhr[i].astype(F32)
        total = total.T
        normed, inverse = normalize(frames_ref[...])
        scaled = total * vec_ref[0:1, :]
        inner = (
            scaled
            - jnp.mean(scaled, axis=-1, keepdims=True)
            - normed * jnp.mean(scaled * normed, axis=-1, keepdims=True)
        )
        ig_ref[...] = gm_ref[...] + inverse * inner
        vb[1] = gv_ref[...]
        vb[1, 0:1, :] = jnp.sum(total * normed, axis=0, keepdims=True)
        vb[1, 1:2, :] = jnp.sum(total, axis=0, keepdims=True)
        vb[1, 2:3, :] = vb[2, 0:1, :]

    def v_core():
        return remote(vb.at[1], vb.at[0], vs.at[0], vr.at[0], at.sibling())

    def v_x(k):
        return remote(vx.at[at.x], vx.at[at.x], vs.at[k], vr.at[k], at.x_peer(k))

    def v_y(m):
        return remote(vy.at[at.hi], vy.at[at.hi], vs.at[nf + m], vr.at[nf + m], at.y_peer(m))

    def v_z(k):
        return remote(
            vz.at[at.z], vz.at[at.z], vs.at[nf + nh + k], vr.at[nf + nh + k], at.z_peer(k)
        )

    def v_step(i):
        if i == 0:
            v_core().start()
        elif i == 1:
            v_core().wait_recv()
            vx[at.x] = vb[0] + vb[1]
            for k in range(1, nf):
                v_x(k).start()
        elif i == 2:
            for k in range(1, nf):
                v_x(k).wait_recv()
            total = vx[0]
            for j in range(1, nf):
                total += vx[j]
            vy[at.hi] = total
            for m in range(1, nh):
                v_y(m).start()
        elif i == 3:
            for m in range(1, nh):
                v_y(m).wait_recv()
            total = vy[0]
            for j in range(1, nh):
                total += vy[j]
            vz[at.z] = total
            for k in range(1, ns):
                v_z(k).start()
        else:
            for k in range(1, ns):
                v_z(k).wait_recv()
            total = vz[0]
            for j in range(1, ns):
                total += vz[j]
            ov_ref[...] = total

    ready = group + 2
    each = -(-ns * pairs // ready)
    done = [-(-pairs * (i + 1) // each) - 1 for i in range(ns)]
    norm = done[ns - 1] + 6
    stages = (stage_x, stage_y, stage_za, stage_zb, stage_gb, stage_ga, stage_ay)
    last = max(chunks + len(stages), norm + 6)
    for n in range(4):
        c_send(n)

    def step(n, carry):
        for k in range(2):
            @pl.when(2 * n + k < 2 * group)
            def _(k=k):
                stage_c(2 * n + k)

                @pl.when(2 * n + k + 4 < 2 * group)
                def _():
                    c_send(2 * n + k + 4)

        for s in range(per):
            @pl.when(n == ready + s + 1)
            def _(s=s):
                for r in range(split):
                    stage_c(2 * group + s * split + r)

        @pl.when(n < ready)
        def _():
            def one(k, carry):
                @pl.when(n * each + k < ns * pairs)
                def _():
                    unit(n * each + k)

                return carry

            lax.fori_loop(0, each, one, 0)

        for i in range(ns):
            @pl.when(n == done[i])
            def _(i=i):
                spread(i)

            if i < ns - 1:
                for late in range(2):
                    @pl.when(n == done[i] + late)
                    def _(i=i, late=late):
                        for t in range(pieces // 2):
                            d_copy(i, late * (pieces // 2) + t).start()

        @pl.when(n == norm)
        def _():
            first_norm()

        for s in range(per):
            @pl.when(n == ready + s)
            def _(s=s):
                weights(s)
                if s == 0:
                    whole = ga.at[:, :, :, :, :, 1, 1]
                    pltpu.make_async_copy(whole, whole, os.at[4]).wait()
                for r in range(split):
                    c_send(2 * group + s * split + r)

        for lag, stage in enumerate(stages):
            @pl.when(jnp.logical_and(n >= lag, n < chunks + lag))
            def _(lag=lag, stage=stage):
                stage(n - lag)

        for i in range(5):
            @pl.when(n == norm + i)
            def _(i=i):
                v_step(i)

        return carry

    lax.fori_loop(0, last, step, 0)
    for n in range(chunks):
        ac_whole(n).wait()

    def drain(n, carry):
        c_whole(n).wait_send()
        za_copy(n).wait_send()
        zb_copy(n).wait_send()
        gb_copy(n).wait_send()
        ga_copy(n).wait_send()
        for k in range(1, nf):
            x_copy(n, k).wait_send()
        for m in range(1, nh):
            y_copy(n, m).wait_send()
            ay_copy(n, m).wait_send()
        return carry

    lax.fori_loop(0, chunks, drain, 0)
    for i in range(ns - 1):
        d_whole(i).wait_send()
    for k in range(1, ns):
        v_z(k).wait_send()
    for k in range(1, nf):
        v_x(k).wait_send()
    for m in range(1, nh):
        v_y(m).wait_send()
    v_core().wait_send()


def back_all(sizes, q, k, v, dc, ctx, lse, ht, w, gm, frames, vec, gv, gc, ge, go):
    nd, nf, ns = sizes
    nh = nd // 2
    rows, width = q.shape
    shard = go.shape[1]
    half = shard // 2
    every = k.shape[0]
    split = 2 if half % 32 == 0 else 1
    strip = half // split
    per = width // nh // 128
    chunks = 3 * per * split
    xn, yn = max(nf - 1, 1), max(nh - 1, 1)
    dma = pltpu.SemaphoreType.DMA
    anywhere = pl.BlockSpec(memory_space=pl.ANY)
    return pl.pallas_call(
        functools.partial(back_kernel, sizes),
        out_shape=(
            jax.ShapeDtypeStruct((3, 2, 2, shard, width), BF),
            jax.ShapeDtypeStruct((rows, width), F32),
            jax.ShapeDtypeStruct((16, width), F32),
        ),
        in_specs=[vmem()] * 12 + [anywhere] * 3,
        out_specs=(vmem(),) * 3,
        scratch_shapes=[
            pltpu.VMEM((per, split, nh, nf, 2, 2, 2, strip, 128), BF),
            pltpu.VMEM((4, nh, nf, 2, 2, strip, 128), BF),
            pltpu.VMEM((chunks, nh, nf, 2, 2, strip, 128), BF),
            pltpu.VMEM((chunks, xn, nh, 2, 2, strip, 128), BF),
            pltpu.VMEM((chunks, yn, 2, 2, strip, 128), BF),
            pltpu.VMEM((chunks, 2, strip, 128), BF),
            pltpu.VMEM((chunks, strip, 128), BF),
            pltpu.VMEM((width, every), BF),
            pltpu.VMEM((width, every), BF),
            pltpu.VMEM((rows, width), F32),
            pltpu.VMEM((ns, width, rows), BF),
            pltpu.VMEM((ns - 1, width, rows), BF),
            pltpu.VMEM((3, 16, width), F32),
            pltpu.VMEM((nf, 16, width), F32),
            pltpu.VMEM((nh, 16, width), F32),
            pltpu.VMEM((ns, 16, width), F32),
            dma((5,)),
            dma((chunks,)), dma((chunks,)),
            dma((chunks, xn)), dma((chunks, xn)),
            dma((chunks, yn)), dma((chunks, yn)),
            dma((chunks,)), dma((chunks,)),
            dma((chunks,)), dma((chunks,)),
            dma((chunks,)), dma((chunks,)),
            dma((chunks,)), dma((chunks,)),
            dma((chunks, yn)), dma((chunks, yn)),
            dma((chunks,)), dma((chunks,)),
            dma((ns,)), dma((ns,)),
            dma((nf + nh + ns,)), dma((nf + nh + ns,)),
        ],
        name="back",
        compiler_params=pltpu.CompilerParams(
            collective_id=1, has_side_effects=True, vmem_limit_bytes=67043328
        ),
    )(q, k, v, dc, ctx, lse, ht, w, gm, frames, vec, gv, gc, ge, go)


def feed_kernel(
    ctx_ref, frames_ref, cot_ref, vec_ref, wo_ref, win_ref, wout_ref,
    fo_ref, gm_ref, dc_ref, gi_ref, gout_ref, go_ref, gv_ref,
    mid, h2, h2t, dyb, acc, dh2,
):
    b = pl.program_id(0)

    @pl.when(b == 0)
    def _():
        middle = frames_ref[...] + nn(ctx_ref[...].astype(BF), wo_ref[...]) + vec_ref[4:5, :]
        mid[...] = middle
        normed, _ = normalize(middle)
        hidden = (normed * vec_ref[5:6, :] + vec_ref[6:7, :]).astype(BF)
        h2[...] = hidden
        h2t[...] = hidden.T
        dyb[...] = cot_ref[...].astype(BF)
        acc[...] = middle + vec_ref[7:8, :]
        dh2[...] = jnp.zeros_like(dh2)
        gv_ref[...] = jnp.zeros_like(gv_ref)

    up = dyb[...]
    u = nn(h2[...], win_ref[...]) + vec_ref[pl.ds(8 + b, 1), :]
    phi = 0.5 * (1.0 + lax.erf(u * 0.7071067811865476))
    activated = (u * phi).astype(BF)
    acc[...] += nn(activated, wout_ref[...])
    gout_ref[...] = tn(activated, up).astype(BF)
    du = nt(up, wout_ref[...]) * (phi + u * jnp.exp(-0.5 * u * u) * 0.3989422804014327)
    gv_ref[pl.ds(8 + b, 1), :] = jnp.sum(du, axis=0, keepdims=True)
    dub = du.astype(BF)
    gi_ref[...] = nn(h2t[...], dub).astype(BF)
    dh2[...] += nt(dub, win_ref[...])

    @pl.when(b == pl.num_programs(0) - 1)
    def _():
        fo_ref[...] = acc[...]
        normed, inverse = normalize(mid[...])
        back, gain, offset = norm_back(dh2[...], normed, inverse, vec_ref[5:6, :])
        upstream = cot_ref[...]
        middle = upstream + back
        gm_ref[...] = middle
        dab = middle.astype(BF)
        go_ref[...] = tn(ctx_ref[...].astype(BF), dab).astype(BF)
        dctx = nt(dab, wo_ref[...]).astype(BF)
        dc_ref[...] = dctx
        gv_ref[3:4, :] = jnp.sum(dctx.astype(F32), axis=0, keepdims=True)
        gv_ref[4:5, :] = jnp.sum(middle, axis=0, keepdims=True)
        gv_ref[5:6, :] = gain[None]
        gv_ref[6:7, :] = offset[None]
        gv_ref[7:8, :] = jnp.sum(upstream, axis=0, keepdims=True)


def feed_all(ctx, frames, cot, vec, aw, ew, cw):
    rows, width = frames.shape
    full = ew.shape[1]
    whole = lambda shape: pl.BlockSpec(shape, lambda b: (0,) * len(shape))
    blocks = full // width
    return pl.pallas_call(
        feed_kernel,
        grid=(blocks,),
        out_shape=(
            jax.ShapeDtypeStruct((rows, width), F32),
            jax.ShapeDtypeStruct((rows, width), F32),
            jax.ShapeDtypeStruct((rows, width), BF),
            jax.ShapeDtypeStruct((width, full), BF),
            jax.ShapeDtypeStruct((full, width), BF),
            jax.ShapeDtypeStruct((width, width), BF),
            jax.ShapeDtypeStruct((16, width), F32),
        ),
        in_specs=[
            whole((rows, width)), whole((rows, width)), whole((rows, width)), whole((16, width)),
            pl.BlockSpec((None, width, width), lambda b: (3, 0, 0)),
            pl.BlockSpec((width, width), lambda b: (0, b)),
            pl.BlockSpec((width, width), lambda b: (b, 0)),
        ],
        out_specs=(
            whole((rows, width)), whole((rows, width)), whole((rows, width)),
            pl.BlockSpec((width, width), lambda b: (0, b)),
            pl.BlockSpec((width, width), lambda b: (b, 0)),
            whole((width, width)), whole((16, width)),
        ),
        scratch_shapes=[
            pltpu.VMEM((rows, width), F32),
            pltpu.VMEM((rows, width), BF),
            pltpu.VMEM((width, rows), BF),
            pltpu.VMEM((rows, width), BF),
            pltpu.VMEM((rows, width), F32),
            pltpu.VMEM((rows, width), F32),
        ],
        name="feed",
        compiler_params=pltpu.CompilerParams(vmem_limit_bytes=67043328),
    )(ctx, frames, cot, vec, aw, ew, cw)


def on_device(
    sizes,
    frames_in,
    cotangent,
    attention_weight,
    expand_weight,
    contract_weight,
    vectors,
    first_attention,
    first_expand,
    first_contract,
    first_vectors,
    second_attention,
    second_expand,
    second_contract,
    second_vectors,
):
    nd, nf, ns = sizes
    frames = frames_in[0]
    upstream = cotangent[0]
    rows, width = frames.shape
    shard = attention_weight.shape[1]
    full = expand_weight.shape[1]
    aw, ew, cw, vec, h_turned, queries, key_rows, value_rows, context_wide, log_total = front_all(
        sizes, frames, vectors, attention_weight, expand_weight, contract_weight
    )
    frames_out, grad_middle, grad_context, grad_expand, grad_contract, grad_output_w, gv = feed_all(
        context_wide, frames, upstream, vec, aw, ew, cw
    )
    out, input_gradient, gv_sum = back_all(
        sizes,
        queries,
        key_rows,
        value_rows,
        grad_context,
        context_wide,
        log_total,
        h_turned,
        aw,
        grad_middle,
        frames,
        vec,
        gv,
        grad_contract.reshape(nf, 4, shard, width),
        grad_expand.reshape(nf, shard, full),
        grad_output_w.reshape(nf, shard, width),
    )
    owned_vec = lax.dynamic_slice_in_dim(
        gv_sum[:12], lax.axis_index("fsdp") * (width // nf), width // nf, 1
    )
    owned = (
        out[2].reshape(4, shard, width).astype(F32),
        jnp.transpose(out[1].reshape(4, shard, width), (1, 0, 2)).reshape(shard, full).astype(F32),
        out[0].reshape(4 * shard, width).astype(F32),
    )
    attention_out = (owned[0],) + adam_update(
        attention_weight, owned[0], first_attention, second_attention, rate_matrix, decay_matrix
    )
    expand_out = (owned[1],) + adam_update(
        expand_weight, owned[1], first_expand, second_expand, rate_matrix, decay_matrix
    )
    contract_out = (owned[2],) + adam_update(
        contract_weight, owned[2], first_contract, second_contract, rate_matrix, decay_matrix
    )
    vector_out = (owned_vec,) + adam_update(
        vectors, owned_vec, first_vectors, second_vectors, rate_vector, 0.0
    )
    result = [frames_out[None], input_gradient[None]]
    for i in range(4):
        result += [attention_out[i], expand_out[i], contract_out[i], vector_out[i]]
    return tuple(result)


def solution(mesh):
    sizes = (mesh.shape["dp"], mesh.shape["fsdp"], mesh.shape["seq"])
    data = P(("dp", "fsdp"), "seq", None)
    state = (P(None, "fsdp", None), P("fsdp", None), P("fsdp", None), P(None, "fsdp"))
    return jax.shard_map(
        functools.partial(on_device, sizes),
        mesh=mesh,
        in_specs=(data, data) + state * 3,
        out_specs=(data, data) + state * 4,
        check_vma=False,
    )
```

```python
import functools

import jax
import jax.numpy as jnp
from jax import lax
from jax.experimental import pallas as pl
from jax.experimental.pallas import tpu as pltpu
from jax.sharding import PartitionSpec as P

HEADS = 12
norm_eps = 1e-05
beta_one = 0.9
beta_two = 0.999
adam_eps = 1e-08
adam_count = 5.0
rate_matrix = 0.02
rate_vector = 0.1
decay_matrix = 0.1
score_scale = 0.125
VMEM_LIMIT = 60 << 20
MESH = pl.DeviceIdType.MESH
BF = jnp.bfloat16
F32 = jnp.float32


def nt(left, right):
    return lax.dot_general(left, right, (((1,), (1,)), ((), ())), preferred_element_type=F32)


def nn(left, right):
    return lax.dot_general(left, right, (((1,), (0,)), ((), ())), preferred_element_type=F32)


def tn(left, right):
    return lax.dot_general(left, right, (((0,), (0,)), ((), ())), preferred_element_type=F32)


def vmem():
    return pl.BlockSpec(memory_space=pltpu.VMEM)


def normalize(values):
    center = values - jnp.mean(values, axis=-1, keepdims=True)
    inverse = lax.rsqrt(jnp.mean(center * center, axis=-1, keepdims=True) + norm_eps)
    return center * inverse, inverse


def norm_back(upstream, normed, inverse, gain):
    scaled = upstream * gain
    inner = (
        scaled
        - jnp.mean(scaled, axis=-1, keepdims=True)
        - normed * jnp.mean(scaled * normed, axis=-1, keepdims=True)
    )
    return (inverse * inner, jnp.sum(upstream * normed, axis=0), jnp.sum(upstream, axis=0))


def adam_update(weight, gradient, first, second, rate, decay):
    first_new = beta_one * first + (1.0 - beta_one) * gradient
    second_new = beta_two * second + (1.0 - beta_two) * gradient * gradient
    first_hat = first_new / (1.0 - beta_one**adam_count)
    second_hat = second_new / (1.0 - beta_two**adam_count)
    updated = weight - rate * (first_hat / (jnp.sqrt(second_hat) + adam_eps) + decay * weight)
    return (updated, first_new, second_new)


class Place:
    def __init__(self, sizes):
        self.nd, self.nf, self.ns = sizes
        self.nh = self.nd // 2
        self.dp = lax.axis_index("dp")
        self.x = lax.axis_index("fsdp")
        self.z = lax.axis_index("seq")
        self.core = lax.rem(self.dp, 2)
        self.hi = self.dp // 2

    def sibling(self):
        return {"dp": self.hi * 2 + 1 - self.core}

    def x_peer(self, k):
        return {"fsdp": lax.rem(self.x + k, self.nf)}

    def y_hi(self, k):
        return lax.rem(self.hi + k, self.nh)

    def y_peer(self, k):
        return {"dp": self.y_hi(k) * 2 + self.core}

    def z_at(self, k):
        return lax.rem(self.z + k + self.ns, self.ns)

    def z_peer(self, k):
        return {"seq": self.z_at(k)}

    def everyone(self):
        out = [self.sibling()]
        out += [self.x_peer(k) for k in range(1, self.nf)]
        out += [self.y_peer(k) for k in range(1, self.nh)]
        out += [self.z_peer(k) for k in range(1, self.ns)]
        return out

    def barrier(self):
        sem = pltpu.get_barrier_semaphore()
        peers = self.everyone()
        for peer in peers:
            pl.semaphore_signal(sem, inc=1, device_id=peer, device_id_type=MESH)
        pl.semaphore_wait(sem, len(peers))


def remote(src, dst, send, recv, peer):
    return pltpu.make_async_remote_copy(
        src_ref=src, dst_ref=dst, send_sem=send, recv_sem=recv, device_id=peer, device_id_type=MESH
    )


def front_kernel(
    sizes, frames_ref, vec_ref, aw_ref, ew_ref, cw_ref,
    a_out, e_ref, c_ref, vec_out, ht_out, q_out, k_out, v_out, ctx_out, lse_ref,
    a_ref, v_buf, h_ref, ht, q_buf, k_buf, v_buf2, ctx_buf, af, ef, cf, eb, cb,
    ls, xs, xr, ys, yr, s1s, s1r, s2s, s2r, vs, vr, rs, hs, hr,
):
    at = Place(sizes)
    nf, nh, ns = at.nf, at.nh, at.ns
    rows, width = frames_ref.shape
    shard = aw_ref.shape[1]
    half = shard // 2
    deep = cw_ref.shape[0]

    def load(i, src, dst):
        return pltpu.make_async_copy(src, dst, ls.at[i])

    loads = [
        load(0, aw_ref.at[pl.ds(0, 3)], af.at[pl.ds(0, 3)]),
        load(1, aw_ref.at[pl.ds(3, 1)], af.at[pl.ds(3, 1)]),
        load(2, ew_ref, ef),
        load(3, cw_ref, cf),
    ]
    for copy in loads:
        copy.start()
    at.barrier()
    v_buf[at.x] = jnp.zeros(v_buf.shape[1:], BF)
    v_buf[at.x, 0 : vec_ref.shape[0], :] = vec_ref[...].astype(BF)
    vec_copies = []
    for k in range(1, nf):
        copy = remote(v_buf.at[at.x], v_buf.at[at.x], vs.at[k], vr.at[k], at.x_peer(k))
        copy.start()
        vec_copies.append(copy)

    def view(chunk, j, hi, core, own=False):
        if chunk < 2:
            first, count = ((0, 3), (3, 1))[chunk]
            cols = width // nh
            return a_ref.at[
                pl.ds(first, count),
                pl.ds(pl.multiple_of(j * shard + core * half, 16), half),
                pl.ds(pl.multiple_of(hi * cols, 128), cols),
            ]
        ref, stage, size = ((e_ref, eb, shard), (c_ref, cb, deep))[chunk - 2]
        cols = ref.shape[1] // nh
        start = core * (size // 2)
        if own:
            ref = stage
        else:
            start = j * size + start
        return ref.at[
            pl.ds(pl.multiple_of(start, 16), size // 2),
            pl.ds(pl.multiple_of(hi * cols, 128), cols),
        ]

    own = pl.multiple_of(at.x * shard, 16)
    x_copies = {}

    def send_chunk(chunk):
        for k in range(1, nf):
            copy = remote(
                view(chunk, at.x, at.hi, at.core, True), view(chunk, at.x, at.hi, at.core),
                xs.at[chunk, k], xr.at[chunk, k], at.x_peer(k),
            )
            copy.start()
            x_copies[chunk, k] = copy

    loads[0].wait()
    for u in range(3):
        a_ref[u, pl.ds(own, shard), :] = af[u].astype(BF)
    send_chunk(0)
    normed, _ = normalize(frames_ref[...])
    for copy in vec_copies:
        copy.wait()
    vec = jnp.concatenate([v_buf[j] for j in range(nf)], axis=1).astype(F32)
    vec_out[...] = vec
    mine = pl.ds(pl.multiple_of(at.z * rows, 128), rows)
    hidden = (normed * vec[0:1] + vec[1:2]).astype(BF)
    h_ref[mine, :] = hidden

    def block(b):
        return h_ref.at[pl.ds(pl.multiple_of(b * rows, 128), rows), :]

    def to_right(b):
        return remote(block(b), block(b), rs.at[b], hr.at[b], {"seq": at.z + 1})

    def to_left(b):
        return remote(block(b), block(b), hs.at[b], hr.at[b], {"seq": at.z - 1})

    @pl.when(at.z < ns - 1)
    def _():
        to_right(at.z).start()

    @pl.when(at.z > 0)
    def _():
        to_left(at.z).start()

    loads[1].wait()
    a_ref[3, pl.ds(own, shard), :] = af[3].astype(BF)
    send_chunk(1)
    loads[2].wait()
    eb[...] = ef[...].astype(BF)
    send_chunk(2)
    loads[3].wait()
    cb[...] = cf[...].astype(BF)
    send_chunk(3)
    stores = [
        load(4, eb, e_ref.at[pl.ds(own, shard), :]),
        load(5, cb, c_ref.at[pl.ds(pl.multiple_of(at.x * deep, 16), deep), :]),
    ]
    for copy in stores:
        copy.start()
    ht[:, mine] = hidden.T

    def first_copy(chunk, k):
        j = lax.rem(at.x - k + nf, nf)
        piece = view(chunk, j, at.hi, at.core)
        return remote(piece, piece, s1s.at[chunk, k], s1r.at[chunk, k], at.sibling())

    def y_copy(chunk, k, m):
        j = lax.rem(at.x - k + nf, nf)
        piece = view(chunk, j, at.hi, at.core)
        return remote(piece, piece, ys.at[chunk, k, m], yr.at[chunk, k, m], at.y_peer(m))

    def second_copy(chunk, k, m):
        j = lax.rem(at.x - k + nf, nf)
        piece = view(chunk, j, lax.rem(at.hi - m + nh, nh), at.core)
        return remote(piece, piece, s2s.at[chunk, k, m], s2r.at[chunk, k, m], at.sibling())

    def forward(chunk):
        for k in range(1, nf):
            x_copies[chunk, k].wait_recv()
            first_copy(chunk, k).start()
            for m in range(1, nh):
                y_copy(chunk, k, m).start()

    def relay(chunk):
        for k in range(1, nf):
            for m in range(1, nh):
                y_copy(chunk, k, m).wait_recv()
                second_copy(chunk, k, m).start()

    def arrived(chunk):
        for k in range(1, nf):
            first_copy(chunk, k).wait_recv()
            for m in range(1, nh):
                second_copy(chunk, k, m).wait_recv()

    def rows_of(b):
        part = pl.ds(pl.multiple_of(b * rows, 128), rows)
        k_buf[part, :] = nn(h_ref[part, :], a_ref[1]).astype(BF)
        v_buf2[part, :] = (nn(h_ref[part, :], a_ref[2]) + vec[3:4]).astype(BF)

    def turn(b):
        part = pl.ds(pl.multiple_of(b * rows, 128), rows)
        ht[:, part] = h_ref[part, :].T

    def hop(s):
        b = at.z - s
        d = at.z + s

        @pl.when(b >= 0)
        def _():
            to_right(b).wait_recv()

            @pl.when(at.z < ns - 1)
            def _():
                to_right(b).start()

        @pl.when(d < ns)
        def _():
            to_left(d).wait_recv()

            @pl.when(at.z > 0)
            def _():
                to_left(d).start()

    def use(s):
        b = at.z - s
        d = at.z + s

        @pl.when(b >= 0)
        def _():
            rows_of(b)
            turn(b)

        @pl.when(d < ns)
        def _():
            rows_of(d)
            turn(d)

    forward(0)
    hop(1)
    forward(1)
    relay(0)
    arrived(0)
    q_buf[...] = (nn(h_ref[mine, :], a_ref[0]) + vec[2:3]).astype(BF)
    stores.append(load(6, q_buf, q_out))
    stores[-1].start()
    rows_of(at.z)
    use(1)
    relay(1)
    forward(2)
    for s in range(2, ns):
        hop(s)
        use(s)
    arrived(1)
    for i, (src, dst) in enumerate(((a_ref, a_out), (ht, ht_out), (k_buf, k_out), (v_buf2, v_out))):
        stores.append(load(7 + i, src, dst))
        stores[-1].start()
    forward(3)
    relay(2)
    lo = lax.broadcasted_iota(jnp.int32, (rows, 128), 1) < 64

    def pair(p, carry):
        col = pl.ds(pl.multiple_of(p * 128, 128), 128)
        k2 = k_buf[:, col]
        v2 = v_buf2[:, col]
        q2 = q_buf[:, col]
        ctx, lse = [], []
        for h in range(2):
            mask = lo if h == 0 else jnp.logical_not(lo)
            s = nt(jnp.where(mask, q2, jnp.zeros_like(q2)), k2) * score_scale
            largest = jnp.max(s, axis=-1, keepdims=True)
            e = jnp.exp(s - largest)
            total = jnp.sum(e, axis=-1, keepdims=True)
            ctx.append(nn((e * (1.0 / total)).astype(BF), v2))
            lse.append(largest + jnp.log(total))
        ctx_buf[:, col] = jnp.where(lo, ctx[0], ctx[1])
        lse_ref[p] = jnp.where(lo, lse[0], lse[1])

        @pl.when(p == 1)
        def _():
            relay(3)

        return carry

    lax.fori_loop(0, width // 128, pair, 0)
    stores.append(load(11, ctx_buf, ctx_out))
    stores[-1].start()
    arrived(2)
    arrived(3)
    for copy in stores:
        copy.wait()
    for copy in x_copies.values():
        copy.wait_send()
    for chunk in range(4):
        for k in range(1, nf):
            first_copy(chunk, k).wait_send()
            for m in range(1, nh):
                y_copy(chunk, k, m).wait_send()
                second_copy(chunk, k, m).wait_send()
    for b in range(ns):
        @pl.when(jnp.logical_and(b <= at.z, at.z < ns - 1))
        def _():
            to_right(b).wait_send()

        @pl.when(jnp.logical_and(b >= at.z, at.z > 0))
        def _():
            to_left(b).wait_send()


def front_all(sizes, frames, vec, aw, ew, cw):
    nd, nf, ns = sizes
    nh = nd // 2
    rows, width = frames.shape
    shard, full = ew.shape
    deep = cw.shape[0]
    every = rows * ns
    dma = pltpu.SemaphoreType.DMA
    anywhere = pl.BlockSpec(memory_space=pl.ANY)
    return pl.pallas_call(
        functools.partial(front_kernel, sizes),
        out_shape=(
            jax.ShapeDtypeStruct((4, width, width), BF),
            jax.ShapeDtypeStruct((width, full), BF),
            jax.ShapeDtypeStruct((deep * nf, width), BF),
            jax.ShapeDtypeStruct((16, width), F32),
            jax.ShapeDtypeStruct((width, every), BF),
            jax.ShapeDtypeStruct((rows, width), BF),
            jax.ShapeDtypeStruct((every, width), BF),
            jax.ShapeDtypeStruct((every, width), BF),
            jax.ShapeDtypeStruct((rows, width), F32),
            jax.ShapeDtypeStruct((width // 128, rows, 128), F32),
        ),
        in_specs=[vmem(), vmem(), anywhere, anywhere, anywhere],
        out_specs=(anywhere, anywhere, anywhere, vmem()) + (anywhere,) * 5 + (vmem(),),
        scratch_shapes=[
            pltpu.VMEM((4, width, width), BF),
            pltpu.VMEM((nf, 16, vec.shape[1]), BF),
            pltpu.VMEM((every, width), BF),
            pltpu.VMEM((width, every), BF),
            pltpu.VMEM((rows, width), BF),
            pltpu.VMEM((every, width), BF),
            pltpu.VMEM((every, width), BF),
            pltpu.VMEM((rows, width), F32),
            pltpu.VMEM((4, shard, width), F32),
            pltpu.VMEM((shard, full), F32),
            pltpu.VMEM((deep, width), F32),
            pltpu.VMEM((shard, full), BF),
            pltpu.VMEM((deep, width), BF),
            dma((12,)),
            dma((4, nf)), dma((4, nf)),
            dma((4, nf, nh)), dma((4, nf, nh)),
            dma((4, nf)), dma((4, nf)),
            dma((4, nf, nh)), dma((4, nf, nh)),
            dma((nf,)), dma((nf,)),
            dma((ns,)), dma((ns,)), dma((ns,)),
        ],
        name="front",
        compiler_params=pltpu.CompilerParams(
            collective_id=0, has_side_effects=True, vmem_limit_bytes=67043328
        ),
    )(frames, vec, aw, ew, cw)


def back_kernel(
    sizes, q_ref, k_ref, v_ref, dc_ref, ctx_ref, lse_ref, ht_ref, w_ref, gm_ref, frames_ref,
    vec_ref, gv_ref, gc_ref, ge_ref, go_ref,
    oc_ref, oe_ref, oa_ref, ig_ref, ov_ref,
    ga, own, rc, rx, ry, rz, ri, dkt, dvt, dqa, dhs, dra, drb, drc, vb, vx, vy, vz,
    os, cs, cr, xs, xr, ys, yr, zs, zr, zis, zir, gs, gr, ays, ayr, acs, acr,
    das, dar, dbs, dbr, dcs, dcr, vs, vr,
):
    at = Place(sizes)
    nf, nh, ns = at.nf, at.nh, at.ns
    rows, width = q_ref.shape
    q = rc.shape[5]
    cols = width // nh
    per = cols // 128
    chunks = rc.shape[0]
    split = chunks // (3 * per)
    half = q * split
    group = per * split
    b0 = lax.rem(at.z, 2)
    b1 = at.z // 2
    at.barrier()

    def strip(core, r):
        return pl.ds(pl.multiple_of(core * half + r * q, 16), q)

    def lanes(s, hi):
        return pl.ds(pl.multiple_of(hi * cols + s * 128, 128), 128)

    def place_of(n):
        return n // group, lax.rem(n, group) // split, lax.rem(n, split)

    for s in range(per):
        for hi in range(nh):
            for part in range(2):
                for r in range(split):
                    pltpu.make_async_copy(
                        go_ref.at[:, pl.ds(part * half + r * q, q), pl.ds(hi * cols + s * 128, 128)],
                        ga.at[s, r, hi, :, part, 1, 1],
                        os.at[4],
                    ).start()

    def own_whole(slot):
        return pltpu.make_async_copy(own.at[slot], own.at[slot], os.at[slot])

    def c_whole(n):
        return remote(rc.at[n], rc.at[n], cs.at[n], cr.at[n], at.sibling())

    def c_send(n):
        slot = lax.rem(n, 4)
        g, s, r = place_of(n)

        @pl.when(n < group)
        def _():
            for hi in range(nh):
                for u in range(4):
                    block = lanes(s, hi)
                    remote(
                        gc_ref.at[:, u, strip(1 - at.core, r), block],
                        rc.at[n, hi, :, u // 2, u % 2], cs.at[n], cr.at[n], at.sibling(),
                    ).start()
                    pltpu.make_async_copy(
                        gc_ref.at[:, u, strip(at.core, r), block],
                        own.at[slot, hi, :, u // 2, u % 2], os.at[slot],
                    ).start()

        @pl.when(jnp.logical_and(n >= group, n < 2 * group))
        def _():
            for hi in range(nh):
                for u in range(4):
                    block = pl.ds(pl.multiple_of(u * width + hi * cols + s * 128, 128), 128)
                    remote(
                        ge_ref.at[:, strip(1 - at.core, r), block],
                        rc.at[n, hi, :, u // 2, u % 2], cs.at[n], cr.at[n], at.sibling(),
                    ).start()
                    pltpu.make_async_copy(
                        ge_ref.at[:, strip(at.core, r), block],
                        own.at[slot, hi, :, u // 2, u % 2], os.at[slot],
                    ).start()

        @pl.when(jnp.logical_and(n >= 2 * group, n < chunks))
        def _():
            remote(
                ga.at[s, r, :, :, 1 - at.core], rc.at[n], cs.at[n], cr.at[n], at.sibling()
            ).start()

    def x_copy(n, k):
        peer = lax.rem(at.x + k, nf)
        return remote(rc.at[n, :, peer], rx.at[n, k - 1], xs.at[n, k - 1], xr.at[n, k - 1], at.x_peer(k))

    def y_copy(n, m):
        return remote(
            rx.at[n, 0, at.y_hi(m)], ry.at[n, m - 1], ys.at[n, m - 1], yr.at[n, m - 1], at.y_peer(m)
        )

    assert ns == 4
    outer = b0 == b1
    inner = b0 != b1
    near = {"seq": at.z + 1 - 2 * b0}
    across = {"seq": 3 - at.z}

    def z_copy(n):
        return remote(ry.at[n, 0], rz.at[n], zs.at[n], zr.at[n], near)

    def zi_copy(n):
        return remote(ry.at[n, 0], ri.at[n], zis.at[n], zir.at[n], across)

    def by_group(n, act):
        g, s, r = place_of(n)

        for which in range(3):
            @pl.when(g == which)
            def _(which=which):
                def place(hi, ua, ub):
                    if which == 1:
                        start = (2 * ua + ub) * width + hi * cols + s * 128
                        return oe_ref.at[strip(at.core, r), pl.ds(pl.multiple_of(start, 128), 128)]
                    ref = oc_ref if which == 0 else oa_ref
                    return ref.at[ua, ub, strip(at.core, r), lanes(s, hi)]

                act(place)

    def g_whole(n):
        return remote(ry.at[n, 0], ry.at[n, 0], gs.at[n], gr.at[n], near)

    def ay_whole(n, m):
        return remote(ry.at[n, 0], ry.at[n, 0], ays.at[n, m - 1], ayr.at[n, m - 1], at.y_peer(m))

    def ac_whole(n):
        return remote(rx.at[n, 0], rx.at[n, 0], acs.at[n], acr.at[n], at.sibling())

    def g_start(n, total):
        def act(place):
            for u in range(4):
                spot = place(at.hi, u // 2, u % 2)
                spot[...] = total[u // 2, u % 2]
                remote(spot, spot, gs.at[n], gr.at[n], near).start()

        by_group(n, act)

    def ay_start(n):
        def act(place):
            for m in range(1, nh):
                for u in range(4):
                    spot = place(at.hi, u // 2, u % 2)
                    remote(spot, spot, ays.at[n, m - 1], ayr.at[n, m - 1], at.y_peer(m)).start()

        by_group(n, act)

    def ac_start(n):
        def act(place):
            for hi in range(nh):
                for u in range(4):
                    spot = place(hi, u // 2, u % 2)
                    remote(spot, spot, acs.at[n], acr.at[n], at.sibling()).start()

        by_group(n, act)

    def plus(left, right):
        if nf == 2:
            return left + right
        return (left.astype(F32) + right.astype(F32)).astype(BF)

    def stage_c(n):
        c_whole(n).wait_recv()
        slot = lax.rem(n, 4)
        _, s, r = place_of(n)

        @pl.when(n < 2 * group)
        def _():
            own_whole(slot).wait()

            def add(i, carry):
                hi, j = i // nf, lax.rem(i, nf)
                rc[n, hi, j] = plus(rc[n, hi, j], own[slot, hi, j])
                return carry

            lax.fori_loop(0, nh * nf, add, 0)

        @pl.when(n >= 2 * group)
        def _():
            def add(i, carry):
                hi, j = i // nf, lax.rem(i, nf)
                rc[n, hi, j] = plus(rc[n, hi, j], ga[s, r, hi, j, at.core])
                return carry

            lax.fori_loop(0, nh * nf, add, 0)

        for k in range(1, nf):
            x_copy(n, k).start()

    def stage_x(n):
        for k in range(1, nf):
            x_copy(n, k).wait_recv()

        def add(hi, carry):
            if nf == 2:
                rx[n, 0, hi] = rc[n, hi, at.x] + rx[n, 0, hi]
            else:
                total = rc[n, hi, at.x].astype(F32)
                for k in range(nf - 1):
                    total += rx[n, k, hi].astype(F32)
                rx[n, 0, hi] = total.astype(BF)
            return carry

        lax.fori_loop(0, nh, add, 0)
        for m in range(1, nh):
            y_copy(n, m).start()

    def stage_y(n):
        for m in range(1, nh):
            y_copy(n, m).wait_recv()
        total = rx[n, 0, at.hi]
        for m in range(nh - 1):
            total = plus(total, ry[n, m])
        ry[n, 0] = total

        @pl.when(outer)
        def _():
            z_copy(n).start()

    def stage_z(n):
        @pl.when(inner)
        def _():
            z_copy(n).wait_recv()
            ry[n, 0] = plus(ry[n, 0], rz[n])
            zi_copy(n).start()

    def stage_zi(n):
        @pl.when(inner)
        def _():
            zi_copy(n).wait_recv()
            g_start(n, plus(ry[n, 0], ri[n]))

    def stage_g(n):
        @pl.when(outer)
        def _():
            g_whole(n).wait_recv()

        ay_start(n)

    def stage_ay(n):
        for m in range(1, nh):
            ay_whole(n, m).wait_recv()
        ac_start(n)

    lo = lax.broadcasted_iota(jnp.int32, (rows, 128), 1) < 64
    pairs = width // 128

    def unit(index):
        i, p = index // pairs, lax.rem(index, pairs)
        there = 1 - b1 - i + 2 * i * b1
        keys = pl.ds(pl.multiple_of(there * (2 * rows), 128), 2 * rows)
        col = pl.ds(pl.multiple_of(p * 128, 128), 128)
        k2 = k_ref[keys, col]
        v2 = v_ref[keys, col]
        q2 = q_ref[:, col]
        dc2 = dc_ref[:, col]
        both = dc2.astype(F32) * ctx_ref[:, col]
        lse2 = lse_ref[p]
        dq, dk, dv = [], None, None
        for h in range(2):
            mask = lo if h == 0 else jnp.logical_not(lo)
            qm = jnp.where(mask, q2, jnp.zeros_like(q2))
            dmask = jnp.where(mask, dc2, jnp.zeros_like(q2))
            lse = lse2[:, 0:1] if h == 0 else lse2[:, 64:65]
            dot = jnp.sum(jnp.where(mask, both, 0.0), axis=-1, keepdims=True)
            probs = jnp.exp(nt(qm, k2) * score_scale - lse)
            slopes = nt(dmask, v2)
            dscore = (probs * (slopes - dot) * score_scale).astype(BF)
            dq.append(nn(dscore, k2))
            a = nn(dmask.T, probs.astype(BF))
            b = nn(qm.T, dscore)
            dv = a if dv is None else dv + a
            dk = b if dk is None else dk + b
        dq2 = jnp.where(lo, dq[0], dq[1])

        @pl.when(i == 0)
        def _():
            dqa[:, col] = dq2

        @pl.when(i > 0)
        def _():
            dqa[:, col] += dq2

        dkt[col, keys] = dk.astype(BF)
        dvt[col, keys] = dv.astype(BF)

    def weights(s):
        frames = pl.ds(pl.multiple_of(at.z * rows, 128), rows)
        for hi in range(nh):
            col = pl.ds(hi * cols + s * 128, 128)
            dq2 = dqa[:, col]
            vb[2, 0:1, col] = jnp.sum(dq2, axis=0, keepdims=True)
            dq2 = dq2.astype(BF)
            dk2 = dkt[col, :]
            dv2 = dvt[col, :]
            for j in range(nf):
                for part in range(2):
                    for r in range(split):
                        here = pl.ds((2 * j + part) * half + r * q, q)
                        ga[s, r, hi, j, part, 0, 0] = nn(ht_ref[here, frames], dq2).astype(BF)
                        ga[s, r, hi, j, part, 0, 1] = nt(ht_ref[here, :], dk2).astype(BF)
                        ga[s, r, hi, j, part, 1, 0] = nt(ht_ref[here, :], dv2).astype(BF)

    pieces = 16
    per_step = 2
    lag = 2
    low = 1 - b1

    def part_of(t):
        return pl.ds(t * (width // pieces), width // pieces)

    def da_copy(t):
        return remote(
            dhs.at[pl.ds(low, 3), part_of(t)], dra.at[:, part_of(t)], das.at[t], dar.at[t], near
        )

    def db_copy(t):
        return remote(
            dhs.at[pl.ds(2 * low, 2), part_of(t)], drb.at[:, part_of(t)], dbs.at[t], dbr.at[t], across
        )

    def dc_copy(t):
        return remote(dhs.at[3 * b1, part_of(t)], drc.at[part_of(t)], dcs.at[t], dcr.at[t], near)

    def d_stage(i, t):
        part = part_of(t)
        if i == 0:
            @pl.when(outer)
            def _():
                da_copy(t).start()
        elif i == 1:
            @pl.when(inner)
            def _():
                da_copy(t).wait_recv()
                for j in range(3):
                    dhs[low + j, part] = dhs[low + j, part] + dra[j, part]
                db_copy(t).start()
        elif i == 2:
            @pl.when(inner)
            def _():
                db_copy(t).wait_recv()
                for j in range(2):
                    dhs[2 * b1 + j, part] = dhs[2 * b1 + j, part] + drb[j, part]
                dc_copy(t).start()
        else:
            @pl.when(outer)
            def _():
                dc_copy(t).wait_recv()

    def spread(i):
        there = 1 - b1 - i + 2 * i * b1
        for ub in range(2):
            part = pl.ds(pl.multiple_of((2 * there + ub) * rows, 128), rows)
            dhs[2 * there + ub] = (nn(w_ref[1], dkt[:, part]) + nn(w_ref[2], dvt[:, part])).astype(BF)

    def first_norm():
        @pl.when(inner)
        def _():
            drc[...] = jnp.zeros_like(drc)

        total = dhs[at.z].astype(F32) + nt(w_ref[0], dqa[...].astype(BF))
        total += drc[...].astype(F32)
        total = total.T
        normed, inverse = normalize(frames_ref[...])
        scaled = total * vec_ref[0:1, :]
        centred = (
            scaled
            - jnp.mean(scaled, axis=-1, keepdims=True)
            - normed * jnp.mean(scaled * normed, axis=-1, keepdims=True)
        )
        ig_ref[...] = gm_ref[...] + inverse * centred
        vb[1] = gv_ref[...]
        vb[1, 0:1, :] = jnp.sum(total * normed, axis=0, keepdims=True)
        vb[1, 1:2, :] = jnp.sum(total, axis=0, keepdims=True)
        vb[1, 2:3, :] = vb[2, 0:1, :]

    def v_core():
        return remote(vb.at[1], vb.at[0], vs.at[0], vr.at[0], at.sibling())

    def v_x(k):
        return remote(vx.at[at.x], vx.at[at.x], vs.at[k], vr.at[k], at.x_peer(k))

    def v_y(m):
        return remote(vy.at[at.hi], vy.at[at.hi], vs.at[nf + m], vr.at[nf + m], at.y_peer(m))

    def v_z(k):
        return remote(
            vz.at[at.z], vz.at[at.z], vs.at[nf + nh + k], vr.at[nf + nh + k], at.z_peer(k)
        )

    def v_step(i):
        if i == 0:
            v_core().start()
        elif i == 1:
            v_core().wait_recv()
            vx[at.x] = vb[0] + vb[1]
            for k in range(1, nf):
                v_x(k).start()
        elif i == 2:
            for k in range(1, nf):
                v_x(k).wait_recv()
            total = vx[0]
            for j in range(1, nf):
                total += vx[j]
            vy[at.hi] = total
            for m in range(1, nh):
                v_y(m).start()
        elif i == 3:
            for m in range(1, nh):
                v_y(m).wait_recv()
            total = vy[0]
            for j in range(1, nh):
                total += vy[j]
            vz[at.z] = total
            for k in range(1, ns):
                v_z(k).start()
        else:
            for k in range(1, ns):
                v_z(k).wait_recv()
            total = vz[0]
            for j in range(1, ns):
                total += vz[j]
            ov_ref[...] = total

    ready = group
    each = -(-2 * pairs // ready)
    done = [-(-pairs * (i + 1) // each) - 1 for i in range(2)]
    away = done[1] + 1
    norm = max(away + (pieces - 1) // per_step + 4, chunks - 2)
    stages = (stage_x, stage_y, stage_z, stage_zi, stage_g, stage_ay)
    last = max(chunks + lag * len(stages), norm + 6)
    for n in range(4):
        c_send(n)

    def step(n, carry):
        for k in range(2):
            @pl.when(2 * n + k < 2 * group)
            def _(k=k):
                stage_c(2 * n + k)

                @pl.when(2 * n + k + 4 < 2 * group)
                def _():
                    c_send(2 * n + k + 4)

        for s in range(per):
            @pl.when(n == ready + s + 1)
            def _(s=s):
                for r in range(split):
                    stage_c(2 * group + s * split + r)

        @pl.when(n < ready)
        def _():
            def one(k, carry):
                @pl.when(n * each + k < 2 * pairs)
                def _():
                    unit(n * each + k)

                return carry

            lax.fori_loop(0, each, one, 0)

        for i in range(2):
            @pl.when(n == done[i])
            def _(i=i):
                spread(i)

        @pl.when(n == norm)
        def _():
            first_norm()

        for s in range(per):
            @pl.when(n == ready + s)
            def _(s=s):
                weights(s)
                if s == 0:
                    whole = ga.at[:, :, :, :, :, 1, 1]
                    pltpu.make_async_copy(whole, whole, os.at[4]).wait()
                for r in range(split):
                    c_send(2 * group + s * split + r)

        for i, stage in enumerate(stages):
            @pl.when(jnp.logical_and(n >= lag * i, n < chunks + lag * i))
            def _(i=i, stage=stage):
                stage(n - lag * i)

        for i in range(4):
            for m in range(pieces // per_step):
                @pl.when(n == away + m + i)
                def _(i=i, m=m):
                    for t in range(m * per_step, (m + 1) * per_step):
                        d_stage(i, t)

        for i in range(5):
            @pl.when(n == norm + i)
            def _(i=i):
                v_step(i)

        return carry

    lax.fori_loop(0, last, step, 0)
    for n in range(chunks):
        ac_whole(n).wait()

    def drain(n, carry):
        c_whole(n).wait_send()

        @pl.when(outer)
        def _():
            z_copy(n).wait_send()

        @pl.when(inner)
        def _():
            zi_copy(n).wait_send()
            g_whole(n).wait_send()

        for k in range(1, nf):
            x_copy(n, k).wait_send()
        for m in range(1, nh):
            y_copy(n, m).wait_send()
            ay_whole(n, m).wait_send()
        return carry

    lax.fori_loop(0, chunks, drain, 0)

    @pl.when(outer)
    def _():
        for t in range(pieces):
            da_copy(t).wait_send()

    @pl.when(inner)
    def _():
        for t in range(pieces):
            db_copy(t).wait_send()
            dc_copy(t).wait_send()

    for k in range(1, ns):
        v_z(k).wait_send()
    for k in range(1, nf):
        v_x(k).wait_send()
    for m in range(1, nh):
        v_y(m).wait_send()
    v_core().wait_send()


def back_all(sizes, q, k, v, dc, ctx, lse, ht, w, gm, frames, vec, gv, gc, ge, go):
    nd, nf, ns = sizes
    nh = nd // 2
    rows, width = q.shape
    shard = go.shape[1]
    half = shard // 2
    every = k.shape[0]
    split = 2 if half % 32 == 0 else 1
    strip = half // split
    per = width // nh // 128
    chunks = 3 * per * split
    xn, yn = max(nf - 1, 1), max(nh - 1, 1)
    dma = pltpu.SemaphoreType.DMA
    anywhere = pl.BlockSpec(memory_space=pl.ANY)
    return pl.pallas_call(
        functools.partial(back_kernel, sizes),
        out_shape=(
            jax.ShapeDtypeStruct((2, 2, shard, width), BF),
            jax.ShapeDtypeStruct((shard, 4 * width), BF),
            jax.ShapeDtypeStruct((2, 2, shard, width), BF),
            jax.ShapeDtypeStruct((rows, width), F32),
            jax.ShapeDtypeStruct((16, width), F32),
        ),
        in_specs=[vmem()] * 12 + [anywhere] * 3,
        out_specs=(vmem(),) * 5,
        scratch_shapes=[
            pltpu.VMEM((per, split, nh, nf, 2, 2, 2, strip, 128), BF),
            pltpu.VMEM((4, nh, nf, 2, 2, strip, 128), BF),
            pltpu.VMEM((chunks, nh, nf, 2, 2, strip, 128), BF),
            pltpu.VMEM((chunks, xn, nh, 2, 2, strip, 128), BF),
            pltpu.VMEM((chunks, yn, 2, 2, strip, 128), BF),
            pltpu.VMEM((chunks, 2, 2, strip, 128), BF),
            pltpu.VMEM((chunks, 2, 2, strip, 128), BF),
            pltpu.VMEM((width, every), BF),
            pltpu.VMEM((width, every), BF),
            pltpu.VMEM((rows, width), F32),
            pltpu.VMEM((ns, width, rows), BF),
            pltpu.VMEM((3, width, rows), BF),
            pltpu.VMEM((2, width, rows), BF),
            pltpu.VMEM((width, rows), BF),
            pltpu.VMEM((3, 16, width), F32),
            pltpu.VMEM((nf, 16, width), F32),
            pltpu.VMEM((nh, 16, width), F32),
            pltpu.VMEM((ns, 16, width), F32),
            dma((5,)),
            dma((chunks,)), dma((chunks,)),
            dma((chunks, xn)), dma((chunks, xn)),
            dma((chunks, yn)), dma((chunks, yn)),
            dma((chunks,)), dma((chunks,)),
            dma((chunks,)), dma((chunks,)),
            dma((chunks,)), dma((chunks,)),
            dma((chunks, yn)), dma((chunks, yn)),
            dma((chunks,)), dma((chunks,)),
            dma((16,)), dma((16,)),
            dma((16,)), dma((16,)),
            dma((16,)), dma((16,)),
            dma((nf + nh + ns,)), dma((nf + nh + ns,)),
        ],
        name="back",
        compiler_params=pltpu.CompilerParams(
            collective_id=1, has_side_effects=True, vmem_limit_bytes=67043328
        ),
    )(q, k, v, dc, ctx, lse, ht, w, gm, frames, vec, gv, gc, ge, go)


def feed_kernel(
    ctx_ref, frames_ref, cot_ref, vec_ref, wo_ref, win_ref, wout_ref,
    fo_ref, gm_ref, dc_ref, gi_ref, gout_ref, go_ref, gv_ref,
    mid, h2, h2t, dyb, acc, dh2,
):
    b = pl.program_id(0)

    @pl.when(b == 0)
    def _():
        middle = frames_ref[...] + nn(ctx_ref[...].astype(BF), wo_ref[...]) + vec_ref[4:5, :]
        mid[...] = middle
        normed, _ = normalize(middle)
        hidden = (normed * vec_ref[5:6, :] + vec_ref[6:7, :]).astype(BF)
        h2[...] = hidden
        h2t[...] = hidden.T
        dyb[...] = cot_ref[...].astype(BF)
        acc[...] = middle + vec_ref[7:8, :]
        dh2[...] = jnp.zeros_like(dh2)
        gv_ref[...] = jnp.zeros_like(gv_ref)

    up = dyb[...]
    u = nn(h2[...], win_ref[...]) + vec_ref[pl.ds(8 + b, 1), :]
    phi = 0.5 * (1.0 + lax.erf(u * 0.7071067811865476))
    activated = (u * phi).astype(BF)
    acc[...] += nn(activated, wout_ref[...])
    gout_ref[...] = tn(activated, up).astype(BF)
    du = nt(up, wout_ref[...]) * (phi + u * jnp.exp(-0.5 * u * u) * 0.3989422804014327)
    gv_ref[pl.ds(8 + b, 1), :] = jnp.sum(du, axis=0, keepdims=True)
    dub = du.astype(BF)
    gi_ref[...] = nn(h2t[...], dub).astype(BF)
    dh2[...] += nt(dub, win_ref[...])

    @pl.when(b == pl.num_programs(0) - 1)
    def _():
        fo_ref[...] = acc[...]
        normed, inverse = normalize(mid[...])
        back, gain, offset = norm_back(dh2[...], normed, inverse, vec_ref[5:6, :])
        upstream = cot_ref[...]
        middle = upstream + back
        gm_ref[...] = middle
        dab = middle.astype(BF)
        go_ref[...] = tn(ctx_ref[...].astype(BF), dab).astype(BF)
        dctx = nt(dab, wo_ref[...]).astype(BF)
        dc_ref[...] = dctx
        gv_ref[3:4, :] = jnp.sum(dctx.astype(F32), axis=0, keepdims=True)
        gv_ref[4:5, :] = jnp.sum(middle, axis=0, keepdims=True)
        gv_ref[5:6, :] = gain[None]
        gv_ref[6:7, :] = offset[None]
        gv_ref[7:8, :] = jnp.sum(upstream, axis=0, keepdims=True)


def feed_all(ctx, frames, cot, vec, aw, ew, cw):
    rows, width = frames.shape
    full = ew.shape[1]
    whole = lambda shape: pl.BlockSpec(shape, lambda b: (0,) * len(shape))
    blocks = full // width
    return pl.pallas_call(
        feed_kernel,
        grid=(blocks,),
        out_shape=(
            jax.ShapeDtypeStruct((rows, width), F32),
            jax.ShapeDtypeStruct((rows, width), F32),
            jax.ShapeDtypeStruct((rows, width), BF),
            jax.ShapeDtypeStruct((width, full), BF),
            jax.ShapeDtypeStruct((full, width), BF),
            jax.ShapeDtypeStruct((width, width), BF),
            jax.ShapeDtypeStruct((16, width), F32),
        ),
        in_specs=[
            whole((rows, width)), whole((rows, width)), whole((rows, width)), whole((16, width)),
            pl.BlockSpec((None, width, width), lambda b: (3, 0, 0)),
            pl.BlockSpec((width, width), lambda b: (0, b)),
            pl.BlockSpec((width, width), lambda b: (b, 0)),
        ],
        out_specs=(
            whole((rows, width)), whole((rows, width)), whole((rows, width)),
            pl.BlockSpec((width, width), lambda b: (0, b)),
            pl.BlockSpec((width, width), lambda b: (b, 0)),
            whole((width, width)), whole((16, width)),
        ),
        scratch_shapes=[
            pltpu.VMEM((rows, width), F32),
            pltpu.VMEM((rows, width), BF),
            pltpu.VMEM((width, rows), BF),
            pltpu.VMEM((rows, width), BF),
            pltpu.VMEM((rows, width), F32),
            pltpu.VMEM((rows, width), F32),
        ],
        name="feed",
        compiler_params=pltpu.CompilerParams(vmem_limit_bytes=67043328),
    )(ctx, frames, cot, vec, aw, ew, cw)


def on_device(
    sizes,
    frames_in,
    cotangent,
    attention_weight,
    expand_weight,
    contract_weight,
    vectors,
    first_attention,
    first_expand,
    first_contract,
    first_vectors,
    second_attention,
    second_expand,
    second_contract,
    second_vectors,
):
    nd, nf, ns = sizes
    frames = frames_in[0]
    upstream = cotangent[0]
    rows, width = frames.shape
    shard = attention_weight.shape[1]
    full = expand_weight.shape[1]
    aw, ew, cw, vec, h_turned, queries, key_rows, value_rows, context_wide, log_total = front_all(
        sizes, frames, vectors, attention_weight, expand_weight, contract_weight
    )
    frames_out, grad_middle, grad_context, grad_expand, grad_contract, grad_output_w, gv = feed_all(
        context_wide, frames, upstream, vec, aw, ew, cw
    )
    oc, oe, oa, input_gradient, gv_sum = back_all(
        sizes,
        queries,
        key_rows,
        value_rows,
        grad_context,
        context_wide,
        log_total,
        h_turned,
        aw,
        grad_middle,
        frames,
        vec,
        gv,
        grad_contract.reshape(nf, 4, shard, width),
        grad_expand.reshape(nf, shard, full),
        grad_output_w.reshape(nf, shard, width),
    )
    owned_vec = lax.dynamic_slice_in_dim(
        gv_sum[:12], lax.axis_index("fsdp") * (width // nf), width // nf, 1
    )
    owned = (
        oa.reshape(4, shard, width).astype(F32),
        oe.astype(F32),
        oc.reshape(4 * shard, width).astype(F32),
    )
    attention_out = (owned[0],) + adam_update(
        attention_weight, owned[0], first_attention, second_attention, rate_matrix, decay_matrix
    )
    expand_out = (owned[1],) + adam_update(
        expand_weight, owned[1], first_expand, second_expand, rate_matrix, decay_matrix
    )
    contract_out = (owned[2],) + adam_update(
        contract_weight, owned[2], first_contract, second_contract, rate_matrix, decay_matrix
    )
    vector_out = (owned_vec,) + adam_update(
        vectors, owned_vec, first_vectors, second_vectors, rate_vector, 0.0
    )
    result = [frames_out[None], input_gradient[None]]
    for i in range(4):
        result += [attention_out[i], expand_out[i], contract_out[i], vector_out[i]]
    return tuple(result)


def solution(mesh):
    sizes = (mesh.shape["dp"], mesh.shape["fsdp"], mesh.shape["seq"])
    data = P(("dp", "fsdp"), "seq", None)
    state = (P(None, "fsdp", None), P("fsdp", None), P("fsdp", None), P(None, "fsdp"))
    return jax.shard_map(
        functools.partial(on_device, sizes),
        mesh=mesh,
        in_specs=(data, data) + state * 3,
        out_specs=(data, data) + state * 4,
        check_vma=False,
    )
```

```python
import functools

import jax
import jax.numpy as jnp
from jax import lax
from jax.experimental import pallas as pl
from jax.experimental.pallas import tpu as pltpu
from jax.sharding import PartitionSpec as P

HEADS = 12
norm_eps = 1e-05
beta_one = 0.9
beta_two = 0.999
adam_eps = 1e-08
adam_count = 5.0
rate_matrix = 0.02
rate_vector = 0.1
decay_matrix = 0.1
score_scale = 0.125
VMEM_LIMIT = 60 << 20
MESH = pl.DeviceIdType.MESH
BF = jnp.bfloat16
F32 = jnp.float32


def nt(left, right):
    return lax.dot_general(left, right, (((1,), (1,)), ((), ())), preferred_element_type=F32)


def nn(left, right):
    return lax.dot_general(left, right, (((1,), (0,)), ((), ())), preferred_element_type=F32)


def tn(left, right):
    return lax.dot_general(left, right, (((0,), (0,)), ((), ())), preferred_element_type=F32)


def vmem():
    return pl.BlockSpec(memory_space=pltpu.VMEM)


def normalize(values):
    center = values - jnp.mean(values, axis=-1, keepdims=True)
    inverse = lax.rsqrt(jnp.mean(center * center, axis=-1, keepdims=True) + norm_eps)
    return center * inverse, inverse


def norm_back(upstream, normed, inverse, gain):
    scaled = upstream * gain
    inner = (
        scaled
        - jnp.mean(scaled, axis=-1, keepdims=True)
        - normed * jnp.mean(scaled * normed, axis=-1, keepdims=True)
    )
    return (inverse * inner, jnp.sum(upstream * normed, axis=0), jnp.sum(upstream, axis=0))


def adam_update(weight, gradient, first, second, rate, decay):
    first_new = beta_one * first + (1.0 - beta_one) * gradient
    second_new = beta_two * second + (1.0 - beta_two) * gradient * gradient
    first_hat = first_new / (1.0 - beta_one**adam_count)
    second_hat = second_new / (1.0 - beta_two**adam_count)
    updated = weight - rate * (first_hat / (jnp.sqrt(second_hat) + adam_eps) + decay * weight)
    return (updated, first_new, second_new)


class Place:
    def __init__(self, sizes):
        self.nd, self.nf, self.ns = sizes
        self.nh = self.nd // 2
        self.dp = lax.axis_index("dp")
        self.x = lax.axis_index("fsdp")
        self.z = lax.axis_index("seq")
        self.core = lax.rem(self.dp, 2)
        self.hi = self.dp // 2

    def sibling(self):
        return {"dp": self.hi * 2 + 1 - self.core}

    def x_peer(self, k):
        return {"fsdp": lax.rem(self.x + k, self.nf)}

    def y_hi(self, k):
        return lax.rem(self.hi + k, self.nh)

    def y_peer(self, k):
        return {"dp": self.y_hi(k) * 2 + self.core}

    def z_at(self, k):
        return lax.rem(self.z + k + self.ns, self.ns)

    def z_peer(self, k):
        return {"seq": self.z_at(k)}

    def everyone(self):
        out = [self.sibling()]
        out += [self.x_peer(k) for k in range(1, self.nf)]
        out += [self.y_peer(k) for k in range(1, self.nh)]
        out += [self.z_peer(k) for k in range(1, self.ns)]
        return out

    def barrier(self):
        sem = pltpu.get_barrier_semaphore()
        peers = self.everyone()
        for peer in peers:
            pl.semaphore_signal(sem, inc=1, device_id=peer, device_id_type=MESH)
        pl.semaphore_wait(sem, len(peers))


def remote(src, dst, send, recv, peer):
    return pltpu.make_async_remote_copy(
        src_ref=src, dst_ref=dst, send_sem=send, recv_sem=recv, device_id=peer, device_id_type=MESH
    )


def front_kernel(
    sizes, frames_ref, vec_ref, aw_ref, ew_ref, cw_ref,
    a_out, e_ref, c_ref, vec_out, ht_out, q_out, k_out, v_out, ctx_out, lse_ref,
    a_ref, v_buf, h_ref, ht, q_buf, k_buf, v_buf2, ctx_buf, af, ef, eb, cb, kept, stat,
    ls, xs, xr, ys, yr, s1s, s1r, s2s, s2r, vs, vr, rs, hs, hr,
):
    at = Place(sizes)
    nf, nh, ns = at.nf, at.nh, at.ns
    rows, width = frames_ref.shape
    shard = aw_ref.shape[1]
    half = shard // 2
    deep = cb.shape[0]
    b0 = lax.rem(at.z, 2)
    b1 = at.z // 2

    def load(i, src, dst):
        return pltpu.make_async_copy(src, dst, ls.at[i])

    loads = [
        load(0, aw_ref.at[pl.ds(0, 3)], af.at[pl.ds(0, 3)]),
        load(1, aw_ref.at[pl.ds(3, 1)], af.at[pl.ds(3, 1)]),
        load(2, ew_ref, ef),
        load(3, cw_ref, af),
    ]
    for copy in loads[:3]:
        copy.start()
    at.barrier()
    v_buf[at.x] = jnp.zeros(v_buf.shape[1:], BF)
    v_buf[at.x, 0 : vec_ref.shape[0], :] = vec_ref[...].astype(BF)
    vec_copies = []
    for k in range(1, nf):
        copy = remote(v_buf.at[at.x], v_buf.at[at.x], vs.at[k], vr.at[k], at.x_peer(k))
        copy.start()
        vec_copies.append(copy)

    def view(chunk, j, hi, core, own=False):
        if chunk < 2:
            first, count = ((0, 3), (3, 1))[chunk]
            cols = width // nh
            return a_ref.at[
                pl.ds(first, count),
                pl.ds(pl.multiple_of(j * shard + core * half, 16), half),
                pl.ds(pl.multiple_of(hi * cols, 128), cols),
            ]
        ref, stage, size = ((e_ref, eb, shard), (c_ref, cb, deep))[chunk - 2]
        cols = ref.shape[1] // nh
        start = core * (size // 2)
        if own:
            ref = stage
        else:
            start = j * size + start
        return ref.at[
            pl.ds(pl.multiple_of(start, 16), size // 2),
            pl.ds(pl.multiple_of(hi * cols, 128), cols),
        ]

    own = pl.multiple_of(at.x * shard, 16)
    x_copies = {}

    def send_chunk(chunk):
        for k in range(1, nf):
            copy = remote(
                view(chunk, at.x, at.hi, at.core, True), view(chunk, at.x, at.hi, at.core),
                xs.at[chunk, k], xr.at[chunk, k], at.x_peer(k),
            )
            copy.start()
            x_copies[chunk, k] = copy

    loads[0].wait()
    for u in range(3):
        a_ref[u, pl.ds(own, shard), :] = af[u].astype(BF)
    send_chunk(0)
    normed, _ = normalize(frames_ref[...])
    for copy in vec_copies:
        copy.wait()
    vec = jnp.concatenate([v_buf[j] for j in range(nf)], axis=1).astype(F32)
    vec_out[...] = vec
    mine = pl.ds(pl.multiple_of(at.z * rows, 128), rows)
    hidden = (normed * vec[0:1] + vec[1:2]).astype(BF)
    h_ref[mine, :] = hidden

    def block(b):
        return h_ref.at[pl.ds(pl.multiple_of(b * rows, 128), rows), :]

    def to_right(b):
        return remote(block(b), block(b), rs.at[b], hr.at[b], {"seq": at.z + 1})

    def to_left(b):
        return remote(block(b), block(b), hs.at[b], hr.at[b], {"seq": at.z - 1})

    @pl.when(at.z < ns - 1)
    def _():
        to_right(at.z).start()

    @pl.when(at.z > 0)
    def _():
        to_left(at.z).start()

    loads[1].wait()
    a_ref[3, pl.ds(own, shard), :] = af[3].astype(BF)
    loads[3].start()
    send_chunk(1)
    loads[2].wait()
    eb[...] = ef[...].astype(BF)
    send_chunk(2)
    loads[3].wait()
    for u in range(4):
        cb[pl.ds(u * shard, shard), :] = af[u].astype(BF)
    send_chunk(3)
    stores = [
        load(4, eb, e_ref.at[pl.ds(own, shard), :]),
        load(5, cb, c_ref.at[pl.ds(pl.multiple_of(at.x * deep, 16), deep), :]),
    ]
    for copy in stores:
        copy.start()
    ht[:, mine] = hidden.T

    def first_copy(chunk, k):
        j = lax.rem(at.x - k + nf, nf)
        piece = view(chunk, j, at.hi, at.core)
        return remote(piece, piece, s1s.at[chunk, k], s1r.at[chunk, k], at.sibling())

    def y_copy(chunk, k, m):
        j = lax.rem(at.x - k + nf, nf)
        piece = view(chunk, j, at.hi, at.core)
        return remote(piece, piece, ys.at[chunk, k, m], yr.at[chunk, k, m], at.y_peer(m))

    def second_copy(chunk, k, m):
        j = lax.rem(at.x - k + nf, nf)
        piece = view(chunk, j, lax.rem(at.hi - m + nh, nh), at.core)
        return remote(piece, piece, s2s.at[chunk, k, m], s2r.at[chunk, k, m], at.sibling())

    def forward(chunk):
        for k in range(1, nf):
            x_copies[chunk, k].wait_recv()
            first_copy(chunk, k).start()
            for m in range(1, nh):
                y_copy(chunk, k, m).start()

    def relay(chunk):
        for k in range(1, nf):
            for m in range(1, nh):
                y_copy(chunk, k, m).wait_recv()
                second_copy(chunk, k, m).start()

    def arrived(chunk):
        for k in range(1, nf):
            first_copy(chunk, k).wait_recv()
            for m in range(1, nh):
                second_copy(chunk, k, m).wait_recv()

    def rows_of(b):
        part = pl.ds(pl.multiple_of(b * rows, 128), rows)
        k_buf[part, :] = nn(h_ref[part, :], a_ref[1]).astype(BF)
        v_buf2[part, :] = (nn(h_ref[part, :], a_ref[2]) + vec[3:4]).astype(BF)

    def turn(b):
        part = pl.ds(pl.multiple_of(b * rows, 128), rows)
        ht[:, part] = h_ref[part, :].T

    def hop(s):
        b = at.z - s
        d = at.z + s

        @pl.when(b >= 0)
        def _():
            to_right(b).wait_recv()

            @pl.when(at.z < ns - 1)
            def _():
                to_right(b).start()

        @pl.when(d < ns)
        def _():
            to_left(d).wait_recv()

            @pl.when(at.z > 0)
            def _():
                to_left(d).start()

    lane = lax.broadcasted_iota(jnp.int32, (rows, 128), 1)
    lo = lane < 64

    def scores(p, h, b):
        col = pl.ds(pl.multiple_of(p * 128, 128), 128)
        part = pl.ds(pl.multiple_of(b * rows, 128), rows)
        q2 = q_buf[:, col]
        mask = lo if h == 0 else jnp.logical_not(lo)
        s = nt(jnp.where(mask, q2, jnp.zeros_like(q2)), k_buf[part, col]) * score_scale
        largest = jnp.max(s, axis=-1, keepdims=True)
        e = jnp.exp(s - largest)
        return e, largest, jnp.sum(e, axis=-1, keepdims=True)

    assert ns == 4
    blocks = (at.z, at.z + 1 - 2 * b0, 2 - b1, 3 - 3 * b1)

    def begin(i):
        b = blocks[i]
        rows_of(b)

        def pair(p, carry):
            found = []
            for h in range(2):
                e, largest, total = scores(p, h, b)
                kept[i, 2 * p + h] = e
                found += [largest, total]
            stat[i, p] = jnp.where(
                lo, jnp.where(lane < 32, found[0], found[1]), jnp.where(lane < 96, found[2], found[3])
            )
            return carry

        lax.fori_loop(0, width // 128, pair, 0)

    forward(0)
    hop(1)
    forward(1)
    relay(0)
    arrived(0)
    q_buf[...] = (nn(h_ref[mine, :], a_ref[0]) + vec[2:3]).astype(BF)
    stores.append(load(6, q_buf, q_out))
    stores[-1].start()
    begin(0)
    hop(2)
    begin(1)
    turn(blocks[1])
    relay(1)
    forward(2)
    begin(2)
    turn(blocks[2])
    hop(3)
    rows_of(blocks[3])
    turn(blocks[3])
    arrived(1)
    for i, (src, dst) in enumerate(((a_ref, a_out), (ht, ht_out), (k_buf, k_out), (v_buf2, v_out))):
        stores.append(load(7 + i, src, dst))
        stores[-1].start()
    forward(3)
    relay(2)

    def pair(p, carry):
        col = pl.ds(pl.multiple_of(p * 128, 128), 128)
        ctx, lse = [], []
        for h in range(2):
            e, peak, count = scores(p, h, blocks[3])
            peaks = [stat[i, p][:, 64 * h : 64 * h + 1] for i in range(3)] + [peak]
            counts = [stat[i, p][:, 64 * h + 32 : 64 * h + 33] for i in range(3)] + [count]
            largest = functools.reduce(jnp.maximum, peaks)
            shares = [jnp.exp(each - largest) for each in peaks]
            total = sum(share * each for share, each in zip(shares, counts))
            inverse = 1.0 / total
            out = None
            for i in range(4):
                part = pl.ds(pl.multiple_of(blocks[i] * rows, 128), rows)
                found = kept[i, 2 * p + h] if i < 3 else e
                term = nn((found * (shares[i] * inverse)).astype(BF), v_buf2[part, col])
                out = term if out is None else out + term
            ctx.append(out)
            lse.append(largest + jnp.log(total))
        ctx_buf[:, col] = jnp.where(lo, ctx[0], ctx[1])
        lse_ref[p] = jnp.where(lo, lse[0], lse[1])

        @pl.when(p == 1)
        def _():
            relay(3)

        return carry

    lax.fori_loop(0, width // 128, pair, 0)
    stores.append(load(11, ctx_buf, ctx_out))
    stores[-1].start()
    arrived(2)
    arrived(3)
    for copy in stores:
        copy.wait()
    for copy in x_copies.values():
        copy.wait_send()
    for chunk in range(4):
        for k in range(1, nf):
            first_copy(chunk, k).wait_send()
            for m in range(1, nh):
                y_copy(chunk, k, m).wait_send()
                second_copy(chunk, k, m).wait_send()
    for b in range(ns):
        @pl.when(jnp.logical_and(b <= at.z, at.z < ns - 1))
        def _():
            to_right(b).wait_send()

        @pl.when(jnp.logical_and(b >= at.z, at.z > 0))
        def _():
            to_left(b).wait_send()


def front_all(sizes, frames, vec, aw, ew, cw):
    nd, nf, ns = sizes
    nh = nd // 2
    rows, width = frames.shape
    shard, full = ew.shape
    deep = cw.shape[0]
    every = rows * ns
    dma = pltpu.SemaphoreType.DMA
    anywhere = pl.BlockSpec(memory_space=pl.ANY)
    return pl.pallas_call(
        functools.partial(front_kernel, sizes),
        out_shape=(
            jax.ShapeDtypeStruct((4, width, width), BF),
            jax.ShapeDtypeStruct((width, full), BF),
            jax.ShapeDtypeStruct((deep * nf, width), BF),
            jax.ShapeDtypeStruct((16, width), F32),
            jax.ShapeDtypeStruct((width, every), BF),
            jax.ShapeDtypeStruct((rows, width), BF),
            jax.ShapeDtypeStruct((every, width), BF),
            jax.ShapeDtypeStruct((every, width), BF),
            jax.ShapeDtypeStruct((rows, width), F32),
            jax.ShapeDtypeStruct((width // 128, rows, 128), F32),
        ),
        in_specs=[vmem(), vmem(), anywhere, anywhere, anywhere],
        out_specs=(anywhere, anywhere, anywhere, vmem()) + (anywhere,) * 5 + (vmem(),),
        scratch_shapes=[
            pltpu.VMEM((4, width, width), BF),
            pltpu.VMEM((nf, 16, vec.shape[1]), BF),
            pltpu.VMEM((every, width), BF),
            pltpu.VMEM((width, every), BF),
            pltpu.VMEM((rows, width), BF),
            pltpu.VMEM((every, width), BF),
            pltpu.VMEM((every, width), BF),
            pltpu.VMEM((rows, width), F32),
            pltpu.VMEM((4, shard, width), F32),
            pltpu.VMEM((shard, full), F32),
            pltpu.VMEM((shard, full), BF),
            pltpu.VMEM((deep, width), BF),
            pltpu.VMEM((ns - 1, width // 64, rows, rows), F32),
            pltpu.VMEM((ns - 1, width // 128, rows, 128), F32),
            dma((12,)),
            dma((4, nf)), dma((4, nf)),
            dma((4, nf, nh)), dma((4, nf, nh)),
            dma((4, nf)), dma((4, nf)),
            dma((4, nf, nh)), dma((4, nf, nh)),
            dma((nf,)), dma((nf,)),
            dma((ns,)), dma((ns,)), dma((ns,)),
        ],
        name="front",
        compiler_params=pltpu.CompilerParams(
            collective_id=0, has_side_effects=True, vmem_limit_bytes=67043328
        ),
    )(frames, vec, aw, ew, cw.reshape(aw.shape))


def back_kernel(
    sizes, q_ref, k_ref, v_ref, dc_ref, ctx_ref, lse_ref, ht_ref, w_ref, gm_ref, frames_ref,
    vec_ref, gv_ref, gc_ref, ge_ref, go_ref,
    oc_ref, oe_ref, oa_ref, ig_ref, ov_ref,
    ga, own, rc, rx, ry, rz, ri, dkt, dvt, dqa, dhs, dra, drb, drc, vb, vx, vy, vz,
    os, cs, cr, xs, xr, ys, yr, zs, zr, zis, zir, gs, gr, ays, ayr, acs, acr,
    das, dar, dbs, dbr, dcs, dcr, vs, vr,
):
    at = Place(sizes)
    nf, nh, ns = at.nf, at.nh, at.ns
    rows, width = q_ref.shape
    q = rc.shape[5]
    cols = width // nh
    per = cols // 128
    chunks = rc.shape[0]
    split = chunks // (3 * per)
    half = q * split
    group = per * split
    b0 = lax.rem(at.z, 2)
    b1 = at.z // 2
    at.barrier()

    def strip(core, r):
        return pl.ds(pl.multiple_of(core * half + r * q, 16), q)

    def lanes(s, hi):
        return pl.ds(pl.multiple_of(hi * cols + s * 128, 128), 128)

    def place_of(n):
        return n // group, lax.rem(n, group) // split, lax.rem(n, split)

    for s in range(per):
        for hi in range(nh):
            for part in range(2):
                for r in range(split):
                    pltpu.make_async_copy(
                        go_ref.at[:, pl.ds(part * half + r * q, q), pl.ds(hi * cols + s * 128, 128)],
                        ga.at[s, r, hi, :, part, 1, 1],
                        os.at[4],
                    ).start()

    def own_whole(slot):
        return pltpu.make_async_copy(own.at[slot], own.at[slot], os.at[slot])

    def c_whole(n):
        return remote(rc.at[n], rc.at[n], cs.at[n], cr.at[n], at.sibling())

    def c_send(n):
        slot = lax.rem(n, 4)
        g, s, r = place_of(n)

        @pl.when(n < group)
        def _():
            for hi in range(nh):
                for u in range(4):
                    block = lanes(s, hi)
                    remote(
                        gc_ref.at[:, u, strip(1 - at.core, r), block],
                        rc.at[n, hi, :, u // 2, u % 2], cs.at[n], cr.at[n], at.sibling(),
                    ).start()
                    pltpu.make_async_copy(
                        gc_ref.at[:, u, strip(at.core, r), block],
                        own.at[slot, hi, :, u // 2, u % 2], os.at[slot],
                    ).start()

        @pl.when(jnp.logical_and(n >= group, n < 2 * group))
        def _():
            for hi in range(nh):
                for u in range(4):
                    block = pl.ds(pl.multiple_of(u * width + hi * cols + s * 128, 128), 128)
                    remote(
                        ge_ref.at[:, strip(1 - at.core, r), block],
                        rc.at[n, hi, :, u // 2, u % 2], cs.at[n], cr.at[n], at.sibling(),
                    ).start()
                    pltpu.make_async_copy(
                        ge_ref.at[:, strip(at.core, r), block],
                        own.at[slot, hi, :, u // 2, u % 2], os.at[slot],
                    ).start()

        @pl.when(jnp.logical_and(n >= 2 * group, n < chunks))
        def _():
            remote(
                ga.at[s, r, :, :, 1 - at.core], rc.at[n], cs.at[n], cr.at[n], at.sibling()
            ).start()

    def x_copy(n, k):
        peer = lax.rem(at.x + k, nf)
        return remote(rc.at[n, :, peer], rx.at[n, k - 1], xs.at[n, k - 1], xr.at[n, k - 1], at.x_peer(k))

    def y_copy(n, m):
        return remote(
            rx.at[n, 0, at.y_hi(m)], ry.at[n, m - 1], ys.at[n, m - 1], yr.at[n, m - 1], at.y_peer(m)
        )

    assert ns == 4
    outer = b0 == b1
    inner = b0 != b1
    near = {"seq": at.z + 1 - 2 * b0}
    across = {"seq": 3 - at.z}

    def z_copy(n):
        return remote(ry.at[n, 0], rz.at[n], zs.at[n], zr.at[n], near)

    def zi_copy(n):
        return remote(ry.at[n, 0], ri.at[n], zis.at[n], zir.at[n], across)

    def by_group(n, act):
        g, s, r = place_of(n)

        for which in range(3):
            @pl.when(g == which)
            def _(which=which):
                def place(hi, ua, ub):
                    if which == 1:
                        start = (2 * ua + ub) * width + hi * cols + s * 128
                        return oe_ref.at[strip(at.core, r), pl.ds(pl.multiple_of(start, 128), 128)]
                    ref = oc_ref if which == 0 else oa_ref
                    return ref.at[ua, ub, strip(at.core, r), lanes(s, hi)]

                act(place)

    def g_whole(n):
        return remote(ry.at[n, 0], ry.at[n, 0], gs.at[n], gr.at[n], near)

    def ay_whole(n, m):
        return remote(ry.at[n, 0], ry.at[n, 0], ays.at[n, m - 1], ayr.at[n, m - 1], at.y_peer(m))

    def ac_whole(n):
        return remote(rx.at[n, 0], rx.at[n, 0], acs.at[n], acr.at[n], at.sibling())

    def g_start(n, total):
        def act(place):
            for u in range(4):
                spot = place(at.hi, u // 2, u % 2)
                spot[...] = total[u // 2, u % 2]
                remote(spot, spot, gs.at[n], gr.at[n], near).start()

        by_group(n, act)

    def ay_start(n):
        def act(place):
            for m in range(1, nh):
                for u in range(4):
                    spot = place(at.hi, u // 2, u % 2)
                    remote(spot, spot, ays.at[n, m - 1], ayr.at[n, m - 1], at.y_peer(m)).start()

        by_group(n, act)

    def ac_start(n):
        def act(place):
            for hi in range(nh):
                for u in range(4):
                    spot = place(hi, u // 2, u % 2)
                    remote(spot, spot, acs.at[n], acr.at[n], at.sibling()).start()

        by_group(n, act)

    def plus(left, right):
        if nf == 2:
            return left + right
        return (left.astype(F32) + right.astype(F32)).astype(BF)

    def stage_c(n):
        c_whole(n).wait_recv()
        slot = lax.rem(n, 4)
        _, s, r = place_of(n)

        @pl.when(n < 2 * group)
        def _():
            own_whole(slot).wait()

            def add(i, carry):
                hi, j = i // nf, lax.rem(i, nf)
                rc[n, hi, j] = plus(rc[n, hi, j], own[slot, hi, j])
                return carry

            lax.fori_loop(0, nh * nf, add, 0)

        @pl.when(n >= 2 * group)
        def _():
            def add(i, carry):
                hi, j = i // nf, lax.rem(i, nf)
                rc[n, hi, j] = plus(rc[n, hi, j], ga[s, r, hi, j, at.core])
                return carry

            lax.fori_loop(0, nh * nf, add, 0)

        for k in range(1, nf):
            x_copy(n, k).start()

    def stage_x(n):
        for k in range(1, nf):
            x_copy(n, k).wait_recv()

        def add(hi, carry):
            if nf == 2:
                rx[n, 0, hi] = rc[n, hi, at.x] + rx[n, 0, hi]
            else:
                total = rc[n, hi, at.x].astype(F32)
                for k in range(nf - 1):
                    total += rx[n, k, hi].astype(F32)
                rx[n, 0, hi] = total.astype(BF)
            return carry

        lax.fori_loop(0, nh, add, 0)
        for m in range(1, nh):
            y_copy(n, m).start()

    def stage_y(n):
        for m in range(1, nh):
            y_copy(n, m).wait_recv()
        total = rx[n, 0, at.hi]
        for m in range(nh - 1):
            total = plus(total, ry[n, m])
        ry[n, 0] = total

        @pl.when(outer)
        def _():
            z_copy(n).start()

    def stage_z(n):
        @pl.when(inner)
        def _():
            z_copy(n).wait_recv()
            ry[n, 0] = plus(ry[n, 0], rz[n])
            zi_copy(n).start()

    def stage_zi(n):
        @pl.when(inner)
        def _():
            zi_copy(n).wait_recv()
            g_start(n, plus(ry[n, 0], ri[n]))

    def stage_g(n):
        @pl.when(outer)
        def _():
            g_whole(n).wait_recv()

        ay_start(n)

    def stage_ay(n):
        for m in range(1, nh):
            ay_whole(n, m).wait_recv()
        ac_start(n)

    lo = lax.broadcasted_iota(jnp.int32, (rows, 128), 1) < 64
    pairs = width // 128

    def unit(index):
        i, p = index // pairs, lax.rem(index, pairs)
        there = 1 - b1 - i + 2 * i * b1
        keys = pl.ds(pl.multiple_of(there * (2 * rows), 128), 2 * rows)
        col = pl.ds(pl.multiple_of(p * 128, 128), 128)
        k2 = k_ref[keys, col]
        v2 = v_ref[keys, col]
        q2 = q_ref[:, col]
        dc2 = dc_ref[:, col]
        both = dc2.astype(F32) * ctx_ref[:, col]
        lse2 = lse_ref[p]
        dq, dk, dv = [], None, None
        for h in range(2):
            mask = lo if h == 0 else jnp.logical_not(lo)
            qm = jnp.where(mask, q2, jnp.zeros_like(q2))
            dmask = jnp.where(mask, dc2, jnp.zeros_like(q2))
            lse = lse2[:, 0:1] if h == 0 else lse2[:, 64:65]
            dot = jnp.sum(jnp.where(mask, both, 0.0), axis=-1, keepdims=True)
            probs = jnp.exp(nt(qm, k2) * score_scale - lse)
            slopes = nt(dmask, v2)
            dscore = (probs * (slopes - dot) * score_scale).astype(BF)
            dq.append(nn(dscore, k2))
            a = nn(dmask.T, probs.astype(BF))
            b = nn(qm.T, dscore)
            dv = a if dv is None else dv + a
            dk = b if dk is None else dk + b
        dq2 = jnp.where(lo, dq[0], dq[1])

        @pl.when(i == 0)
        def _():
            dqa[:, col] = dq2

        @pl.when(i > 0)
        def _():
            dqa[:, col] += dq2

        dkt[col, keys] = dk.astype(BF)
        dvt[col, keys] = dv.astype(BF)

    def weights(s):
        frames = pl.ds(pl.multiple_of(at.z * rows, 128), rows)
        for hi in range(nh):
            col = lanes(s, hi)
            dq2 = dqa[:, col]
            vb[2, 0:1, col] = jnp.sum(dq2, axis=0, keepdims=True)
            dq2 = dq2.astype(BF)
            dk2 = dkt[col, :]
            dv2 = dvt[col, :]
            for j in range(nf):
                for part in range(2):
                    for r in range(split):
                        here = pl.ds((2 * j + part) * half + r * q, q)
                        ga[s, r, hi, j, part, 0, 0] = nn(ht_ref[here, frames], dq2).astype(BF)
                        ga[s, r, hi, j, part, 0, 1] = nt(ht_ref[here, :], dk2).astype(BF)
                        ga[s, r, hi, j, part, 1, 0] = nt(ht_ref[here, :], dv2).astype(BF)

    pieces = 16
    per_step = 2
    lag = 2
    low = 1 - b1

    def part_of(t):
        return pl.ds(pl.multiple_of(t * (width // pieces), 16), width // pieces)

    def da_copy(t):
        return remote(
            dhs.at[pl.ds(low, 3), part_of(t)], dra.at[:, part_of(t)], das.at[t], dar.at[t], near
        )

    def db_copy(t):
        return remote(
            dhs.at[pl.ds(2 * low, 2), part_of(t)], drb.at[:, part_of(t)], dbs.at[t], dbr.at[t], across
        )

    def dc_copy(t):
        return remote(dhs.at[3 * b1, part_of(t)], drc.at[part_of(t)], dcs.at[t], dcr.at[t], near)

    def d_stage(i, t):
        part = part_of(t)
        if i == 0:
            @pl.when(outer)
            def _():
                da_copy(t).start()
        elif i == 1:
            @pl.when(inner)
            def _():
                da_copy(t).wait_recv()
                for j in range(3):
                    dhs[low + j, part] = dhs[low + j, part] + dra[j, part]
                db_copy(t).start()
        elif i == 2:
            @pl.when(inner)
            def _():
                db_copy(t).wait_recv()
                for j in range(2):
                    dhs[2 * b1 + j, part] = dhs[2 * b1 + j, part] + drb[j, part]
                dc_copy(t).start()
        else:
            @pl.when(outer)
            def _():
                dc_copy(t).wait_recv()

    def spread(i):
        there = 1 - b1 - i + 2 * i * b1
        for ub in range(2):
            part = pl.ds(pl.multiple_of((2 * there + ub) * rows, 128), rows)
            dhs[2 * there + ub] = (nn(w_ref[1], dkt[:, part]) + nn(w_ref[2], dvt[:, part])).astype(BF)

    def first_norm():
        @pl.when(inner)
        def _():
            drc[...] = jnp.zeros_like(drc)

        total = dhs[at.z].astype(F32) + nt(w_ref[0], dqa[...].astype(BF))
        total += drc[...].astype(F32)
        total = total.T
        normed, inverse = normalize(frames_ref[...])
        scaled = total * vec_ref[0:1, :]
        centred = (
            scaled
            - jnp.mean(scaled, axis=-1, keepdims=True)
            - normed * jnp.mean(scaled * normed, axis=-1, keepdims=True)
        )
        ig_ref[...] = gm_ref[...] + inverse * centred
        vb[1] = gv_ref[...]
        vb[1, 0:1, :] = jnp.sum(total * normed, axis=0, keepdims=True)
        vb[1, 1:2, :] = jnp.sum(total, axis=0, keepdims=True)
        vb[1, 2:3, :] = vb[2, 0:1, :]

    def v_core():
        return remote(vb.at[1], vb.at[0], vs.at[0], vr.at[0], at.sibling())

    def v_x(k):
        return remote(vx.at[at.x], vx.at[at.x], vs.at[k], vr.at[k], at.x_peer(k))

    def v_y(m):
        return remote(vy.at[at.hi], vy.at[at.hi], vs.at[nf + m], vr.at[nf + m], at.y_peer(m))

    def v_z(k):
        return remote(
            vz.at[at.z], vz.at[at.z], vs.at[nf + nh + k], vr.at[nf + nh + k], at.z_peer(k)
        )

    def v_step(i):
        if i == 0:
            v_core().start()
        elif i == 1:
            v_core().wait_recv()
            vx[at.x] = vb[0] + vb[1]
            for k in range(1, nf):
                v_x(k).start()
        elif i == 2:
            for k in range(1, nf):
                v_x(k).wait_recv()
            total = vx[0]
            for j in range(1, nf):
                total += vx[j]
            vy[at.hi] = total
            for m in range(1, nh):
                v_y(m).start()
        elif i == 3:
            for m in range(1, nh):
                v_y(m).wait_recv()
            total = vy[0]
            for j in range(1, nh):
                total += vy[j]
            vz[at.z] = total
            for k in range(1, ns):
                v_z(k).start()
        else:
            for k in range(1, ns):
                v_z(k).wait_recv()
            total = vz[0]
            for j in range(1, ns):
                total += vz[j]
            ov_ref[...] = total

    ready = group
    each = -(-2 * pairs // ready)
    done = [-(-pairs * (i + 1) // each) - 1 for i in range(2)]
    away = done[1] + 1
    norm = max(away + (pieces - 1) // per_step + 4, chunks - 2)
    stages = (stage_x, stage_y, stage_z, stage_zi, stage_g, stage_ay)
    last = max(chunks + lag * len(stages), norm + 6)
    for n in range(4):
        c_send(n)

    def step(n, carry):
        for k in range(2):
            @pl.when(2 * n + k < 2 * group)
            def _(k=k):
                stage_c(2 * n + k)

                @pl.when(2 * n + k + 4 < 2 * group)
                def _():
                    c_send(2 * n + k + 4)

        @pl.when(jnp.logical_and(n >= ready + 1, n < ready + 1 + per))
        def _():
            for r in range(split):
                stage_c(2 * group + (n - ready - 1) * split + r)

        @pl.when(n < ready)
        def _():
            def one(k, carry):
                @pl.when(n * each + k < 2 * pairs)
                def _():
                    unit(n * each + k)

                return carry

            lax.fori_loop(0, each, one, 0)

        @pl.when(jnp.logical_or(n == done[0], n == done[1]))
        def _():
            spread(n // done[1])

        @pl.when(n == norm)
        def _():
            first_norm()

        @pl.when(n == ready)
        def _():
            whole = ga.at[:, :, :, :, :, 1, 1]
            pltpu.make_async_copy(whole, whole, os.at[4]).wait()

        @pl.when(jnp.logical_and(n >= ready, n < ready + per))
        def _():
            weights(n - ready)
            for r in range(split):
                c_send(2 * group + (n - ready) * split + r)

        for i, stage in enumerate(stages):
            @pl.when(jnp.logical_and(n >= lag * i, n < chunks + lag * i))
            def _(i=i, stage=stage):
                stage(n - lag * i)

        for i in range(4):
            first = away + i

            @pl.when(jnp.logical_and(n >= first, n < first + pieces // per_step))
            def _(i=i, first=first):
                for t in range(per_step):
                    d_stage(i, (n - first) * per_step + t)

        for i in range(5):
            @pl.when(n == norm + i)
            def _(i=i):
                v_step(i)

        return carry

    lax.fori_loop(0, last, step, 0)
    for n in range(chunks):
        ac_whole(n).wait()

    def drain(n, carry):
        c_whole(n).wait_send()

        @pl.when(outer)
        def _():
            z_copy(n).wait_send()

        @pl.when(inner)
        def _():
            zi_copy(n).wait_send()
            g_whole(n).wait_send()

        for k in range(1, nf):
            x_copy(n, k).wait_send()
        for m in range(1, nh):
            y_copy(n, m).wait_send()
            ay_whole(n, m).wait_send()
        return carry

    lax.fori_loop(0, chunks, drain, 0)

    @pl.when(outer)
    def _():
        def sent(t, carry):
            da_copy(t).wait_send()
            return carry

        lax.fori_loop(0, pieces, sent, 0)

    @pl.when(inner)
    def _():
        def sent(t, carry):
            db_copy(t).wait_send()
            dc_copy(t).wait_send()
            return carry

        lax.fori_loop(0, pieces, sent, 0)

    for k in range(1, ns):
        v_z(k).wait_send()
    for k in range(1, nf):
        v_x(k).wait_send()
    for m in range(1, nh):
        v_y(m).wait_send()
    v_core().wait_send()


def back_all(sizes, q, k, v, dc, ctx, lse, ht, w, gm, frames, vec, gv, gc, ge, go):
    nd, nf, ns = sizes
    nh = nd // 2
    rows, width = q.shape
    shard = go.shape[1]
    half = shard // 2
    every = k.shape[0]
    split = 2 if half % 32 == 0 else 1
    strip = half // split
    per = width // nh // 128
    chunks = 3 * per * split
    xn, yn = max(nf - 1, 1), max(nh - 1, 1)
    dma = pltpu.SemaphoreType.DMA
    anywhere = pl.BlockSpec(memory_space=pl.ANY)
    return pl.pallas_call(
        functools.partial(back_kernel, sizes),
        out_shape=(
            jax.ShapeDtypeStruct((2, 2, shard, width), BF),
            jax.ShapeDtypeStruct((shard, 4 * width), BF),
            jax.ShapeDtypeStruct((2, 2, shard, width), BF),
            jax.ShapeDtypeStruct((rows, width), F32),
            jax.ShapeDtypeStruct((16, width), F32),
        ),
        in_specs=[vmem()] * 12 + [anywhere] * 3,
        out_specs=(vmem(),) * 5,
        scratch_shapes=[
            pltpu.VMEM((per, split, nh, nf, 2, 2, 2, strip, 128), BF),
            pltpu.VMEM((4, nh, nf, 2, 2, strip, 128), BF),
            pltpu.VMEM((chunks, nh, nf, 2, 2, strip, 128), BF),
            pltpu.VMEM((chunks, xn, nh, 2, 2, strip, 128), BF),
            pltpu.VMEM((chunks, yn, 2, 2, strip, 128), BF),
            pltpu.VMEM((chunks, 2, 2, strip, 128), BF),
            pltpu.VMEM((chunks, 2, 2, strip, 128), BF),
            pltpu.VMEM((width, every), BF),
            pltpu.VMEM((width, every), BF),
            pltpu.VMEM((rows, width), F32),
            pltpu.VMEM((ns, width, rows), BF),
            pltpu.VMEM((3, width, rows), BF),
            pltpu.VMEM((2, width, rows), BF),
            pltpu.VMEM((width, rows), BF),
            pltpu.VMEM((3, 16, width), F32),
            pltpu.VMEM((nf, 16, width), F32),
            pltpu.VMEM((nh, 16, width), F32),
            pltpu.VMEM((ns, 16, width), F32),
            dma((5,)),
            dma((chunks,)), dma((chunks,)),
            dma((chunks, xn)), dma((chunks, xn)),
            dma((chunks, yn)), dma((chunks, yn)),
            dma((chunks,)), dma((chunks,)),
            dma((chunks,)), dma((chunks,)),
            dma((chunks,)), dma((chunks,)),
            dma((chunks, yn)), dma((chunks, yn)),
            dma((chunks,)), dma((chunks,)),
            dma((16,)), dma((16,)),
            dma((16,)), dma((16,)),
            dma((16,)), dma((16,)),
            dma((nf + nh + ns,)), dma((nf + nh + ns,)),
        ],
        name="back",
        compiler_params=pltpu.CompilerParams(
            collective_id=1, has_side_effects=True, vmem_limit_bytes=67043328
        ),
    )(q, k, v, dc, ctx, lse, ht, w, gm, frames, vec, gv, gc, ge, go)


def feed_kernel(
    ctx_ref, frames_ref, cot_ref, vec_ref, wo_ref, win_ref, wout_ref,
    fo_ref, gm_ref, dc_ref, gi_ref, gout_ref, go_ref, gv_ref,
    mid, h2, h2t, dyb, acc, dh2,
):
    b = pl.program_id(0)

    @pl.when(b == 0)
    def _():
        middle = frames_ref[...] + nn(ctx_ref[...].astype(BF), wo_ref[...]) + vec_ref[4:5, :]
        mid[...] = middle
        normed, _ = normalize(middle)
        hidden = (normed * vec_ref[5:6, :] + vec_ref[6:7, :]).astype(BF)
        h2[...] = hidden
        h2t[...] = hidden.T
        dyb[...] = cot_ref[...].astype(BF)
        acc[...] = middle + vec_ref[7:8, :]
        dh2[...] = jnp.zeros_like(dh2)
        gv_ref[...] = jnp.zeros_like(gv_ref)

    up = dyb[...]
    u = nn(h2[...], win_ref[...]) + vec_ref[pl.ds(8 + b, 1), :]
    phi = 0.5 * (1.0 + lax.erf(u * 0.7071067811865476))
    activated = (u * phi).astype(BF)
    acc[...] += nn(activated, wout_ref[...])
    gout_ref[...] = tn(activated, up).astype(BF)
    du = nt(up, wout_ref[...]) * (phi + u * jnp.exp(-0.5 * u * u) * 0.3989422804014327)
    gv_ref[pl.ds(8 + b, 1), :] = jnp.sum(du, axis=0, keepdims=True)
    dub = du.astype(BF)
    gi_ref[...] = nn(h2t[...], dub).astype(BF)
    dh2[...] += nt(dub, win_ref[...])

    @pl.when(b == pl.num_programs(0) - 1)
    def _():
        fo_ref[...] = acc[...]
        normed, inverse = normalize(mid[...])
        back, gain, offset = norm_back(dh2[...], normed, inverse, vec_ref[5:6, :])
        upstream = cot_ref[...]
        middle = upstream + back
        gm_ref[...] = middle
        dab = middle.astype(BF)
        go_ref[...] = tn(ctx_ref[...].astype(BF), dab).astype(BF)
        dctx = nt(dab, wo_ref[...]).astype(BF)
        dc_ref[...] = dctx
        gv_ref[3:4, :] = jnp.sum(dctx.astype(F32), axis=0, keepdims=True)
        gv_ref[4:5, :] = jnp.sum(middle, axis=0, keepdims=True)
        gv_ref[5:6, :] = gain[None]
        gv_ref[6:7, :] = offset[None]
        gv_ref[7:8, :] = jnp.sum(upstream, axis=0, keepdims=True)


def feed_all(ctx, frames, cot, vec, aw, ew, cw):
    rows, width = frames.shape
    full = ew.shape[1]
    whole = lambda shape: pl.BlockSpec(shape, lambda b: (0,) * len(shape))
    blocks = full // width
    return pl.pallas_call(
        feed_kernel,
        grid=(blocks,),
        out_shape=(
            jax.ShapeDtypeStruct((rows, width), F32),
            jax.ShapeDtypeStruct((rows, width), F32),
            jax.ShapeDtypeStruct((rows, width), BF),
            jax.ShapeDtypeStruct((width, full), BF),
            jax.ShapeDtypeStruct((full, width), BF),
            jax.ShapeDtypeStruct((width, width), BF),
            jax.ShapeDtypeStruct((16, width), F32),
        ),
        in_specs=[
            whole((rows, width)), whole((rows, width)), whole((rows, width)), whole((16, width)),
            pl.BlockSpec((None, width, width), lambda b: (3, 0, 0)),
            pl.BlockSpec((width, width), lambda b: (0, b)),
            pl.BlockSpec((width, width), lambda b: (b, 0)),
        ],
        out_specs=(
            whole((rows, width)), whole((rows, width)), whole((rows, width)),
            pl.BlockSpec((width, width), lambda b: (0, b)),
            pl.BlockSpec((width, width), lambda b: (b, 0)),
            whole((width, width)), whole((16, width)),
        ),
        scratch_shapes=[
            pltpu.VMEM((rows, width), F32),
            pltpu.VMEM((rows, width), BF),
            pltpu.VMEM((width, rows), BF),
            pltpu.VMEM((rows, width), BF),
            pltpu.VMEM((rows, width), F32),
            pltpu.VMEM((rows, width), F32),
        ],
        name="feed",
        compiler_params=pltpu.CompilerParams(vmem_limit_bytes=67043328),
    )(ctx, frames, cot, vec, aw, ew, cw)


def on_device(
    sizes,
    frames_in,
    cotangent,
    attention_weight,
    expand_weight,
    contract_weight,
    vectors,
    first_attention,
    first_expand,
    first_contract,
    first_vectors,
    second_attention,
    second_expand,
    second_contract,
    second_vectors,
):
    nd, nf, ns = sizes
    frames = frames_in[0]
    upstream = cotangent[0]
    rows, width = frames.shape
    shard = attention_weight.shape[1]
    full = expand_weight.shape[1]
    aw, ew, cw, vec, h_turned, queries, key_rows, value_rows, context_wide, log_total = front_all(
        sizes, frames, vectors, attention_weight, expand_weight, contract_weight
    )
    frames_out, grad_middle, grad_context, grad_expand, grad_contract, grad_output_w, gv = feed_all(
        context_wide, frames, upstream, vec, aw, ew, cw
    )
    oc, oe, oa, input_gradient, gv_sum = back_all(
        sizes,
        queries,
        key_rows,
        value_rows,
        grad_context,
        context_wide,
        log_total,
        h_turned,
        aw,
        grad_middle,
        frames,
        vec,
        gv,
        grad_contract.reshape(nf, 4, shard, width),
        grad_expand.reshape(nf, shard, full),
        grad_output_w.reshape(nf, shard, width),
    )
    owned_vec = lax.dynamic_slice_in_dim(
        gv_sum[:12], lax.axis_index("fsdp") * (width // nf), width // nf, 1
    )
    owned = (
        oa.reshape(4, shard, width).astype(F32),
        oe.astype(F32),
        oc.reshape(4 * shard, width).astype(F32),
    )
    attention_out = (owned[0],) + adam_update(
        attention_weight, owned[0], first_attention, second_attention, rate_matrix, decay_matrix
    )
    expand_out = (owned[1],) + adam_update(
        expand_weight, owned[1], first_expand, second_expand, rate_matrix, decay_matrix
    )
    contract_out = (owned[2],) + adam_update(
        contract_weight, owned[2], first_contract, second_contract, rate_matrix, decay_matrix
    )
    vector_out = (owned_vec,) + adam_update(
        vectors, owned_vec, first_vectors, second_vectors, rate_vector, 0.0
    )
    result = [frames_out[None], input_gradient[None]]
    for i in range(4):
        result += [attention_out[i], expand_out[i], contract_out[i], vector_out[i]]
    return tuple(result)


def solution(mesh):
    sizes = (mesh.shape["dp"], mesh.shape["fsdp"], mesh.shape["seq"])
    data = P(("dp", "fsdp"), "seq", None)
    state = (P(None, "fsdp", None), P("fsdp", None), P("fsdp", None), P(None, "fsdp"))
    return jax.shard_map(
        functools.partial(on_device, sizes),
        mesh=mesh,
        in_specs=(data, data) + state * 3,
        out_specs=(data, data) + state * 4,
        check_vma=False,
    )
```

```python
import functools

import jax
import jax.numpy as jnp
from jax import lax
from jax.experimental import pallas as pl
from jax.experimental.pallas import tpu as pltpu
from jax.sharding import PartitionSpec as P

HEADS = 12
norm_eps = 1e-05
beta_one = 0.9
beta_two = 0.999
adam_eps = 1e-08
adam_count = 5.0
rate_matrix = 0.02
rate_vector = 0.1
decay_matrix = 0.1
score_scale = 0.125
VMEM_LIMIT = 60 << 20
MESH = pl.DeviceIdType.MESH
BF = jnp.bfloat16
F32 = jnp.float32


def nt(left, right):
    return lax.dot_general(left, right, (((1,), (1,)), ((), ())), preferred_element_type=F32)


def nn(left, right):
    return lax.dot_general(left, right, (((1,), (0,)), ((), ())), preferred_element_type=F32)


def tn(left, right):
    return lax.dot_general(left, right, (((0,), (0,)), ((), ())), preferred_element_type=F32)


def vmem():
    return pl.BlockSpec(memory_space=pltpu.VMEM)


def normalize(values):
    center = values - jnp.mean(values, axis=-1, keepdims=True)
    inverse = lax.rsqrt(jnp.mean(center * center, axis=-1, keepdims=True) + norm_eps)
    return center * inverse, inverse


def norm_back(upstream, normed, inverse, gain):
    scaled = upstream * gain
    inner = (
        scaled
        - jnp.mean(scaled, axis=-1, keepdims=True)
        - normed * jnp.mean(scaled * normed, axis=-1, keepdims=True)
    )
    return (inverse * inner, jnp.sum(upstream * normed, axis=0), jnp.sum(upstream, axis=0))


def adam_update(weight, gradient, first, second, rate, decay):
    first_new = beta_one * first + (1.0 - beta_one) * gradient
    second_new = beta_two * second + (1.0 - beta_two) * gradient * gradient
    first_hat = first_new / (1.0 - beta_one**adam_count)
    second_hat = second_new / (1.0 - beta_two**adam_count)
    updated = weight - rate * (first_hat / (jnp.sqrt(second_hat) + adam_eps) + decay * weight)
    return (updated, first_new, second_new)


class Place:
    def __init__(self, sizes):
        self.nd, self.nf, self.ns = sizes
        self.nh = self.nd // 2
        self.dp = lax.axis_index("dp")
        self.x = lax.axis_index("fsdp")
        self.z = lax.axis_index("seq")
        self.core = lax.rem(self.dp, 2)
        self.hi = self.dp // 2

    def sibling(self):
        return {"dp": self.hi * 2 + 1 - self.core}

    def x_peer(self, k):
        return {"fsdp": lax.rem(self.x + k, self.nf)}

    def y_hi(self, k):
        return lax.rem(self.hi + k, self.nh)

    def y_peer(self, k):
        return {"dp": self.y_hi(k) * 2 + self.core}

    def z_at(self, k):
        return lax.rem(self.z + k + self.ns, self.ns)

    def z_peer(self, k):
        return {"seq": self.z_at(k)}

    def everyone(self):
        out = [self.sibling()]
        out += [self.x_peer(k) for k in range(1, self.nf)]
        out += [self.y_peer(k) for k in range(1, self.nh)]
        out += [self.z_peer(k) for k in range(1, self.ns)]
        return out

    def barrier(self):
        sem = pltpu.get_barrier_semaphore()
        peers = self.everyone()
        for peer in peers:
            pl.semaphore_signal(sem, inc=1, device_id=peer, device_id_type=MESH)
        pl.semaphore_wait(sem, len(peers))


def remote(src, dst, send, recv, peer):
    return pltpu.make_async_remote_copy(
        src_ref=src, dst_ref=dst, send_sem=send, recv_sem=recv, device_id=peer, device_id_type=MESH
    )


def front_kernel(
    sizes, frames_ref, vec_ref, aw_ref, ew_ref, cw_ref,
    a_out, e_ref, c_ref, vec_out, ht_out, q_out, k_out, v_out, ctx_out, lse_ref,
    a_ref, v_buf, h_ref, ht, q_buf, k_buf, v_buf2, ctx_buf, af, ef, eb, cb, kept, stat,
    ls, xs, xr, ys, yr, s1s, s1r, s2s, s2r, vs, vr, rs, hs, hr,
):
    at = Place(sizes)
    nf, nh, ns = at.nf, at.nh, at.ns
    rows, width = frames_ref.shape
    shard = aw_ref.shape[1]
    half = shard // 2
    deep = cb.shape[0]
    b0 = lax.rem(at.z, 2)
    b1 = at.z // 2

    def load(i, src, dst):
        return pltpu.make_async_copy(src, dst, ls.at[i])

    loads = [
        load(0, aw_ref.at[pl.ds(0, 3)], af.at[pl.ds(0, 3)]),
        load(1, aw_ref.at[pl.ds(3, 1)], af.at[pl.ds(3, 1)]),
        load(2, ew_ref, ef),
        load(3, cw_ref, af),
    ]
    for copy in loads[:3]:
        copy.start()
    at.barrier()
    v_buf[at.x] = jnp.zeros(v_buf.shape[1:], BF)
    v_buf[at.x, 0 : vec_ref.shape[0], :] = vec_ref[...].astype(BF)
    vec_copies = []
    for k in range(1, nf):
        copy = remote(v_buf.at[at.x], v_buf.at[at.x], vs.at[k], vr.at[k], at.x_peer(k))
        copy.start()
        vec_copies.append(copy)

    order = (1, 2, 0, 3)

    def view(chunk, j, hi, core, own=False):
        cols = width // nh
        if chunk < 4:
            return a_ref.at[
                order[chunk],
                pl.ds(pl.multiple_of(j * shard + core * half, 16), half),
                pl.ds(pl.multiple_of(hi * cols, 128), cols),
            ]
        if chunk < 8:
            start = 0 if own else j * shard
            wide = eb.shape[1] // nh
            return (eb if own else e_ref).at[
                pl.ds(pl.multiple_of(start + core * half, 16), half),
                pl.ds(pl.multiple_of(hi * wide + (chunk - 4) * (wide // 4), 128), wide // 4),
            ]
        start = 0 if own else j * deep
        tall = deep // 8
        return (cb if own else c_ref).at[
            pl.ds(pl.multiple_of(start + core * (deep // 2) + (chunk - 8) * tall, 16), tall),
            pl.ds(pl.multiple_of(hi * cols, 128), cols),
        ]

    own = pl.multiple_of(at.x * shard, 16)
    x_copies = {}

    def send_chunk(chunk):
        for k in range(1, nf):
            copy = remote(
                view(chunk, at.x, at.hi, at.core, True), view(chunk, at.x, at.hi, at.core),
                xs.at[chunk, k - 1], xr.at[chunk, k - 1], at.x_peer(k),
            )
            copy.start()
            x_copies[chunk, k] = copy

    loads[0].wait()
    for i, u in enumerate(order[:3]):
        a_ref[u, pl.ds(own, shard), :] = af[u].astype(BF)
        send_chunk(i)
    normed, _ = normalize(frames_ref[...])
    for copy in vec_copies:
        copy.wait()
    vec = jnp.concatenate([v_buf[j] for j in range(nf)], axis=1).astype(F32)
    vec_out[...] = vec
    mine = pl.ds(pl.multiple_of(at.z * rows, 128), rows)
    hidden = (normed * vec[0:1] + vec[1:2]).astype(BF)
    h_ref[mine, :] = hidden

    def block(b):
        return h_ref.at[pl.ds(pl.multiple_of(b * rows, 128), rows), :]

    def to_right(b):
        return remote(block(b), block(b), rs.at[b], hr.at[b], {"seq": at.z + 1})

    def to_left(b):
        return remote(block(b), block(b), hs.at[b], hr.at[b], {"seq": at.z - 1})

    @pl.when(at.z < ns - 1)
    def _():
        to_right(at.z).start()

    @pl.when(at.z > 0)
    def _():
        to_left(at.z).start()

    loads[1].wait()
    a_ref[3, pl.ds(own, shard), :] = af[3].astype(BF)
    loads[3].start()
    send_chunk(3)
    loads[2].wait()
    eb[...] = ef[...].astype(BF)
    for i in range(4, 8):
        send_chunk(i)
    loads[3].wait()
    for u in range(4):
        cb[pl.ds(u * shard, shard), :] = af[u].astype(BF)
    for i in range(8, 12):
        send_chunk(i)
    stores = [
        load(4, eb, e_ref.at[pl.ds(own, shard), :]),
        load(5, cb, c_ref.at[pl.ds(pl.multiple_of(at.x * deep, 16), deep), :]),
    ]
    for copy in stores:
        copy.start()
    ht[:, mine] = hidden.T

    def first_copy(chunk, k):
        j = lax.rem(at.x - k + nf, nf)
        piece = view(chunk, j, at.hi, at.core)
        return remote(piece, piece, s1s.at[chunk, k - 1], s1r.at[chunk, k - 1], at.sibling())

    def y_copy(chunk, k, m):
        j = lax.rem(at.x - k + nf, nf)
        piece = view(chunk, j, at.hi, at.core)
        return remote(piece, piece, ys.at[chunk, k - 1, m - 1], yr.at[chunk, k - 1, m - 1], at.y_peer(m))

    def second_copy(chunk, k, m):
        j = lax.rem(at.x - k + nf, nf)
        piece = view(chunk, j, lax.rem(at.hi - m + nh, nh), at.core)
        return remote(piece, piece, s2s.at[chunk, k - 1, m - 1], s2r.at[chunk, k - 1, m - 1], at.sibling())

    def forward(chunk):
        for k in range(1, nf):
            x_copies[chunk, k].wait_recv()
            first_copy(chunk, k).start()
            for m in range(1, nh):
                y_copy(chunk, k, m).start()

    def relay(chunk):
        for k in range(1, nf):
            for m in range(1, nh):
                y_copy(chunk, k, m).wait_recv()
                second_copy(chunk, k, m).start()

    def arrived(chunk):
        for k in range(1, nf):
            first_copy(chunk, k).wait_recv()
            for m in range(1, nh):
                second_copy(chunk, k, m).wait_recv()

    def rows_of(b):
        part = pl.ds(pl.multiple_of(b * rows, 128), rows)
        k_buf[part, :] = nn(h_ref[part, :], a_ref[1]).astype(BF)
        v_buf2[part, :] = (nn(h_ref[part, :], a_ref[2]) + vec[3:4]).astype(BF)

    def turn(b):
        part = pl.ds(pl.multiple_of(b * rows, 128), rows)
        ht[:, part] = h_ref[part, :].T

    def hop(s):
        b = at.z - s
        d = at.z + s

        @pl.when(b >= 0)
        def _():
            to_right(b).wait_recv()

            @pl.when(at.z < ns - 1)
            def _():
                to_right(b).start()

        @pl.when(d < ns)
        def _():
            to_left(d).wait_recv()

            @pl.when(at.z > 0)
            def _():
                to_left(d).start()

    lane = lax.broadcasted_iota(jnp.int32, (rows, 128), 1)
    lo = lane < 64

    def scores(p, h, b):
        col = pl.ds(pl.multiple_of(p * 128, 128), 128)
        part = pl.ds(pl.multiple_of(b * rows, 128), rows)
        q2 = q_buf[:, col]
        mask = lo if h == 0 else jnp.logical_not(lo)
        s = nt(jnp.where(mask, q2, jnp.zeros_like(q2)), k_buf[part, col]) * score_scale
        largest = jnp.max(s, axis=-1, keepdims=True)
        e = jnp.exp(s - largest)
        return e, largest, jnp.sum(e, axis=-1, keepdims=True)

    assert ns == 4
    blocks = (at.z, at.z + 1 - 2 * b0, 2 - b1, 3 - 3 * b1)

    def tick(i):
        if i < 12:
            forward(i)
        if i > 0:
            relay(i - 1)

    def begin(i, ticks):
        b = blocks[i]
        rows_of(b)

        def pair(p, carry):
            found = []
            for h in range(2):
                e, largest, total = scores(p, h, b)
                kept[i, 2 * p + h] = e
                found += [largest, total]
            stat[i, p] = jnp.where(
                lo, jnp.where(lane < 32, found[0], found[1]), jnp.where(lane < 96, found[2], found[3])
            )
            for when, which in ticks:
                @pl.when(p == when)
                def _(which=which):
                    tick(which)

            return carry

        lax.fori_loop(0, width // 128, pair, 0)

    tick(0)
    tick(1)
    tick(2)
    hop(1)
    tick(3)
    for i in range(3):
        arrived(i)
    q_buf[...] = (nn(h_ref[mine, :], a_ref[0]) + vec[2:3]).astype(BF)
    stores.append(load(6, q_buf, q_out))
    stores[-1].start()
    tick(4)
    begin(0, ((2, 5), (5, 6)))
    hop(2)
    begin(1, ((1, 7), (4, 8)))
    turn(blocks[1])
    begin(2, ((0, 9), (3, 10)))
    turn(blocks[2])
    hop(3)
    rows_of(blocks[3])
    turn(blocks[3])
    tick(11)
    arrived(3)
    for i, (src, dst) in enumerate(((a_ref, a_out), (ht, ht_out), (k_buf, k_out), (v_buf2, v_out))):
        stores.append(load(7 + i, src, dst))
        stores[-1].start()
    def pair(p, carry):
        col = pl.ds(pl.multiple_of(p * 128, 128), 128)
        ctx, lse = [], []
        for h in range(2):
            e, peak, count = scores(p, h, blocks[3])
            peaks = [stat[i, p][:, 64 * h : 64 * h + 1] for i in range(3)] + [peak]
            counts = [stat[i, p][:, 64 * h + 32 : 64 * h + 33] for i in range(3)] + [count]
            largest = functools.reduce(jnp.maximum, peaks)
            shares = [jnp.exp(each - largest) for each in peaks]
            total = sum(share * each for share, each in zip(shares, counts))
            inverse = 1.0 / total
            out = None
            for i in range(4):
                part = pl.ds(pl.multiple_of(blocks[i] * rows, 128), rows)
                found = kept[i, 2 * p + h] if i < 3 else e
                term = nn((found * (shares[i] * inverse)).astype(BF), v_buf2[part, col])
                out = term if out is None else out + term
            ctx.append(out)
            lse.append(largest + jnp.log(total))
        ctx_buf[:, col] = jnp.where(lo, ctx[0], ctx[1])
        lse_ref[p] = jnp.where(lo, lse[0], lse[1])

        @pl.when(p == 1)
        def _():
            tick(12)

        return carry

    lax.fori_loop(0, width // 128, pair, 0)
    stores.append(load(11, ctx_buf, ctx_out))
    stores[-1].start()
    for i in range(4, 12):
        arrived(i)
    for copy in stores:
        copy.wait()
    for copy in x_copies.values():
        copy.wait_send()
    for chunk in range(12):
        for k in range(1, nf):
            first_copy(chunk, k).wait_send()
            for m in range(1, nh):
                y_copy(chunk, k, m).wait_send()
                second_copy(chunk, k, m).wait_send()
    for b in range(ns):
        @pl.when(jnp.logical_and(b <= at.z, at.z < ns - 1))
        def _():
            to_right(b).wait_send()

        @pl.when(jnp.logical_and(b >= at.z, at.z > 0))
        def _():
            to_left(b).wait_send()


def front_all(sizes, frames, vec, aw, ew, cw):
    nd, nf, ns = sizes
    nh = nd // 2
    rows, width = frames.shape
    shard, full = ew.shape
    deep = cw.shape[0]
    every = rows * ns
    dma = pltpu.SemaphoreType.DMA
    anywhere = pl.BlockSpec(memory_space=pl.ANY)
    return pl.pallas_call(
        functools.partial(front_kernel, sizes),
        out_shape=(
            jax.ShapeDtypeStruct((4, width, width), BF),
            jax.ShapeDtypeStruct((width, full), BF),
            jax.ShapeDtypeStruct((deep * nf, width), BF),
            jax.ShapeDtypeStruct((16, width), F32),
            jax.ShapeDtypeStruct((width, every), BF),
            jax.ShapeDtypeStruct((rows, width), BF),
            jax.ShapeDtypeStruct((every, width), BF),
            jax.ShapeDtypeStruct((every, width), BF),
            jax.ShapeDtypeStruct((rows, width), F32),
            jax.ShapeDtypeStruct((width // 128, rows, 128), F32),
        ),
        in_specs=[vmem(), vmem(), anywhere, anywhere, anywhere],
        out_specs=(anywhere, anywhere, anywhere, vmem()) + (anywhere,) * 5 + (vmem(),),
        scratch_shapes=[
            pltpu.VMEM((4, width, width), BF),
            pltpu.VMEM((nf, 16, vec.shape[1]), BF),
            pltpu.VMEM((every, width), BF),
            pltpu.VMEM((width, every), BF),
            pltpu.VMEM((rows, width), BF),
            pltpu.VMEM((every, width), BF),
            pltpu.VMEM((every, width), BF),
            pltpu.VMEM((rows, width), F32),
            pltpu.VMEM((4, shard, width), F32),
            pltpu.VMEM((shard, full), F32),
            pltpu.VMEM((shard, full), BF),
            pltpu.VMEM((deep, width), BF),
            pltpu.VMEM((ns - 1, width // 64, rows, rows), F32),
            pltpu.VMEM((ns - 1, width // 128, rows, 128), F32),
            dma((12,)),
            dma((12, nf - 1)), dma((12, nf - 1)),
            dma((12, nf - 1, nh - 1)), dma((12, nf - 1, nh - 1)),
            dma((12, nf - 1)), dma((12, nf - 1)),
            dma((12, nf - 1, nh - 1)), dma((12, nf - 1, nh - 1)),
            dma((nf,)), dma((nf,)),
            dma((ns,)), dma((ns,)), dma((ns,)),
        ],
        name="front",
        compiler_params=pltpu.CompilerParams(
            collective_id=0, has_side_effects=True, vmem_limit_bytes=67043328
        ),
    )(frames, vec, aw, ew, cw.reshape(aw.shape))


def back_kernel(
    sizes, q_ref, k_ref, v_ref, dc_ref, ctx_ref, lse_ref, ht_ref, w_ref, gm_ref, frames_ref,
    vec_ref, gv_ref, gc_ref, ge_ref, go_ref,
    oc_ref, oe_ref, oa_ref, ig_ref, ov_ref,
    ga, own, rc, rx, ry, rz, ri, dkt, dvt, dqa, dhs, dra, drb, drc, vb, vx, vy, vz,
    os, cs, cr, xs, xr, ys, yr, zs, zr, zis, zir, gs, gr, ays, ayr, acs, acr,
    das, dar, dbs, dbr, dcs, dcr, vs, vr,
):
    at = Place(sizes)
    nf, nh, ns = at.nf, at.nh, at.ns
    rows, width = q_ref.shape
    q = rc.shape[5]
    cols = width // nh
    per = cols // 128
    chunks = rc.shape[0]
    split = chunks // (3 * per)
    half = q * split
    group = per * split
    b0 = lax.rem(at.z, 2)
    b1 = at.z // 2
    at.barrier()

    def strip(core, r):
        return pl.ds(pl.multiple_of(core * half + r * q, 16), q)

    def lanes(s, hi):
        return pl.ds(pl.multiple_of(hi * cols + s * 128, 128), 128)

    def place_of(n):
        return n // group, lax.rem(n, group) // split, lax.rem(n, split)

    for s in range(per):
        for hi in range(nh):
            for part in range(2):
                for r in range(split):
                    pltpu.make_async_copy(
                        go_ref.at[:, pl.ds(part * half + r * q, q), pl.ds(hi * cols + s * 128, 128)],
                        ga.at[s, r, hi, :, part, 1, 1],
                        os.at[4],
                    ).start()

    def own_whole(slot):
        return pltpu.make_async_copy(own.at[slot], own.at[slot], os.at[slot])

    def c_whole(n):
        return remote(rc.at[n], rc.at[n], cs.at[n], cr.at[n], at.sibling())

    def c_send(n):
        slot = lax.rem(n, 4)
        g, s, r = place_of(n)

        @pl.when(n < group)
        def _():
            for hi in range(nh):
                for u in range(4):
                    block = lanes(s, hi)
                    remote(
                        gc_ref.at[:, u, strip(1 - at.core, r), block],
                        rc.at[n, hi, :, u // 2, u % 2], cs.at[n], cr.at[n], at.sibling(),
                    ).start()
                    pltpu.make_async_copy(
                        gc_ref.at[:, u, strip(at.core, r), block],
                        own.at[slot, hi, :, u // 2, u % 2], os.at[slot],
                    ).start()

        @pl.when(jnp.logical_and(n >= group, n < 2 * group))
        def _():
            for hi in range(nh):
                for u in range(4):
                    block = pl.ds(pl.multiple_of(u * width + hi * cols + s * 128, 128), 128)
                    remote(
                        ge_ref.at[:, strip(1 - at.core, r), block],
                        rc.at[n, hi, :, u // 2, u % 2], cs.at[n], cr.at[n], at.sibling(),
                    ).start()
                    pltpu.make_async_copy(
                        ge_ref.at[:, strip(at.core, r), block],
                        own.at[slot, hi, :, u // 2, u % 2], os.at[slot],
                    ).start()

        @pl.when(jnp.logical_and(n >= 2 * group, n < chunks))
        def _():
            remote(
                ga.at[s, r, :, :, 1 - at.core], rc.at[n], cs.at[n], cr.at[n], at.sibling()
            ).start()

    def x_copy(n, k):
        peer = lax.rem(at.x + k, nf)
        return remote(rc.at[n, :, peer], rx.at[n, k - 1], xs.at[n, k - 1], xr.at[n, k - 1], at.x_peer(k))

    def y_copy(n, m):
        return remote(
            rx.at[n, 0, at.y_hi(m)], ry.at[n, m - 1], ys.at[n, m - 1], yr.at[n, m - 1], at.y_peer(m)
        )

    assert ns == 4
    outer = b0 == b1
    inner = b0 != b1
    near = {"seq": at.z + 1 - 2 * b0}
    across = {"seq": 3 - at.z}

    def z_copy(n):
        return remote(ry.at[n, 0], rz.at[n], zs.at[n], zr.at[n], near)

    def zi_copy(n):
        return remote(ry.at[n, 0], ri.at[n], zis.at[n], zir.at[n], across)

    def by_group(n, act):
        g, s, r = place_of(n)

        for which in range(3):
            @pl.when(g == which)
            def _(which=which):
                def place(hi, ua, ub):
                    if which == 1:
                        start = (2 * ua + ub) * width + hi * cols + s * 128
                        return oe_ref.at[strip(at.core, r), pl.ds(pl.multiple_of(start, 128), 128)]
                    ref = oc_ref if which == 0 else oa_ref
                    return ref.at[ua, ub, strip(at.core, r), lanes(s, hi)]

                act(place)

    def g_whole(n):
        return remote(ry.at[n, 0], ry.at[n, 0], gs.at[n], gr.at[n], near)

    def ay_whole(n, m):
        return remote(ry.at[n, 0], ry.at[n, 0], ays.at[n, m - 1], ayr.at[n, m - 1], at.y_peer(m))

    def ac_whole(n):
        return remote(rx.at[n, 0], rx.at[n, 0], acs.at[n], acr.at[n], at.sibling())

    def g_start(n, total):
        def act(place):
            for u in range(4):
                spot = place(at.hi, u // 2, u % 2)
                spot[...] = total[u // 2, u % 2]
                remote(spot, spot, gs.at[n], gr.at[n], near).start()

        by_group(n, act)

    def ay_start(n):
        def act(place):
            for m in range(1, nh):
                for u in range(4):
                    spot = place(at.hi, u // 2, u % 2)
                    remote(spot, spot, ays.at[n, m - 1], ayr.at[n, m - 1], at.y_peer(m)).start()

        by_group(n, act)

    def ac_start(n):
        def act(place):
            for hi in range(nh):
                for u in range(4):
                    spot = place(hi, u // 2, u % 2)
                    remote(spot, spot, acs.at[n], acr.at[n], at.sibling()).start()

        by_group(n, act)

    def plus(left, right):
        if nf == 2:
            return left + right
        return (left.astype(F32) + right.astype(F32)).astype(BF)

    def stage_c(n):
        c_whole(n).wait_recv()
        slot = lax.rem(n, 4)
        _, s, r = place_of(n)

        @pl.when(n < 2 * group)
        def _():
            own_whole(slot).wait()

            def add(i, carry):
                hi, j = i // nf, lax.rem(i, nf)
                rc[n, hi, j] = plus(rc[n, hi, j], own[slot, hi, j])
                return carry

            lax.fori_loop(0, nh * nf, add, 0)

        @pl.when(n >= 2 * group)
        def _():
            def add(i, carry):
                hi, j = i // nf, lax.rem(i, nf)
                rc[n, hi, j] = plus(rc[n, hi, j], ga[s, r, hi, j, at.core])
                return carry

            lax.fori_loop(0, nh * nf, add, 0)

        for k in range(1, nf):
            x_copy(n, k).start()

    def stage_x(n):
        for k in range(1, nf):
            x_copy(n, k).wait_recv()

        def add(hi, carry):
            if nf == 2:
                rx[n, 0, hi] = rc[n, hi, at.x] + rx[n, 0, hi]
            else:
                total = rc[n, hi, at.x].astype(F32)
                for k in range(nf - 1):
                    total += rx[n, k, hi].astype(F32)
                rx[n, 0, hi] = total.astype(BF)
            return carry

        lax.fori_loop(0, nh, add, 0)
        for m in range(1, nh):
            y_copy(n, m).start()

    def stage_y(n):
        for m in range(1, nh):
            y_copy(n, m).wait_recv()
        total = rx[n, 0, at.hi]
        for m in range(nh - 1):
            total = plus(total, ry[n, m])
        ry[n, 0] = total

        @pl.when(outer)
        def _():
            z_copy(n).start()

    def stage_z(n):
        @pl.when(inner)
        def _():
            z_copy(n).wait_recv()
            ry[n, 0] = plus(ry[n, 0], rz[n])
            zi_copy(n).start()

    def stage_zi(n):
        @pl.when(inner)
        def _():
            zi_copy(n).wait_recv()
            g_start(n, plus(ry[n, 0], ri[n]))

    def stage_g(n):
        @pl.when(outer)
        def _():
            g_whole(n).wait_recv()

        ay_start(n)

    def stage_ay(n):
        for m in range(1, nh):
            ay_whole(n, m).wait_recv()
        ac_start(n)

    lo = lax.broadcasted_iota(jnp.int32, (rows, 128), 1) < 64
    pairs = width // 128

    def unit(index):
        i, p = index // pairs, lax.rem(index, pairs)
        there = 1 - b1 - i + 2 * i * b1
        keys = pl.ds(pl.multiple_of(there * (2 * rows), 128), 2 * rows)
        col = pl.ds(pl.multiple_of(p * 128, 128), 128)
        k2 = k_ref[keys, col]
        v2 = v_ref[keys, col]
        q2 = q_ref[:, col]
        dc2 = dc_ref[:, col]
        both = dc2.astype(F32) * ctx_ref[:, col]
        lse2 = lse_ref[p]
        dq, dk, dv = [], None, None
        for h in range(2):
            mask = lo if h == 0 else jnp.logical_not(lo)
            qm = jnp.where(mask, q2, jnp.zeros_like(q2))
            dmask = jnp.where(mask, dc2, jnp.zeros_like(q2))
            lse = lse2[:, 0:1] if h == 0 else lse2[:, 64:65]
            dot = jnp.sum(jnp.where(mask, both, 0.0), axis=-1, keepdims=True)
            probs = jnp.exp(nt(qm, k2) * score_scale - lse)
            slopes = nt(dmask, v2)
            dscore = (probs * (slopes - dot) * score_scale).astype(BF)
            dq.append(nn(dscore, k2))
            a = nn(dmask.T, probs.astype(BF))
            b = nn(qm.T, dscore)
            dv = a if dv is None else dv + a
            dk = b if dk is None else dk + b
        dq2 = jnp.where(lo, dq[0], dq[1])

        @pl.when(i == 0)
        def _():
            dqa[:, col] = dq2

        @pl.when(i > 0)
        def _():
            dqa[:, col] += dq2

        dkt[col, keys] = dk.astype(BF)
        dvt[col, keys] = dv.astype(BF)

    def weights(s):
        frames = pl.ds(pl.multiple_of(at.z * rows, 128), rows)
        for hi in range(nh):
            col = lanes(s, hi)
            dq2 = dqa[:, col]
            vb[2, 0:1, col] = jnp.sum(dq2, axis=0, keepdims=True)
            dq2 = dq2.astype(BF)
            dk2 = dkt[col, :]
            dv2 = dvt[col, :]
            for j in range(nf):
                for part in range(2):
                    for r in range(split):
                        here = pl.ds((2 * j + part) * half + r * q, q)
                        ga[s, r, hi, j, part, 0, 0] = nn(ht_ref[here, frames], dq2).astype(BF)
                        ga[s, r, hi, j, part, 0, 1] = nt(ht_ref[here, :], dk2).astype(BF)
                        ga[s, r, hi, j, part, 1, 0] = nt(ht_ref[here, :], dv2).astype(BF)

    pieces = 16
    per_step = 2
    lag = 2
    low = 1 - b1

    def part_of(t):
        return pl.ds(pl.multiple_of(t * (width // pieces), 16), width // pieces)

    def da_copy(t):
        return remote(
            dhs.at[pl.ds(low, 3), part_of(t)], dra.at[:, part_of(t)], das.at[t], dar.at[t], near
        )

    def db_copy(t):
        return remote(
            dhs.at[pl.ds(2 * low, 2), part_of(t)], drb.at[:, part_of(t)], dbs.at[t], dbr.at[t], across
        )

    def dc_copy(t):
        return remote(dhs.at[3 * b1, part_of(t)], drc.at[part_of(t)], dcs.at[t], dcr.at[t], near)

    def d_stage(i, t):
        part = part_of(t)
        if i == 0:
            @pl.when(outer)
            def _():
                da_copy(t).start()
        elif i == 1:
            @pl.when(inner)
            def _():
                da_copy(t).wait_recv()
                for j in range(3):
                    dhs[low + j, part] = dhs[low + j, part] + dra[j, part]
                db_copy(t).start()
        elif i == 2:
            @pl.when(inner)
            def _():
                db_copy(t).wait_recv()
                for j in range(2):
                    dhs[2 * b1 + j, part] = dhs[2 * b1 + j, part] + drb[j, part]
                dc_copy(t).start()
        else:
            @pl.when(outer)
            def _():
                dc_copy(t).wait_recv()

    def spread(i):
        there = 1 - b1 - i + 2 * i * b1
        for ub in range(2):
            part = pl.ds(pl.multiple_of((2 * there + ub) * rows, 128), rows)
            dhs[2 * there + ub] = (nn(w_ref[1], dkt[:, part]) + nn(w_ref[2], dvt[:, part])).astype(BF)

    def first_norm():
        @pl.when(inner)
        def _():
            drc[...] = jnp.zeros_like(drc)

        total = dhs[at.z].astype(F32) + nt(w_ref[0], dqa[...].astype(BF))
        total += drc[...].astype(F32)
        total = total.T
        normed, inverse = normalize(frames_ref[...])
        scaled = total * vec_ref[0:1, :]
        centred = (
            scaled
            - jnp.mean(scaled, axis=-1, keepdims=True)
            - normed * jnp.mean(scaled * normed, axis=-1, keepdims=True)
        )
        ig_ref[...] = gm_ref[...] + inverse * centred
        vb[1] = gv_ref[...]
        vb[1, 0:1, :] = jnp.sum(total * normed, axis=0, keepdims=True)
        vb[1, 1:2, :] = jnp.sum(total, axis=0, keepdims=True)
        vb[1, 2:3, :] = vb[2, 0:1, :]

    def v_core():
        return remote(vb.at[1], vb.at[0], vs.at[0], vr.at[0], at.sibling())

    def v_x(k):
        return remote(vx.at[at.x], vx.at[at.x], vs.at[k], vr.at[k], at.x_peer(k))

    def v_y(m):
        return remote(vy.at[at.hi], vy.at[at.hi], vs.at[nf + m], vr.at[nf + m], at.y_peer(m))

    def v_z(k):
        return remote(
            vz.at[at.z], vz.at[at.z], vs.at[nf + nh + k], vr.at[nf + nh + k], at.z_peer(k)
        )

    def v_step(i):
        if i == 0:
            v_core().start()
        elif i == 1:
            v_core().wait_recv()
            vx[at.x] = vb[0] + vb[1]
            for k in range(1, nf):
                v_x(k).start()
        elif i == 2:
            for k in range(1, nf):
                v_x(k).wait_recv()
            total = vx[0]
            for j in range(1, nf):
                total += vx[j]
            vy[at.hi] = total
            for m in range(1, nh):
                v_y(m).start()
        elif i == 3:
            for m in range(1, nh):
                v_y(m).wait_recv()
            total = vy[0]
            for j in range(1, nh):
                total += vy[j]
            vz[at.z] = total
            for k in range(1, ns):
                v_z(k).start()
        else:
            for k in range(1, ns):
                v_z(k).wait_recv()
            total = vz[0]
            for j in range(1, ns):
                total += vz[j]
            ov_ref[...] = total

    ready = group
    each = -(-2 * pairs // ready)
    done = [-(-pairs * (i + 1) // each) - 1 for i in range(2)]
    away = done[1] + 1
    norm = max(away + (pieces - 1) // per_step + 4, chunks - 2)
    stages = (stage_x, stage_y, stage_z, stage_zi, stage_g, stage_ay)
    last = max(chunks + lag * len(stages), norm + 6)
    for n in range(4):
        c_send(n)

    def step(n, carry):
        for k in range(2):
            @pl.when(2 * n + k < 2 * group)
            def _(k=k):
                stage_c(2 * n + k)

                @pl.when(2 * n + k + 4 < 2 * group)
                def _():
                    c_send(2 * n + k + 4)

        @pl.when(jnp.logical_and(n >= ready + 1, n < ready + 1 + per))
        def _():
            for r in range(split):
                stage_c(2 * group + (n - ready - 1) * split + r)

        @pl.when(n < ready)
        def _():
            def one(k, carry):
                @pl.when(n * each + k < 2 * pairs)
                def _():
                    unit(n * each + k)

                return carry

            lax.fori_loop(0, each, one, 0)

        @pl.when(jnp.logical_or(n == done[0], n == done[1]))
        def _():
            spread(n // done[1])

        @pl.when(n == norm)
        def _():
            first_norm()

        @pl.when(n == ready)
        def _():
            whole = ga.at[:, :, :, :, :, 1, 1]
            pltpu.make_async_copy(whole, whole, os.at[4]).wait()

        @pl.when(jnp.logical_and(n >= ready, n < ready + per))
        def _():
            weights(n - ready)
            for r in range(split):
                c_send(2 * group + (n - ready) * split + r)

        for i, stage in enumerate(stages):
            @pl.when(jnp.logical_and(n >= lag * i, n < chunks + lag * i))
            def _(i=i, stage=stage):
                stage(n - lag * i)

        for i in range(4):
            first = away + i

            @pl.when(jnp.logical_and(n >= first, n < first + pieces // per_step))
            def _(i=i, first=first):
                for t in range(per_step):
                    d_stage(i, (n - first) * per_step + t)

        for i in range(5):
            @pl.when(n == norm + i)
            def _(i=i):
                v_step(i)

        return carry

    lax.fori_loop(0, last, step, 0)
    for n in range(chunks):
        ac_whole(n).wait()

    def drain(n, carry):
        c_whole(n).wait_send()

        @pl.when(outer)
        def _():
            z_copy(n).wait_send()

        @pl.when(inner)
        def _():
            zi_copy(n).wait_send()
            g_whole(n).wait_send()

        for k in range(1, nf):
            x_copy(n, k).wait_send()
        for m in range(1, nh):
            y_copy(n, m).wait_send()
            ay_whole(n, m).wait_send()
        return carry

    lax.fori_loop(0, chunks, drain, 0)

    @pl.when(outer)
    def _():
        def sent(t, carry):
            da_copy(t).wait_send()
            return carry

        lax.fori_loop(0, pieces, sent, 0)

    @pl.when(inner)
    def _():
        def sent(t, carry):
            db_copy(t).wait_send()
            dc_copy(t).wait_send()
            return carry

        lax.fori_loop(0, pieces, sent, 0)

    for k in range(1, ns):
        v_z(k).wait_send()
    for k in range(1, nf):
        v_x(k).wait_send()
    for m in range(1, nh):
        v_y(m).wait_send()
    v_core().wait_send()


def back_all(sizes, q, k, v, dc, ctx, lse, ht, w, gm, frames, vec, gv, gc, ge, go):
    nd, nf, ns = sizes
    nh = nd // 2
    rows, width = q.shape
    shard = go.shape[1]
    half = shard // 2
    every = k.shape[0]
    split = 2 if half % 32 == 0 else 1
    strip = half // split
    per = width // nh // 128
    chunks = 3 * per * split
    xn, yn = max(nf - 1, 1), max(nh - 1, 1)
    dma = pltpu.SemaphoreType.DMA
    anywhere = pl.BlockSpec(memory_space=pl.ANY)
    return pl.pallas_call(
        functools.partial(back_kernel, sizes),
        out_shape=(
            jax.ShapeDtypeStruct((2, 2, shard, width), BF),
            jax.ShapeDtypeStruct((shard, 4 * width), BF),
            jax.ShapeDtypeStruct((2, 2, shard, width), BF),
            jax.ShapeDtypeStruct((rows, width), F32),
            jax.ShapeDtypeStruct((16, width), F32),
        ),
        in_specs=[vmem()] * 12 + [anywhere] * 3,
        out_specs=(vmem(),) * 5,
        scratch_shapes=[
            pltpu.VMEM((per, split, nh, nf, 2, 2, 2, strip, 128), BF),
            pltpu.VMEM((4, nh, nf, 2, 2, strip, 128), BF),
            pltpu.VMEM((chunks, nh, nf, 2, 2, strip, 128), BF),
            pltpu.VMEM((chunks, xn, nh, 2, 2, strip, 128), BF),
            pltpu.VMEM((chunks, yn, 2, 2, strip, 128), BF),
            pltpu.VMEM((chunks, 2, 2, strip, 128), BF),
            pltpu.VMEM((chunks, 2, 2, strip, 128), BF),
            pltpu.VMEM((width, every), BF),
            pltpu.VMEM((width, every), BF),
            pltpu.VMEM((rows, width), F32),
            pltpu.VMEM((ns, width, rows), BF),
            pltpu.VMEM((3, width, rows), BF),
            pltpu.VMEM((2, width, rows), BF),
            pltpu.VMEM((width, rows), BF),
            pltpu.VMEM((3, 16, width), F32),
            pltpu.VMEM((nf, 16, width), F32),
            pltpu.VMEM((nh, 16, width), F32),
            pltpu.VMEM((ns, 16, width), F32),
            dma((5,)),
            dma((chunks,)), dma((chunks,)),
            dma((chunks, xn)), dma((chunks, xn)),
            dma((chunks, yn)), dma((chunks, yn)),
            dma((chunks,)), dma((chunks,)),
            dma((chunks,)), dma((chunks,)),
            dma((chunks,)), dma((chunks,)),
            dma((chunks, yn)), dma((chunks, yn)),
            dma((chunks,)), dma((chunks,)),
            dma((16,)), dma((16,)),
            dma((16,)), dma((16,)),
            dma((16,)), dma((16,)),
            dma((nf + nh + ns,)), dma((nf + nh + ns,)),
        ],
        name="back",
        compiler_params=pltpu.CompilerParams(
            collective_id=1, has_side_effects=True, vmem_limit_bytes=67043328
        ),
    )(q, k, v, dc, ctx, lse, ht, w, gm, frames, vec, gv, gc, ge, go)


def feed_kernel(
    ctx_ref, frames_ref, cot_ref, vec_ref, wo_ref, win_ref, wout_ref,
    fo_ref, gm_ref, dc_ref, gi_ref, gout_ref, go_ref, gv_ref,
    mid, h2, h2t, dyb, acc, dh2,
):
    b = pl.program_id(0)

    @pl.when(b == 0)
    def _():
        middle = frames_ref[...] + nn(ctx_ref[...].astype(BF), wo_ref[...]) + vec_ref[4:5, :]
        mid[...] = middle
        normed, _ = normalize(middle)
        hidden = (normed * vec_ref[5:6, :] + vec_ref[6:7, :]).astype(BF)
        h2[...] = hidden
        h2t[...] = hidden.T
        dyb[...] = cot_ref[...].astype(BF)
        acc[...] = middle + vec_ref[7:8, :]
        dh2[...] = jnp.zeros_like(dh2)
        gv_ref[...] = jnp.zeros_like(gv_ref)

    up = dyb[...]
    u = nn(h2[...], win_ref[...]) + vec_ref[pl.ds(8 + b, 1), :]
    phi = 0.5 * (1.0 + lax.erf(u * 0.7071067811865476))
    activated = (u * phi).astype(BF)
    acc[...] += nn(activated, wout_ref[...])
    gout_ref[...] = tn(activated, up).astype(BF)
    du = nt(up, wout_ref[...]) * (phi + u * jnp.exp(-0.5 * u * u) * 0.3989422804014327)
    gv_ref[pl.ds(8 + b, 1), :] = jnp.sum(du, axis=0, keepdims=True)
    dub = du.astype(BF)
    gi_ref[...] = nn(h2t[...], dub).astype(BF)
    dh2[...] += nt(dub, win_ref[...])

    @pl.when(b == pl.num_programs(0) - 1)
    def _():
        fo_ref[...] = acc[...]
        normed, inverse = normalize(mid[...])
        back, gain, offset = norm_back(dh2[...], normed, inverse, vec_ref[5:6, :])
        upstream = cot_ref[...]
        middle = upstream + back
        gm_ref[...] = middle
        dab = middle.astype(BF)
        go_ref[...] = tn(ctx_ref[...].astype(BF), dab).astype(BF)
        dctx = nt(dab, wo_ref[...]).astype(BF)
        dc_ref[...] = dctx
        gv_ref[3:4, :] = jnp.sum(dctx.astype(F32), axis=0, keepdims=True)
        gv_ref[4:5, :] = jnp.sum(middle, axis=0, keepdims=True)
        gv_ref[5:6, :] = gain[None]
        gv_ref[6:7, :] = offset[None]
        gv_ref[7:8, :] = jnp.sum(upstream, axis=0, keepdims=True)


def feed_all(ctx, frames, cot, vec, aw, ew, cw):
    rows, width = frames.shape
    full = ew.shape[1]
    whole = lambda shape: pl.BlockSpec(shape, lambda b: (0,) * len(shape))
    blocks = full // width
    return pl.pallas_call(
        feed_kernel,
        grid=(blocks,),
        out_shape=(
            jax.ShapeDtypeStruct((rows, width), F32),
            jax.ShapeDtypeStruct((rows, width), F32),
            jax.ShapeDtypeStruct((rows, width), BF),
            jax.ShapeDtypeStruct((width, full), BF),
            jax.ShapeDtypeStruct((full, width), BF),
            jax.ShapeDtypeStruct((width, width), BF),
            jax.ShapeDtypeStruct((16, width), F32),
        ),
        in_specs=[
            whole((rows, width)), whole((rows, width)), whole((rows, width)), whole((16, width)),
            pl.BlockSpec((None, width, width), lambda b: (3, 0, 0)),
            pl.BlockSpec((width, width), lambda b: (0, b)),
            pl.BlockSpec((width, width), lambda b: (b, 0)),
        ],
        out_specs=(
            whole((rows, width)), whole((rows, width)), whole((rows, width)),
            pl.BlockSpec((width, width), lambda b: (0, b)),
            pl.BlockSpec((width, width), lambda b: (b, 0)),
            whole((width, width)), whole((16, width)),
        ),
        scratch_shapes=[
            pltpu.VMEM((rows, width), F32),
            pltpu.VMEM((rows, width), BF),
            pltpu.VMEM((width, rows), BF),
            pltpu.VMEM((rows, width), BF),
            pltpu.VMEM((rows, width), F32),
            pltpu.VMEM((rows, width), F32),
        ],
        name="feed",
        compiler_params=pltpu.CompilerParams(vmem_limit_bytes=67043328),
    )(ctx, frames, cot, vec, aw, ew, cw)


def on_device(
    sizes,
    frames_in,
    cotangent,
    attention_weight,
    expand_weight,
    contract_weight,
    vectors,
    first_attention,
    first_expand,
    first_contract,
    first_vectors,
    second_attention,
    second_expand,
    second_contract,
    second_vectors,
):
    nd, nf, ns = sizes
    frames = frames_in[0]
    upstream = cotangent[0]
    rows, width = frames.shape
    shard = attention_weight.shape[1]
    full = expand_weight.shape[1]
    aw, ew, cw, vec, h_turned, queries, key_rows, value_rows, context_wide, log_total = front_all(
        sizes, frames, vectors, attention_weight, expand_weight, contract_weight
    )
    frames_out, grad_middle, grad_context, grad_expand, grad_contract, grad_output_w, gv = feed_all(
        context_wide, frames, upstream, vec, aw, ew, cw
    )
    oc, oe, oa, input_gradient, gv_sum = back_all(
        sizes,
        queries,
        key_rows,
        value_rows,
        grad_context,
        context_wide,
        log_total,
        h_turned,
        aw,
        grad_middle,
        frames,
        vec,
        gv,
        grad_contract.reshape(nf, 4, shard, width),
        grad_expand.reshape(nf, shard, full),
        grad_output_w.reshape(nf, shard, width),
    )
    owned_vec = lax.dynamic_slice_in_dim(
        gv_sum[:12], lax.axis_index("fsdp") * (width // nf), width // nf, 1
    )
    owned = (
        oa.reshape(4, shard, width).astype(F32),
        oe.astype(F32),
        oc.reshape(4 * shard, width).astype(F32),
    )
    attention_out = (owned[0],) + adam_update(
        attention_weight, owned[0], first_attention, second_attention, rate_matrix, decay_matrix
    )
    expand_out = (owned[1],) + adam_update(
        expand_weight, owned[1], first_expand, second_expand, rate_matrix, decay_matrix
    )
    contract_out = (owned[2],) + adam_update(
        contract_weight, owned[2], first_contract, second_contract, rate_matrix, decay_matrix
    )
    vector_out = (owned_vec,) + adam_update(
        vectors, owned_vec, first_vectors, second_vectors, rate_vector, 0.0
    )
    result = [frames_out[None], input_gradient[None]]
    for i in range(4):
        result += [attention_out[i], expand_out[i], contract_out[i], vector_out[i]]
    return tuple(result)


def solution(mesh):
    sizes = (mesh.shape["dp"], mesh.shape["fsdp"], mesh.shape["seq"])
    data = P(("dp", "fsdp"), "seq", None)
    state = (P(None, "fsdp", None), P("fsdp", None), P("fsdp", None), P(None, "fsdp"))
    return jax.shard_map(
        functools.partial(on_device, sizes),
        mesh=mesh,
        in_specs=(data, data) + state * 3,
        out_specs=(data, data) + state * 4,
        check_vma=False,
    )
```

```python
import functools

import jax
import jax.numpy as jnp
from jax import lax
from jax.experimental import pallas as pl
from jax.experimental.pallas import tpu as pltpu
from jax.sharding import PartitionSpec as P

HEADS = 12
norm_eps = 1e-05
beta_one = 0.9
beta_two = 0.999
adam_eps = 1e-08
adam_count = 5.0
rate_matrix = 0.02
rate_vector = 0.1
decay_matrix = 0.1
score_scale = 0.125
VMEM_LIMIT = 60 << 20
MESH = pl.DeviceIdType.MESH
BF = jnp.bfloat16
F32 = jnp.float32


def nt(left, right):
    return lax.dot_general(left, right, (((1,), (1,)), ((), ())), preferred_element_type=F32)


def nn(left, right):
    return lax.dot_general(left, right, (((1,), (0,)), ((), ())), preferred_element_type=F32)


def tn(left, right):
    return lax.dot_general(left, right, (((0,), (0,)), ((), ())), preferred_element_type=F32)


def vmem():
    return pl.BlockSpec(memory_space=pltpu.VMEM)


def normalize(values):
    center = values - jnp.mean(values, axis=-1, keepdims=True)
    inverse = lax.rsqrt(jnp.mean(center * center, axis=-1, keepdims=True) + norm_eps)
    return center * inverse, inverse


def norm_back(upstream, normed, inverse, gain):
    scaled = upstream * gain
    inner = (
        scaled
        - jnp.mean(scaled, axis=-1, keepdims=True)
        - normed * jnp.mean(scaled * normed, axis=-1, keepdims=True)
    )
    return (inverse * inner, jnp.sum(upstream * normed, axis=0), jnp.sum(upstream, axis=0))


def adam_update(weight, gradient, first, second, rate, decay):
    first_new = beta_one * first + (1.0 - beta_one) * gradient
    second_new = beta_two * second + (1.0 - beta_two) * gradient * gradient
    first_hat = first_new / (1.0 - beta_one**adam_count)
    second_hat = second_new / (1.0 - beta_two**adam_count)
    updated = weight - rate * (first_hat / (jnp.sqrt(second_hat) + adam_eps) + decay * weight)
    return (updated, first_new, second_new)


class Place:
    def __init__(self, sizes):
        self.nd, self.nf, self.ns = sizes
        self.nh = self.nd // 2
        self.dp = lax.axis_index("dp")
        self.x = lax.axis_index("fsdp")
        self.z = lax.axis_index("seq")
        self.core = lax.rem(self.dp, 2)
        self.hi = self.dp // 2

    def sibling(self):
        return {"dp": self.hi * 2 + 1 - self.core}

    def x_peer(self, k):
        return {"fsdp": lax.rem(self.x + k, self.nf)}

    def y_hi(self, k):
        return lax.rem(self.hi + k, self.nh)

    def y_peer(self, k):
        return {"dp": self.y_hi(k) * 2 + self.core}

    def z_at(self, k):
        return lax.rem(self.z + k + self.ns, self.ns)

    def z_peer(self, k):
        return {"seq": self.z_at(k)}

    def everyone(self):
        out = [self.sibling()]
        out += [self.x_peer(k) for k in range(1, self.nf)]
        out += [self.y_peer(k) for k in range(1, self.nh)]
        out += [self.z_peer(k) for k in range(1, self.ns)]
        return out

    def barrier(self):
        sem = pltpu.get_barrier_semaphore()
        peers = self.everyone()
        for peer in peers:
            pl.semaphore_signal(sem, inc=1, device_id=peer, device_id_type=MESH)
        pl.semaphore_wait(sem, len(peers))


def remote(src, dst, send, recv, peer):
    return pltpu.make_async_remote_copy(
        src_ref=src, dst_ref=dst, send_sem=send, recv_sem=recv, device_id=peer, device_id_type=MESH
    )


def front_kernel(
    sizes, frames_ref, vec_ref, aw_ref, ew_ref, cw_ref,
    a_out, e_ref, c_ref, vec_out, ht_out, q_out, k_out, v_out, ctx_out, lse_ref,
    a_ref, v_buf, h_ref, ht, q_buf, k_buf, v_buf2, ctx_buf, af, ef, eb, cb, kept, stat,
    ls, xs, xr, ys, yr, s1s, s1r, s2s, s2r, vs, vr, rs, hs, hr,
):
    at = Place(sizes)
    nf, nh, ns = at.nf, at.nh, at.ns
    rows, width = frames_ref.shape
    shard = aw_ref.shape[1]
    half = shard // 2
    deep = cb.shape[0]
    b0 = lax.rem(at.z, 2)
    b1 = at.z // 2

    def load(i, src, dst):
        return pltpu.make_async_copy(src, dst, ls.at[i])

    loads = [
        load(0, aw_ref.at[pl.ds(0, 3)], af.at[pl.ds(0, 3)]),
        load(1, aw_ref.at[pl.ds(3, 1)], af.at[pl.ds(3, 1)]),
        load(2, ew_ref, ef),
        load(3, cw_ref, af),
    ]
    for copy in loads[:3]:
        copy.start()
    at.barrier()
    v_buf[at.x] = jnp.zeros(v_buf.shape[1:], BF)
    v_buf[at.x, 0 : vec_ref.shape[0], :] = vec_ref[...].astype(BF)
    vec_copies = []
    for k in range(1, nf):
        copy = remote(v_buf.at[at.x], v_buf.at[at.x], vs.at[k], vr.at[k], at.x_peer(k))
        copy.start()
        vec_copies.append(copy)

    order = (1, 2, 0, 3)

    def view(chunk, j, hi, core, own=False):
        cols = width // nh
        if chunk < 4:
            return a_ref.at[
                order[chunk],
                pl.ds(pl.multiple_of(j * shard + core * half, 16), half),
                pl.ds(pl.multiple_of(hi * cols, 128), cols),
            ]
        if chunk < 8:
            start = 0 if own else j * shard
            wide = eb.shape[1] // nh
            return (eb if own else e_ref).at[
                pl.ds(pl.multiple_of(start + core * half, 16), half),
                pl.ds(pl.multiple_of(hi * wide + (chunk - 4) * (wide // 4), 128), wide // 4),
            ]
        start = 0 if own else j * deep
        tall = deep // 8
        return (cb if own else c_ref).at[
            pl.ds(pl.multiple_of(start + core * (deep // 2) + (chunk - 8) * tall, 16), tall),
            pl.ds(pl.multiple_of(hi * cols, 128), cols),
        ]

    own = pl.multiple_of(at.x * shard, 16)
    x_copies = {}

    def send_chunk(chunk):
        for k in range(1, nf):
            copy = remote(
                view(chunk, at.x, at.hi, at.core, True), view(chunk, at.x, at.hi, at.core),
                xs.at[chunk, k - 1], xr.at[chunk, k - 1], at.x_peer(k),
            )
            copy.start()
            x_copies[chunk, k] = copy

    loads[0].wait()
    for i, u in enumerate(order[:3]):
        a_ref[u, pl.ds(own, shard), :] = af[u].astype(BF)
        send_chunk(i)
    normed, _ = normalize(frames_ref[...])
    for copy in vec_copies:
        copy.wait()
    vec = jnp.concatenate([v_buf[j] for j in range(nf)], axis=1).astype(F32)
    vec_out[...] = vec
    mine = pl.ds(pl.multiple_of(at.z * rows, 128), rows)
    hidden = (normed * vec[0:1] + vec[1:2]).astype(BF)
    h_ref[mine, :] = hidden

    def block(b):
        return h_ref.at[pl.ds(pl.multiple_of(b * rows, 128), rows), :]

    def to_right(b):
        return remote(block(b), block(b), rs.at[b], hr.at[b], {"seq": at.z + 1})

    def to_left(b):
        return remote(block(b), block(b), hs.at[b], hr.at[b], {"seq": at.z - 1})

    @pl.when(at.z < ns - 1)
    def _():
        to_right(at.z).start()

    @pl.when(at.z > 0)
    def _():
        to_left(at.z).start()

    loads[1].wait()
    a_ref[3, pl.ds(own, shard), :] = af[3].astype(BF)
    loads[3].start()
    send_chunk(3)
    loads[2].wait()
    eb[...] = ef[...].astype(BF)
    for i in range(4, 8):
        send_chunk(i)
    loads[3].wait()
    for u in range(4):
        cb[pl.ds(u * shard, shard), :] = af[u].astype(BF)
    for i in range(8, 12):
        send_chunk(i)
    stores = [
        load(4, eb, e_ref.at[pl.ds(own, shard), :]),
        load(5, cb, c_ref.at[pl.ds(pl.multiple_of(at.x * deep, 16), deep), :]),
    ]
    for copy in stores:
        copy.start()
    ht[:, mine] = hidden.T

    def first_copy(chunk, k):
        j = lax.rem(at.x - k + nf, nf)
        piece = view(chunk, j, at.hi, at.core)
        return remote(piece, piece, s1s.at[chunk, k - 1], s1r.at[chunk, k - 1], at.sibling())

    def y_copy(chunk, k, m):
        j = lax.rem(at.x - k + nf, nf)
        piece = view(chunk, j, at.hi, at.core)
        return remote(piece, piece, ys.at[chunk, k - 1, m - 1], yr.at[chunk, k - 1, m - 1], at.y_peer(m))

    def second_copy(chunk, k, m):
        j = lax.rem(at.x - k + nf, nf)
        piece = view(chunk, j, lax.rem(at.hi - m + nh, nh), at.core)
        return remote(piece, piece, s2s.at[chunk, k - 1, m - 1], s2r.at[chunk, k - 1, m - 1], at.sibling())

    def forward(chunk):
        for k in range(1, nf):
            x_copies[chunk, k].wait_recv()
            first_copy(chunk, k).start()
            for m in range(1, nh):
                y_copy(chunk, k, m).start()

    def relay(chunk):
        for k in range(1, nf):
            for m in range(1, nh):
                y_copy(chunk, k, m).wait_recv()
                second_copy(chunk, k, m).start()

    def arrived(chunk):
        for k in range(1, nf):
            first_copy(chunk, k).wait_recv()
            for m in range(1, nh):
                second_copy(chunk, k, m).wait_recv()

    def rows_of(b):
        part = pl.ds(pl.multiple_of(b * rows, 128), rows)
        k_buf[part, :] = nn(h_ref[part, :], a_ref[1]).astype(BF)
        v_buf2[part, :] = (nn(h_ref[part, :], a_ref[2]) + vec[3:4]).astype(BF)

    def turn(b):
        part = pl.ds(pl.multiple_of(b * rows, 128), rows)
        ht[:, part] = h_ref[part, :].T

    def hop(s):
        b = at.z - s
        d = at.z + s

        @pl.when(b >= 0)
        def _():
            to_right(b).wait_recv()

            @pl.when(at.z < ns - 1)
            def _():
                to_right(b).start()

        @pl.when(d < ns)
        def _():
            to_left(d).wait_recv()

            @pl.when(at.z > 0)
            def _():
                to_left(d).start()

    lane = lax.broadcasted_iota(jnp.int32, (rows, 128), 1)
    lo = lane < 64

    def scores(p, h, b):
        col = pl.ds(pl.multiple_of(p * 128, 128), 128)
        part = pl.ds(pl.multiple_of(b * rows, 128), rows)
        q2 = q_buf[:, col]
        mask = lo if h == 0 else jnp.logical_not(lo)
        s = nt(jnp.where(mask, q2, jnp.zeros_like(q2)), k_buf[part, col]) * score_scale
        largest = jnp.max(s, axis=-1, keepdims=True)
        e = jnp.exp(s - largest)
        return e, largest, jnp.sum(e, axis=-1, keepdims=True)

    assert ns == 4
    blocks = (at.z, at.z + 1 - 2 * b0, 2 - b1, 3 - 3 * b1)

    def tick(i):
        if i < 12:
            forward(i)
        if i > 0:
            relay(i - 1)

    def begin(i, ticks):
        b = blocks[i]
        rows_of(b)

        def pair(p, carry):
            found = []
            for h in range(2):
                e, largest, total = scores(p, h, b)
                kept[i, 2 * p + h] = e
                found += [largest, total]
            stat[i, p] = jnp.where(
                lo, jnp.where(lane < 32, found[0], found[1]), jnp.where(lane < 96, found[2], found[3])
            )
            for when, which in ticks:
                @pl.when(p == when)
                def _(which=which):
                    tick(which)

            return carry

        lax.fori_loop(0, width // 128, pair, 0)

    tick(0)
    tick(1)
    tick(2)
    hop(1)
    tick(3)
    for i in range(3):
        arrived(i)
    q_buf[...] = (nn(h_ref[mine, :], a_ref[0]) + vec[2:3]).astype(BF)
    stores.append(load(6, q_buf, q_out))
    stores[-1].start()
    tick(4)
    begin(0, ((2, 5), (5, 6)))
    hop(2)
    begin(1, ((1, 7), (4, 8)))
    turn(blocks[1])
    begin(2, ((0, 9), (3, 10)))
    turn(blocks[2])
    hop(3)
    rows_of(blocks[3])
    turn(blocks[3])
    tick(11)
    arrived(3)
    for i, (src, dst) in enumerate(((a_ref, a_out), (ht, ht_out), (k_buf, k_out), (v_buf2, v_out))):
        stores.append(load(7 + i, src, dst))
        stores[-1].start()
    def pair(p, carry):
        col = pl.ds(pl.multiple_of(p * 128, 128), 128)
        ctx, lse = [], []
        for h in range(2):
            e, peak, count = scores(p, h, blocks[3])
            peaks = [stat[i, p][:, 64 * h : 64 * h + 1] for i in range(3)] + [peak]
            counts = [stat[i, p][:, 64 * h + 32 : 64 * h + 33] for i in range(3)] + [count]
            largest = functools.reduce(jnp.maximum, peaks)
            shares = [jnp.exp(each - largest) for each in peaks]
            total = sum(share * each for share, each in zip(shares, counts))
            inverse = 1.0 / total
            out = None
            for i in range(4):
                part = pl.ds(pl.multiple_of(blocks[i] * rows, 128), rows)
                found = kept[i, 2 * p + h] if i < 3 else e
                term = nn((found * (shares[i] * inverse)).astype(BF), v_buf2[part, col])
                out = term if out is None else out + term
            ctx.append(out)
            lse.append(largest + jnp.log(total))
        ctx_buf[:, col] = jnp.where(lo, ctx[0], ctx[1])
        lse_ref[p] = jnp.where(lo, lse[0], lse[1])

        @pl.when(p == 1)
        def _():
            tick(12)

        return carry

    lax.fori_loop(0, width // 128, pair, 0)
    stores.append(load(11, ctx_buf, ctx_out))
    stores[-1].start()
    for i in range(4, 12):
        arrived(i)
    for copy in stores:
        copy.wait()
    for copy in x_copies.values():
        copy.wait_send()
    for chunk in range(12):
        for k in range(1, nf):
            first_copy(chunk, k).wait_send()
            for m in range(1, nh):
                y_copy(chunk, k, m).wait_send()
                second_copy(chunk, k, m).wait_send()
    for b in range(ns):
        @pl.when(jnp.logical_and(b <= at.z, at.z < ns - 1))
        def _():
            to_right(b).wait_send()

        @pl.when(jnp.logical_and(b >= at.z, at.z > 0))
        def _():
            to_left(b).wait_send()


def front_all(sizes, frames, vec, aw, ew, cw):
    nd, nf, ns = sizes
    nh = nd // 2
    rows, width = frames.shape
    shard, full = ew.shape
    deep = cw.shape[0]
    every = rows * ns
    dma = pltpu.SemaphoreType.DMA
    anywhere = pl.BlockSpec(memory_space=pl.ANY)
    return pl.pallas_call(
        functools.partial(front_kernel, sizes),
        out_shape=(
            jax.ShapeDtypeStruct((4, width, width), BF),
            jax.ShapeDtypeStruct((width, full), BF),
            jax.ShapeDtypeStruct((deep * nf, width), BF),
            jax.ShapeDtypeStruct((16, width), F32),
            jax.ShapeDtypeStruct((width, every), BF),
            jax.ShapeDtypeStruct((rows, width), BF),
            jax.ShapeDtypeStruct((every, width), BF),
            jax.ShapeDtypeStruct((every, width), BF),
            jax.ShapeDtypeStruct((rows, width), F32),
            jax.ShapeDtypeStruct((width // 128, rows, 128), F32),
        ),
        in_specs=[vmem(), vmem(), anywhere, anywhere, anywhere],
        out_specs=(anywhere, anywhere, anywhere, vmem()) + (anywhere,) * 5 + (vmem(),),
        scratch_shapes=[
            pltpu.VMEM((4, width, width), BF),
            pltpu.VMEM((nf, 16, vec.shape[1]), BF),
            pltpu.VMEM((every, width), BF),
            pltpu.VMEM((width, every), BF),
            pltpu.VMEM((rows, width), BF),
            pltpu.VMEM((every, width), BF),
            pltpu.VMEM((every, width), BF),
            pltpu.VMEM((rows, width), F32),
            pltpu.VMEM((4, shard, width), F32),
            pltpu.VMEM((shard, full), F32),
            pltpu.VMEM((shard, full), BF),
            pltpu.VMEM((deep, width), BF),
            pltpu.VMEM((ns - 1, width // 64, rows, rows), F32),
            pltpu.VMEM((ns - 1, width // 128, rows, 128), F32),
            dma((12,)),
            dma((12, nf - 1)), dma((12, nf - 1)),
            dma((12, nf - 1, nh - 1)), dma((12, nf - 1, nh - 1)),
            dma((12, nf - 1)), dma((12, nf - 1)),
            dma((12, nf - 1, nh - 1)), dma((12, nf - 1, nh - 1)),
            dma((nf,)), dma((nf,)),
            dma((ns,)), dma((ns,)), dma((ns,)),
        ],
        name="front",
        compiler_params=pltpu.CompilerParams(
            collective_id=0, has_side_effects=True, vmem_limit_bytes=67043328
        ),
    )(frames, vec, aw, ew, cw.reshape(aw.shape))


def back_kernel(
    sizes, q_ref, k_ref, v_ref, dc_ref, ctx_ref, lse_ref, ht_ref, w_ref, gm_ref, frames_ref,
    vec_ref, gv_ref, gc_ref, ge_ref, go_ref,
    oc_ref, oe_ref, oa_ref, ig_ref, ov_ref,
    ga, own, rc, rx, ry, rz, ri, dkt, dvt, dqa, dhs, dra, drb, drc, vb, vx, vy, vz,
    os, cs, cr, xs, xr, ys, yr, zs, zr, zis, zir, gs, gr, ays, ayr, acs, acr,
    das, dar, dbs, dbr, dcs, dcr, dns, dnr, vs, vr,
):
    at = Place(sizes)
    nf, nh, ns = at.nf, at.nh, at.ns
    rows, width = q_ref.shape
    q = rc.shape[5]
    cols = width // nh
    per = cols // 128
    chunks = rc.shape[0]
    split = chunks // (3 * per)
    half = q * split
    group = per * split
    b0 = lax.rem(at.z, 2)
    b1 = at.z // 2
    at.barrier()

    def strip(core, r):
        return pl.ds(pl.multiple_of(core * half + r * q, 16), q)

    def lanes(s, hi):
        return pl.ds(pl.multiple_of(hi * cols + s * 128, 128), 128)

    def place_of(n):
        return n // group, lax.rem(n, group) // split, lax.rem(n, split)

    for s in range(per):
        for hi in range(nh):
            for part in range(2):
                for r in range(split):
                    pltpu.make_async_copy(
                        go_ref.at[:, pl.ds(part * half + r * q, q), pl.ds(hi * cols + s * 128, 128)],
                        ga.at[s, r, hi, :, part, 1, 1],
                        os.at[4],
                    ).start()

    def own_whole(slot):
        return pltpu.make_async_copy(own.at[slot], own.at[slot], os.at[slot])

    def c_whole(n):
        return remote(rc.at[n], rc.at[n], cs.at[n], cr.at[n], at.sibling())

    def c_send(n):
        slot = lax.rem(n, 4)
        g, s, r = place_of(n)

        @pl.when(n < group)
        def _():
            for hi in range(nh):
                for u in range(4):
                    block = lanes(s, hi)
                    remote(
                        gc_ref.at[:, u, strip(1 - at.core, r), block],
                        rc.at[n, hi, :, u // 2, u % 2], cs.at[n], cr.at[n], at.sibling(),
                    ).start()
                    pltpu.make_async_copy(
                        gc_ref.at[:, u, strip(at.core, r), block],
                        own.at[slot, hi, :, u // 2, u % 2], os.at[slot],
                    ).start()

        @pl.when(jnp.logical_and(n >= group, n < 2 * group))
        def _():
            for hi in range(nh):
                for u in range(4):
                    block = pl.ds(pl.multiple_of(u * width + hi * cols + s * 128, 128), 128)
                    remote(
                        ge_ref.at[:, strip(1 - at.core, r), block],
                        rc.at[n, hi, :, u // 2, u % 2], cs.at[n], cr.at[n], at.sibling(),
                    ).start()
                    pltpu.make_async_copy(
                        ge_ref.at[:, strip(at.core, r), block],
                        own.at[slot, hi, :, u // 2, u % 2], os.at[slot],
                    ).start()

        @pl.when(jnp.logical_and(n >= 2 * group, n < chunks))
        def _():
            remote(
                ga.at[s, r, :, :, 1 - at.core], rc.at[n], cs.at[n], cr.at[n], at.sibling()
            ).start()

    def x_copy(n, k):
        peer = lax.rem(at.x + k, nf)
        return remote(rc.at[n, :, peer], rx.at[n, k - 1], xs.at[n, k - 1], xr.at[n, k - 1], at.x_peer(k))

    def y_copy(n, m):
        return remote(
            rx.at[n, 0, at.y_hi(m)], ry.at[n, m - 1], ys.at[n, m - 1], yr.at[n, m - 1], at.y_peer(m)
        )

    assert ns == 4
    outer = b0 == b1
    inner = b0 != b1
    near = {"seq": at.z + 1 - 2 * b0}
    across = {"seq": 3 - at.z}

    def z_copy(n):
        return remote(ry.at[n, 0], rz.at[n], zs.at[n], zr.at[n], near)

    def zi_copy(n):
        return remote(ry.at[n, 0], ri.at[n], zis.at[n], zir.at[n], across)

    def by_group(n, act):
        g, s, r = place_of(n)

        for which in range(3):
            @pl.when(g == which)
            def _(which=which):
                def place(hi, ua, ub):
                    if which == 1:
                        start = (2 * ua + ub) * width + hi * cols + s * 128
                        return oe_ref.at[strip(at.core, r), pl.ds(pl.multiple_of(start, 128), 128)]
                    ref = oc_ref if which == 0 else oa_ref
                    return ref.at[ua, ub, strip(at.core, r), lanes(s, hi)]

                act(place)

    def g_whole(n):
        return remote(ry.at[n, 0], ry.at[n, 0], gs.at[n], gr.at[n], near)

    def ay_whole(n, m):
        return remote(ry.at[n, 0], ry.at[n, 0], ays.at[n, m - 1], ayr.at[n, m - 1], at.y_peer(m))

    def ac_whole(n):
        return remote(rx.at[n, 0], rx.at[n, 0], acs.at[n], acr.at[n], at.sibling())

    def g_start(n, total):
        def act(place):
            for u in range(4):
                spot = place(at.hi, u // 2, u % 2)
                spot[...] = total[u // 2, u % 2]
                remote(spot, spot, gs.at[n], gr.at[n], near).start()

        by_group(n, act)

    def ay_start(n):
        def act(place):
            for m in range(1, nh):
                for u in range(4):
                    spot = place(at.hi, u // 2, u % 2)
                    remote(spot, spot, ays.at[n, m - 1], ayr.at[n, m - 1], at.y_peer(m)).start()

        by_group(n, act)

    def ac_start(n):
        def act(place):
            for hi in range(nh):
                for u in range(4):
                    spot = place(hi, u // 2, u % 2)
                    remote(spot, spot, acs.at[n], acr.at[n], at.sibling()).start()

        by_group(n, act)

    def plus(left, right):
        if nf == 2:
            return left + right
        return (left.astype(F32) + right.astype(F32)).astype(BF)

    def stage_c(n):
        c_whole(n).wait_recv()
        slot = lax.rem(n, 4)
        _, s, r = place_of(n)

        @pl.when(n < 2 * group)
        def _():
            own_whole(slot).wait()

            def add(i, carry):
                hi, j = i // nf, lax.rem(i, nf)
                rc[n, hi, j] = plus(rc[n, hi, j], own[slot, hi, j])
                return carry

            lax.fori_loop(0, nh * nf, add, 0)

        @pl.when(n >= 2 * group)
        def _():
            def add(i, carry):
                hi, j = i // nf, lax.rem(i, nf)
                rc[n, hi, j] = plus(rc[n, hi, j], ga[s, r, hi, j, at.core])
                return carry

            lax.fori_loop(0, nh * nf, add, 0)

        for k in range(1, nf):
            x_copy(n, k).start()

    def stage_x(n):
        for k in range(1, nf):
            x_copy(n, k).wait_recv()

        def add(hi, carry):
            if nf == 2:
                rx[n, 0, hi] = rc[n, hi, at.x] + rx[n, 0, hi]
            else:
                total = rc[n, hi, at.x].astype(F32)
                for k in range(nf - 1):
                    total += rx[n, k, hi].astype(F32)
                rx[n, 0, hi] = total.astype(BF)
            return carry

        lax.fori_loop(0, nh, add, 0)
        for m in range(1, nh):
            y_copy(n, m).start()

    def stage_y(n):
        for m in range(1, nh):
            y_copy(n, m).wait_recv()
        total = rx[n, 0, at.hi]
        for m in range(nh - 1):
            total = plus(total, ry[n, m])
        ry[n, 0] = total

        @pl.when(outer)
        def _():
            z_copy(n).start()

    def stage_z(n):
        @pl.when(inner)
        def _():
            z_copy(n).wait_recv()
            ry[n, 0] = plus(ry[n, 0], rz[n])
            zi_copy(n).start()

    def stage_zi(n):
        @pl.when(inner)
        def _():
            zi_copy(n).wait_recv()
            g_start(n, plus(ry[n, 0], ri[n]))

    def stage_g(n):
        @pl.when(outer)
        def _():
            g_whole(n).wait_recv()

        ay_start(n)

    def stage_ay(n):
        for m in range(1, nh):
            ay_whole(n, m).wait_recv()
        ac_start(n)

    lo = lax.broadcasted_iota(jnp.int32, (rows, 128), 1) < 64
    pairs = width // 128

    def unit(index):
        i, p = index // pairs, lax.rem(index, pairs)
        there = 1 - b1 - i + 2 * i * b1
        keys = pl.ds(pl.multiple_of(there * (2 * rows), 128), 2 * rows)
        col = pl.ds(pl.multiple_of(p * 128, 128), 128)
        k2 = k_ref[keys, col]
        v2 = v_ref[keys, col]
        q2 = q_ref[:, col]
        dc2 = dc_ref[:, col]
        both = dc2.astype(F32) * ctx_ref[:, col]
        lse2 = lse_ref[p]
        dq, dk, dv = [], None, None
        for h in range(2):
            mask = lo if h == 0 else jnp.logical_not(lo)
            qm = jnp.where(mask, q2, jnp.zeros_like(q2))
            dmask = jnp.where(mask, dc2, jnp.zeros_like(q2))
            lse = lse2[:, 0:1] if h == 0 else lse2[:, 64:65]
            dot = jnp.sum(jnp.where(mask, both, 0.0), axis=-1, keepdims=True)
            probs = jnp.exp(nt(qm, k2) * score_scale - lse)
            slopes = nt(dmask, v2)
            dscore = (probs * (slopes - dot) * score_scale).astype(BF)
            dq.append(nn(dscore, k2))
            a = nn(dmask.T, probs.astype(BF))
            b = nn(qm.T, dscore)
            dv = a if dv is None else dv + a
            dk = b if dk is None else dk + b
        dq2 = jnp.where(lo, dq[0], dq[1])

        @pl.when(i == 0)
        def _():
            dqa[:, col] = dq2

        @pl.when(i > 0)
        def _():
            dqa[:, col] += dq2

        dkt[col, keys] = dk.astype(BF)
        dvt[col, keys] = dv.astype(BF)

    def weights(s):
        frames = pl.ds(pl.multiple_of(at.z * rows, 128), rows)
        for hi in range(nh):
            col = lanes(s, hi)
            dq2 = dqa[:, col]
            vb[2, 0:1, col] = jnp.sum(dq2, axis=0, keepdims=True)
            dq2 = dq2.astype(BF)
            dk2 = dkt[col, :]
            dv2 = dvt[col, :]
            for j in range(nf):
                for part in range(2):
                    for r in range(split):
                        here = pl.ds((2 * j + part) * half + r * q, q)
                        ga[s, r, hi, j, part, 0, 0] = nn(ht_ref[here, frames], dq2).astype(BF)
                        ga[s, r, hi, j, part, 0, 1] = nt(ht_ref[here, :], dk2).astype(BF)
                        ga[s, r, hi, j, part, 1, 0] = nt(ht_ref[here, :], dv2).astype(BF)

    pieces = 16
    per_step = 2
    lag = 1
    low = 1 - b1

    def part_of(t):
        return pl.ds(pl.multiple_of(t * (width // pieces), 16), width // pieces)

    def da_copy(t):
        return remote(
            dhs.at[pl.ds(2 * low, 2), part_of(t)], dra.at[:, part_of(t)], das.at[t], dar.at[t], near
        )

    def dn_start(t):
        remote(
            dhs.at[at.z + 1 - 2 * b0, part_of(t)], drc.at[part_of(t)], dns.at[0], dnr.at[0], near
        ).start()

    def dn_whole():
        return remote(dhs.at[0], drc, dns.at[0], dnr.at[0], near)

    def db_copy(t):
        return remote(
            dhs.at[pl.ds(2 * low, 2), part_of(t)], drb.at[:, part_of(t)], dbs.at[t], dbr.at[t], across
        )

    def dc_copy(t):
        return remote(dhs.at[3 * b1, part_of(t)], drc.at[part_of(t)], dcs.at[t], dcr.at[t], near)

    def d_stage(i, t):
        part = part_of(t)
        if i == 0:
            @pl.when(outer)
            def _():
                da_copy(t).start()
        elif i == 1:
            @pl.when(inner)
            def _():
                da_copy(t).wait_recv()
                for j in range(2):
                    dhs[2 * low + j, part] = dhs[2 * low + j, part] + dra[j, part]
                db_copy(t).start()
        elif i == 2:
            @pl.when(inner)
            def _():
                db_copy(t).wait_recv()
                for j in range(2):
                    dhs[2 * b1 + j, part] = dhs[2 * b1 + j, part] + drb[j, part]
                dc_copy(t).start()
        else:
            @pl.when(outer)
            def _():
                dc_copy(t).wait_recv()

    def spread(i):
        there = 1 - b1 - i + 2 * i * b1
        for ub in range(2):
            part = pl.ds(pl.multiple_of((2 * there + ub) * rows, 128), rows)
            dhs[2 * there + ub] = (nn(w_ref[1], dkt[:, part]) + nn(w_ref[2], dvt[:, part])).astype(BF)

    def first_norm():
        @pl.when(inner)
        def _():
            dn_whole().wait_recv()

        total = dhs[at.z].astype(F32) + nt(w_ref[0], dqa[...].astype(BF))
        total += drc[...].astype(F32)
        total = total.T
        normed, inverse = normalize(frames_ref[...])
        scaled = total * vec_ref[0:1, :]
        centred = (
            scaled
            - jnp.mean(scaled, axis=-1, keepdims=True)
            - normed * jnp.mean(scaled * normed, axis=-1, keepdims=True)
        )
        ig_ref[...] = gm_ref[...] + inverse * centred
        vb[1] = gv_ref[...]
        vb[1, 0:1, :] = jnp.sum(total * normed, axis=0, keepdims=True)
        vb[1, 1:2, :] = jnp.sum(total, axis=0, keepdims=True)
        vb[1, 2:3, :] = vb[2, 0:1, :]

    def v_core():
        return remote(vb.at[1], vb.at[0], vs.at[0], vr.at[0], at.sibling())

    def v_x(k):
        return remote(vx.at[at.x], vx.at[at.x], vs.at[k], vr.at[k], at.x_peer(k))

    def v_y(m):
        return remote(vy.at[at.hi], vy.at[at.hi], vs.at[nf + m], vr.at[nf + m], at.y_peer(m))

    def v_z(k):
        return remote(
            vz.at[at.z], vz.at[at.z], vs.at[nf + nh + k], vr.at[nf + nh + k], at.z_peer(k)
        )

    def v_step(i):
        if i == 0:
            v_core().start()
        elif i == 1:
            v_core().wait_recv()
            vx[at.x] = vb[0] + vb[1]
            for k in range(1, nf):
                v_x(k).start()
        elif i == 2:
            for k in range(1, nf):
                v_x(k).wait_recv()
            total = vx[0]
            for j in range(1, nf):
                total += vx[j]
            vy[at.hi] = total
            for m in range(1, nh):
                v_y(m).start()
        elif i == 3:
            for m in range(1, nh):
                v_y(m).wait_recv()
            total = vy[0]
            for j in range(1, nh):
                total += vy[j]
            vz[at.z] = total
            for k in range(1, ns):
                v_z(k).start()
        else:
            for k in range(1, ns):
                v_z(k).wait_recv()
            total = vz[0]
            for j in range(1, ns):
                total += vz[j]
            ov_ref[...] = total

    ready = group
    each = -(-2 * pairs // ready)
    done = [-(-pairs * (i + 1) // each) - 1 for i in range(2)]
    away = done[0] + 1
    slack = 2
    turns = pieces // per_step
    rest = away + turns
    norm = max(away + turns + 3 * slack, rest + turns // 2 + 1, chunks - 2)
    stages = (stage_x, stage_y, stage_z, stage_zi, stage_g, stage_ay)
    last = max(chunks + lag * len(stages), norm + 6)
    for n in range(4):
        c_send(n)

    def step(n, carry):
        for k in range(2):
            @pl.when(2 * n + k < 2 * group)
            def _(k=k):
                stage_c(2 * n + k)

                @pl.when(2 * n + k + 4 < 2 * group)
                def _():
                    c_send(2 * n + k + 4)

        @pl.when(jnp.logical_and(n >= ready + 1, n < ready + 1 + per))
        def _():
            for r in range(split):
                stage_c(2 * group + (n - ready - 1) * split + r)

        @pl.when(n < ready)
        def _():
            def one(k, carry):
                @pl.when(n * each + k < 2 * pairs)
                def _():
                    unit(n * each + k)

                return carry

            lax.fori_loop(0, each, one, 0)

        @pl.when(jnp.logical_or(n == done[0], n == done[1]))
        def _():
            spread(n // done[1])

        @pl.when(n == norm)
        def _():
            first_norm()

        @pl.when(n == ready)
        def _():
            whole = ga.at[:, :, :, :, :, 1, 1]
            pltpu.make_async_copy(whole, whole, os.at[4]).wait()

        @pl.when(jnp.logical_and(n >= ready, n < ready + per))
        def _():
            weights(n - ready)
            for r in range(split):
                c_send(2 * group + (n - ready) * split + r)

        for i, stage in enumerate(stages):
            @pl.when(jnp.logical_and(n >= lag * i, n < chunks + lag * i))
            def _(i=i, stage=stage):
                stage(n - lag * i)

        for i in range(4):
            first = away + slack * i

            @pl.when(jnp.logical_and(n >= first, n < first + turns))
            def _(i=i, first=first):
                for t in range(per_step):
                    d_stage(i, (n - first) * per_step + t)

        @pl.when(jnp.logical_and(outer, jnp.logical_and(n >= rest, n < rest + turns // 2)))
        def _():
            for t in range(2 * per_step):
                dn_start((n - rest) * (2 * per_step) + t)

        for i in range(5):
            @pl.when(n == norm + i)
            def _(i=i):
                v_step(i)

        return carry

    lax.fori_loop(0, last, step, 0)
    for n in range(chunks):
        ac_whole(n).wait()

    def drain(n, carry):
        c_whole(n).wait_send()

        @pl.when(outer)
        def _():
            z_copy(n).wait_send()

        @pl.when(inner)
        def _():
            zi_copy(n).wait_send()
            g_whole(n).wait_send()

        for k in range(1, nf):
            x_copy(n, k).wait_send()
        for m in range(1, nh):
            y_copy(n, m).wait_send()
            ay_whole(n, m).wait_send()
        return carry

    lax.fori_loop(0, chunks, drain, 0)

    @pl.when(outer)
    def _():
        dn_whole().wait_send()

        def sent(t, carry):
            da_copy(t).wait_send()
            return carry

        lax.fori_loop(0, pieces, sent, 0)

    @pl.when(inner)
    def _():
        def sent(t, carry):
            db_copy(t).wait_send()
            dc_copy(t).wait_send()
            return carry

        lax.fori_loop(0, pieces, sent, 0)

    for k in range(1, ns):
        v_z(k).wait_send()
    for k in range(1, nf):
        v_x(k).wait_send()
    for m in range(1, nh):
        v_y(m).wait_send()
    v_core().wait_send()


def back_all(sizes, q, k, v, dc, ctx, lse, ht, w, gm, frames, vec, gv, gc, ge, go):
    nd, nf, ns = sizes
    nh = nd // 2
    rows, width = q.shape
    shard = go.shape[1]
    half = shard // 2
    every = k.shape[0]
    split = 2 if half % 32 == 0 else 1
    strip = half // split
    per = width // nh // 128
    chunks = 3 * per * split
    xn, yn = max(nf - 1, 1), max(nh - 1, 1)
    dma = pltpu.SemaphoreType.DMA
    anywhere = pl.BlockSpec(memory_space=pl.ANY)
    return pl.pallas_call(
        functools.partial(back_kernel, sizes),
        out_shape=(
            jax.ShapeDtypeStruct((2, 2, shard, width), BF),
            jax.ShapeDtypeStruct((shard, 4 * width), BF),
            jax.ShapeDtypeStruct((2, 2, shard, width), BF),
            jax.ShapeDtypeStruct((rows, width), F32),
            jax.ShapeDtypeStruct((16, width), F32),
        ),
        in_specs=[vmem()] * 12 + [anywhere] * 3,
        out_specs=(vmem(),) * 5,
        scratch_shapes=[
            pltpu.VMEM((per, split, nh, nf, 2, 2, 2, strip, 128), BF),
            pltpu.VMEM((4, nh, nf, 2, 2, strip, 128), BF),
            pltpu.VMEM((chunks, nh, nf, 2, 2, strip, 128), BF),
            pltpu.VMEM((chunks, xn, nh, 2, 2, strip, 128), BF),
            pltpu.VMEM((chunks, yn, 2, 2, strip, 128), BF),
            pltpu.VMEM((chunks, 2, 2, strip, 128), BF),
            pltpu.VMEM((chunks, 2, 2, strip, 128), BF),
            pltpu.VMEM((width, every), BF),
            pltpu.VMEM((width, every), BF),
            pltpu.VMEM((rows, width), F32),
            pltpu.VMEM((ns, width, rows), BF),
            pltpu.VMEM((2, width, rows), BF),
            pltpu.VMEM((2, width, rows), BF),
            pltpu.VMEM((width, rows), BF),
            pltpu.VMEM((3, 16, width), F32),
            pltpu.VMEM((nf, 16, width), F32),
            pltpu.VMEM((nh, 16, width), F32),
            pltpu.VMEM((ns, 16, width), F32),
            dma((5,)),
            dma((chunks,)), dma((chunks,)),
            dma((chunks, xn)), dma((chunks, xn)),
            dma((chunks, yn)), dma((chunks, yn)),
            dma((chunks,)), dma((chunks,)),
            dma((chunks,)), dma((chunks,)),
            dma((chunks,)), dma((chunks,)),
            dma((chunks, yn)), dma((chunks, yn)),
            dma((chunks,)), dma((chunks,)),
            dma((16,)), dma((16,)),
            dma((16,)), dma((16,)),
            dma((16,)), dma((16,)),
            dma((1,)), dma((1,)),
            dma((nf + nh + ns,)), dma((nf + nh + ns,)),
        ],
        name="back",
        compiler_params=pltpu.CompilerParams(
            collective_id=1, has_side_effects=True, vmem_limit_bytes=67043328
        ),
    )(q, k, v, dc, ctx, lse, ht, w, gm, frames, vec, gv, gc, ge, go)


def feed_kernel(
    ctx_ref, frames_ref, cot_ref, vec_ref, wo_ref, win_ref, wout_ref,
    fo_ref, gm_ref, dc_ref, gi_ref, gout_ref, go_ref, gv_ref,
    mid, h2, h2t, dyb, acc, dh2,
):
    b = pl.program_id(0)

    @pl.when(b == 0)
    def _():
        middle = frames_ref[...] + nn(ctx_ref[...].astype(BF), wo_ref[...]) + vec_ref[4:5, :]
        mid[...] = middle
        normed, _ = normalize(middle)
        hidden = (normed * vec_ref[5:6, :] + vec_ref[6:7, :]).astype(BF)
        h2[...] = hidden
        h2t[...] = hidden.T
        dyb[...] = cot_ref[...].astype(BF)
        acc[...] = middle + vec_ref[7:8, :]
        dh2[...] = jnp.zeros_like(dh2)
        gv_ref[...] = jnp.zeros_like(gv_ref)

    up = dyb[...]
    u = nn(h2[...], win_ref[...]) + vec_ref[pl.ds(8 + b, 1), :]
    phi = 0.5 * (1.0 + lax.erf(u * 0.7071067811865476))
    activated = (u * phi).astype(BF)
    acc[...] += nn(activated, wout_ref[...])
    gout_ref[...] = tn(activated, up).astype(BF)
    du = nt(up, wout_ref[...]) * (phi + u * jnp.exp(-0.5 * u * u) * 0.3989422804014327)
    gv_ref[pl.ds(8 + b, 1), :] = jnp.sum(du, axis=0, keepdims=True)
    dub = du.astype(BF)
    gi_ref[...] = nn(h2t[...], dub).astype(BF)
    dh2[...] += nt(dub, win_ref[...])

    @pl.when(b == pl.num_programs(0) - 1)
    def _():
        fo_ref[...] = acc[...]
        normed, inverse = normalize(mid[...])
        back, gain, offset = norm_back(dh2[...], normed, inverse, vec_ref[5:6, :])
        upstream = cot_ref[...]
        middle = upstream + back
        gm_ref[...] = middle
        dab = middle.astype(BF)
        go_ref[...] = tn(ctx_ref[...].astype(BF), dab).astype(BF)
        dctx = nt(dab, wo_ref[...]).astype(BF)
        dc_ref[...] = dctx
        gv_ref[3:4, :] = jnp.sum(dctx.astype(F32), axis=0, keepdims=True)
        gv_ref[4:5, :] = jnp.sum(middle, axis=0, keepdims=True)
        gv_ref[5:6, :] = gain[None]
        gv_ref[6:7, :] = offset[None]
        gv_ref[7:8, :] = jnp.sum(upstream, axis=0, keepdims=True)


def feed_all(ctx, frames, cot, vec, aw, ew, cw):
    rows, width = frames.shape
    full = ew.shape[1]
    whole = lambda shape: pl.BlockSpec(shape, lambda b: (0,) * len(shape))
    blocks = full // width
    return pl.pallas_call(
        feed_kernel,
        grid=(blocks,),
        out_shape=(
            jax.ShapeDtypeStruct((rows, width), F32),
            jax.ShapeDtypeStruct((rows, width), F32),
            jax.ShapeDtypeStruct((rows, width), BF),
            jax.ShapeDtypeStruct((width, full), BF),
            jax.ShapeDtypeStruct((full, width), BF),
            jax.ShapeDtypeStruct((width, width), BF),
            jax.ShapeDtypeStruct((16, width), F32),
        ),
        in_specs=[
            whole((rows, width)), whole((rows, width)), whole((rows, width)), whole((16, width)),
            pl.BlockSpec((None, width, width), lambda b: (3, 0, 0)),
            pl.BlockSpec((width, width), lambda b: (0, b)),
            pl.BlockSpec((width, width), lambda b: (b, 0)),
        ],
        out_specs=(
            whole((rows, width)), whole((rows, width)), whole((rows, width)),
            pl.BlockSpec((width, width), lambda b: (0, b)),
            pl.BlockSpec((width, width), lambda b: (b, 0)),
            whole((width, width)), whole((16, width)),
        ),
        scratch_shapes=[
            pltpu.VMEM((rows, width), F32),
            pltpu.VMEM((rows, width), BF),
            pltpu.VMEM((width, rows), BF),
            pltpu.VMEM((rows, width), BF),
            pltpu.VMEM((rows, width), F32),
            pltpu.VMEM((rows, width), F32),
        ],
        name="feed",
        compiler_params=pltpu.CompilerParams(vmem_limit_bytes=67043328),
    )(ctx, frames, cot, vec, aw, ew, cw)


def on_device(
    sizes,
    frames_in,
    cotangent,
    attention_weight,
    expand_weight,
    contract_weight,
    vectors,
    first_attention,
    first_expand,
    first_contract,
    first_vectors,
    second_attention,
    second_expand,
    second_contract,
    second_vectors,
):
    nd, nf, ns = sizes
    frames = frames_in[0]
    upstream = cotangent[0]
    rows, width = frames.shape
    shard = attention_weight.shape[1]
    full = expand_weight.shape[1]
    aw, ew, cw, vec, h_turned, queries, key_rows, value_rows, context_wide, log_total = front_all(
        sizes, frames, vectors, attention_weight, expand_weight, contract_weight
    )
    frames_out, grad_middle, grad_context, grad_expand, grad_contract, grad_output_w, gv = feed_all(
        context_wide, frames, upstream, vec, aw, ew, cw
    )
    oc, oe, oa, input_gradient, gv_sum = back_all(
        sizes,
        queries,
        key_rows,
        value_rows,
        grad_context,
        context_wide,
        log_total,
        h_turned,
        aw,
        grad_middle,
        frames,
        vec,
        gv,
        grad_contract.reshape(nf, 4, shard, width),
        grad_expand.reshape(nf, shard, full),
        grad_output_w.reshape(nf, shard, width),
    )
    owned_vec = lax.dynamic_slice_in_dim(
        gv_sum[:12], lax.axis_index("fsdp") * (width // nf), width // nf, 1
    )
    owned = (
        oa.reshape(4, shard, width).astype(F32),
        oe.astype(F32),
        oc.reshape(4 * shard, width).astype(F32),
    )
    attention_out = (owned[0],) + adam_update(
        attention_weight, owned[0], first_attention, second_attention, rate_matrix, decay_matrix
    )
    expand_out = (owned[1],) + adam_update(
        expand_weight, owned[1], first_expand, second_expand, rate_matrix, decay_matrix
    )
    contract_out = (owned[2],) + adam_update(
        contract_weight, owned[2], first_contract, second_contract, rate_matrix, decay_matrix
    )
    vector_out = (owned_vec,) + adam_update(
        vectors, owned_vec, first_vectors, second_vectors, rate_vector, 0.0
    )
    result = [frames_out[None], input_gradient[None]]
    for i in range(4):
        result += [attention_out[i], expand_out[i], contract_out[i], vector_out[i]]
    return tuple(result)


def solution(mesh):
    sizes = (mesh.shape["dp"], mesh.shape["fsdp"], mesh.shape["seq"])
    data = P(("dp", "fsdp"), "seq", None)
    state = (P(None, "fsdp", None), P("fsdp", None), P("fsdp", None), P(None, "fsdp"))
    return jax.shard_map(
        functools.partial(on_device, sizes),
        mesh=mesh,
        in_specs=(data, data) + state * 3,
        out_specs=(data, data) + state * 4,
        check_vma=False,
    )
```

```python
import functools

import jax
import jax.numpy as jnp
from jax import lax
from jax.experimental import pallas as pl
from jax.experimental.pallas import tpu as pltpu
from jax.sharding import PartitionSpec as P

HEADS = 12
norm_eps = 1e-05
beta_one = 0.9
beta_two = 0.999
adam_eps = 1e-08
adam_count = 5.0
rate_matrix = 0.02
rate_vector = 0.1
decay_matrix = 0.1
score_scale = 0.125
VMEM_LIMIT = 60 << 20
MESH = pl.DeviceIdType.MESH
BF = jnp.bfloat16
F32 = jnp.float32


def nt(left, right):
    return lax.dot_general(left, right, (((1,), (1,)), ((), ())), preferred_element_type=F32)


def nn(left, right):
    return lax.dot_general(left, right, (((1,), (0,)), ((), ())), preferred_element_type=F32)


def tn(left, right):
    return lax.dot_general(left, right, (((0,), (0,)), ((), ())), preferred_element_type=F32)


def vmem():
    return pl.BlockSpec(memory_space=pltpu.VMEM)


def normalize(values):
    center = values - jnp.mean(values, axis=-1, keepdims=True)
    inverse = lax.rsqrt(jnp.mean(center * center, axis=-1, keepdims=True) + norm_eps)
    return center * inverse, inverse


def norm_back(upstream, normed, inverse, gain):
    scaled = upstream * gain
    inner = (
        scaled
        - jnp.mean(scaled, axis=-1, keepdims=True)
        - normed * jnp.mean(scaled * normed, axis=-1, keepdims=True)
    )
    return (inverse * inner, jnp.sum(upstream * normed, axis=0), jnp.sum(upstream, axis=0))


def adam_update(weight, gradient, first, second, rate, decay):
    first_new = beta_one * first + (1.0 - beta_one) * gradient
    second_new = beta_two * second + (1.0 - beta_two) * gradient * gradient
    first_hat = first_new / (1.0 - beta_one**adam_count)
    second_hat = second_new / (1.0 - beta_two**adam_count)
    updated = weight - rate * (first_hat / (jnp.sqrt(second_hat) + adam_eps) + decay * weight)
    return (updated, first_new, second_new)


class Place:
    def __init__(self, sizes):
        self.nd, self.nf, self.ns = sizes
        self.nh = self.nd // 2
        self.dp = lax.axis_index("dp")
        self.x = lax.axis_index("fsdp")
        self.z = lax.axis_index("seq")
        self.core = lax.rem(self.dp, 2)
        self.hi = self.dp // 2

    def sibling(self):
        return {"dp": self.hi * 2 + 1 - self.core}

    def x_peer(self, k):
        return {"fsdp": lax.rem(self.x + k, self.nf)}

    def y_hi(self, k):
        return lax.rem(self.hi + k, self.nh)

    def y_peer(self, k):
        return {"dp": self.y_hi(k) * 2 + self.core}

    def z_at(self, k):
        return lax.rem(self.z + k + self.ns, self.ns)

    def z_peer(self, k):
        return {"seq": self.z_at(k)}

    def everyone(self):
        out = [self.sibling()]
        out += [self.x_peer(k) for k in range(1, self.nf)]
        out += [self.y_peer(k) for k in range(1, self.nh)]
        out += [self.z_peer(k) for k in range(1, self.ns)]
        return out

    def barrier(self):
        sem = pltpu.get_barrier_semaphore()
        peers = self.everyone()
        for peer in peers:
            pl.semaphore_signal(sem, inc=1, device_id=peer, device_id_type=MESH)
        pl.semaphore_wait(sem, len(peers))


def remote(src, dst, send, recv, peer):
    return pltpu.make_async_remote_copy(
        src_ref=src, dst_ref=dst, send_sem=send, recv_sem=recv, device_id=peer, device_id_type=MESH
    )


def front_kernel(
    sizes, frames_ref, vec_ref, aw_ref, ew_ref, cw_ref,
    a_out, e_ref, c_ref, vec_out, ht_out, q_out, k_out, v_out, ctx_out, lse_ref,
    a_ref, v_buf, h_ref, ht, q_buf, k_buf, v_buf2, ctx_buf, af, ef, eb, cb, kept, stat,
    ls, xs, xr, ys, yr, s1s, s1r, s2s, s2r, vs, vr, rs, hs, hr,
):
    at = Place(sizes)
    nf, nh, ns = at.nf, at.nh, at.ns
    rows, width = frames_ref.shape
    shard = aw_ref.shape[1]
    half = shard // 2
    deep = cb.shape[0]
    b0 = lax.rem(at.z, 2)
    b1 = at.z // 2

    def load(i, src, dst):
        return pltpu.make_async_copy(src, dst, ls.at[i])

    loads = [
        load(0, aw_ref.at[pl.ds(0, 3)], af.at[pl.ds(0, 3)]),
        load(1, aw_ref.at[pl.ds(3, 1)], af.at[pl.ds(3, 1)]),
        load(2, ew_ref, ef),
        load(3, cw_ref, af),
    ]
    for copy in loads[:3]:
        copy.start()
    at.barrier()
    v_buf[at.x] = jnp.zeros(v_buf.shape[1:], BF)
    v_buf[at.x, 0 : vec_ref.shape[0], :] = vec_ref[...].astype(BF)
    vec_copies = []
    for k in range(1, nf):
        copy = remote(v_buf.at[at.x], v_buf.at[at.x], vs.at[k], vr.at[k], at.x_peer(k))
        copy.start()
        vec_copies.append(copy)

    order = (1, 2, 0, 3)

    def view(chunk, j, hi, core, own=False):
        cols = width // nh
        if chunk < 4:
            return a_ref.at[
                order[chunk],
                pl.ds(pl.multiple_of(j * shard + core * half, 16), half),
                pl.ds(pl.multiple_of(hi * cols, 128), cols),
            ]
        if chunk < 8:
            start = 0 if own else j * shard
            wide = eb.shape[1] // nh
            return (eb if own else e_ref).at[
                pl.ds(pl.multiple_of(start + core * half, 16), half),
                pl.ds(pl.multiple_of(hi * wide + (chunk - 4) * (wide // 4), 128), wide // 4),
            ]
        start = 0 if own else j * deep
        tall = deep // 8
        return (cb if own else c_ref).at[
            pl.ds(pl.multiple_of(start + core * (deep // 2) + (chunk - 8) * tall, 16), tall),
            pl.ds(pl.multiple_of(hi * cols, 128), cols),
        ]

    own = pl.multiple_of(at.x * shard, 16)
    x_copies = {}

    def send_chunk(chunk):
        for k in range(1, nf):
            copy = remote(
                view(chunk, at.x, at.hi, at.core, True), view(chunk, at.x, at.hi, at.core),
                xs.at[chunk, k - 1], xr.at[chunk, k - 1], at.x_peer(k),
            )
            copy.start()
            x_copies[chunk, k] = copy

    loads[0].wait()
    for i, u in enumerate(order[:3]):
        a_ref[u, pl.ds(own, shard), :] = af[u].astype(BF)
        send_chunk(i)
    normed, _ = normalize(frames_ref[...])
    for copy in vec_copies:
        copy.wait()
    vec = jnp.concatenate([v_buf[j] for j in range(nf)], axis=1).astype(F32)
    vec_out[...] = vec
    mine = pl.ds(pl.multiple_of(at.z * rows, 128), rows)
    hidden = (normed * vec[0:1] + vec[1:2]).astype(BF)
    h_ref[mine, :] = hidden

    def block(b):
        return h_ref.at[pl.ds(pl.multiple_of(b * rows, 128), rows), :]

    def to_right(b):
        return remote(block(b), block(b), rs.at[b], hr.at[b], {"seq": at.z + 1})

    def to_left(b):
        return remote(block(b), block(b), hs.at[b], hr.at[b], {"seq": at.z - 1})

    @pl.when(at.z < ns - 1)
    def _():
        to_right(at.z).start()

    @pl.when(at.z > 0)
    def _():
        to_left(at.z).start()

    loads[1].wait()
    a_ref[3, pl.ds(own, shard), :] = af[3].astype(BF)
    loads[3].start()
    send_chunk(3)
    loads[2].wait()
    eb[...] = ef[...].astype(BF)
    for i in range(4, 8):
        send_chunk(i)
    loads[3].wait()
    for u in range(4):
        cb[pl.ds(u * shard, shard), :] = af[u].astype(BF)
    for i in range(8, 12):
        send_chunk(i)
    stores = [
        load(4, eb, e_ref.at[pl.ds(own, shard), :]),
        load(5, cb, c_ref.at[pl.ds(pl.multiple_of(at.x * deep, 16), deep), :]),
    ]
    for copy in stores:
        copy.start()
    ht[:, mine] = hidden.T

    def first_copy(chunk, k):
        j = lax.rem(at.x - k + nf, nf)
        piece = view(chunk, j, at.hi, at.core)
        return remote(piece, piece, s1s.at[chunk, k - 1], s1r.at[chunk, k - 1], at.sibling())

    def y_copy(chunk, k, m):
        j = lax.rem(at.x - k + nf, nf)
        piece = view(chunk, j, at.hi, at.core)
        return remote(piece, piece, ys.at[chunk, k - 1, m - 1], yr.at[chunk, k - 1, m - 1], at.y_peer(m))

    def second_copy(chunk, k, m):
        j = lax.rem(at.x - k + nf, nf)
        piece = view(chunk, j, lax.rem(at.hi - m + nh, nh), at.core)
        return remote(piece, piece, s2s.at[chunk, k - 1, m - 1], s2r.at[chunk, k - 1, m - 1], at.sibling())

    def forward(chunk):
        for k in range(1, nf):
            x_copies[chunk, k].wait_recv()
            first_copy(chunk, k).start()
            for m in range(1, nh):
                y_copy(chunk, k, m).start()

    def relay(chunk):
        for k in range(1, nf):
            for m in range(1, nh):
                y_copy(chunk, k, m).wait_recv()
                second_copy(chunk, k, m).start()

    def arrived(chunk):
        for k in range(1, nf):
            first_copy(chunk, k).wait_recv()
            for m in range(1, nh):
                second_copy(chunk, k, m).wait_recv()

    def rows_of(b):
        part = pl.ds(pl.multiple_of(b * rows, 128), rows)
        k_buf[part, :] = nn(h_ref[part, :], a_ref[1]).astype(BF)
        v_buf2[part, :] = (nn(h_ref[part, :], a_ref[2]) + vec[3:4]).astype(BF)

    def turn(b):
        part = pl.ds(pl.multiple_of(b * rows, 128), rows)
        ht[:, part] = h_ref[part, :].T

    def hop(s):
        b = at.z - s
        d = at.z + s

        @pl.when(b >= 0)
        def _():
            to_right(b).wait_recv()

            @pl.when(at.z < ns - 1)
            def _():
                to_right(b).start()

        @pl.when(d < ns)
        def _():
            to_left(d).wait_recv()

            @pl.when(at.z > 0)
            def _():
                to_left(d).start()

    lane = lax.broadcasted_iota(jnp.int32, (rows, 128), 1)
    lo = lane < 64

    def scores(p, h, b):
        col = pl.ds(pl.multiple_of(p * 128, 128), 128)
        part = pl.ds(pl.multiple_of(b * rows, 128), rows)
        q2 = q_buf[:, col]
        mask = lo if h == 0 else jnp.logical_not(lo)
        s = nt(jnp.where(mask, q2, jnp.zeros_like(q2)), k_buf[part, col]) * score_scale
        largest = jnp.max(s, axis=-1, keepdims=True)
        e = jnp.exp(s - largest)
        return e, largest, jnp.sum(e, axis=-1, keepdims=True)

    assert ns == 4
    blocks = (at.z, at.z + 1 - 2 * b0, 2 - b1, 3 - 3 * b1)

    def tick(i):
        if i < 12:
            forward(i)
        if i > 0:
            relay(i - 1)

    def begin(i, ticks):
        b = blocks[i]
        rows_of(b)

        def pair(p, carry):
            found = []
            for h in range(2):
                e, largest, total = scores(p, h, b)
                kept[i, 2 * p + h] = e
                found += [largest, total]
            stat[i, p] = jnp.where(
                lo, jnp.where(lane < 32, found[0], found[1]), jnp.where(lane < 96, found[2], found[3])
            )
            for when, which in ticks:
                @pl.when(p == when)
                def _(which=which):
                    tick(which)

            return carry

        lax.fori_loop(0, width // 128, pair, 0)

    tick(0)
    tick(1)
    tick(2)
    hop(1)
    tick(3)
    for i in range(3):
        arrived(i)
    q_buf[...] = (nn(h_ref[mine, :], a_ref[0]) + vec[2:3]).astype(BF)
    stores.append(load(6, q_buf, q_out))
    stores[-1].start()
    tick(4)
    begin(0, ((2, 5), (5, 6)))
    hop(2)
    begin(1, ((1, 7), (4, 8)))
    turn(blocks[1])
    begin(2, ((0, 9), (3, 10)))
    turn(blocks[2])
    hop(3)
    rows_of(blocks[3])
    turn(blocks[3])
    tick(11)
    arrived(3)
    for i, (src, dst) in enumerate(((a_ref, a_out), (ht, ht_out), (k_buf, k_out), (v_buf2, v_out))):
        stores.append(load(7 + i, src, dst))
        stores[-1].start()
    def pair(p, carry):
        col = pl.ds(pl.multiple_of(p * 128, 128), 128)
        ctx, lse = [], []
        for h in range(2):
            e, peak, count = scores(p, h, blocks[3])
            peaks = [stat[i, p][:, 64 * h : 64 * h + 1] for i in range(3)] + [peak]
            counts = [stat[i, p][:, 64 * h + 32 : 64 * h + 33] for i in range(3)] + [count]
            largest = functools.reduce(jnp.maximum, peaks)
            shares = [jnp.exp(each - largest) for each in peaks]
            total = sum(share * each for share, each in zip(shares, counts))
            inverse = 1.0 / total
            out = None
            for i in range(4):
                part = pl.ds(pl.multiple_of(blocks[i] * rows, 128), rows)
                found = kept[i, 2 * p + h] if i < 3 else e
                term = nn((found * (shares[i] * inverse)).astype(BF), v_buf2[part, col])
                out = term if out is None else out + term
            ctx.append(out)
            lse.append(largest + jnp.log(total))
        ctx_buf[:, col] = jnp.where(lo, ctx[0], ctx[1])
        lse_ref[p] = jnp.where(lo, lse[0], lse[1])

        @pl.when(p == 1)
        def _():
            tick(12)

        return carry

    lax.fori_loop(0, width // 128, pair, 0)
    stores.append(load(11, ctx_buf, ctx_out))
    stores[-1].start()
    for i in range(4, 12):
        arrived(i)
    for copy in stores:
        copy.wait()
    for copy in x_copies.values():
        copy.wait_send()
    for chunk in range(12):
        for k in range(1, nf):
            first_copy(chunk, k).wait_send()
            for m in range(1, nh):
                y_copy(chunk, k, m).wait_send()
                second_copy(chunk, k, m).wait_send()
    for b in range(ns):
        @pl.when(jnp.logical_and(b <= at.z, at.z < ns - 1))
        def _():
            to_right(b).wait_send()

        @pl.when(jnp.logical_and(b >= at.z, at.z > 0))
        def _():
            to_left(b).wait_send()


def front_all(sizes, frames, vec, aw, ew, cw):
    nd, nf, ns = sizes
    nh = nd // 2
    rows, width = frames.shape
    shard, full = ew.shape
    deep = cw.shape[0]
    every = rows * ns
    dma = pltpu.SemaphoreType.DMA
    anywhere = pl.BlockSpec(memory_space=pl.ANY)
    return pl.pallas_call(
        functools.partial(front_kernel, sizes),
        out_shape=(
            jax.ShapeDtypeStruct((4, width, width), BF),
            jax.ShapeDtypeStruct((width, full), BF),
            jax.ShapeDtypeStruct((deep * nf, width), BF),
            jax.ShapeDtypeStruct((16, width), F32),
            jax.ShapeDtypeStruct((width, every), BF),
            jax.ShapeDtypeStruct((rows, width), BF),
            jax.ShapeDtypeStruct((every, width), BF),
            jax.ShapeDtypeStruct((every, width), BF),
            jax.ShapeDtypeStruct((rows, width), F32),
            jax.ShapeDtypeStruct((width // 128, rows, 128), F32),
        ),
        in_specs=[vmem(), vmem(), anywhere, anywhere, anywhere],
        out_specs=(anywhere, anywhere, anywhere, vmem()) + (anywhere,) * 5 + (vmem(),),
        scratch_shapes=[
            pltpu.VMEM((4, width, width), BF),
            pltpu.VMEM((nf, 16, vec.shape[1]), BF),
            pltpu.VMEM((every, width), BF),
            pltpu.VMEM((width, every), BF),
            pltpu.VMEM((rows, width), BF),
            pltpu.VMEM((every, width), BF),
            pltpu.VMEM((every, width), BF),
            pltpu.VMEM((rows, width), F32),
            pltpu.VMEM((4, shard, width), F32),
            pltpu.VMEM((shard, full), F32),
            pltpu.VMEM((shard, full), BF),
            pltpu.VMEM((deep, width), BF),
            pltpu.VMEM((ns - 1, width // 64, rows, rows), F32),
            pltpu.VMEM((ns - 1, width // 128, rows, 128), F32),
            dma((12,)),
            dma((12, nf - 1)), dma((12, nf - 1)),
            dma((12, nf - 1, nh - 1)), dma((12, nf - 1, nh - 1)),
            dma((12, nf - 1)), dma((12, nf - 1)),
            dma((12, nf - 1, nh - 1)), dma((12, nf - 1, nh - 1)),
            dma((nf,)), dma((nf,)),
            dma((ns,)), dma((ns,)), dma((ns,)),
        ],
        name="front",
        compiler_params=pltpu.CompilerParams(
            collective_id=0, has_side_effects=True, vmem_limit_bytes=67043328
        ),
    )(frames, vec, aw, ew, cw.reshape(aw.shape))


def back_kernel(
    sizes, q_ref, k_ref, v_ref, dc_ref, ctx_ref, lse_ref, ht_ref, w_ref, gm_ref, frames_ref,
    vec_ref, gv_ref, gc_ref, ge_ref, go_ref,
    oc_ref, oe_ref, oa_ref, ig_ref, ov_ref,
    ga, own, rc, rx, ry, rz, ri, dkt, dvt, dqa, dhs, dra, drb, drc, vb, vx, vy, vz,
    os, cs, cr, xs, xr, ys, yr, zs, zr, zis, zir, gs, gr, ays, ayr, acs, acr,
    das, dar, dbs, dbr, dcs, dcr, dns, dnr, vs, vr,
):
    at = Place(sizes)
    nf, nh, ns = at.nf, at.nh, at.ns
    rows, width = q_ref.shape
    q = rc.shape[5]
    cols = width // nh
    per = cols // 128
    chunks = rc.shape[0]
    split = chunks // (3 * per)
    half = q * split
    group = per * split
    b0 = lax.rem(at.z, 2)
    b1 = at.z // 2
    at.barrier()

    def strip(core, r):
        return pl.ds(pl.multiple_of(core * half + r * q, 16), q)

    def lanes(s, hi):
        return pl.ds(pl.multiple_of(hi * cols + s * 128, 128), 128)

    def place_of(n):
        return n // group, lax.rem(n, group) // split, lax.rem(n, split)

    for s in range(per):
        for hi in range(nh):
            for part in range(2):
                for r in range(split):
                    pltpu.make_async_copy(
                        go_ref.at[:, pl.ds(part * half + r * q, q), pl.ds(hi * cols + s * 128, 128)],
                        ga.at[s, r, hi, :, part, 1, 1],
                        os.at[4],
                    ).start()

    def own_whole(slot):
        return pltpu.make_async_copy(own.at[slot], own.at[slot], os.at[slot])

    def c_whole(n):
        return remote(rc.at[n], rc.at[n], cs.at[n], cr.at[n], at.sibling())

    def c_send(n):
        slot = lax.rem(n, 4)
        g, s, r = place_of(n)

        @pl.when(n < group)
        def _():
            for hi in range(nh):
                for u in range(4):
                    block = lanes(s, hi)
                    remote(
                        gc_ref.at[:, u, strip(1 - at.core, r), block],
                        rc.at[n, hi, :, u // 2, u % 2], cs.at[n], cr.at[n], at.sibling(),
                    ).start()
                    pltpu.make_async_copy(
                        gc_ref.at[:, u, strip(at.core, r), block],
                        own.at[slot, hi, :, u // 2, u % 2], os.at[slot],
                    ).start()

        @pl.when(jnp.logical_and(n >= group, n < 2 * group))
        def _():
            for hi in range(nh):
                for u in range(4):
                    block = pl.ds(pl.multiple_of(u * width + hi * cols + s * 128, 128), 128)
                    remote(
                        ge_ref.at[:, strip(1 - at.core, r), block],
                        rc.at[n, hi, :, u // 2, u % 2], cs.at[n], cr.at[n], at.sibling(),
                    ).start()
                    pltpu.make_async_copy(
                        ge_ref.at[:, strip(at.core, r), block],
                        own.at[slot, hi, :, u // 2, u % 2], os.at[slot],
                    ).start()

        @pl.when(jnp.logical_and(n >= 2 * group, n < chunks))
        def _():
            remote(
                ga.at[s, r, :, :, 1 - at.core], rc.at[n], cs.at[n], cr.at[n], at.sibling()
            ).start()

    def x_copy(n, k):
        peer = lax.rem(at.x + k, nf)
        return remote(rc.at[n, :, peer], rx.at[n, k - 1], xs.at[n, k - 1], xr.at[n, k - 1], at.x_peer(k))

    def y_copy(n, m):
        return remote(
            rx.at[n, 0, at.y_hi(m)], ry.at[n, m - 1], ys.at[n, m - 1], yr.at[n, m - 1], at.y_peer(m)
        )

    assert ns == 4
    outer = b0 == b1
    inner = b0 != b1
    near = {"seq": at.z + 1 - 2 * b0}
    across = {"seq": 3 - at.z}

    def z_copy(n):
        return remote(ry.at[n, 0], rz.at[n], zs.at[n], zr.at[n], near)

    def zi_copy(n):
        return remote(ry.at[n, 0], ri.at[n], zis.at[n], zir.at[n], across)

    def by_group(n, act):
        g, s, r = place_of(n)

        for which in range(3):
            @pl.when(g == which)
            def _(which=which):
                def place(hi, ua, ub):
                    if which == 1:
                        start = (2 * ua + ub) * width + hi * cols + s * 128
                        return oe_ref.at[strip(at.core, r), pl.ds(pl.multiple_of(start, 128), 128)]
                    ref = oc_ref if which == 0 else oa_ref
                    return ref.at[ua, ub, strip(at.core, r), lanes(s, hi)]

                act(place)

    def g_whole(n):
        return remote(ry.at[n, 0], ry.at[n, 0], gs.at[n], gr.at[n], near)

    def ay_whole(n, m):
        return remote(ry.at[n, 0], ry.at[n, 0], ays.at[n, m - 1], ayr.at[n, m - 1], at.y_peer(m))

    def ac_whole(n):
        return remote(rx.at[n, 0], rx.at[n, 0], acs.at[n], acr.at[n], at.sibling())

    def g_start(n, total):
        def act(place):
            for u in range(4):
                spot = place(at.hi, u // 2, u % 2)
                spot[...] = total[u // 2, u % 2]
                remote(spot, spot, gs.at[n], gr.at[n], near).start()

        by_group(n, act)

    def ay_start(n):
        def act(place):
            for m in range(1, nh):
                for u in range(4):
                    spot = place(at.hi, u // 2, u % 2)
                    remote(spot, spot, ays.at[n, m - 1], ayr.at[n, m - 1], at.y_peer(m)).start()

        by_group(n, act)

    def ac_start(n):
        def act(place):
            for hi in range(nh):
                for u in range(4):
                    spot = place(hi, u // 2, u % 2)
                    remote(spot, spot, acs.at[n], acr.at[n], at.sibling()).start()

        by_group(n, act)

    def plus(left, right):
        if nf == 2:
            return left + right
        return (left.astype(F32) + right.astype(F32)).astype(BF)

    def stage_c(n):
        c_whole(n).wait_recv()
        slot = lax.rem(n, 4)
        _, s, r = place_of(n)

        @pl.when(n < 2 * group)
        def _():
            own_whole(slot).wait()

            def add(i, carry):
                hi, j = i // nf, lax.rem(i, nf)
                rc[n, hi, j] = plus(rc[n, hi, j], own[slot, hi, j])
                return carry

            lax.fori_loop(0, nh * nf, add, 0)

        @pl.when(n >= 2 * group)
        def _():
            def add(i, carry):
                hi, j = i // nf, lax.rem(i, nf)
                rc[n, hi, j] = plus(rc[n, hi, j], ga[s, r, hi, j, at.core])
                return carry

            lax.fori_loop(0, nh * nf, add, 0)

        for k in range(1, nf):
            x_copy(n, k).start()

    def stage_x(n):
        for k in range(1, nf):
            x_copy(n, k).wait_recv()

        def add(hi, carry):
            if nf == 2:
                rx[n, 0, hi] = rc[n, hi, at.x] + rx[n, 0, hi]
            else:
                total = rc[n, hi, at.x].astype(F32)
                for k in range(nf - 1):
                    total += rx[n, k, hi].astype(F32)
                rx[n, 0, hi] = total.astype(BF)
            return carry

        lax.fori_loop(0, nh, add, 0)
        for m in range(1, nh):
            y_copy(n, m).start()

    def stage_y(n):
        for m in range(1, nh):
            y_copy(n, m).wait_recv()
        total = rx[n, 0, at.hi]
        for m in range(nh - 1):
            total = plus(total, ry[n, m])
        ry[n, 0] = total

        @pl.when(outer)
        def _():
            z_copy(n).start()

    def stage_z(n):
        @pl.when(inner)
        def _():
            z_copy(n).wait_recv()
            ry[n, 0] = plus(ry[n, 0], rz[n])
            zi_copy(n).start()

    def stage_zi(n):
        @pl.when(inner)
        def _():
            zi_copy(n).wait_recv()
            g_start(n, plus(ry[n, 0], ri[n]))

    def stage_g(n):
        @pl.when(outer)
        def _():
            g_whole(n).wait_recv()

        ay_start(n)

    def stage_ay(n):
        for m in range(1, nh):
            ay_whole(n, m).wait_recv()
        ac_start(n)

    lo = lax.broadcasted_iota(jnp.int32, (rows, 128), 1) < 64
    pairs = width // 128

    def unit(index):
        i, p = index // pairs, lax.rem(index, pairs)
        there = 1 - b1 - i + 2 * i * b1
        keys = pl.ds(pl.multiple_of(there * (2 * rows), 128), 2 * rows)
        col = pl.ds(pl.multiple_of(p * 128, 128), 128)
        k2 = k_ref[keys, col]
        v2 = v_ref[keys, col]
        q2 = q_ref[:, col]
        dc2 = dc_ref[:, col]
        both = dc2.astype(F32) * ctx_ref[:, col]
        lse2 = lse_ref[p]
        dq, dk, dv = [], None, None
        for h in range(2):
            mask = lo if h == 0 else jnp.logical_not(lo)
            qm = jnp.where(mask, q2, jnp.zeros_like(q2))
            dmask = jnp.where(mask, dc2, jnp.zeros_like(q2))
            lse = lse2[:, 0:1] if h == 0 else lse2[:, 64:65]
            dot = jnp.sum(jnp.where(mask, both, 0.0), axis=-1, keepdims=True)
            probs = jnp.exp(nt(qm, k2) * score_scale - lse)
            slopes = nt(dmask, v2)
            dscore = (probs * (slopes - dot) * score_scale).astype(BF)
            dq.append(nn(dscore, k2))
            a = nn(dmask.T, probs.astype(BF))
            b = nn(qm.T, dscore)
            dv = a if dv is None else dv + a
            dk = b if dk is None else dk + b
        dq2 = jnp.where(lo, dq[0], dq[1])

        @pl.when(i == 0)
        def _():
            dqa[:, col] = dq2

        @pl.when(i > 0)
        def _():
            dqa[:, col] += dq2

        dkt[col, keys] = dk.astype(BF)
        dvt[col, keys] = dv.astype(BF)

    def weights(s):
        frames = pl.ds(pl.multiple_of(at.z * rows, 128), rows)
        for hi in range(nh):
            col = lanes(s, hi)
            dq2 = dqa[:, col]
            vb[2, 0:1, col] = jnp.sum(dq2, axis=0, keepdims=True)
            dq2 = dq2.astype(BF)
            dk2 = dkt[col, :]
            dv2 = dvt[col, :]
            for j in range(nf):
                for part in range(2):
                    for r in range(split):
                        here = pl.ds((2 * j + part) * half + r * q, q)
                        ga[s, r, hi, j, part, 0, 0] = nn(ht_ref[here, frames], dq2).astype(BF)
                        ga[s, r, hi, j, part, 0, 1] = nt(ht_ref[here, :], dk2).astype(BF)
                        ga[s, r, hi, j, part, 1, 0] = nt(ht_ref[here, :], dv2).astype(BF)

    pieces = 16
    per_step = 2
    offsets = (0, 1, 3, 4, 5, 7)
    low = 1 - b1

    def part_of(t):
        return pl.ds(pl.multiple_of(t * (width // pieces), 16), width // pieces)

    def da_copy(t):
        return remote(
            dhs.at[pl.ds(2 * low, 2), part_of(t)], dra.at[:, part_of(t)], das.at[t], dar.at[t], near
        )

    def dn_start(t):
        remote(
            dhs.at[at.z + 1 - 2 * b0, part_of(t)], drc.at[part_of(t)], dns.at[0], dnr.at[0], near
        ).start()

    def dn_whole():
        return remote(dhs.at[0], drc, dns.at[0], dnr.at[0], near)

    def db_copy(t):
        return remote(
            dhs.at[pl.ds(2 * low, 2), part_of(t)], drb.at[:, part_of(t)], dbs.at[t], dbr.at[t], across
        )

    def dc_copy(t):
        return remote(dhs.at[3 * b1, part_of(t)], drc.at[part_of(t)], dcs.at[t], dcr.at[t], near)

    def d_stage(i, t):
        part = part_of(t)
        if i == 0:
            @pl.when(outer)
            def _():
                da_copy(t).start()
        elif i == 1:
            @pl.when(inner)
            def _():
                da_copy(t).wait_recv()
                for j in range(2):
                    dhs[2 * low + j, part] = dhs[2 * low + j, part] + dra[j, part]
                db_copy(t).start()
        elif i == 2:
            @pl.when(inner)
            def _():
                db_copy(t).wait_recv()
                for j in range(2):
                    dhs[2 * b1 + j, part] = dhs[2 * b1 + j, part] + drb[j, part]
                dc_copy(t).start()
        else:
            @pl.when(outer)
            def _():
                dc_copy(t).wait_recv()

    def spread(i):
        there = 1 - b1 - i + 2 * i * b1
        for ub in range(2):
            part = pl.ds(pl.multiple_of((2 * there + ub) * rows, 128), rows)
            dhs[2 * there + ub] = (nn(w_ref[1], dkt[:, part]) + nn(w_ref[2], dvt[:, part])).astype(BF)

    def first_norm():
        @pl.when(inner)
        def _():
            dn_whole().wait_recv()

        total = dhs[at.z].astype(F32) + nt(w_ref[0], dqa[...].astype(BF))
        total += drc[...].astype(F32)
        total = total.T
        normed, inverse = normalize(frames_ref[...])
        scaled = total * vec_ref[0:1, :]
        centred = (
            scaled
            - jnp.mean(scaled, axis=-1, keepdims=True)
            - normed * jnp.mean(scaled * normed, axis=-1, keepdims=True)
        )
        ig_ref[...] = gm_ref[...] + inverse * centred
        vb[1] = gv_ref[...]
        vb[1, 0:1, :] = jnp.sum(total * normed, axis=0, keepdims=True)
        vb[1, 1:2, :] = jnp.sum(total, axis=0, keepdims=True)
        vb[1, 2:3, :] = vb[2, 0:1, :]

    def v_core():
        return remote(vb.at[1], vb.at[0], vs.at[0], vr.at[0], at.sibling())

    def v_x(k):
        return remote(vx.at[at.x], vx.at[at.x], vs.at[k], vr.at[k], at.x_peer(k))

    def v_y(m):
        return remote(vy.at[at.hi], vy.at[at.hi], vs.at[nf + m], vr.at[nf + m], at.y_peer(m))

    def v_z(k):
        return remote(
            vz.at[at.z], vz.at[at.z], vs.at[nf + nh + k], vr.at[nf + nh + k], at.z_peer(k)
        )

    def v_step(i):
        if i == 0:
            v_core().start()
        elif i == 1:
            v_core().wait_recv()
            vx[at.x] = vb[0] + vb[1]
            for k in range(1, nf):
                v_x(k).start()
        elif i == 2:
            for k in range(1, nf):
                v_x(k).wait_recv()
            total = vx[0]
            for j in range(1, nf):
                total += vx[j]
            vy[at.hi] = total
            for m in range(1, nh):
                v_y(m).start()
        elif i == 3:
            for m in range(1, nh):
                v_y(m).wait_recv()
            total = vy[0]
            for j in range(1, nh):
                total += vy[j]
            vz[at.z] = total
            for k in range(1, ns):
                v_z(k).start()
        else:
            for k in range(1, ns):
                v_z(k).wait_recv()
            total = vz[0]
            for j in range(1, ns):
                total += vz[j]
            ov_ref[...] = total

    ready = 8 if split == 2 else group
    each = -(-2 * pairs // ready)

    def units_before(n):
        return (2 * pairs * n + ready - 1) // ready

    done = [
        next(n for n in range(ready) if units_before(n + 1) >= pairs * (i + 1)) for i in range(2)
    ]
    away = done[0] + 1
    slack = 2
    turns = pieces // per_step
    rest = away + turns
    norm = max(away + turns + 3 * slack, rest + turns // 2 + 1, chunks - 2)
    stages = (stage_x, stage_y, stage_z, stage_zi, stage_g, stage_ay)
    last = max(chunks + offsets[-1] + 1, norm + 6)
    for n in range(4):
        c_send(n)

    def step(n, carry):
        for k in range(3):
            @pl.when(3 * n + k < 2 * group)
            def _(k=k):
                stage_c(3 * n + k)

                @pl.when(3 * n + k + 4 < 2 * group)
                def _():
                    c_send(3 * n + k + 4)

        @pl.when(jnp.logical_and(n >= ready + 1, n < ready + 1 + per))
        def _():
            for r in range(split):
                stage_c(2 * group + (n - ready - 1) * split + r)

        @pl.when(n < ready)
        def _():
            def one(k, carry):
                @pl.when(units_before(n) + k < units_before(n + 1))
                def _():
                    unit(units_before(n) + k)

                return carry

            lax.fori_loop(0, each, one, 0)

        @pl.when(jnp.logical_or(n == done[0], n == done[1]))
        def _():
            spread(n // done[1])

        @pl.when(n == norm)
        def _():
            first_norm()

        @pl.when(n == ready)
        def _():
            whole = ga.at[:, :, :, :, :, 1, 1]
            pltpu.make_async_copy(whole, whole, os.at[4]).wait()

        @pl.when(jnp.logical_and(n >= ready, n < ready + per))
        def _():
            weights(n - ready)
            for r in range(split):
                c_send(2 * group + (n - ready) * split + r)

        for i, stage in enumerate(stages):
            @pl.when(jnp.logical_and(n >= offsets[i], n < chunks + offsets[i]))
            def _(i=i, stage=stage):
                stage(n - offsets[i])

        for i in range(4):
            first = away + slack * i

            @pl.when(jnp.logical_and(n >= first, n < first + turns))
            def _(i=i, first=first):
                for t in range(per_step):
                    d_stage(i, (n - first) * per_step + t)

        @pl.when(jnp.logical_and(outer, jnp.logical_and(n >= rest, n < rest + turns // 2)))
        def _():
            for t in range(2 * per_step):
                dn_start((n - rest) * (2 * per_step) + t)

        for i in range(5):
            @pl.when(n == norm + i)
            def _(i=i):
                v_step(i)

        return carry

    lax.fori_loop(0, last, step, 0)
    for n in range(chunks):
        ac_whole(n).wait()

    def drain(n, carry):
        c_whole(n).wait_send()

        @pl.when(outer)
        def _():
            z_copy(n).wait_send()

        @pl.when(inner)
        def _():
            zi_copy(n).wait_send()
            g_whole(n).wait_send()

        for k in range(1, nf):
            x_copy(n, k).wait_send()
        for m in range(1, nh):
            y_copy(n, m).wait_send()
            ay_whole(n, m).wait_send()
        return carry

    lax.fori_loop(0, chunks, drain, 0)

    @pl.when(outer)
    def _():
        dn_whole().wait_send()

        def sent(t, carry):
            da_copy(t).wait_send()
            return carry

        lax.fori_loop(0, pieces, sent, 0)

    @pl.when(inner)
    def _():
        def sent(t, carry):
            db_copy(t).wait_send()
            dc_copy(t).wait_send()
            return carry

        lax.fori_loop(0, pieces, sent, 0)

    for k in range(1, ns):
        v_z(k).wait_send()
    for k in range(1, nf):
        v_x(k).wait_send()
    for m in range(1, nh):
        v_y(m).wait_send()
    v_core().wait_send()


def back_all(sizes, q, k, v, dc, ctx, lse, ht, w, gm, frames, vec, gv, gc, ge, go):
    nd, nf, ns = sizes
    nh = nd // 2
    rows, width = q.shape
    shard = go.shape[1]
    half = shard // 2
    every = k.shape[0]
    split = 2 if half % 32 == 0 else 1
    strip = half // split
    per = width // nh // 128
    chunks = 3 * per * split
    xn, yn = max(nf - 1, 1), max(nh - 1, 1)
    dma = pltpu.SemaphoreType.DMA
    anywhere = pl.BlockSpec(memory_space=pl.ANY)
    return pl.pallas_call(
        functools.partial(back_kernel, sizes),
        out_shape=(
            jax.ShapeDtypeStruct((2, 2, shard, width), BF),
            jax.ShapeDtypeStruct((shard, 4 * width), BF),
            jax.ShapeDtypeStruct((2, 2, shard, width), BF),
            jax.ShapeDtypeStruct((rows, width), F32),
            jax.ShapeDtypeStruct((16, width), F32),
        ),
        in_specs=[vmem()] * 12 + [anywhere] * 3,
        out_specs=(vmem(),) * 5,
        scratch_shapes=[
            pltpu.VMEM((per, split, nh, nf, 2, 2, 2, strip, 128), BF),
            pltpu.VMEM((4, nh, nf, 2, 2, strip, 128), BF),
            pltpu.VMEM((chunks, nh, nf, 2, 2, strip, 128), BF),
            pltpu.VMEM((chunks, xn, nh, 2, 2, strip, 128), BF),
            pltpu.VMEM((chunks, yn, 2, 2, strip, 128), BF),
            pltpu.VMEM((chunks, 2, 2, strip, 128), BF),
            pltpu.VMEM((chunks, 2, 2, strip, 128), BF),
            pltpu.VMEM((width, every), BF),
            pltpu.VMEM((width, every), BF),
            pltpu.VMEM((rows, width), F32),
            pltpu.VMEM((ns, width, rows), BF),
            pltpu.VMEM((2, width, rows), BF),
            pltpu.VMEM((2, width, rows), BF),
            pltpu.VMEM((width, rows), BF),
            pltpu.VMEM((3, 16, width), F32),
            pltpu.VMEM((nf, 16, width), F32),
            pltpu.VMEM((nh, 16, width), F32),
            pltpu.VMEM((ns, 16, width), F32),
            dma((5,)),
            dma((chunks,)), dma((chunks,)),
            dma((chunks, xn)), dma((chunks, xn)),
            dma((chunks, yn)), dma((chunks, yn)),
            dma((chunks,)), dma((chunks,)),
            dma((chunks,)), dma((chunks,)),
            dma((chunks,)), dma((chunks,)),
            dma((chunks, yn)), dma((chunks, yn)),
            dma((chunks,)), dma((chunks,)),
            dma((16,)), dma((16,)),
            dma((16,)), dma((16,)),
            dma((16,)), dma((16,)),
            dma((1,)), dma((1,)),
            dma((nf + nh + ns,)), dma((nf + nh + ns,)),
        ],
        name="back",
        compiler_params=pltpu.CompilerParams(
            collective_id=1, has_side_effects=True, vmem_limit_bytes=67043328
        ),
    )(q, k, v, dc, ctx, lse, ht, w, gm, frames, vec, gv, gc, ge, go)


def feed_kernel(
    ctx_ref, frames_ref, cot_ref, vec_ref, wo_ref, win_ref, wout_ref,
    fo_ref, gm_ref, dc_ref, gi_ref, gout_ref, go_ref, gv_ref,
    mid, h2, h2t, dyb, acc, dh2,
):
    b = pl.program_id(0)

    @pl.when(b == 0)
    def _():
        middle = frames_ref[...] + nn(ctx_ref[...].astype(BF), wo_ref[...]) + vec_ref[4:5, :]
        mid[...] = middle
        normed, _ = normalize(middle)
        hidden = (normed * vec_ref[5:6, :] + vec_ref[6:7, :]).astype(BF)
        h2[...] = hidden
        h2t[...] = hidden.T
        dyb[...] = cot_ref[...].astype(BF)
        acc[...] = middle + vec_ref[7:8, :]
        dh2[...] = jnp.zeros_like(dh2)
        gv_ref[...] = jnp.zeros_like(gv_ref)

    up = dyb[...]
    u = nn(h2[...], win_ref[...]) + vec_ref[pl.ds(8 + b, 1), :]
    phi = 0.5 * (1.0 + lax.erf(u * 0.7071067811865476))
    activated = (u * phi).astype(BF)
    acc[...] += nn(activated, wout_ref[...])
    gout_ref[...] = tn(activated, up).astype(BF)
    du = nt(up, wout_ref[...]) * (phi + u * jnp.exp(-0.5 * u * u) * 0.3989422804014327)
    gv_ref[pl.ds(8 + b, 1), :] = jnp.sum(du, axis=0, keepdims=True)
    dub = du.astype(BF)
    gi_ref[...] = nn(h2t[...], dub).astype(BF)
    dh2[...] += nt(dub, win_ref[...])

    @pl.when(b == pl.num_programs(0) - 1)
    def _():
        fo_ref[...] = acc[...]
        normed, inverse = normalize(mid[...])
        back, gain, offset = norm_back(dh2[...], normed, inverse, vec_ref[5:6, :])
        upstream = cot_ref[...]
        middle = upstream + back
        gm_ref[...] = middle
        dab = middle.astype(BF)
        go_ref[...] = tn(ctx_ref[...].astype(BF), dab).astype(BF)
        dctx = nt(dab, wo_ref[...]).astype(BF)
        dc_ref[...] = dctx
        gv_ref[3:4, :] = jnp.sum(dctx.astype(F32), axis=0, keepdims=True)
        gv_ref[4:5, :] = jnp.sum(middle, axis=0, keepdims=True)
        gv_ref[5:6, :] = gain[None]
        gv_ref[6:7, :] = offset[None]
        gv_ref[7:8, :] = jnp.sum(upstream, axis=0, keepdims=True)


def feed_all(ctx, frames, cot, vec, aw, ew, cw):
    rows, width = frames.shape
    full = ew.shape[1]
    whole = lambda shape: pl.BlockSpec(shape, lambda b: (0,) * len(shape))
    blocks = full // width
    return pl.pallas_call(
        feed_kernel,
        grid=(blocks,),
        out_shape=(
            jax.ShapeDtypeStruct((rows, width), F32),
            jax.ShapeDtypeStruct((rows, width), F32),
            jax.ShapeDtypeStruct((rows, width), BF),
            jax.ShapeDtypeStruct((width, full), BF),
            jax.ShapeDtypeStruct((full, width), BF),
            jax.ShapeDtypeStruct((width, width), BF),
            jax.ShapeDtypeStruct((16, width), F32),
        ),
        in_specs=[
            whole((rows, width)), whole((rows, width)), whole((rows, width)), whole((16, width)),
            pl.BlockSpec((None, width, width), lambda b: (3, 0, 0)),
            pl.BlockSpec((width, width), lambda b: (0, b)),
            pl.BlockSpec((width, width), lambda b: (b, 0)),
        ],
        out_specs=(
            whole((rows, width)), whole((rows, width)), whole((rows, width)),
            pl.BlockSpec((width, width), lambda b: (0, b)),
            pl.BlockSpec((width, width), lambda b: (b, 0)),
            whole((width, width)), whole((16, width)),
        ),
        scratch_shapes=[
            pltpu.VMEM((rows, width), F32),
            pltpu.VMEM((rows, width), BF),
            pltpu.VMEM((width, rows), BF),
            pltpu.VMEM((rows, width), BF),
            pltpu.VMEM((rows, width), F32),
            pltpu.VMEM((rows, width), F32),
        ],
        name="feed",
        compiler_params=pltpu.CompilerParams(vmem_limit_bytes=67043328),
    )(ctx, frames, cot, vec, aw, ew, cw)


def on_device(
    sizes,
    frames_in,
    cotangent,
    attention_weight,
    expand_weight,
    contract_weight,
    vectors,
    first_attention,
    first_expand,
    first_contract,
    first_vectors,
    second_attention,
    second_expand,
    second_contract,
    second_vectors,
):
    nd, nf, ns = sizes
    frames = frames_in[0]
    upstream = cotangent[0]
    rows, width = frames.shape
    shard = attention_weight.shape[1]
    full = expand_weight.shape[1]
    aw, ew, cw, vec, h_turned, queries, key_rows, value_rows, context_wide, log_total = front_all(
        sizes, frames, vectors, attention_weight, expand_weight, contract_weight
    )
    frames_out, grad_middle, grad_context, grad_expand, grad_contract, grad_output_w, gv = feed_all(
        context_wide, frames, upstream, vec, aw, ew, cw
    )
    oc, oe, oa, input_gradient, gv_sum = back_all(
        sizes,
        queries,
        key_rows,
        value_rows,
        grad_context,
        context_wide,
        log_total,
        h_turned,
        aw,
        grad_middle,
        frames,
        vec,
        gv,
        grad_contract.reshape(nf, 4, shard, width),
        grad_expand.reshape(nf, shard, full),
        grad_output_w.reshape(nf, shard, width),
    )
    owned_vec = lax.dynamic_slice_in_dim(
        gv_sum[:12], lax.axis_index("fsdp") * (width // nf), width // nf, 1
    )
    owned = (
        oa.reshape(4, shard, width).astype(F32),
        oe.astype(F32),
        oc.reshape(4 * shard, width).astype(F32),
    )
    attention_out = (owned[0],) + adam_update(
        attention_weight, owned[0], first_attention, second_attention, rate_matrix, decay_matrix
    )
    expand_out = (owned[1],) + adam_update(
        expand_weight, owned[1], first_expand, second_expand, rate_matrix, decay_matrix
    )
    contract_out = (owned[2],) + adam_update(
        contract_weight, owned[2], first_contract, second_contract, rate_matrix, decay_matrix
    )
    vector_out = (owned_vec,) + adam_update(
        vectors, owned_vec, first_vectors, second_vectors, rate_vector, 0.0
    )
    result = [frames_out[None], input_gradient[None]]
    for i in range(4):
        result += [attention_out[i], expand_out[i], contract_out[i], vector_out[i]]
    return tuple(result)


def solution(mesh):
    sizes = (mesh.shape["dp"], mesh.shape["fsdp"], mesh.shape["seq"])
    data = P(("dp", "fsdp"), "seq", None)
    state = (P(None, "fsdp", None), P("fsdp", None), P("fsdp", None), P(None, "fsdp"))
    return jax.shard_map(
        functools.partial(on_device, sizes),
        mesh=mesh,
        in_specs=(data, data) + state * 3,
        out_specs=(data, data) + state * 4,
        check_vma=False,
    )
```

```python
import functools

import jax
import jax.numpy as jnp
from jax import lax
from jax.experimental import pallas as pl
from jax.experimental.pallas import tpu as pltpu
from jax.sharding import PartitionSpec as P

HEADS = 12
norm_eps = 1e-05
beta_one = 0.9
beta_two = 0.999
adam_eps = 1e-08
adam_count = 5.0
rate_matrix = 0.02
rate_vector = 0.1
decay_matrix = 0.1
score_scale = 0.125
VMEM_LIMIT = 60 << 20
MESH = pl.DeviceIdType.MESH
BF = jnp.bfloat16
F32 = jnp.float32


def nt(left, right):
    return lax.dot_general(left, right, (((1,), (1,)), ((), ())), preferred_element_type=F32)


def nn(left, right):
    return lax.dot_general(left, right, (((1,), (0,)), ((), ())), preferred_element_type=F32)


def tn(left, right):
    return lax.dot_general(left, right, (((0,), (0,)), ((), ())), preferred_element_type=F32)


def vmem():
    return pl.BlockSpec(memory_space=pltpu.VMEM)


def normalize(values):
    center = values - jnp.mean(values, axis=-1, keepdims=True)
    inverse = lax.rsqrt(jnp.mean(center * center, axis=-1, keepdims=True) + norm_eps)
    return center * inverse, inverse


def norm_back(upstream, normed, inverse, gain):
    scaled = upstream * gain
    inner = (
        scaled
        - jnp.mean(scaled, axis=-1, keepdims=True)
        - normed * jnp.mean(scaled * normed, axis=-1, keepdims=True)
    )
    return (inverse * inner, jnp.sum(upstream * normed, axis=0), jnp.sum(upstream, axis=0))


def adam_update(weight, gradient, first, second, rate, decay):
    first_new = beta_one * first + (1.0 - beta_one) * gradient
    second_new = beta_two * second + (1.0 - beta_two) * gradient * gradient
    first_hat = first_new / (1.0 - beta_one**adam_count)
    second_hat = second_new / (1.0 - beta_two**adam_count)
    updated = weight - rate * (first_hat / (jnp.sqrt(second_hat) + adam_eps) + decay * weight)
    return (updated, first_new, second_new)


class Place:
    def __init__(self, sizes):
        self.nd, self.nf, self.ns = sizes
        self.nh = self.nd // 2
        self.dp = lax.axis_index("dp")
        self.x = lax.axis_index("fsdp")
        self.z = lax.axis_index("seq")
        self.core = lax.rem(self.dp, 2)
        self.hi = self.dp // 2

    def sibling(self):
        return {"dp": self.hi * 2 + 1 - self.core}

    def x_peer(self, k):
        return {"fsdp": lax.rem(self.x + k, self.nf)}

    def y_hi(self, k):
        return lax.rem(self.hi + k, self.nh)

    def y_peer(self, k):
        return {"dp": self.y_hi(k) * 2 + self.core}

    def z_at(self, k):
        return lax.rem(self.z + k + self.ns, self.ns)

    def z_peer(self, k):
        return {"seq": self.z_at(k)}

    def everyone(self):
        out = [self.sibling()]
        out += [self.x_peer(k) for k in range(1, self.nf)]
        out += [self.y_peer(k) for k in range(1, self.nh)]
        out += [self.z_peer(k) for k in range(1, self.ns)]
        return out

    def barrier(self):
        sem = pltpu.get_barrier_semaphore()
        peers = self.everyone()
        for peer in peers:
            pl.semaphore_signal(sem, inc=1, device_id=peer, device_id_type=MESH)
        pl.semaphore_wait(sem, len(peers))


def remote(src, dst, send, recv, peer):
    return pltpu.make_async_remote_copy(
        src_ref=src, dst_ref=dst, send_sem=send, recv_sem=recv, device_id=peer, device_id_type=MESH
    )


def front_kernel(
    sizes, frames_ref, vec_ref, aw_ref, ew_ref, cw_ref,
    a_out, e_ref, c_ref, vec_out, ht_out, q_out, k_out, v_out, ctx_out, lse_ref,
    a_ref, v_buf, h_ref, ht, q_buf, k_buf, v_buf2, ctx_buf, af, ef, eb, cb, kept, stat,
    ls, xs, xr, ys, yr, s1s, s1r, s2s, s2r, vs, vr, rs, hs, hr,
):
    at = Place(sizes)
    nf, nh, ns = at.nf, at.nh, at.ns
    rows, width = frames_ref.shape
    shard = aw_ref.shape[1]
    half = shard // 2
    deep = cb.shape[0]
    b0 = lax.rem(at.z, 2)
    b1 = at.z // 2

    def load(i, src, dst):
        return pltpu.make_async_copy(src, dst, ls.at[i])

    loads = [
        load(0, aw_ref.at[pl.ds(0, 3)], af.at[pl.ds(0, 3)]),
        load(1, aw_ref.at[pl.ds(3, 1)], af.at[pl.ds(3, 1)]),
        load(2, ew_ref, ef),
        load(3, cw_ref, af),
    ]
    for copy in loads[:3]:
        copy.start()
    at.barrier()
    v_buf[at.x] = jnp.zeros(v_buf.shape[1:], BF)
    v_buf[at.x, 0 : vec_ref.shape[0], :] = vec_ref[...].astype(BF)
    vec_copies = []
    for k in range(1, nf):
        copy = remote(v_buf.at[at.x], v_buf.at[at.x], vs.at[k], vr.at[k], at.x_peer(k))
        copy.start()
        vec_copies.append(copy)

    order = (1, 2, 0, 3)

    def view(chunk, j, hi, core, own=False):
        cols = width // nh
        if chunk < 4:
            return a_ref.at[
                order[chunk],
                pl.ds(pl.multiple_of(j * shard + core * half, 16), half),
                pl.ds(pl.multiple_of(hi * cols, 128), cols),
            ]
        if chunk < 8:
            start = 0 if own else j * shard
            wide = eb.shape[1] // nh
            return (eb if own else e_ref).at[
                pl.ds(pl.multiple_of(start + core * half, 16), half),
                pl.ds(pl.multiple_of(hi * wide + (chunk - 4) * (wide // 4), 128), wide // 4),
            ]
        start = 0 if own else j * deep
        tall = deep // 8
        return (cb if own else c_ref).at[
            pl.ds(pl.multiple_of(start + core * (deep // 2) + (chunk - 8) * tall, 16), tall),
            pl.ds(pl.multiple_of(hi * cols, 128), cols),
        ]

    own = pl.multiple_of(at.x * shard, 16)
    x_copies = {}

    def send_chunk(chunk):
        for k in range(1, nf):
            copy = remote(
                view(chunk, at.x, at.hi, at.core, True), view(chunk, at.x, at.hi, at.core),
                xs.at[chunk, k - 1], xr.at[chunk, k - 1], at.x_peer(k),
            )
            copy.start()
            x_copies[chunk, k] = copy

    loads[0].wait()
    for i, u in enumerate(order[:3]):
        a_ref[u, pl.ds(own, shard), :] = af[u].astype(BF)
        send_chunk(i)
    normed, _ = normalize(frames_ref[...])
    for copy in vec_copies:
        copy.wait()
    vec = jnp.concatenate([v_buf[j] for j in range(nf)], axis=1).astype(F32)
    vec_out[...] = vec
    mine = pl.ds(pl.multiple_of(at.z * rows, 128), rows)
    hidden = (normed * vec[0:1] + vec[1:2]).astype(BF)
    h_ref[mine, :] = hidden

    def block(b):
        return h_ref.at[pl.ds(pl.multiple_of(b * rows, 128), rows), :]

    def to_right(b):
        return remote(block(b), block(b), rs.at[b], hr.at[b], {"seq": at.z + 1})

    def to_left(b):
        return remote(block(b), block(b), hs.at[b], hr.at[b], {"seq": at.z - 1})

    @pl.when(at.z < ns - 1)
    def _():
        to_right(at.z).start()

    @pl.when(at.z > 0)
    def _():
        to_left(at.z).start()

    loads[1].wait()
    a_ref[3, pl.ds(own, shard), :] = af[3].astype(BF)
    loads[3].start()
    send_chunk(3)
    loads[2].wait()
    eb[...] = ef[...].astype(BF)
    for i in range(4, 8):
        send_chunk(i)
    loads[3].wait()
    for u in range(4):
        cb[pl.ds(u * shard, shard), :] = af[u].astype(BF)
    for i in range(8, 12):
        send_chunk(i)
    stores = [
        load(4, eb, e_ref.at[pl.ds(own, shard), :]),
        load(5, cb, c_ref.at[pl.ds(pl.multiple_of(at.x * deep, 16), deep), :]),
    ]
    for copy in stores:
        copy.start()
    ht[:, mine] = hidden.T

    def first_copy(chunk, k):
        j = lax.rem(at.x - k + nf, nf)
        piece = view(chunk, j, at.hi, at.core)
        return remote(piece, piece, s1s.at[chunk, k - 1], s1r.at[chunk, k - 1], at.sibling())

    def y_copy(chunk, k, m):
        j = lax.rem(at.x - k + nf, nf)
        piece = view(chunk, j, at.hi, at.core)
        return remote(piece, piece, ys.at[chunk, k - 1, m - 1], yr.at[chunk, k - 1, m - 1], at.y_peer(m))

    def second_copy(chunk, k, m):
        j = lax.rem(at.x - k + nf, nf)
        piece = view(chunk, j, lax.rem(at.hi - m + nh, nh), at.core)
        return remote(piece, piece, s2s.at[chunk, k - 1, m - 1], s2r.at[chunk, k - 1, m - 1], at.sibling())

    def forward(chunk):
        for k in range(1, nf):
            x_copies[chunk, k].wait_recv()
            first_copy(chunk, k).start()
            for m in range(1, nh):
                y_copy(chunk, k, m).start()

    def relay(chunk):
        for k in range(1, nf):
            for m in range(1, nh):
                y_copy(chunk, k, m).wait_recv()
                second_copy(chunk, k, m).start()

    def arrived(chunk):
        for k in range(1, nf):
            first_copy(chunk, k).wait_recv()
            for m in range(1, nh):
                second_copy(chunk, k, m).wait_recv()

    def rows_of(b):
        part = pl.ds(pl.multiple_of(b * rows, 128), rows)
        k_buf[part, :] = nn(h_ref[part, :], a_ref[1]).astype(BF)
        v_buf2[part, :] = (nn(h_ref[part, :], a_ref[2]) + vec[3:4]).astype(BF)

    def turn(b):
        part = pl.ds(pl.multiple_of(b * rows, 128), rows)
        ht[:, part] = h_ref[part, :].T

    def hop(s):
        b = at.z - s
        d = at.z + s

        @pl.when(b >= 0)
        def _():
            to_right(b).wait_recv()

            @pl.when(at.z < ns - 1)
            def _():
                to_right(b).start()

        @pl.when(d < ns)
        def _():
            to_left(d).wait_recv()

            @pl.when(at.z > 0)
            def _():
                to_left(d).start()

    lane = lax.broadcasted_iota(jnp.int32, (rows, 128), 1)
    lo = lane < 64

    def scores(p, h, b):
        col = pl.ds(pl.multiple_of(p * 128, 128), 128)
        part = pl.ds(pl.multiple_of(b * rows, 128), rows)
        q2 = q_buf[:, col]
        mask = lo if h == 0 else jnp.logical_not(lo)
        s = nt(jnp.where(mask, q2, jnp.zeros_like(q2)), k_buf[part, col]) * score_scale
        largest = jnp.max(s, axis=-1, keepdims=True)
        e = jnp.exp(s - largest)
        return e, largest, jnp.sum(e, axis=-1, keepdims=True)

    assert ns == 4
    blocks = (at.z, at.z + 1 - 2 * b0, 2 - b1, 3 - 3 * b1)

    def tick(i):
        if i < 12:
            forward(i)
        if i > 0:
            relay(i - 1)

    def begin(i, ticks):
        b = blocks[i]
        rows_of(b)

        def pair(p, carry):
            found = []
            for h in range(2):
                e, largest, total = scores(p, h, b)
                kept[i, 2 * p + h] = e
                found += [largest, total]
            stat[i, p] = jnp.where(
                lo, jnp.where(lane < 32, found[0], found[1]), jnp.where(lane < 96, found[2], found[3])
            )
            for when, which in ticks:
                @pl.when(p == when)
                def _(which=which):
                    tick(which)

            return carry

        lax.fori_loop(0, width // 128, pair, 0)

    tick(0)
    tick(1)
    tick(2)
    hop(1)
    tick(3)
    for i in range(3):
        arrived(i)
    q_buf[...] = (nn(h_ref[mine, :], a_ref[0]) + vec[2:3]).astype(BF)
    stores.append(load(6, q_buf, q_out))
    stores[-1].start()
    tick(4)
    begin(0, ((2, 5), (5, 6)))
    hop(2)
    begin(1, ((1, 7), (4, 8)))
    turn(blocks[1])
    begin(2, ((0, 9), (3, 10)))
    turn(blocks[2])
    hop(3)
    rows_of(blocks[3])
    turn(blocks[3])
    tick(11)
    arrived(3)
    for i, (src, dst) in enumerate(((a_ref, a_out), (ht, ht_out), (k_buf, k_out), (v_buf2, v_out))):
        stores.append(load(7 + i, src, dst))
        stores[-1].start()
    def pair(p, carry):
        col = pl.ds(pl.multiple_of(p * 128, 128), 128)
        ctx, lse = [], []
        for h in range(2):
            e, peak, count = scores(p, h, blocks[3])
            peaks = [stat[i, p][:, 64 * h : 64 * h + 1] for i in range(3)] + [peak]
            counts = [stat[i, p][:, 64 * h + 32 : 64 * h + 33] for i in range(3)] + [count]
            largest = functools.reduce(jnp.maximum, peaks)
            shares = [jnp.exp(each - largest) for each in peaks]
            total = sum(share * each for share, each in zip(shares, counts))
            inverse = 1.0 / total
            out = None
            for i in range(4):
                part = pl.ds(pl.multiple_of(blocks[i] * rows, 128), rows)
                found = kept[i, 2 * p + h] if i < 3 else e
                term = nn((found * (shares[i] * inverse)).astype(BF), v_buf2[part, col])
                out = term if out is None else out + term
            ctx.append(out)
            lse.append(largest + jnp.log(total))
        ctx_buf[:, col] = jnp.where(lo, ctx[0], ctx[1])
        lse_ref[p] = jnp.where(lo, lse[0], lse[1])

        @pl.when(p == 1)
        def _():
            tick(12)

        return carry

    lax.fori_loop(0, width // 128, pair, 0)
    stores.append(load(11, ctx_buf, ctx_out))
    stores[-1].start()
    for i in range(4, 12):
        arrived(i)
    for copy in stores:
        copy.wait()
    for copy in x_copies.values():
        copy.wait_send()
    for chunk in range(12):
        for k in range(1, nf):
            first_copy(chunk, k).wait_send()
            for m in range(1, nh):
                y_copy(chunk, k, m).wait_send()
                second_copy(chunk, k, m).wait_send()
    for b in range(ns):
        @pl.when(jnp.logical_and(b <= at.z, at.z < ns - 1))
        def _():
            to_right(b).wait_send()

        @pl.when(jnp.logical_and(b >= at.z, at.z > 0))
        def _():
            to_left(b).wait_send()


def front_all(sizes, frames, vec, aw, ew, cw):
    nd, nf, ns = sizes
    nh = nd // 2
    rows, width = frames.shape
    shard, full = ew.shape
    deep = cw.shape[0]
    every = rows * ns
    dma = pltpu.SemaphoreType.DMA
    anywhere = pl.BlockSpec(memory_space=pl.ANY)
    return pl.pallas_call(
        functools.partial(front_kernel, sizes),
        out_shape=(
            jax.ShapeDtypeStruct((4, width, width), BF),
            jax.ShapeDtypeStruct((width, full), BF),
            jax.ShapeDtypeStruct((deep * nf, width), BF),
            jax.ShapeDtypeStruct((16, width), F32),
            jax.ShapeDtypeStruct((width, every), BF),
            jax.ShapeDtypeStruct((rows, width), BF),
            jax.ShapeDtypeStruct((every, width), BF),
            jax.ShapeDtypeStruct((every, width), BF),
            jax.ShapeDtypeStruct((rows, width), F32),
            jax.ShapeDtypeStruct((width // 128, rows, 128), F32),
        ),
        in_specs=[vmem(), vmem(), anywhere, anywhere, anywhere],
        out_specs=(anywhere, anywhere, anywhere, vmem()) + (anywhere,) * 5 + (vmem(),),
        scratch_shapes=[
            pltpu.VMEM((4, width, width), BF),
            pltpu.VMEM((nf, 16, vec.shape[1]), BF),
            pltpu.VMEM((every, width), BF),
            pltpu.VMEM((width, every), BF),
            pltpu.VMEM((rows, width), BF),
            pltpu.VMEM((every, width), BF),
            pltpu.VMEM((every, width), BF),
            pltpu.VMEM((rows, width), F32),
            pltpu.VMEM((4, shard, width), F32),
            pltpu.VMEM((shard, full), F32),
            pltpu.VMEM((shard, full), BF),
            pltpu.VMEM((deep, width), BF),
            pltpu.VMEM((ns - 1, width // 64, rows, rows), F32),
            pltpu.VMEM((ns - 1, width // 128, rows, 128), F32),
            dma((12,)),
            dma((12, nf - 1)), dma((12, nf - 1)),
            dma((12, nf - 1, nh - 1)), dma((12, nf - 1, nh - 1)),
            dma((12, nf - 1)), dma((12, nf - 1)),
            dma((12, nf - 1, nh - 1)), dma((12, nf - 1, nh - 1)),
            dma((nf,)), dma((nf,)),
            dma((ns,)), dma((ns,)), dma((ns,)),
        ],
        name="front",
        compiler_params=pltpu.CompilerParams(
            collective_id=0, has_side_effects=True, vmem_limit_bytes=67043328
        ),
    )(frames, vec, aw, ew, cw.reshape(aw.shape))


def back_kernel(
    sizes, q_ref, k_ref, v_ref, dc_ref, ctx_ref, lse_ref, ht_ref, w_ref, gm_ref, frames_ref,
    vec_ref, gv_ref, gc_ref, ge_ref, go_ref,
    oc_ref, oe_ref, oa_ref, ig_ref, ov_ref,
    ga, own, rc, rx, ry, rz, ri, dkt, dvt, dqa, dhs, dra, drb, drc, vb, vx, vy, vz,
    os, cs, cr, xs, xr, ys, yr, zs, zr, zis, zir, gs, gr, ays, ayr, acs, acr,
    das, dar, dbs, dbr, dcs, dcr, dns, dnr, vs, vr,
):
    at = Place(sizes)
    nf, nh, ns = at.nf, at.nh, at.ns
    rows, width = q_ref.shape
    q = rc.shape[5]
    cols = width // nh
    per = cols // 128
    chunks = rc.shape[0]
    split = chunks // (3 * per)
    half = q * split
    group = per * split
    b0 = lax.rem(at.z, 2)
    b1 = at.z // 2
    at.barrier()

    def strip(core, r):
        return pl.ds(pl.multiple_of(core * half + r * q, 16), q)

    def lanes(s, hi):
        return pl.ds(pl.multiple_of(hi * cols + s * 128, 128), 128)

    def place_of(n):
        return n // group, lax.rem(n, group) // split, lax.rem(n, split)

    for s in range(per):
        for hi in range(nh):
            for part in range(2):
                for r in range(split):
                    pltpu.make_async_copy(
                        go_ref.at[:, pl.ds(part * half + r * q, q), pl.ds(hi * cols + s * 128, 128)],
                        ga.at[s, r, hi, :, part, 1, 1],
                        os.at[4],
                    ).start()

    def own_whole(slot):
        return pltpu.make_async_copy(own.at[slot], own.at[slot], os.at[slot])

    def c_whole(n):
        return remote(rc.at[n], rc.at[n], cs.at[n], cr.at[n], at.sibling())

    def c_send(n):
        slot = lax.rem(n, 4)
        g, s, r = place_of(n)

        @pl.when(n < group)
        def _():
            for hi in range(nh):
                for u in range(4):
                    block = lanes(s, hi)
                    remote(
                        gc_ref.at[:, u, strip(1 - at.core, r), block],
                        rc.at[n, hi, :, u // 2, u % 2], cs.at[n], cr.at[n], at.sibling(),
                    ).start()
                    pltpu.make_async_copy(
                        gc_ref.at[:, u, strip(at.core, r), block],
                        own.at[slot, hi, :, u // 2, u % 2], os.at[slot],
                    ).start()

        @pl.when(jnp.logical_and(n >= group, n < 2 * group))
        def _():
            for hi in range(nh):
                for u in range(4):
                    block = pl.ds(pl.multiple_of(u * width + hi * cols + s * 128, 128), 128)
                    remote(
                        ge_ref.at[:, strip(1 - at.core, r), block],
                        rc.at[n, hi, :, u // 2, u % 2], cs.at[n], cr.at[n], at.sibling(),
                    ).start()
                    pltpu.make_async_copy(
                        ge_ref.at[:, strip(at.core, r), block],
                        own.at[slot, hi, :, u // 2, u % 2], os.at[slot],
                    ).start()

        @pl.when(jnp.logical_and(n >= 2 * group, n < chunks))
        def _():
            remote(
                ga.at[s, r, :, :, 1 - at.core], rc.at[n], cs.at[n], cr.at[n], at.sibling()
            ).start()

    def x_copy(n, k):
        peer = lax.rem(at.x + k, nf)
        return remote(rc.at[n, :, peer], rx.at[n, k - 1], xs.at[n, k - 1], xr.at[n, k - 1], at.x_peer(k))

    def y_copy(n, m):
        return remote(
            rx.at[n, 0, at.y_hi(m)], ry.at[n, m - 1], ys.at[n, m - 1], yr.at[n, m - 1], at.y_peer(m)
        )

    assert ns == 4
    outer = b0 == b1
    inner = b0 != b1
    near = {"seq": at.z + 1 - 2 * b0}
    across = {"seq": 3 - at.z}

    def z_copy(n):
        return remote(ry.at[n, 0], rz.at[n], zs.at[n], zr.at[n], near)

    def zi_copy(n):
        return remote(ry.at[n, 0], ri.at[n], zis.at[n], zir.at[n], across)

    def by_group(n, act):
        g, s, r = place_of(n)

        for which in range(3):
            @pl.when(g == which)
            def _(which=which):
                def place(hi, ua, ub):
                    if which == 1:
                        start = (2 * ua + ub) * width + hi * cols + s * 128
                        return oe_ref.at[strip(at.core, r), pl.ds(pl.multiple_of(start, 128), 128)]
                    ref = oc_ref if which == 0 else oa_ref
                    return ref.at[ua, ub, strip(at.core, r), lanes(s, hi)]

                act(place)

    def g_whole(n):
        return remote(ry.at[n, 0], ry.at[n, 0], gs.at[n], gr.at[n], near)

    def ay_whole(n, m):
        return remote(ry.at[n, 0], ry.at[n, 0], ays.at[n, m - 1], ayr.at[n, m - 1], at.y_peer(m))

    def ac_whole(n):
        return remote(rx.at[n, 0], rx.at[n, 0], acs.at[n], acr.at[n], at.sibling())

    def g_start(n, total):
        def act(place):
            for u in range(4):
                spot = place(at.hi, u // 2, u % 2)
                spot[...] = total[u // 2, u % 2]
                remote(spot, spot, gs.at[n], gr.at[n], near).start()

        by_group(n, act)

    def ay_start(n):
        def act(place):
            for m in range(1, nh):
                for u in range(4):
                    spot = place(at.hi, u // 2, u % 2)
                    remote(spot, spot, ays.at[n, m - 1], ayr.at[n, m - 1], at.y_peer(m)).start()

        by_group(n, act)

    def ac_start(n):
        def act(place):
            for hi in range(nh):
                for u in range(4):
                    spot = place(hi, u // 2, u % 2)
                    remote(spot, spot, acs.at[n], acr.at[n], at.sibling()).start()

        by_group(n, act)

    def plus(left, right):
        if nf == 2:
            return left + right
        return (left.astype(F32) + right.astype(F32)).astype(BF)

    def stage_c(n):
        c_whole(n).wait_recv()
        slot = lax.rem(n, 4)
        _, s, r = place_of(n)

        @pl.when(n < 2 * group)
        def _():
            own_whole(slot).wait()

            def add(i, carry):
                hi, j = i // nf, lax.rem(i, nf)
                rc[n, hi, j] = plus(rc[n, hi, j], own[slot, hi, j])
                return carry

            lax.fori_loop(0, nh * nf, add, 0)

        @pl.when(n >= 2 * group)
        def _():
            def add(i, carry):
                hi, j = i // nf, lax.rem(i, nf)
                rc[n, hi, j] = plus(rc[n, hi, j], ga[s, r, hi, j, at.core])
                return carry

            lax.fori_loop(0, nh * nf, add, 0)

        for k in range(1, nf):
            x_copy(n, k).start()

    def stage_x(n):
        for k in range(1, nf):
            x_copy(n, k).wait_recv()

        def add(hi, carry):
            if nf == 2:
                rx[n, 0, hi] = rc[n, hi, at.x] + rx[n, 0, hi]
            else:
                total = rc[n, hi, at.x].astype(F32)
                for k in range(nf - 1):
                    total += rx[n, k, hi].astype(F32)
                rx[n, 0, hi] = total.astype(BF)
            return carry

        lax.fori_loop(0, nh, add, 0)
        for m in range(1, nh):
            y_copy(n, m).start()

    def stage_y(n):
        for m in range(1, nh):
            y_copy(n, m).wait_recv()
        total = rx[n, 0, at.hi]
        for m in range(nh - 1):
            total = plus(total, ry[n, m])
        ry[n, 0] = total

        @pl.when(outer)
        def _():
            z_copy(n).start()

    def stage_z(n):
        @pl.when(inner)
        def _():
            z_copy(n).wait_recv()
            ry[n, 0] = plus(ry[n, 0], rz[n])
            zi_copy(n).start()

    def stage_zi(n):
        @pl.when(inner)
        def _():
            zi_copy(n).wait_recv()
            g_start(n, plus(ry[n, 0], ri[n]))

    def stage_g(n):
        @pl.when(outer)
        def _():
            g_whole(n).wait_recv()

        ay_start(n)

    def stage_ay(n):
        for m in range(1, nh):
            ay_whole(n, m).wait_recv()
        ac_start(n)

    lo = lax.broadcasted_iota(jnp.int32, (rows, 128), 1) < 64
    pairs = width // 128

    def unit(index):
        i, p = index // pairs, lax.rem(index, pairs)
        there = 1 - b1 - i + 2 * i * b1
        keys = pl.ds(pl.multiple_of(there * (2 * rows), 128), 2 * rows)
        col = pl.ds(pl.multiple_of(p * 128, 128), 128)
        k2 = k_ref[keys, col]
        v2 = v_ref[keys, col]
        q2 = q_ref[:, col]
        dc2 = dc_ref[:, col]
        both = dc2.astype(F32) * ctx_ref[:, col]
        lse2 = lse_ref[p]
        dq, dk, dv = [], None, None
        for h in range(2):
            mask = lo if h == 0 else jnp.logical_not(lo)
            qm = jnp.where(mask, q2, jnp.zeros_like(q2))
            dmask = jnp.where(mask, dc2, jnp.zeros_like(q2))
            lse = lse2[:, 0:1] if h == 0 else lse2[:, 64:65]
            dot = jnp.sum(jnp.where(mask, both, 0.0), axis=-1, keepdims=True)
            probs = jnp.exp(nt(qm, k2) * score_scale - lse)
            slopes = nt(dmask, v2)
            dscore = (probs * (slopes - dot) * score_scale).astype(BF)
            dq.append(nn(dscore, k2))
            a = nn(dmask.T, probs.astype(BF))
            b = nn(qm.T, dscore)
            dv = a if dv is None else dv + a
            dk = b if dk is None else dk + b
        dq2 = jnp.where(lo, dq[0], dq[1])

        @pl.when(i == 0)
        def _():
            dqa[:, col] = dq2

        @pl.when(i > 0)
        def _():
            dqa[:, col] += dq2

        dkt[col, keys] = dk.astype(BF)
        dvt[col, keys] = dv.astype(BF)

    def weights(s):
        frames = pl.ds(pl.multiple_of(at.z * rows, 128), rows)
        for hi in range(nh):
            col = lanes(s, hi)
            dq2 = dqa[:, col]
            vb[2, 0:1, col] = jnp.sum(dq2, axis=0, keepdims=True)
            dq2 = dq2.astype(BF)
            dk2 = dkt[col, :]
            dv2 = dvt[col, :]
            for j in range(nf):
                for part in range(2):
                    for r in range(split):
                        here = pl.ds((2 * j + part) * half + r * q, q)
                        ga[s, r, hi, j, part, 0, 0] = nn(ht_ref[here, frames], dq2).astype(BF)
                        ga[s, r, hi, j, part, 0, 1] = nt(ht_ref[here, :], dk2).astype(BF)
                        ga[s, r, hi, j, part, 1, 0] = nt(ht_ref[here, :], dv2).astype(BF)

    pieces = 16
    per_step = 2
    offsets = (0, 1, 3, 4, 5, 6)
    low = 1 - b1

    def part_of(t):
        return pl.ds(pl.multiple_of(t * (width // pieces), 16), width // pieces)

    def da_copy(t):
        return remote(
            dhs.at[pl.ds(2 * low, 2), part_of(t)], dra.at[:, part_of(t)], das.at[t], dar.at[t], near
        )

    def dn_start(t):
        remote(
            dhs.at[at.z + 1 - 2 * b0, part_of(t)], drc.at[part_of(t)], dns.at[0], dnr.at[0], near
        ).start()

    def dn_whole():
        return remote(dhs.at[0], drc, dns.at[0], dnr.at[0], near)

    def db_copy(t):
        return remote(
            dhs.at[pl.ds(2 * low, 2), part_of(t)], drb.at[:, part_of(t)], dbs.at[t], dbr.at[t], across
        )

    def dc_copy(t):
        return remote(dhs.at[3 * b1, part_of(t)], drc.at[part_of(t)], dcs.at[t], dcr.at[t], near)

    def d_stage(i, t):
        part = part_of(t)
        if i == 0:
            @pl.when(outer)
            def _():
                da_copy(t).start()
        elif i == 1:
            @pl.when(inner)
            def _():
                da_copy(t).wait_recv()
                for j in range(2):
                    dhs[2 * low + j, part] = dhs[2 * low + j, part] + dra[j, part]
                db_copy(t).start()
        elif i == 2:
            @pl.when(inner)
            def _():
                db_copy(t).wait_recv()
                for j in range(2):
                    dhs[2 * b1 + j, part] = dhs[2 * b1 + j, part] + drb[j, part]
                dc_copy(t).start()
        else:
            @pl.when(outer)
            def _():
                dc_copy(t).wait_recv()

    def spread(i):
        there = 1 - b1 - i + 2 * i * b1
        for ub in range(2):
            part = pl.ds(pl.multiple_of((2 * there + ub) * rows, 128), rows)
            dhs[2 * there + ub] = (nn(w_ref[1], dkt[:, part]) + nn(w_ref[2], dvt[:, part])).astype(BF)

    def first_norm():
        @pl.when(inner)
        def _():
            dn_whole().wait_recv()

        total = dhs[at.z].astype(F32) + nt(w_ref[0], dqa[...].astype(BF))
        total += drc[...].astype(F32)
        total = total.T
        normed, inverse = normalize(frames_ref[...])
        scaled = total * vec_ref[0:1, :]
        centred = (
            scaled
            - jnp.mean(scaled, axis=-1, keepdims=True)
            - normed * jnp.mean(scaled * normed, axis=-1, keepdims=True)
        )
        ig_ref[...] = gm_ref[...] + inverse * centred
        vb[1] = gv_ref[...]
        vb[1, 0:1, :] = jnp.sum(total * normed, axis=0, keepdims=True)
        vb[1, 1:2, :] = jnp.sum(total, axis=0, keepdims=True)
        vb[1, 2:3, :] = vb[2, 0:1, :]

    def v_core():
        return remote(vb.at[1], vb.at[0], vs.at[0], vr.at[0], at.sibling())

    def v_x(k):
        return remote(vx.at[at.x], vx.at[at.x], vs.at[k], vr.at[k], at.x_peer(k))

    def v_y(m):
        return remote(vy.at[at.hi], vy.at[at.hi], vs.at[nf + m], vr.at[nf + m], at.y_peer(m))

    def v_z(k):
        return remote(
            vz.at[at.z], vz.at[at.z], vs.at[nf + nh + k], vr.at[nf + nh + k], at.z_peer(k)
        )

    def v_step(i):
        if i == 0:
            v_core().start()
        elif i == 1:
            v_core().wait_recv()
            vx[at.x] = vb[0] + vb[1]
            for k in range(1, nf):
                v_x(k).start()
        elif i == 2:
            for k in range(1, nf):
                v_x(k).wait_recv()
            total = vx[0]
            for j in range(1, nf):
                total += vx[j]
            vy[at.hi] = total
            for m in range(1, nh):
                v_y(m).start()
        elif i == 3:
            for m in range(1, nh):
                v_y(m).wait_recv()
            total = vy[0]
            for j in range(1, nh):
                total += vy[j]
            vz[at.z] = total
            for k in range(1, ns):
                v_z(k).start()
        else:
            for k in range(1, ns):
                v_z(k).wait_recv()
            total = vz[0]
            for j in range(1, ns):
                total += vz[j]
            ov_ref[...] = total

    ready = 8 if split == 2 else group
    each = -(-2 * pairs // ready)

    def units_before(n):
        return (2 * pairs * n + ready - 1) // ready

    done = [
        next(n for n in range(ready) if units_before(n + 1) >= pairs * (i + 1)) for i in range(2)
    ]
    away = done[0] + 1
    slack = 2
    turns = pieces // per_step
    rest = away + turns
    norm = max(away + turns + 3 * slack, rest + turns // 2 + 1, chunks - 2)
    stages = (stage_x, stage_y, stage_z, stage_zi, stage_g, stage_ay)
    last = max(chunks + offsets[-1] + 1, norm + 6)
    for n in range(4):
        c_send(n)

    def step(n, carry):
        for k in range(3):
            @pl.when(3 * n + k < 2 * group)
            def _(k=k):
                stage_c(3 * n + k)

                @pl.when(3 * n + k + 4 < 2 * group)
                def _():
                    c_send(3 * n + k + 4)

        @pl.when(jnp.logical_and(n >= ready + 1, n < ready + 1 + per))
        def _():
            for r in range(split):
                stage_c(2 * group + (n - ready - 1) * split + r)

        @pl.when(n < ready)
        def _():
            def one(k, carry):
                @pl.when(units_before(n) + k < units_before(n + 1))
                def _():
                    unit(units_before(n) + k)

                return carry

            lax.fori_loop(0, each, one, 0)

        @pl.when(jnp.logical_or(n == done[0], n == done[1]))
        def _():
            spread(n // done[1])

        @pl.when(n == norm)
        def _():
            first_norm()

        @pl.when(n == ready)
        def _():
            whole = ga.at[:, :, :, :, :, 1, 1]
            pltpu.make_async_copy(whole, whole, os.at[4]).wait()

        @pl.when(jnp.logical_and(n >= ready, n < ready + per))
        def _():
            weights(n - ready)
            for r in range(split):
                c_send(2 * group + (n - ready) * split + r)

        for i, stage in enumerate(stages):
            @pl.when(jnp.logical_and(n >= offsets[i], n < chunks + offsets[i]))
            def _(i=i, stage=stage):
                stage(n - offsets[i])

        for i in range(4):
            first = away + slack * i

            @pl.when(jnp.logical_and(n >= first, n < first + turns))
            def _(i=i, first=first):
                for t in range(per_step):
                    d_stage(i, (n - first) * per_step + t)

        @pl.when(jnp.logical_and(outer, jnp.logical_and(n >= rest, n < rest + turns // 2)))
        def _():
            for t in range(2 * per_step):
                dn_start((n - rest) * (2 * per_step) + t)

        for i in range(5):
            @pl.when(n == norm + i)
            def _(i=i):
                v_step(i)

        return carry

    lax.fori_loop(0, last, step, 0)
    for n in range(chunks):
        ac_whole(n).wait()

    def drain(n, carry):
        c_whole(n).wait_send()

        @pl.when(outer)
        def _():
            z_copy(n).wait_send()

        @pl.when(inner)
        def _():
            zi_copy(n).wait_send()
            g_whole(n).wait_send()

        for k in range(1, nf):
            x_copy(n, k).wait_send()
        for m in range(1, nh):
            y_copy(n, m).wait_send()
            ay_whole(n, m).wait_send()
        return carry

    lax.fori_loop(0, chunks, drain, 0)

    @pl.when(outer)
    def _():
        dn_whole().wait_send()

        def sent(t, carry):
            da_copy(t).wait_send()
            return carry

        lax.fori_loop(0, pieces, sent, 0)

    @pl.when(inner)
    def _():
        def sent(t, carry):
            db_copy(t).wait_send()
            dc_copy(t).wait_send()
            return carry

        lax.fori_loop(0, pieces, sent, 0)

    for k in range(1, ns):
        v_z(k).wait_send()
    for k in range(1, nf):
        v_x(k).wait_send()
    for m in range(1, nh):
        v_y(m).wait_send()
    v_core().wait_send()


def back_all(sizes, q, k, v, dc, ctx, lse, ht, w, gm, frames, vec, gv, gc, ge, go):
    nd, nf, ns = sizes
    nh = nd // 2
    rows, width = q.shape
    shard = go.shape[1]
    half = shard // 2
    every = k.shape[0]
    split = 2 if half % 32 == 0 else 1
    strip = half // split
    per = width // nh // 128
    chunks = 3 * per * split
    xn, yn = max(nf - 1, 1), max(nh - 1, 1)
    dma = pltpu.SemaphoreType.DMA
    anywhere = pl.BlockSpec(memory_space=pl.ANY)
    return pl.pallas_call(
        functools.partial(back_kernel, sizes),
        out_shape=(
            jax.ShapeDtypeStruct((2, 2, shard, width), BF),
            jax.ShapeDtypeStruct((shard, 4 * width), BF),
            jax.ShapeDtypeStruct((2, 2, shard, width), BF),
            jax.ShapeDtypeStruct((rows, width), F32),
            jax.ShapeDtypeStruct((16, width), F32),
        ),
        in_specs=[vmem()] * 12 + [anywhere] * 3,
        out_specs=(vmem(),) * 5,
        scratch_shapes=[
            pltpu.VMEM((per, split, nh, nf, 2, 2, 2, strip, 128), BF),
            pltpu.VMEM((4, nh, nf, 2, 2, strip, 128), BF),
            pltpu.VMEM((chunks, nh, nf, 2, 2, strip, 128), BF),
            pltpu.VMEM((chunks, xn, nh, 2, 2, strip, 128), BF),
            pltpu.VMEM((chunks, yn, 2, 2, strip, 128), BF),
            pltpu.VMEM((chunks, 2, 2, strip, 128), BF),
            pltpu.VMEM((chunks, 2, 2, strip, 128), BF),
            pltpu.VMEM((width, every), BF),
            pltpu.VMEM((width, every), BF),
            pltpu.VMEM((rows, width), F32),
            pltpu.VMEM((ns, width, rows), BF),
            pltpu.VMEM((2, width, rows), BF),
            pltpu.VMEM((2, width, rows), BF),
            pltpu.VMEM((width, rows), BF),
            pltpu.VMEM((3, 16, width), F32),
            pltpu.VMEM((nf, 16, width), F32),
            pltpu.VMEM((nh, 16, width), F32),
            pltpu.VMEM((ns, 16, width), F32),
            dma((5,)),
            dma((chunks,)), dma((chunks,)),
            dma((chunks, xn)), dma((chunks, xn)),
            dma((chunks, yn)), dma((chunks, yn)),
            dma((chunks,)), dma((chunks,)),
            dma((chunks,)), dma((chunks,)),
            dma((chunks,)), dma((chunks,)),
            dma((chunks, yn)), dma((chunks, yn)),
            dma((chunks,)), dma((chunks,)),
            dma((16,)), dma((16,)),
            dma((16,)), dma((16,)),
            dma((16,)), dma((16,)),
            dma((1,)), dma((1,)),
            dma((nf + nh + ns,)), dma((nf + nh + ns,)),
        ],
        name="back",
        compiler_params=pltpu.CompilerParams(
            collective_id=1, has_side_effects=True, vmem_limit_bytes=67043328
        ),
    )(q, k, v, dc, ctx, lse, ht, w, gm, frames, vec, gv, gc, ge, go)


def feed_kernel(
    ctx_ref, frames_ref, cot_ref, vec_ref, wo_ref, win_ref, wout_ref,
    fo_ref, gm_ref, dc_ref, gi_ref, gout_ref, go_ref, gv_ref,
    mid, h2, h2t, dyb, acc, dh2, act, dub,
):
    b = pl.program_id(0)

    @pl.when(b == 0)
    def _():
        middle = frames_ref[...] + nn(ctx_ref[...].astype(BF), wo_ref[...]) + vec_ref[4:5, :]
        mid[...] = middle
        normed, _ = normalize(middle)
        hidden = (normed * vec_ref[5:6, :] + vec_ref[6:7, :]).astype(BF)
        h2[...] = hidden
        h2t[...] = hidden.T
        dyb[...] = cot_ref[...].astype(BF)
        acc[...] = middle + vec_ref[7:8, :]
        dh2[...] = jnp.zeros_like(dh2)
        gv_ref[...] = jnp.zeros_like(gv_ref)

    bias = vec_ref[pl.ds(8 + b, 1), :]
    size = h2.shape[0] // 1
    total = None
    for i in range(1):
        part = pl.ds(i * size, size)
        u = nn(h2[part, :], win_ref[...]) + bias
        da = nt(dyb[part, :], wout_ref[...])
        phi = 0.5 * (1.0 + lax.erf(u * 0.7071067811865476))
        act[part, :] = (u * phi).astype(BF)
        du = da * (phi + u * jnp.exp(-0.5 * u * u) * 0.3989422804014327)
        found = jnp.sum(du, axis=0, keepdims=True)
        total = found if total is None else total + found
        dub[part, :] = du.astype(BF)
    gv_ref[pl.ds(8 + b, 1), :] = total
    acc[...] += nn(act[...], wout_ref[...])
    gout_ref[...] = tn(act[...], dyb[...]).astype(BF)
    gi_ref[...] = nn(h2t[...], dub[...]).astype(BF)
    dh2[...] += nt(dub[...], win_ref[...])

    @pl.when(b == pl.num_programs(0) - 1)
    def _():
        fo_ref[...] = acc[...]
        normed, inverse = normalize(mid[...])
        back, gain, offset = norm_back(dh2[...], normed, inverse, vec_ref[5:6, :])
        upstream = cot_ref[...]
        middle = upstream + back
        gm_ref[...] = middle
        dab = middle.astype(BF)
        go_ref[...] = tn(ctx_ref[...].astype(BF), dab).astype(BF)
        dctx = nt(dab, wo_ref[...]).astype(BF)
        dc_ref[...] = dctx
        gv_ref[3:4, :] = jnp.sum(dctx.astype(F32), axis=0, keepdims=True)
        gv_ref[4:5, :] = jnp.sum(middle, axis=0, keepdims=True)
        gv_ref[5:6, :] = gain[None]
        gv_ref[6:7, :] = offset[None]
        gv_ref[7:8, :] = jnp.sum(upstream, axis=0, keepdims=True)


def feed_all(ctx, frames, cot, vec, aw, ew, cw):
    rows, width = frames.shape
    full = ew.shape[1]
    whole = lambda shape: pl.BlockSpec(shape, lambda b: (0,) * len(shape))
    blocks = full // width
    return pl.pallas_call(
        feed_kernel,
        grid=(blocks,),
        out_shape=(
            jax.ShapeDtypeStruct((rows, width), F32),
            jax.ShapeDtypeStruct((rows, width), F32),
            jax.ShapeDtypeStruct((rows, width), BF),
            jax.ShapeDtypeStruct((width, full), BF),
            jax.ShapeDtypeStruct((full, width), BF),
            jax.ShapeDtypeStruct((width, width), BF),
            jax.ShapeDtypeStruct((16, width), F32),
        ),
        in_specs=[
            whole((rows, width)), whole((rows, width)), whole((rows, width)), whole((16, width)),
            pl.BlockSpec((None, width, width), lambda b: (3, 0, 0)),
            pl.BlockSpec((width, width), lambda b: (0, b)),
            pl.BlockSpec((width, width), lambda b: (b, 0)),
        ],
        out_specs=(
            whole((rows, width)), whole((rows, width)), whole((rows, width)),
            pl.BlockSpec((width, width), lambda b: (0, b)),
            pl.BlockSpec((width, width), lambda b: (b, 0)),
            whole((width, width)), whole((16, width)),
        ),
        scratch_shapes=[
            pltpu.VMEM((rows, width), F32),
            pltpu.VMEM((rows, width), BF),
            pltpu.VMEM((width, rows), BF),
            pltpu.VMEM((rows, width), BF),
            pltpu.VMEM((rows, width), F32),
            pltpu.VMEM((rows, width), F32),
            pltpu.VMEM((rows, width), BF),
            pltpu.VMEM((rows, width), BF),
        ],
        name="feed",
        compiler_params=pltpu.CompilerParams(vmem_limit_bytes=67043328),
    )(ctx, frames, cot, vec, aw, ew, cw)


def on_device(
    sizes,
    frames_in,
    cotangent,
    attention_weight,
    expand_weight,
    contract_weight,
    vectors,
    first_attention,
    first_expand,
    first_contract,
    first_vectors,
    second_attention,
    second_expand,
    second_contract,
    second_vectors,
):
    nd, nf, ns = sizes
    frames = frames_in[0]
    upstream = cotangent[0]
    rows, width = frames.shape
    shard = attention_weight.shape[1]
    full = expand_weight.shape[1]
    aw, ew, cw, vec, h_turned, queries, key_rows, value_rows, context_wide, log_total = front_all(
        sizes, frames, vectors, attention_weight, expand_weight, contract_weight
    )
    frames_out, grad_middle, grad_context, grad_expand, grad_contract, grad_output_w, gv = feed_all(
        context_wide, frames, upstream, vec, aw, ew, cw
    )
    oc, oe, oa, input_gradient, gv_sum = back_all(
        sizes,
        queries,
        key_rows,
        value_rows,
        grad_context,
        context_wide,
        log_total,
        h_turned,
        aw,
        grad_middle,
        frames,
        vec,
        gv,
        grad_contract.reshape(nf, 4, shard, width),
        grad_expand.reshape(nf, shard, full),
        grad_output_w.reshape(nf, shard, width),
    )
    owned_vec = lax.dynamic_slice_in_dim(
        gv_sum[:12], lax.axis_index("fsdp") * (width // nf), width // nf, 1
    )
    owned = (
        oa.reshape(4, shard, width).astype(F32),
        oe.astype(F32),
        oc.reshape(4 * shard, width).astype(F32),
    )
    attention_out = (owned[0],) + adam_update(
        attention_weight, owned[0], first_attention, second_attention, rate_matrix, decay_matrix
    )
    expand_out = (owned[1],) + adam_update(
        expand_weight, owned[1], first_expand, second_expand, rate_matrix, decay_matrix
    )
    contract_out = (owned[2],) + adam_update(
        contract_weight, owned[2], first_contract, second_contract, rate_matrix, decay_matrix
    )
    vector_out = (owned_vec,) + adam_update(
        vectors, owned_vec, first_vectors, second_vectors, rate_vector, 0.0
    )
    result = [frames_out[None], input_gradient[None]]
    for i in range(4):
        result += [attention_out[i], expand_out[i], contract_out[i], vector_out[i]]
    return tuple(result)


def solution(mesh):
    sizes = (mesh.shape["dp"], mesh.shape["fsdp"], mesh.shape["seq"])
    data = P(("dp", "fsdp"), "seq", None)
    state = (P(None, "fsdp", None), P("fsdp", None), P("fsdp", None), P(None, "fsdp"))
    return jax.shard_map(
        functools.partial(on_device, sizes),
        mesh=mesh,
        in_specs=(data, data) + state * 3,
        out_specs=(data, data) + state * 4,
        check_vma=False,
    )
```
